32 devices in a mesh: batch: 4 (over z), ulysses: 2 (over x), blk: 4 (over y, core).
Axes of the slice: x: 2, y: 2, z: 4, core: 2. Of those that a mesh axis runs over, the one named last changes fastest.
Arguments:
- residual_in: bfloat16 [512, 8, 1024], P(('ulysses', 'blk'), 'batch'), may hold values from -6 to 6
- qkv_weight: bfloat16 [1024, 3072], P(('batch', 'ulysses', 'blk')), may hold values from -3 to 3
- qkv_bias: bfloat16 [3072], P(('batch', 'ulysses', 'blk')), may hold values from -0.4375 to 0.4375
- dense_weight: bfloat16 [1024, 1024], P(('batch', 'ulysses', 'blk')), may hold values from -0.5 to 0.5
- dense_bias: bfloat16 [1024], P(('batch', 'ulysses', 'blk')), may hold values from -4 to 4
- norm1_gain: bfloat16 [1024], P(('batch', 'ulysses', 'blk')), may hold values from 0.5 to 1.5
- norm1_bias: bfloat16 [1024], P(('batch', 'ulysses', 'blk')), may hold values from -3 to 3
- norm2_gain: bfloat16 [1024], P(('batch', 'ulysses', 'blk')), may hold values from 0.5 to 1.5
- norm2_bias: bfloat16 [1024], P(('batch', 'ulysses', 'blk')), may hold values from -3 to 3
- up_weight: bfloat16 [1024, 4096], P(('batch', 'ulysses', 'blk')), may hold values from -0.1875 to 0.1875
- up_bias: bfloat16 [4096], P(('batch', 'ulysses', 'blk')), may hold values from -6 to 6
- down_weight: bfloat16 [4096, 1024], P(('batch', 'ulysses', 'blk')), may hold values from -0.09375 to 0.09375
- down_bias: bfloat16 [1024], P(('batch', 'ulysses', 'blk')), may hold values from -4 to 4
- cotangent: bfloat16 [512, 8, 1024], P(('ulysses', 'blk'), 'batch'), may hold values from -6 to 6
Outputs:
- output: bfloat16 [512, 8, 1024], P(('ulysses', 'blk'), 'batch')
- input_grad: float32 [512, 8, 1024], P(('ulysses', 'blk'), 'batch')
- qkv_weight_grad: float32 [1024, 3072], P(('batch', 'ulysses', 'blk'))
- qkv_bias_grad: float32 [3072], P(('batch', 'ulysses', 'blk'))
- dense_weight_grad: float32 [1024, 1024], P(('batch', 'ulysses', 'blk'))
- dense_bias_grad: float32 [1024], P(('batch', 'ulysses', 'blk'))
- norm1_gain_grad: float32 [1024], P(('batch', 'ulysses', 'blk'))
- norm1_bias_grad: float32 [1024], P(('batch', 'ulysses', 'blk'))
- norm2_gain_grad: float32 [1024], P(('batch', 'ulysses', 'blk'))
- norm2_bias_grad: float32 [1024], P(('batch', 'ulysses', 'blk'))
- up_weight_grad: float32 [1024, 4096], P(('batch', 'ulysses', 'blk'))
- up_bias_grad: float32 [4096], P(('batch', 'ulysses', 'blk'))
- down_weight_grad: float32 [4096, 1024], P(('batch', 'ulysses', 'blk'))
- down_bias_grad: float32 [1024], P(('batch', 'ulysses', 'blk'))
The draws below stay inside these ranges and needn't reach their ends.
All inputs are finite; a program needn't handle non-finite values.
Results may differ from the reference program's by a relative error of at most 0.0091.
Values may be sent and summed in bfloat16 or wider, within the bound.
A program may use at most 192 MiB of HBM per device.

```python
import math
import jax
import jax.numpy as jnp
from jax import lax

D = 1024
HD = 64
FF = 4096
LEN = 512
SEQS = 8


def draw_qkv_weight(key, part):
    base_draw = jnp.clip(jax.random.normal(key, (D, 3 * D), jnp.float32), -4.0, 4.0) / math.sqrt(D)
    return base_draw.astype(jnp.bfloat16)


def shard_levels(own_key, extent, pieces, smallest, high):
    level, own = 1.0, jax.random.fold_in(own_key, 6)
    for position, blocks in pieces:
        steps = jnp.exp(jax.random.uniform(jax.random.fold_in(own, position), (blocks,), jnp.float32, smallest / len(pieces), high / len(pieces)))
        level = level * jnp.repeat(steps, extent[position] // blocks).reshape([-1 if axis == position else 1 for axis in range(len(extent))])
    return level


def bell_draw(rng, shape, spread, bound, pieces=(), held_as=jnp.bfloat16):
    entries = spread * jax.random.normal(rng, shape, jnp.float32)
    if pieces:
        entries = entries * shard_levels(rng, shape, pieces, -0.22, 0.18)
    return jnp.clip(entries, -bound, bound).astype(held_as)


def setup_inputs(seed: int = 0) -> dict:
    seeds = jax.random.split(jax.random.key(seed), 15)
    return {
        "residual_in": bell_draw(seeds[0], (LEN, SEQS, D), 1.0, 6.0, ((0, 8), (1, 4))),
        "qkv_weight": draw_qkv_weight(jax.random.fold_in(seeds[14], 71), 0),
        "qkv_bias": bell_draw(seeds[2], (3 * D,), 0.03, 0.4375, ((0, 32),)),
        "dense_weight": bell_draw(seeds[3], (D, D), (max(1, D * 64 // LEN)) ** -0.5, 0.5, ((0, 32),)),
        "dense_bias": bell_draw(seeds[4], (D,), 0.3, 4.0, ((0, 32),)),
        "norm1_gain": jnp.clip(1.0 + 0.1 * jax.random.normal(seeds[5], (D,), jnp.float32), 0.5, 1.5).astype(jnp.bfloat16),
        "norm1_bias": bell_draw(seeds[6], (D,), 0.2, 3.0, ((0, 32),)),
        "norm2_gain": jnp.clip(1.0 + 0.1 * jax.random.normal(seeds[7], (D,), jnp.float32), 0.5, 1.5).astype(jnp.bfloat16),
        "norm2_bias": bell_draw(seeds[8], (D,), 0.2, 3.0, ((0, 32),)),
        "up_weight": bell_draw(seeds[9], (D, FF), D ** -0.5, 0.1875, ((0, 32),)),
        "up_bias": bell_draw(seeds[10], (FF,), 0.5, 6.0, ((0, 32),)),
        "down_weight": bell_draw(seeds[11], (FF, D), FF ** -0.5, 0.09375, ((0, 32),)),
        "down_bias": bell_draw(seeds[12], (D,), 0.3, 4.0, ((0, 32),)),
        "cotangent": bell_draw(seeds[13], (LEN, SEQS, D), 1.0, 6.0, ((0, 8), (1, 4))),
    }


EPSILON = 1e-05
INV_ROOT_TWO = 0.7071067811865476
INV_ROOT_TWO_PI = 0.3989422804014327

def layer_norm(values):
    center = lax.optimization_barrier(jnp.mean(values, axis=-1, keepdims=True))
    shifted = values - center
    inverse = lax.rsqrt(lax.optimization_barrier(jnp.mean(shifted * shifted, axis=-1, keepdims=True)) + EPSILON)
    return (shifted * inverse, inverse)

def norm_back(gradient, normed, inverse, gain_vec):
    scaled = gradient * gain_vec
    return inverse * (scaled - lax.optimization_barrier(jnp.mean(scaled, axis=-1, keepdims=True)) - normed * lax.optimization_barrier(jnp.mean(scaled * normed, axis=-1, keepdims=True)))

def gelu_value(pre_values):
    return 0.5 * pre_values * (1.0 + jax.scipy.special.erf(pre_values * INV_ROOT_TWO))

def gelu_slope(pre_values):
    normal_cdf = 0.5 * (1.0 + jax.scipy.special.erf(pre_values * INV_ROOT_TWO))
    return normal_cdf + pre_values * jnp.exp(-0.5 * pre_values * pre_values) * INV_ROOT_TWO_PI

def rotary_tables(positions, rotary):
    half_rot = rotary // 2
    frequency = 1.0 / 10000.0 ** (jnp.arange(half_rot, dtype=jnp.float32) * (2.0 / rotary))
    angles = positions.astype(jnp.float32)[:, None] * frequency[None, :]
    cosine = jnp.concatenate([jnp.cos(angles), jnp.cos(angles)], axis=-1)
    sine_table = jnp.concatenate([jnp.sin(angles), jnp.sin(angles)], axis=-1)
    return (cosine, sine_table)

def expand_table(table, tensor):
    extra_dims = (1,) * (tensor.ndim - 2)
    return table.reshape((table.shape[0],) + extra_dims + (table.shape[1],))

def rotate_fwd(tensor, cosine, sine_table, rotary):
    half_rot = rotary // 2
    cos_full = expand_table(cosine, tensor)
    sin_full = expand_table(sine_table, tensor)
    rot_part = tensor[..., :rotary]
    turned = jnp.concatenate([-rot_part[..., half_rot:], rot_part[..., :half_rot]], axis=-1)
    return jnp.concatenate([rot_part * cos_full + turned * sin_full, tensor[..., rotary:]], axis=-1)

def rotate_back(tensor, cosine, sine_table, rotary):
    half_rot = rotary // 2
    cos_full = expand_table(cosine, tensor)
    sin_full = expand_table(sine_table, tensor)
    rot_part = tensor[..., :rotary]
    weighted = rot_part * sin_full
    turned = jnp.concatenate([weighted[..., half_rot:], -weighted[..., :half_rot]], axis=-1)
    return jnp.concatenate([rot_part * cos_full + turned, tensor[..., rotary:]], axis=-1)

def reference(residual_in, qkv_weight, qkv_bias, dense_weight, dense_bias, norm1_gain, norm1_bias, norm2_gain, norm2_bias, up_weight, up_bias, down_weight, down_bias, cotangent):
    single = jnp.float32
    half_type = jnp.bfloat16
    head_count = D // HD
    rotary = HD // 4
    scale_factor = 1.0 / math.sqrt(HD)
    block_rows = math.gcd(512, LEN)
    n_blocks = LEN // block_rows
    positions = jnp.arange(LEN, dtype=jnp.int32)
    cosine, sine_table = rotary_tables(positions, rotary)
    w_qkv = qkv_weight.astype(single)
    w_dense = dense_weight.astype(single)
    w_up = up_weight.astype(single)
    w_down = down_weight.astype(single)
    b_qkv = qkv_bias.astype(single)
    b_dense = dense_bias.astype(single)
    b_up = up_bias.astype(single)
    b_down = down_bias.astype(single)
    gain_one = norm1_gain.astype(single)
    shift_one = norm1_bias.astype(single)
    gain_two = norm2_gain.astype(single)
    shift_two = norm2_bias.astype(single)
    head_shape = (LEN, 1, head_count, HD)
    block_ids = jnp.arange(n_blocks, dtype=jnp.int32)

    def masked_scores(query_rows, key_heads, row_pos):
        scores = jnp.einsum('qshd,kshd->shqk', query_rows.astype(single), key_heads.astype(single)) * scale_factor
        allowed = (positions[None, :] <= row_pos[:, None])[None, None]
        return jnp.where(allowed, scores, -jnp.inf)

    def per_seq(running, seq_pair):
        seq_in, seq_cot = seq_pair
        inputs_f = seq_in.astype(single)[:, None, :]
        grad_out = seq_cot[:, None, :]
        grad_f = grad_out.astype(single)
        normed, inverse = layer_norm(inputs_f)
        act_one = (normed * gain_one + shift_one).astype(half_type)
        act_two = (normed * gain_two + shift_two).astype(half_type)
        qkv_full = jnp.einsum('tsd,df->tsf', act_one.astype(single), w_qkv) + b_qkv
        query_heads = rotate_fwd(qkv_full[..., :D].reshape(head_shape), cosine, sine_table, rotary).astype(half_type)
        key_heads = rotate_fwd(qkv_full[..., D:2 * D].reshape(head_shape), cosine, sine_table, rotary).astype(half_type)
        value_heads = qkv_full[..., 2 * D:].reshape(head_shape).astype(half_type)

        def forward_block(block_index):
            row_start = block_index * block_rows
            query_rows = lax.dynamic_slice_in_dim(query_heads, row_start, block_rows, 0)
            row_pos = lax.dynamic_slice_in_dim(positions, row_start, block_rows, 0)
            masked = masked_scores(query_rows, key_heads, row_pos)
            row_max = lax.optimization_barrier(jnp.max(masked, axis=-1))
            log_total = row_max + jnp.log(lax.optimization_barrier(jnp.sum(jnp.exp(masked - row_max[..., None]), axis=-1)))
            weights_b = jnp.exp(masked - log_total[..., None]).astype(half_type)
            result = jnp.einsum('shqk,kshd->qshd', weights_b.astype(single), value_heads.astype(single)).astype(half_type)
            return (result, log_total)
        results, log_totals = lax.map(forward_block, block_ids)
        attn_heads = results.reshape(head_shape)
        attn_flat = attn_heads.reshape(LEN, 1, D)
        proj_out = jnp.einsum('tsd,de->tse', attn_flat.astype(single), w_dense) + b_dense
        pre_act = jnp.einsum('tsd,df->tsf', act_two.astype(single), w_up) + b_up
        gelu_out = gelu_value(pre_act).astype(half_type)
        mlp_out = jnp.einsum('tsf,fd->tsd', gelu_out.astype(single), w_down) + b_down
        output = (inputs_f + proj_out + mlp_out).astype(half_type)
        bias_sum = lax.optimization_barrier(jnp.sum(grad_f, axis=(0, 1)))
        down_w_grad = jnp.einsum('tsf,tsd->fd', gelu_out.astype(single), grad_f)
        gelu_grad = jnp.einsum('tsd,fd->tsf', grad_f, w_down)
        pre_grad = (gelu_grad * gelu_slope(pre_act)).astype(half_type)
        up_w_grad = jnp.einsum('tsd,tsf->df', act_two.astype(single), pre_grad.astype(single))
        up_b_grad = lax.optimization_barrier(jnp.sum(pre_grad.astype(single), axis=(0, 1)))
        act_two_grad = jnp.einsum('tsf,df->tsd', pre_grad.astype(single), w_up)
        dense_w_grad = jnp.einsum('tsd,tse->de', attn_flat.astype(single), grad_f)
        attn_grad = jnp.einsum('tse,de->tsd', grad_f, w_dense).astype(half_type)
        grad_heads = attn_grad.reshape(head_shape)

        def backward_block(acc_pair, block_index):
            key_acc, value_acc = acc_pair
            row_start = block_index * block_rows
            query_rows = lax.dynamic_slice_in_dim(query_heads, row_start, block_rows, 0)
            out_rows = lax.dynamic_slice_in_dim(attn_heads, row_start, block_rows, 0)
            grad_rows = lax.dynamic_slice_in_dim(grad_heads, row_start, block_rows, 0)
            row_pos = lax.dynamic_slice_in_dim(positions, row_start, block_rows, 0)
            masked = masked_scores(query_rows, key_heads, row_pos)
            probs_f = jnp.exp(masked - log_totals[block_index][..., None])
            value_acc = value_acc + jnp.einsum('shqk,qshd->kshd', probs_f.astype(half_type).astype(single), grad_rows.astype(single))
            grad_prob = jnp.einsum('qshd,kshd->shqk', grad_rows.astype(single), value_heads.astype(single))
            delta_row = jnp.transpose(lax.optimization_barrier(jnp.sum(grad_rows.astype(single) * out_rows.astype(single), axis=-1)), (1, 2, 0))
            grad_score = (probs_f * (grad_prob - delta_row[..., None]) * scale_factor).astype(half_type)
            query_part = jnp.einsum('shqk,kshd->qshd', grad_score.astype(single), key_heads.astype(single))
            key_acc = key_acc + jnp.einsum('shqk,qshd->kshd', grad_score.astype(single), query_rows.astype(single))
            return ((key_acc, value_acc), query_part)
        acc_zero = jnp.zeros(head_shape, single)
        (key_acc, value_acc), query_parts = lax.scan(backward_block, (acc_zero, acc_zero), block_ids)
        query_grad = query_parts.reshape(head_shape)
        query_send = rotate_back(query_grad, cosine, sine_table, rotary).reshape(LEN, 1, D).astype(half_type)
        key_send = rotate_back(key_acc, cosine, sine_table, rotary).reshape(LEN, 1, D).astype(half_type)
        value_send = value_acc.reshape(LEN, 1, D).astype(half_type)
        qkv_grad = jnp.concatenate([query_send, key_send, value_send], axis=-1).astype(single)
        qkv_w_grad = jnp.einsum('tsd,tsf->df', act_one.astype(single), qkv_grad)
        qkv_b_grad = lax.optimization_barrier(jnp.sum(qkv_grad, axis=(0, 1)))
        act_one_grad = jnp.einsum('tsf,df->tsd', qkv_grad, w_qkv)
        gain_one_grad = lax.optimization_barrier(jnp.sum(act_one_grad * normed, axis=(0, 1)))
        shift_one_grad = lax.optimization_barrier(jnp.sum(act_one_grad, axis=(0, 1)))
        gain_two_grad = lax.optimization_barrier(jnp.sum(act_two_grad * normed, axis=(0, 1)))
        shift_two_grad = lax.optimization_barrier(jnp.sum(act_two_grad, axis=(0, 1)))
        input_grad = grad_f + norm_back(act_one_grad, normed, inverse, gain_one) + norm_back(act_two_grad, normed, inverse, gain_two)
        terms = (qkv_w_grad, qkv_b_grad, dense_w_grad, bias_sum, gain_one_grad, shift_one_grad, gain_two_grad, shift_two_grad, up_w_grad, up_b_grad, down_w_grad, bias_sum)
        new_running = jax.tree.map(jnp.add, running, terms)
        return (new_running, (output[:, 0, :], input_grad[:, 0, :]))
    zero_grads = jax.tree.map(lambda array_in: jnp.zeros(array_in.shape, single), (qkv_weight, qkv_bias, dense_weight, dense_bias, norm1_gain, norm1_bias, norm2_gain, norm2_bias, up_weight, up_bias, down_weight, down_bias))
    grads, seq_outs = lax.scan(per_seq, zero_grads, (jnp.swapaxes(residual_in, 0, 1), jnp.swapaxes(cotangent, 0, 1)))
    outputs, input_grads = seq_outs
    qkv_weight_grad, qkv_bias_grad, dense_weight_grad, dense_bias_grad, norm1_gain_grad, norm1_bias_grad, norm2_gain_grad, norm2_bias_grad, up_weight_grad, up_bias_grad, down_weight_grad, down_bias_grad = grads
    return (jnp.swapaxes(outputs, 0, 1), jnp.swapaxes(input_grads, 0, 1), qkv_weight_grad, qkv_bias_grad, dense_weight_grad, dense_bias_grad, norm1_gain_grad, norm1_bias_grad, norm2_gain_grad, norm2_bias_grad, up_weight_grad, up_bias_grad, down_weight_grad, down_bias_grad)
```

```python
import functools
import math

import jax
import jax.numpy as jnp
from jax import lax
from jax.experimental import pallas as pl
from jax.experimental.pallas import tpu as pltpu
from jax.sharding import PartitionSpec as P

HD = 64
BATCH, ULY, BLK = "batch", "ulysses", "blk"
AXES = (BATCH, ULY, BLK)
TOKENS = (ULY, BLK)


EPSILON = 1e-05
INV_ROOT_TWO = 0.7071067811865476
INV_ROOT_TWO_PI = 0.3989422804014327


def layer_norm(values):
    center = jnp.mean(values, axis=-1, keepdims=True)
    shifted = values - center
    inverse = lax.rsqrt(jnp.mean(shifted * shifted, axis=-1, keepdims=True) + EPSILON)
    return (shifted * inverse, inverse)


def norm_back(gradient, normed, inverse, gain_vec):
    scaled = gradient * gain_vec
    return inverse * (
        scaled
        - jnp.mean(scaled, axis=-1, keepdims=True)
        - normed * jnp.mean(scaled * normed, axis=-1, keepdims=True)
    )


def gelu_value(pre_values):
    return 0.5 * pre_values * (1.0 + jax.scipy.special.erf(pre_values * INV_ROOT_TWO))


def gelu_slope(pre_values):
    normal_cdf = 0.5 * (1.0 + jax.scipy.special.erf(pre_values * INV_ROOT_TWO))
    return normal_cdf + pre_values * jnp.exp(-0.5 * pre_values * pre_values) * INV_ROOT_TWO_PI


def rotary_tables(positions, rotary):
    half_rot = rotary // 2
    frequency = 1.0 / 10000.0 ** (jnp.arange(half_rot, dtype=jnp.float32) * (2.0 / rotary))
    angles = positions.astype(jnp.float32)[:, None] * frequency[None, :]
    cosine = jnp.concatenate([jnp.cos(angles), jnp.cos(angles)], axis=-1)
    sine_table = jnp.concatenate([jnp.sin(angles), jnp.sin(angles)], axis=-1)
    return (cosine, sine_table)


def expand_table(table, tensor):
    extra_dims = (1,) * (tensor.ndim - 2)
    return table.reshape((table.shape[0],) + extra_dims + (table.shape[1],))


def rotate_fwd(tensor, cosine, sine_table, rotary):
    half_rot = rotary // 2
    cos_full = expand_table(cosine, tensor)
    sin_full = expand_table(sine_table, tensor)
    rot_part = tensor[..., :rotary]
    turned = jnp.concatenate([-rot_part[..., half_rot:], rot_part[..., :half_rot]], axis=-1)
    return jnp.concatenate([rot_part * cos_full + turned * sin_full, tensor[..., rotary:]], axis=-1)


def rotate_back(tensor, cosine, sine_table, rotary):
    half_rot = rotary // 2
    cos_full = expand_table(cosine, tensor)
    sin_full = expand_table(sine_table, tensor)
    rot_part = tensor[..., :rotary]
    weighted = rot_part * sin_full
    turned = jnp.concatenate([weighted[..., half_rot:], -weighted[..., :half_rot]], axis=-1)
    return jnp.concatenate([rot_part * cos_full + turned, tensor[..., rotary:]], axis=-1)


def general_body(
    residual_in,
    qkv_weight,
    qkv_bias,
    dense_weight,
    dense_bias,
    norm1_gain,
    norm1_bias,
    norm2_gain,
    norm2_bias,
    up_weight,
    up_bias,
    down_weight,
    down_bias,
    cotangent,
):
    single = jnp.float32
    half_type = jnp.bfloat16
    gathered = (
        lax.all_gather(qkv_weight, AXES, axis=0, tiled=True),
        lax.all_gather(qkv_bias, AXES, axis=0, tiled=True),
        lax.all_gather(dense_weight, AXES, axis=0, tiled=True),
        lax.all_gather(dense_bias, AXES, axis=0, tiled=True),
        lax.all_gather(norm1_gain, AXES, axis=0, tiled=True),
        lax.all_gather(norm1_bias, AXES, axis=0, tiled=True),
        lax.all_gather(norm2_gain, AXES, axis=0, tiled=True),
        lax.all_gather(norm2_bias, AXES, axis=0, tiled=True),
        lax.all_gather(up_weight, AXES, axis=0, tiled=True),
        lax.all_gather(up_bias, AXES, axis=0, tiled=True),
        lax.all_gather(down_weight, AXES, axis=0, tiled=True),
        lax.all_gather(down_bias, AXES, axis=0, tiled=True),
    )
    (
        w_qkv,
        b_qkv,
        w_dense,
        b_dense,
        gain_one,
        shift_one,
        gain_two,
        shift_two,
        w_up,
        b_up,
        w_down,
        b_down,
    ) = gathered
    tok_rows = residual_in.shape[0]
    seq_count = residual_in.shape[1]
    model_width = residual_in.shape[2]
    head_count = model_width // HD
    rotary = HD // 4
    scale_factor = 1.0 / math.sqrt(HD)
    blk_size = lax.axis_size(BLK)
    uly_size = lax.axis_size(ULY)
    blk_index = lax.axis_index(BLK)
    block_id = lax.axis_index(ULY) * blk_size + blk_index
    seq_pos = block_id * tok_rows + jnp.arange(tok_rows, dtype=jnp.int32)
    inputs_f = residual_in.astype(single)
    normed, inverse = layer_norm(inputs_f)
    act_one = (normed * gain_one.astype(single) + shift_one.astype(single)).astype(half_type)
    act_two = (normed * gain_two.astype(single) + shift_two.astype(single)).astype(half_type)
    qkv_full = jnp.einsum(
        "tsd,df->tsf", act_one, w_qkv, preferred_element_type=single
    ) + b_qkv.astype(single)
    cos_seq, sin_seq = rotary_tables(seq_pos, rotary)
    head_shape = (tok_rows, seq_count, head_count, HD)
    query_seq = (
        rotate_fwd(qkv_full[..., :model_width].reshape(head_shape), cos_seq, sin_seq, rotary)
        .reshape(tok_rows, seq_count, model_width)
        .astype(half_type)
    )
    key_seq = (
        rotate_fwd(
            qkv_full[..., model_width : 2 * model_width].reshape(head_shape),
            cos_seq,
            sin_seq,
            rotary,
        )
        .reshape(tok_rows, seq_count, model_width)
        .astype(half_type)
    )
    value_seq = qkv_full[..., 2 * model_width :].astype(half_type)
    query_loc, key_loc, value_loc = (
        lax.all_to_all(query_seq, ULY, split_axis=2, concat_axis=0, tiled=True),
        lax.all_to_all(key_seq, ULY, split_axis=2, concat_axis=0, tiled=True),
        lax.all_to_all(value_seq, ULY, split_axis=2, concat_axis=0, tiled=True),
    )
    local_rows = query_loc.shape[0]
    features = query_loc.shape[2]
    local_heads = features // HD
    key_all, value_all = (
        lax.all_gather(key_loc, BLK, axis=0, tiled=True),
        lax.all_gather(value_loc, BLK, axis=0, tiled=True),
    )
    total_rows = key_all.shape[0]
    row_ids = jnp.arange(local_rows, dtype=jnp.int32)
    query_pos = (row_ids // tok_rows * blk_size + blk_index) * tok_rows + row_ids % tok_rows
    block_rows = math.gcd(512, local_rows)
    n_blocks = local_rows // block_rows
    query_h = query_loc.reshape(local_rows, seq_count, local_heads, HD)
    key_h = jnp.transpose(
        key_all.reshape(blk_size, uly_size, tok_rows, seq_count, features), (1, 0, 2, 3, 4)
    ).reshape(total_rows, seq_count, local_heads, HD)
    value_h = jnp.transpose(
        value_all.reshape(blk_size, uly_size, tok_rows, seq_count, features), (1, 0, 2, 3, 4)
    ).reshape(total_rows, seq_count, local_heads, HD)
    zero_idx = jnp.zeros((), jnp.int32)
    step_ids = jnp.arange(n_blocks * seq_count, dtype=jnp.int32)
    row_shape = (block_rows, 1, local_heads, HD)

    def select(step_index):
        row_start = step_index // seq_count * block_rows
        seq_index = step_index % seq_count
        query_rows = lax.dynamic_slice(
            query_h, (row_start, seq_index, zero_idx, zero_idx), row_shape
        )
        limit = jnp.max(query_pos) // block_rows + 1
        return (row_start, seq_index, query_rows, query_pos, limit)

    def block_scores(query_rows, row_pos, key_index, seq_index):
        key_start = key_index * block_rows
        slot = (key_start, seq_index, zero_idx, zero_idx)
        key_rows = lax.dynamic_slice(key_h, slot, (block_rows, 1, local_heads, HD))
        value_rows = lax.dynamic_slice(value_h, slot, (block_rows, 1, local_heads, HD))
        scores = (
            jnp.einsum("qshd,kshd->shqk", query_rows, key_rows, preferred_element_type=single)
            * scale_factor
        )
        key_ids = key_start + jnp.arange(block_rows, dtype=jnp.int32)
        allowed = (key_ids[None, :] <= row_pos[:, None])[None, None]
        return (jnp.where(allowed, scores, -jnp.inf), key_rows, value_rows, slot)

    def forward_block(step_index):
        row_start, seq_index, query_rows, row_pos, limit = select(step_index)

        def total_step(key_index, carry):
            running_max, running_sum = carry
            masked, key_rows, value_rows, slot = block_scores(
                query_rows, row_pos, key_index, seq_index
            )
            new_max = jnp.maximum(running_max, jnp.max(masked, axis=-1))
            new_sum = running_sum * jnp.exp(running_max - new_max) + jnp.sum(
                jnp.exp(masked - new_max[..., None]), axis=-1
            )
            return (new_max, new_sum)

        start_max = jnp.full((1, local_heads, block_rows), -jnp.inf, single)
        start_sum = jnp.zeros((1, local_heads, block_rows), single)
        final_max, final_sum = lax.fori_loop(zero_idx, limit, total_step, (start_max, start_sum))
        log_total = final_max + jnp.log(final_sum)

        def value_step(key_index, acc):
            masked, key_rows, value_rows, slot = block_scores(
                query_rows, row_pos, key_index, seq_index
            )
            weights_b = jnp.exp(masked - log_total[..., None]).astype(half_type)
            return acc + jnp.einsum(
                "shqk,kshd->qshd", weights_b, value_rows, preferred_element_type=single
            )

        result = lax.fori_loop(zero_idx, limit, value_step, jnp.zeros(row_shape, single)).astype(
            half_type
        )
        return (result[:, 0], log_total)

    results, log_totals = lax.map(forward_block, step_ids)
    attn_h = jnp.transpose(
        results.reshape(n_blocks, seq_count, block_rows, local_heads, HD), (0, 2, 1, 3, 4)
    ).reshape(local_rows, seq_count, local_heads, HD)
    attn_seq = lax.all_to_all(
        attn_h.reshape(local_rows, seq_count, features),
        ULY,
        split_axis=0,
        concat_axis=2,
        tiled=True,
    )
    proj_out = jnp.einsum(
        "tsd,de->tse", attn_seq, w_dense, preferred_element_type=single
    ) + b_dense.astype(single)
    pre_act = jnp.einsum("tsd,df->tsf", act_two, w_up, preferred_element_type=single) + b_up.astype(
        single
    )
    gelu_out = gelu_value(pre_act).astype(half_type)
    mlp_out = jnp.einsum(
        "tsf,fd->tsd", gelu_out, w_down, preferred_element_type=single
    ) + b_down.astype(single)
    output = (inputs_f + proj_out + mlp_out).astype(half_type)
    back_params = (
        lax.all_gather(qkv_weight, AXES, axis=0, tiled=True),
        lax.all_gather(qkv_bias, AXES, axis=0, tiled=True),
        lax.all_gather(dense_weight, AXES, axis=0, tiled=True),
        lax.all_gather(dense_bias, AXES, axis=0, tiled=True),
        lax.all_gather(norm1_gain, AXES, axis=0, tiled=True),
        lax.all_gather(norm1_bias, AXES, axis=0, tiled=True),
        lax.all_gather(norm2_gain, AXES, axis=0, tiled=True),
        lax.all_gather(norm2_bias, AXES, axis=0, tiled=True),
        lax.all_gather(up_weight, AXES, axis=0, tiled=True),
        lax.all_gather(up_bias, AXES, axis=0, tiled=True),
        lax.all_gather(down_weight, AXES, axis=0, tiled=True),
        lax.all_gather(down_bias, AXES, axis=0, tiled=True),
    )
    back_qkv = back_params[0]
    back_dense = back_params[2]
    back_gain_one = back_params[4].astype(single)
    back_gain_two = back_params[6].astype(single)
    back_up = back_params[8]
    back_down = back_params[10]
    grad_f = cotangent.astype(single)
    bias_sum = jnp.sum(grad_f, axis=(0, 1))
    down_w_grad = jnp.einsum("tsf,tsd->fd", gelu_out, cotangent, preferred_element_type=single)
    gelu_grad = jnp.einsum("tsd,fd->tsf", cotangent, back_down, preferred_element_type=single)
    pre_grad = (gelu_grad * gelu_slope(pre_act)).astype(half_type)
    up_w_grad = jnp.einsum("tsd,tsf->df", act_two, pre_grad, preferred_element_type=single)
    up_b_grad = jnp.sum(pre_grad.astype(single), axis=(0, 1))
    act_two_grad = jnp.einsum("tsf,df->tsd", pre_grad, back_up, preferred_element_type=single)
    gain_two_grad = jnp.sum(act_two_grad * normed, axis=(0, 1))
    shift_two_grad = jnp.sum(act_two_grad, axis=(0, 1))
    dense_w_grad = jnp.einsum("tsd,tse->de", attn_seq, cotangent, preferred_element_type=single)
    attn_grad = jnp.einsum(
        "tse,de->tsd", cotangent, back_dense, preferred_element_type=single
    ).astype(half_type)
    grad_loc = lax.all_to_all(attn_grad, ULY, split_axis=2, concat_axis=0, tiled=True)
    grad_h = grad_loc.reshape(local_rows, seq_count, local_heads, HD)

    def backward_block(acc_pair, step_index):
        row_start, seq_index, query_rows, row_pos, limit = select(step_index)
        own_slot = (row_start, seq_index, zero_idx, zero_idx)
        out_rows = lax.dynamic_slice(attn_h, own_slot, row_shape)
        grad_rows = lax.dynamic_slice(grad_h, own_slot, row_shape)
        log_total = log_totals[step_index]
        delta_row = jnp.transpose(
            jnp.sum(grad_rows.astype(single) * out_rows.astype(single), axis=-1), (1, 2, 0)
        )

        def grad_step(key_index, carry):
            key_acc, value_acc, query_acc = carry
            masked, key_rows, value_rows, slot = block_scores(
                query_rows, row_pos, key_index, seq_index
            )
            probs_f = jnp.exp(masked - log_total[..., None])
            value_part = jnp.einsum(
                "shqk,qshd->kshd",
                probs_f.astype(half_type),
                grad_rows,
                preferred_element_type=single,
            )
            grad_prob = jnp.einsum(
                "qshd,kshd->shqk", grad_rows, value_rows, preferred_element_type=single
            )
            grad_score = (probs_f * (grad_prob - delta_row[..., None]) * scale_factor).astype(
                half_type
            )
            query_acc = query_acc + jnp.einsum(
                "shqk,kshd->qshd", grad_score, key_rows, preferred_element_type=single
            )
            key_part = jnp.einsum(
                "shqk,qshd->kshd", grad_score, query_rows, preferred_element_type=single
            )
            key_acc = lax.dynamic_update_slice(
                key_acc, lax.dynamic_slice(key_acc, slot, key_part.shape) + key_part, slot
            )
            value_acc = lax.dynamic_update_slice(
                value_acc, lax.dynamic_slice(value_acc, slot, value_part.shape) + value_part, slot
            )
            return (key_acc, value_acc, query_acc)

        key_acc, value_acc, query_acc = lax.fori_loop(
            zero_idx, limit, grad_step, (acc_pair[0], acc_pair[1], jnp.zeros(row_shape, single))
        )
        return ((key_acc, value_acc), query_acc[:, 0])

    acc_zero = jnp.zeros((total_rows, seq_count, local_heads, HD), single)
    acc_final, query_parts = lax.scan(backward_block, (acc_zero, acc_zero), step_ids)
    query_grad = jnp.transpose(
        query_parts.reshape(n_blocks, seq_count, block_rows, local_heads, HD), (0, 2, 1, 3, 4)
    ).reshape(local_rows, seq_count, local_heads, HD)
    key_terms = jnp.transpose(
        acc_final[0].reshape(uly_size, blk_size, tok_rows, seq_count, features), (1, 0, 2, 3, 4)
    ).reshape(total_rows, seq_count, features)
    value_terms = jnp.transpose(
        acc_final[1].reshape(uly_size, blk_size, tok_rows, seq_count, features), (1, 0, 2, 3, 4)
    ).reshape(total_rows, seq_count, features)
    key_back, value_back = (
        lax.psum_scatter(key_terms, BLK, scatter_dimension=0, tiled=True),
        lax.psum_scatter(value_terms, BLK, scatter_dimension=0, tiled=True),
    )
    cos_h, sin_h = rotary_tables(query_pos, rotary)
    query_send = (
        rotate_back(query_grad, cos_h, sin_h, rotary)
        .reshape(local_rows, seq_count, features)
        .astype(half_type)
    )
    key_send = (
        rotate_back(key_back.reshape(local_rows, seq_count, local_heads, HD), cos_h, sin_h, rotary)
        .reshape(local_rows, seq_count, features)
        .astype(half_type)
    )
    value_send = value_back.astype(half_type)
    query_ret, key_ret, value_ret = (
        lax.all_to_all(query_send, ULY, split_axis=0, concat_axis=2, tiled=True),
        lax.all_to_all(key_send, ULY, split_axis=0, concat_axis=2, tiled=True),
        lax.all_to_all(value_send, ULY, split_axis=0, concat_axis=2, tiled=True),
    )
    qkv_grad = jnp.concatenate([query_ret, key_ret, value_ret], axis=-1)
    qkv_w_grad = jnp.einsum("tsd,tsf->df", act_one, qkv_grad, preferred_element_type=single)
    qkv_b_grad = jnp.sum(qkv_grad.astype(single), axis=(0, 1))
    act_one_grad = jnp.einsum("tsf,df->tsd", qkv_grad, back_qkv, preferred_element_type=single)
    gain_one_grad = jnp.sum(act_one_grad * normed, axis=(0, 1))
    shift_one_grad = jnp.sum(act_one_grad, axis=(0, 1))
    input_grad = (
        grad_f
        + norm_back(act_one_grad, normed, inverse, back_gain_one)
        + norm_back(act_two_grad, normed, inverse, back_gain_two)
    )
    summed = (
        lax.psum_scatter(qkv_w_grad, AXES, scatter_dimension=0, tiled=True),
        lax.psum_scatter(qkv_b_grad, AXES, scatter_dimension=0, tiled=True),
        lax.psum_scatter(
            dense_w_grad, AXES, scatter_dimension=0, tiled=True
        ),
        lax.psum_scatter(bias_sum, AXES, scatter_dimension=0, tiled=True),
        lax.psum_scatter(
            gain_one_grad, AXES, scatter_dimension=0, tiled=True
        ),
        lax.psum_scatter(
            shift_one_grad, AXES, scatter_dimension=0, tiled=True
        ),
        lax.psum_scatter(
            gain_two_grad, AXES, scatter_dimension=0, tiled=True
        ),
        lax.psum_scatter(
            shift_two_grad, AXES, scatter_dimension=0, tiled=True
        ),
        lax.psum_scatter(up_w_grad, AXES, scatter_dimension=0, tiled=True),
        lax.psum_scatter(up_b_grad, AXES, scatter_dimension=0, tiled=True),
        lax.psum_scatter(down_w_grad, AXES, scatter_dimension=0, tiled=True),
        lax.psum_scatter(bias_sum, AXES, scatter_dimension=0, tiled=True),
    )
    return (
        output,
        input_grad,
        summed[0],
        summed[1],
        summed[2],
        summed[3],
        summed[4],
        summed[5],
        summed[6],
        summed[7],
        summed[8],
        summed[9],
        summed[10],
        summed[11],
    )


MESH = pl.DeviceIdType.MESH


class Place:
    def __init__(self, planes):
        self.planes = planes
        self.b = lax.axis_index(BATCH)
        self.u = lax.axis_index(ULY)
        k = lax.axis_index(BLK)
        self.y, self.c = k // 2, k % 2
        self.t = self.u * 4 + k
        self.xn, self.yn, self.pn = self.peer(4), self.peer(2), self.peer(1)

    def rank(self, d):
        u = 1 - self.u if d & 4 else self.u
        y = 1 - self.y if d & 2 else self.y
        c = 1 - self.c if d & 1 else self.c
        return u * 4 + y * 2 + c

    def chip(self, d):
        return self.rank(d) // 2

    def peer(self, d):
        u = 1 - self.u if d & 4 else self.u
        y = 1 - self.y if d & 2 else self.y
        c = 1 - self.c if d & 1 else self.c
        return {BATCH: self.b, ULY: u, BLK: y * 2 + c}

    def along(self, step):
        return {BATCH: self.b + step, ULY: self.u, BLK: self.y * 2 + self.c}

    def barrier(self):
        sem = pltpu.get_barrier_semaphore()
        for d in range(1, 8):
            pl.semaphore_signal(sem, inc=1, device_id=self.peer(d), device_id_type=MESH)

        @pl.when(self.b > 0)
        def _():
            pl.semaphore_signal(sem, inc=1, device_id=self.along(-1), device_id_type=MESH)

        @pl.when(self.b < self.planes - 1)
        def _():
            pl.semaphore_signal(sem, inc=1, device_id=self.along(1), device_id_type=MESH)

        below = (self.b > 0).astype(jnp.int32)
        above = (self.b < self.planes - 1).astype(jnp.int32)
        pl.semaphore_wait(sem, 7 + below + above)


class Mail:
    def __init__(self, send, recv):
        self.send, self.recv, self.used, self.open = send, recv, 0, []

    def slots(self, n):
        first = self.used
        self.used += n
        return first

    def copy(self, src, dst, slot, device, recv_slot=None):
        return pltpu.make_async_remote_copy(
            src_ref=src,
            dst_ref=dst,
            send_sem=self.send.at[slot],
            recv_sem=self.recv.at[slot if recv_slot is None else recv_slot],
            device_id=device,
            device_id_type=MESH,
        )

    def post(self, src, dst, slot, device):
        made = self.copy(src, dst, slot, device)
        made.start()
        self.open.append(made)

    def arrived(self, dst, slot, device):
        self.copy(dst, dst, slot, device).wait_recv()

    def close(self):
        for made in self.open:
            made.wait_send()


class PlaneGather:
    def __init__(self, at, mail, shard, whole):
        self.at, self.mail, self.shard, self.whole = at, mail, shard, whole
        self.rows = shard.shape[1]
        self.base = mail.slots(8)

    def block(self, d, half=None):
        rows = pl.ds(pl.multiple_of(self.at.rank(d) * self.rows, self.rows), self.rows)
        halves = self.shard.shape[0] // 2
        if half is None:
            return self.whole.at[:, rows, :]
        return self.whole.at[pl.ds(half * halves, halves), rows, :]

    def start(self):
        at, mail, s = self.at, self.mail, self.base
        mine = self.block(0)
        mail.post(self.shard, mine, s, at.xn)
        mail.post(self.shard, mine, s + 1, at.yn)
        mail.post(self.shard, mine, s + 2, at.pn)
        mine[...] = self.shard[...]

    def relay(self):
        at, mail, s = self.at, self.mail, self.base
        mail.arrived(self.block(2), s + 1, at.yn)
        mail.post(self.block(2, 0), self.block(2, 0), s + 3, at.xn)
        mail.arrived(self.block(4), s, at.xn)
        mail.post(self.block(4, 1), self.block(4, 1), s + 4, at.yn)
        mail.post(self.block(2), self.block(2), s + 5, at.pn)
        mail.post(self.block(4), self.block(4), s + 6, at.pn)

    def finish(self):
        at, mail, s = self.at, self.mail, self.base
        mail.arrived(self.block(6, 0), s + 3, at.xn)
        mail.arrived(self.block(6, 1), s + 4, at.yn)
        mail.post(self.block(6), self.block(6), s + 7, at.pn)
        mail.arrived(self.block(1), s + 2, at.pn)
        mail.arrived(self.block(3), s + 5, at.pn)
        mail.arrived(self.block(5), s + 6, at.pn)
        mail.arrived(self.block(7), s + 7, at.pn)


class LineGather:
    def __init__(self, at, mail, held):
        self.at, self.mail, self.held = at, mail, held
        self.up, self.down = mail.slots(at.planes), mail.slots(at.planes)

    def pass_on(self, slot, src=None):
        at = self.at
        part = self.held.at[slot]
        src = part if src is None else src

        @pl.when((slot <= at.b) & (at.b < at.planes - 1))
        def _():
            self.mail.copy(src, part, self.up + slot, at.along(1)).start()

        @pl.when((slot >= at.b) & (at.b > 0))
        def _():
            self.mail.copy(src, part, self.down + slot, at.along(-1)).start()

    def start(self, src=None):
        self.pass_on(self.at.b, src)

    def take(self, distance):
        at = self.at

        @pl.when(at.b >= distance)
        def _():
            slot = at.b - distance
            self.mail.arrived(self.held.at[slot], self.up + slot, at.along(-1))
            self.pass_on(slot)

        @pl.when(at.b + distance < at.planes)
        def _():
            slot = at.b + distance
            self.mail.arrived(self.held.at[slot], self.down + slot, at.along(1))
            self.pass_on(slot)

    def close(self):
        at = self.at
        for slot in range(at.planes):
            part = self.held.at[slot]

            @pl.when((slot <= at.b) & (at.b < at.planes - 1))
            def _():
                self.mail.copy(part, part, self.up + slot, at.along(1)).wait_send()

            @pl.when((slot >= at.b) & (at.b > 0))
            def _():
                self.mail.copy(part, part, self.down + slot, at.along(-1)).wait_send()


class PlaneExchange:
    def __init__(self, at, mail, piece, landing):
        self.at, self.mail, self.piece, self.landing = at, mail, piece, landing
        self.base = mail.slots(8)

    def start(self):
        at = self.at
        for d in range(1, 8):
            self.mail.post(
                self.piece(at.rank(d)), self.landing(at.t), self.base + d, at.peer(d)
            )
        self.landing(at.t)[...] = self.piece(at.t)[...]

    def finish(self):
        at = self.at
        for d in range(1, 8):
            self.mail.arrived(self.landing(at.rank(d)), self.base + d, at.peer(d))


class PairExchange:
    def __init__(self, at, mail, src, dst, landed):
        self.at, self.mail, self.src, self.dst, self.landed = at, mail, src, dst, landed
        self.base = mail.slots(1)

    def start(self):
        self.mail.post(self.src, self.dst, self.base, self.at.pn)

    def finish(self):
        self.mail.arrived(self.landed, self.base, self.at.pn)


GATHER_SLOTS = 16 + 5 * 8 + 3 * 8 + 1


def gather_kernel(planes, x, cot, wq_s, wu_s, wd_s, wo_s, vec, xa, ca, wq, wu, wd, wo2, va, wo, send, recv):
    at = Place(planes)
    at.barrier()
    mail = Mail(send, recv)
    b, t, c = at.b, at.t, at.c
    rows = wq_s.shape[1]
    depth = wd_s.shape[0]
    pair = planes // 2
    gx = PlaneGather(at, mail, x, xa)
    gc = PlaneGather(at, mail, cot, ca)
    line_wd, line_wo, line_v = LineGather(at, mail, wd), LineGather(at, mail, wo), LineGather(at, mail, va)
    line_wq, line_wu = LineGather(at, mail, wq), LineGather(at, mail, wu)

    def strip(whole):
        return lambda rank: whole.at[b, pl.ds(pl.multiple_of(rank * rows, rows), rows), :]

    ex_q = PlaneExchange(at, mail, lambda rank: wq_s.at[rank], strip(wq))
    ex_u = PlaneExchange(at, mail, lambda rank: wu_s.at[rank], strip(wu))
    ex_v = PlaneExchange(at, mail, lambda rank: vec, lambda rank: va.at[b, rank])
    line_wd.start(wd_s)
    ex_q.start()
    gx.start()
    ex_u.start()
    ex_v.start()
    line_wo.start(wo_s)
    gc.start()
    wd[b] = wd_s[...]
    wo[b] = wo_s[...]
    ex_q.finish()
    line_wq.start()
    gx.relay()
    ex_u.finish()
    line_wu.start()
    ex_v.finish()
    line_v.start()
    gx.finish()
    gc.relay()
    lines = (line_wd, line_wo, line_wq, line_wu, line_v)
    for distance in range(1, planes):
        for line in lines:
            line.take(distance)
        if distance == 1:
            gc.finish()
    mine = wo2.at[:, c]
    swap = PairExchange(
        at, mail, wo.at[pl.ds(pair * (1 - c), pair)], mine, wo2.at[:, 1 - c]
    )
    swap.start()
    mine[...] = wo[pl.ds(pair * c, pair)]
    swap.finish()
    mail.close()
    for line in lines:
        line.close()


class PlaneReduce:
    def __init__(self, at, mail, terms, out, pairs, sums, side):
        self.at, self.mail, self.terms, self.out = at, mail, terms, out
        self.pairs, self.sums, self.side = pairs, sums, side
        self.base = mail.slots(8)
        self.order = (6, 4, 2, 0)
        self.halves = terms.shape[0] // 2

    def start(self):
        at = self.at
        for i, d in enumerate(self.order):
            chip = at.chip(d)
            self.mail.post(
                self.terms.at[:, chip, 1 - at.c], self.pairs.at[:, chip], self.base + i, at.pn
            )

    def half(self, ref, i):
        return ref.at[pl.ds(i * self.halves, self.halves)]

    def fold(self):
        at, mail, s = self.at, self.mail, self.base
        for i, d in enumerate(self.order):
            chip = at.chip(d)
            mail.arrived(self.pairs.at[:, chip], s + i, at.pn)
            total = self.terms[:, chip, at.c].astype(jnp.float32) + self.pairs[:, chip].astype(
                jnp.float32
            )
            self.sums[:, chip] = total.astype(self.sums.dtype)
            if d == 6:
                far = self.sums.at[:, chip]
                mail.post(self.half(far, 0), self.half(self.side.at[0], 0), s + 4, at.xn)
                mail.post(self.half(far, 1), self.half(self.side.at[0], 1), s + 5, at.yn)

    def turn(self):
        at, mail, s = self.at, self.mail, self.base
        for i, d, other, slot, nbr in ((1, 4, at.yn, 5, at.xn), (0, 2, at.xn, 4, at.yn)):
            chip = at.chip(d)
            landed = self.half(self.side.at[0], i)
            mail.arrived(landed, s + slot, other)
            part = self.half(self.sums.at[:, chip], i)
            part[...] = (part[...].astype(jnp.float32) + landed[...].astype(jnp.float32)).astype(
                self.sums.dtype
            )
            whole = self.sums.at[:, chip]
            mail.post(whole, self.side.at[2 - i], s + 6 + i, nbr)

    def finish(self):
        at, mail, s = self.at, self.mail, self.base
        mail.arrived(self.side.at[1], s + 7, at.xn)
        mail.arrived(self.side.at[2], s + 6, at.yn)
        self.out[...] = (
            self.sums[:, at.chip(0)].astype(jnp.float32)
            + self.side[1].astype(jnp.float32)
            + self.side[2].astype(jnp.float32)
        )


class LineReduce:
    def __init__(self, at, mail, terms, above, below):
        self.at, self.mail, self.terms = at, mail, terms
        self.above, self.below = above, below
        self.up, self.down = mail.slots(at.planes), mail.slots(at.planes)

    def run(self, rank):
        last = self.at.planes - 1
        self.forward_up(last - rank)
        self.forward_down(rank)

    def forward_up(self, slot):
        self._forward(slot, self.below, self.up, 1, self.at.b < slot, self.at.b == 0)

    def forward_down(self, slot):
        self._forward(
            slot, self.above, self.down, -1, self.at.b > slot, self.at.b == self.at.planes - 1
        )

    def _forward(self, slot, held, base, step, ahead, edge):
        at, mail = self.at, self.mail
        part = held.at[slot]

        @pl.when(ahead & edge)
        def _():
            mail.copy(self.terms.at[slot], part, base + slot, at.along(step)).start()

        @pl.when(ahead & jnp.logical_not(edge))
        def _():
            mail.arrived(part, base + slot, at.along(-step))
            total = self.terms[slot].astype(jnp.float32) + part[...].astype(jnp.float32)
            part[...] = total.astype(part.dtype)
            mail.copy(part, part, base + slot, at.along(step)).start()

    def finish(self, out):
        at, mail = self.at, self.mail
        b = at.b
        kind = out.dtype

        @pl.when(b == 0)
        def _():
            mail.arrived(self.above.at[b], self.down + b, at.along(1))
            out[...] = (
                self.terms[b].astype(jnp.float32) + self.above[b].astype(jnp.float32)
            ).astype(kind)

        @pl.when(b == at.planes - 1)
        def _():
            mail.arrived(self.below.at[b], self.up + b, at.along(-1))
            out[...] = (
                self.terms[b].astype(jnp.float32) + self.below[b].astype(jnp.float32)
            ).astype(kind)

        @pl.when((b > 0) & (b < at.planes - 1))
        def _():
            mail.arrived(self.below.at[b], self.up + b, at.along(-1))
            mail.arrived(self.above.at[b], self.down + b, at.along(1))
            out[...] = (
                self.terms[b].astype(jnp.float32)
                + self.below[b].astype(jnp.float32)
                + self.above[b].astype(jnp.float32)
            ).astype(kind)

    def close(self):
        at = self.at
        for slot in range(at.planes):
            part = self.terms.at[slot]

            @pl.when(at.b < slot)
            def _():
                self.mail.copy(part, part, self.up + slot, at.along(1)).wait_send()

            @pl.when(at.b > slot)
            def _():
                self.mail.copy(part, part, self.down + slot, at.along(-1)).wait_send()


REDUCE_SLOTS = 16 + 5 * 8 + 3 * 8 + 1


def reduce_kernel(
    planes, po, pg, gq, gu, gd, go, vec,
    out, gin, dq, du, dd, do, dv,
    pairs_o, sums_o, side_o, pairs_g, sums_g, side_g,
    go4, go_in, vec_in, vec_sum, fq, fu, aq, bq, au, bu, ad, bd, ao, bo, av, bv, send, recv,
):
    at = Place(planes)
    at.barrier()
    mail = Mail(send, recv)
    t, c = at.t, at.c
    rows = dq.shape[1]
    pair = planes // 2
    ro = PlaneReduce(at, mail, po, out, pairs_o, sums_o, side_o)
    rg = PlaneReduce(at, mail, pg, gin, pairs_g, sums_g, side_g)
    swap = PairExchange(
        at, mail, go.at[:, 1 - c], go4.at[pl.ds(pair * c, pair)], go4.at[pl.ds(pair * (1 - c), pair)]
    )
    ex_v = PlaneExchange(at, mail, lambda rank: vec.at[:, rank], lambda rank: vec_in.at[rank])
    line_d, line_o = LineReduce(at, mail, gd, ad, bd), LineReduce(at, mail, go4, ao, bo)
    line_q, line_u = LineReduce(at, mail, gq, aq, bq), LineReduce(at, mail, gu, au, bu)
    line_v = LineReduce(at, mail, vec_sum, av, bv)

    def strip(whole):
        return lambda rank: whole.at[pl.ds(pl.multiple_of(rank * rows, rows), rows), :]

    ex_q = PlaneExchange(at, mail, strip(fq), lambda rank: dq.at[rank])
    ex_u = PlaneExchange(at, mail, strip(fu), lambda rank: du.at[rank])
    line_u.run(0)
    line_q.run(0)
    swap.start()
    ex_v.start()
    ro.start()
    rg.start()
    go4[pl.ds(pair * c, pair)] = go[:, c]
    line_u.run(1)
    line_q.run(1)
    line_u.run(2)
    line_q.run(2)
    line_d.run(0)
    ex_v.finish()
    swap.finish()
    vec_sum[...] = jnp.sum(vec_in[...], axis=0)
    line_o.run(0)
    line_v.run(0)
    ro.fold()
    rg.fold()
    line_d.run(1)
    ro.turn()
    rg.turn()
    for line in (line_o, line_v):
        line.run(1)
    for line in (line_d, line_o, line_v):
        line.run(2)
    line_u.finish(fu)
    ex_u.start()
    line_q.finish(fq)
    ex_q.start()
    ro.finish()
    rg.finish()
    line_d.finish(dd)
    line_o.finish(do)
    line_v.finish(dv)
    ex_u.finish()
    ex_q.finish()
    mail.close()
    for line in (line_u, line_q, line_d, line_o, line_v):
        line.close()


VMEM = pl.BlockSpec(memory_space=pltpu.VMEM)


def call(kernel, outs, scratch, slots, number, *operands):
    return pl.pallas_call(
        kernel,
        out_shape=[jax.ShapeDtypeStruct(shape, kind) for shape, kind in outs],
        in_specs=[VMEM] * len(operands),
        out_specs=[VMEM] * len(outs),
        scratch_shapes=[pltpu.VMEM(shape, kind) for shape, kind in scratch]
        + [pltpu.SemaphoreType.DMA((slots,)), pltpu.SemaphoreType.DMA((slots,))],
        compiler_params=pltpu.CompilerParams(
            collective_id=number, has_side_effects=True, vmem_limit_bytes=60 * 2**20
        ),
    )(*operands)


def body(shape, *operands):
    residual_in, qkv_weight, down_weight = operands[0], operands[1], operands[11]
    planes = shape[BATCH]
    ranks = shape[ULY] * shape[BLK]
    heads = residual_in.shape[2] // HD
    fits = (
        shape[ULY] == 2
        and shape[BLK] == 4
        and planes % 2 == 0
        and residual_in.shape[1] % 2 == 0
        and 2 * qkv_weight.shape[0] == HD
        and heads == ranks * planes // 2
        and down_weight.shape[0] % 128 == 0
    )
    return fast_body(planes, *operands) if fits else general_body(*operands)


def fast_body(
    planes,
    residual_in,
    qkv_weight,
    qkv_bias,
    dense_weight,
    dense_bias,
    norm1_gain,
    norm1_bias,
    norm2_gain,
    norm2_bias,
    up_weight,
    up_bias,
    down_weight,
    down_bias,
    cotangent,
):
    single = jnp.float32
    half_type = jnp.bfloat16
    ranks = 8
    tok_rows, seqs, width = residual_in.shape
    rows = qkv_weight.shape[0]
    depth = down_weight.shape[0]
    hidden = planes * depth
    pair = planes // 2
    own_heads = pair
    head_cols = own_heads * HD
    length = ranks * tok_rows
    rotary = HD // 4
    scale_factor = 1.0 / math.sqrt(HD)
    k_index = lax.axis_index(BLK)
    rank = lax.axis_index(ULY) * 4 + k_index
    chip, core = rank // 2, rank % 2

    x_own = jnp.transpose(residual_in, (1, 0, 2))
    cot_own = jnp.transpose(cotangent, (1, 0, 2))
    wq_send = jnp.transpose(
        qkv_weight.reshape(rows, 3, 2, pair, ranks // 2, HD), (4, 2, 0, 1, 3, 5)
    ).reshape(ranks, rows, 3 * head_cols)
    wu_send = jnp.transpose(
        up_weight.reshape(rows, planes, ranks, depth), (2, 0, 1, 3)
    ).reshape(ranks, rows, hidden)
    vectors = (
        qkv_bias, up_bias, dense_bias, norm1_gain, norm1_bias, norm2_gain, norm2_bias, down_bias,
    )
    sizes = [v.shape[0] for v in vectors]
    room = -(-sum(sizes) // 1024) * 1024
    lanes = (room // 128, 128)
    vec = jnp.concatenate(
        [v.astype(single) for v in vectors] + [jnp.zeros((room - sum(sizes),), single)]
    ).reshape(lanes)

    x_all, cot_all, wq, wu, wd, wo, vec_all = call(
        functools.partial(gather_kernel, planes),
        [
            ((seqs, length, width), half_type),
            ((seqs, length, width), half_type),
            ((planes, ranks * rows, 3 * head_cols), half_type),
            ((planes, ranks * rows, hidden), half_type),
            ((planes, depth, width), half_type),
            ((pair, 2, rows, width), half_type),
            ((planes, ranks) + lanes, single),
        ],
        [((planes, rows, width), half_type)],
        GATHER_SLOTS,
        0,
        x_own,
        cot_own,
        wq_send,
        wu_send,
        down_weight,
        dense_weight,
        vec,
    )
    wq = wq.reshape(width, 3 * head_cols)
    wu = wu.reshape(width, hidden)
    wd = wd.reshape(hidden, width)
    wo = wo.reshape(head_cols, width)
    flat = vec_all.reshape(planes * ranks, room)
    ends = [sum(sizes[:i]) for i in range(len(sizes) + 1)]
    b_qkv, b_up, b_dense, gain_one, shift_one, gain_two, shift_two, b_down = [
        flat[:, ends[i] : ends[i + 1]].reshape(-1) for i in range(len(sizes))
    ]
    bq = lax.dynamic_slice(
        b_qkv.reshape(3, 2, pair, ranks // 2, HD), (0, core, 0, chip, 0), (3, 1, pair, 1, HD)
    ).reshape(3 * head_cols)
    bu = lax.dynamic_slice(
        b_up.reshape(planes, ranks, depth), (0, rank, 0), (planes, 1, depth)
    ).reshape(hidden)

    inputs_f = x_all.astype(single)
    normed, inverse = layer_norm(inputs_f)
    act_one = (normed * gain_one + shift_one).astype(half_type)
    act_two = (normed * gain_two + shift_two).astype(half_type)
    qkv = jnp.einsum("std,df->tsf", act_one, wq, preferred_element_type=single) + bq
    cosine, sine_table = rotary_tables(jnp.arange(length, dtype=jnp.int32), rotary)
    qkv = qkv.reshape(length, seqs, 3, own_heads, HD)
    query = rotate_fwd(qkv[:, :, 0], cosine, sine_table, rotary).astype(half_type)
    key = rotate_fwd(qkv[:, :, 1], cosine, sine_table, rotary).astype(half_type)
    value = qkv[:, :, 2].astype(half_type)
    scores = jnp.einsum("qshd,kshd->shqk", query, key, preferred_element_type=single) * scale_factor
    places = jnp.arange(length, dtype=jnp.int32)
    scores = jnp.where((places[None, :] <= places[:, None])[None, None], scores, -jnp.inf)
    top = jnp.max(scores, axis=-1, keepdims=True)
    log_total = top + jnp.log(jnp.sum(jnp.exp(scores - top), axis=-1, keepdims=True))
    probs = jnp.exp(scores - log_total)
    probs_b = probs.astype(half_type)
    attn = jnp.einsum("shqk,kshd->sqhd", probs_b, value, preferred_element_type=single).astype(
        half_type
    )
    attn_flat = attn.reshape(seqs, length, head_cols)
    pre = jnp.einsum("std,df->stf", act_two, wu, preferred_element_type=single) + bu
    gelu_out = gelu_value(pre).astype(half_type)
    out_terms = jnp.einsum("std,de->ste", attn_flat, wo, preferred_element_type=single) + jnp.einsum(
        "stf,fd->std", gelu_out, wd, preferred_element_type=single
    )
    down_w_grad = jnp.einsum("stf,std->fd", gelu_out, cot_all, preferred_element_type=single)
    gelu_grad = jnp.einsum("std,fd->stf", cot_all, wd, preferred_element_type=single)
    pre_grad = (gelu_grad * gelu_slope(pre)).astype(half_type)
    up_w_grad = jnp.einsum("std,stf->df", act_two, pre_grad, preferred_element_type=single)
    up_b_grad = jnp.sum(pre_grad.astype(single), axis=(0, 1))
    act_two_grad = jnp.einsum("stf,df->std", pre_grad, wu, preferred_element_type=single)
    dense_w_grad = jnp.einsum("std,ste->de", attn_flat, cot_all, preferred_element_type=single)
    attn_grad = jnp.einsum("ste,de->std", cot_all, wo, preferred_element_type=single).astype(
        half_type
    ).reshape(seqs, length, own_heads, HD)
    value_grad = jnp.einsum("shqk,sqhd->kshd", probs_b, attn_grad, preferred_element_type=single)
    grad_prob = jnp.einsum("sqhd,kshd->shqk", attn_grad, value, preferred_element_type=single)
    delta = jnp.transpose(
        jnp.sum(attn_grad.astype(single) * attn.astype(single), axis=-1), (0, 2, 1)
    )
    grad_score = (probs * (grad_prob - delta[..., None]) * scale_factor).astype(half_type)
    query_grad = jnp.einsum("shqk,kshd->qshd", grad_score, key, preferred_element_type=single)
    key_grad = jnp.einsum("shqk,qshd->kshd", grad_score, query, preferred_element_type=single)
    qkv_grad = jnp.stack(
        [
            rotate_back(query_grad, cosine, sine_table, rotary),
            rotate_back(key_grad, cosine, sine_table, rotary),
            value_grad,
        ],
        axis=2,
    ).astype(half_type).reshape(length, seqs, 3 * head_cols)
    qkv_w_grad = jnp.einsum("std,tsf->df", act_one, qkv_grad, preferred_element_type=single)
    qkv_b_grad = jnp.sum(qkv_grad.astype(single), axis=(0, 1))
    act_one_grad = jnp.einsum("tsf,df->std", qkv_grad, wq, preferred_element_type=single)
    in_terms = act_one_grad * gain_one + act_two_grad * gain_two
    bias_sum = jnp.sum(cot_own.astype(single), axis=(0, 1))
    small = (
        lax.dynamic_update_slice(
            jnp.zeros((3, 2, pair, ranks // 2, HD), single),
            qkv_b_grad.reshape(3, 1, pair, 1, HD),
            (0, core, 0, chip, 0),
        ),
        lax.dynamic_update_slice(
            jnp.zeros((planes, ranks, depth), single),
            up_b_grad.reshape(planes, 1, depth),
            (0, rank, 0),
        ),
        bias_sum,
        jnp.sum(act_one_grad * normed, axis=(0, 1)),
        jnp.sum(act_one_grad, axis=(0, 1)),
        jnp.sum(act_two_grad * normed, axis=(0, 1)),
        jnp.sum(act_two_grad, axis=(0, 1)),
    )
    small_vec = jnp.concatenate(
        [v.reshape(planes, ranks, -1) for v in small]
        + [jnp.zeros((planes, ranks, room - sum(sizes[:-1])), single)],
        axis=-1,
    ).reshape((planes, ranks) + lanes)

    plane_terms = (seqs, ranks // 2, 2, tok_rows, width)
    shard = (seqs, tok_rows, width)
    plane_scratch = [
        ((seqs, ranks // 2, tok_rows, width), half_type),
        ((seqs, ranks // 2, tok_rows, width), half_type),
        ((3,) + shard, half_type),
    ]
    q_shape = (planes, ranks * rows, 3 * head_cols)
    u_shape = (planes, ranks * rows, hidden)
    d_shape = (planes, depth, width)
    o_shape = (planes, rows, width)
    v_shape = (planes,) + lanes
    out_sum, in_sum, dq, du, dd, do, dv = call(
        functools.partial(reduce_kernel, planes),
        [
            (shard, single),
            (shard, single),
            ((ranks, rows, 3 * head_cols), half_type),
            ((ranks, rows, hidden), half_type),
            ((depth, width), single),
            ((rows, width), single),
            (lanes, single),
        ],
        plane_scratch * 2
        + [
            (o_shape, half_type),
            (o_shape, half_type),
            ((ranks,) + v_shape, single),
            (v_shape, single),
            (q_shape[1:], half_type),
            (u_shape[1:], half_type),
        ]
        + [
            (s, k)
            for s, k in (
                (q_shape, half_type),
                (u_shape, half_type),
                (d_shape, half_type),
                (o_shape, half_type),
                (v_shape, single),
            )
            for _ in range(2)
        ],
        REDUCE_SLOTS,
        1,
        out_terms.astype(half_type).reshape(plane_terms),
        in_terms.astype(half_type).reshape(plane_terms),
        qkv_w_grad.astype(half_type).reshape(q_shape),
        up_w_grad.astype(half_type).reshape(u_shape),
        down_w_grad.astype(half_type).reshape(d_shape),
        dense_w_grad.astype(half_type).reshape(pair, 2, rows, width),
        small_vec,
    )
    x_f = x_own.astype(single)
    own_normed, own_inverse = layer_norm(x_f)
    output = jnp.transpose((x_f + out_sum + b_dense + b_down).astype(half_type), (1, 0, 2))
    input_grad = jnp.transpose(
        cot_own.astype(single) + norm_back(in_sum, own_normed, own_inverse, 1.0), (1, 0, 2)
    )
    qkv_grad_out = jnp.transpose(
        dq.reshape(ranks // 2, 2, rows, 3, pair, HD), (2, 3, 1, 4, 0, 5)
    ).reshape(qkv_weight.shape).astype(single)
    up_grad_out = jnp.transpose(
        du.reshape(ranks, rows, planes, depth), (1, 2, 0, 3)
    ).reshape(up_weight.shape).astype(single)
    flat_v = dv.reshape(room)
    pieces = [flat_v[ends[i] : ends[i + 1]] for i in range(7)]
    return (
        output,
        input_grad,
        qkv_grad_out,
        pieces[0],
        do,
        pieces[2],
        pieces[3],
        pieces[4],
        pieces[5],
        pieces[6],
        up_grad_out,
        pieces[1],
        dd,
        pieces[2],
    )


def solution(mesh):
    placed = (
        P(TOKENS, BATCH, None),
        P(AXES, None),
        P(AXES),
        P(AXES, None),
        P(AXES),
        P(AXES),
        P(AXES),
        P(AXES),
        P(AXES),
        P(AXES, None),
        P(AXES),
        P(AXES, None),
        P(AXES),
        P(TOKENS, BATCH, None),
    )
    return jax.shard_map(
        functools.partial(body, dict(mesh.shape)),
        mesh=mesh,
        in_specs=placed,
        out_specs=(
            P(TOKENS, BATCH, None),
            P(TOKENS, BATCH, None),
            P(AXES, None),
            P(AXES),
            P(AXES, None),
            P(AXES),
            P(AXES),
            P(AXES),
            P(AXES),
            P(AXES),
            P(AXES, None),
            P(AXES),
            P(AXES, None),
            P(AXES),
        ),
        check_vma=False,
    )
```

```python
import functools
import math

import jax
import jax.numpy as jnp
import numpy as np
from jax import lax
from jax.experimental import pallas as pl
from jax.experimental.pallas import tpu as pltpu
from jax.sharding import PartitionSpec as P

HD = 64
BATCH, ULY, BLK = "batch", "ulysses", "blk"
AXES = (BATCH, ULY, BLK)
TOKENS = (ULY, BLK)


EPSILON = 1e-05
INV_ROOT_TWO = 0.7071067811865476
INV_ROOT_TWO_PI = 0.3989422804014327


def layer_norm(values):
    center = jnp.mean(values, axis=-1, keepdims=True)
    shifted = values - center
    inverse = lax.rsqrt(jnp.mean(shifted * shifted, axis=-1, keepdims=True) + EPSILON)
    return (shifted * inverse, inverse)


def norm_back(gradient, normed, inverse, gain_vec):
    scaled = gradient * gain_vec
    return inverse * (
        scaled
        - jnp.mean(scaled, axis=-1, keepdims=True)
        - normed * jnp.mean(scaled * normed, axis=-1, keepdims=True)
    )


def gelu_value(pre_values):
    return 0.5 * pre_values * (1.0 + jax.scipy.special.erf(pre_values * INV_ROOT_TWO))


def gelu_slope(pre_values):
    normal_cdf = 0.5 * (1.0 + jax.scipy.special.erf(pre_values * INV_ROOT_TWO))
    return normal_cdf + pre_values * jnp.exp(-0.5 * pre_values * pre_values) * INV_ROOT_TWO_PI


def rotary_tables(positions, rotary):
    half_rot = rotary // 2
    frequency = 1.0 / 10000.0 ** (jnp.arange(half_rot, dtype=jnp.float32) * (2.0 / rotary))
    angles = positions.astype(jnp.float32)[:, None] * frequency[None, :]
    cosine = jnp.concatenate([jnp.cos(angles), jnp.cos(angles)], axis=-1)
    sine_table = jnp.concatenate([jnp.sin(angles), jnp.sin(angles)], axis=-1)
    return (cosine, sine_table)


def expand_table(table, tensor):
    extra_dims = (1,) * (tensor.ndim - 2)
    return table.reshape((table.shape[0],) + extra_dims + (table.shape[1],))


def rotate_fwd(tensor, cosine, sine_table, rotary):
    half_rot = rotary // 2
    cos_full = expand_table(cosine, tensor)
    sin_full = expand_table(sine_table, tensor)
    rot_part = tensor[..., :rotary]
    turned = jnp.concatenate([-rot_part[..., half_rot:], rot_part[..., :half_rot]], axis=-1)
    return jnp.concatenate([rot_part * cos_full + turned * sin_full, tensor[..., rotary:]], axis=-1)


def rotate_back(tensor, cosine, sine_table, rotary):
    half_rot = rotary // 2
    cos_full = expand_table(cosine, tensor)
    sin_full = expand_table(sine_table, tensor)
    rot_part = tensor[..., :rotary]
    weighted = rot_part * sin_full
    turned = jnp.concatenate([weighted[..., half_rot:], -weighted[..., :half_rot]], axis=-1)
    return jnp.concatenate([rot_part * cos_full + turned, tensor[..., rotary:]], axis=-1)


def general_body(
    residual_in,
    qkv_weight,
    qkv_bias,
    dense_weight,
    dense_bias,
    norm1_gain,
    norm1_bias,
    norm2_gain,
    norm2_bias,
    up_weight,
    up_bias,
    down_weight,
    down_bias,
    cotangent,
):
    single = jnp.float32
    half_type = jnp.bfloat16
    gathered = (
        lax.all_gather(qkv_weight, AXES, axis=0, tiled=True),
        lax.all_gather(qkv_bias, AXES, axis=0, tiled=True),
        lax.all_gather(dense_weight, AXES, axis=0, tiled=True),
        lax.all_gather(dense_bias, AXES, axis=0, tiled=True),
        lax.all_gather(norm1_gain, AXES, axis=0, tiled=True),
        lax.all_gather(norm1_bias, AXES, axis=0, tiled=True),
        lax.all_gather(norm2_gain, AXES, axis=0, tiled=True),
        lax.all_gather(norm2_bias, AXES, axis=0, tiled=True),
        lax.all_gather(up_weight, AXES, axis=0, tiled=True),
        lax.all_gather(up_bias, AXES, axis=0, tiled=True),
        lax.all_gather(down_weight, AXES, axis=0, tiled=True),
        lax.all_gather(down_bias, AXES, axis=0, tiled=True),
    )
    (
        w_qkv,
        b_qkv,
        w_dense,
        b_dense,
        gain_one,
        shift_one,
        gain_two,
        shift_two,
        w_up,
        b_up,
        w_down,
        b_down,
    ) = gathered
    tok_rows = residual_in.shape[0]
    seq_count = residual_in.shape[1]
    model_width = residual_in.shape[2]
    head_count = model_width // HD
    rotary = HD // 4
    scale_factor = 1.0 / math.sqrt(HD)
    blk_size = lax.axis_size(BLK)
    uly_size = lax.axis_size(ULY)
    blk_index = lax.axis_index(BLK)
    block_id = lax.axis_index(ULY) * blk_size + blk_index
    seq_pos = block_id * tok_rows + jnp.arange(tok_rows, dtype=jnp.int32)
    inputs_f = residual_in.astype(single)
    normed, inverse = layer_norm(inputs_f)
    act_one = (normed * gain_one.astype(single) + shift_one.astype(single)).astype(half_type)
    act_two = (normed * gain_two.astype(single) + shift_two.astype(single)).astype(half_type)
    qkv_full = jnp.einsum(
        "tsd,df->tsf", act_one, w_qkv, preferred_element_type=single
    ) + b_qkv.astype(single)
    cos_seq, sin_seq = rotary_tables(seq_pos, rotary)
    head_shape = (tok_rows, seq_count, head_count, HD)
    query_seq = (
        rotate_fwd(qkv_full[..., :model_width].reshape(head_shape), cos_seq, sin_seq, rotary)
        .reshape(tok_rows, seq_count, model_width)
        .astype(half_type)
    )
    key_seq = (
        rotate_fwd(
            qkv_full[..., model_width : 2 * model_width].reshape(head_shape),
            cos_seq,
            sin_seq,
            rotary,
        )
        .reshape(tok_rows, seq_count, model_width)
        .astype(half_type)
    )
    value_seq = qkv_full[..., 2 * model_width :].astype(half_type)
    query_loc, key_loc, value_loc = (
        lax.all_to_all(query_seq, ULY, split_axis=2, concat_axis=0, tiled=True),
        lax.all_to_all(key_seq, ULY, split_axis=2, concat_axis=0, tiled=True),
        lax.all_to_all(value_seq, ULY, split_axis=2, concat_axis=0, tiled=True),
    )
    local_rows = query_loc.shape[0]
    features = query_loc.shape[2]
    local_heads = features // HD
    key_all, value_all = (
        lax.all_gather(key_loc, BLK, axis=0, tiled=True),
        lax.all_gather(value_loc, BLK, axis=0, tiled=True),
    )
    total_rows = key_all.shape[0]
    row_ids = jnp.arange(local_rows, dtype=jnp.int32)
    query_pos = (row_ids // tok_rows * blk_size + blk_index) * tok_rows + row_ids % tok_rows
    block_rows = math.gcd(512, local_rows)
    n_blocks = local_rows // block_rows
    query_h = query_loc.reshape(local_rows, seq_count, local_heads, HD)
    key_h = jnp.transpose(
        key_all.reshape(blk_size, uly_size, tok_rows, seq_count, features), (1, 0, 2, 3, 4)
    ).reshape(total_rows, seq_count, local_heads, HD)
    value_h = jnp.transpose(
        value_all.reshape(blk_size, uly_size, tok_rows, seq_count, features), (1, 0, 2, 3, 4)
    ).reshape(total_rows, seq_count, local_heads, HD)
    zero_idx = jnp.zeros((), jnp.int32)
    step_ids = jnp.arange(n_blocks * seq_count, dtype=jnp.int32)
    row_shape = (block_rows, 1, local_heads, HD)

    def select(step_index):
        row_start = step_index // seq_count * block_rows
        seq_index = step_index % seq_count
        query_rows = lax.dynamic_slice(
            query_h, (row_start, seq_index, zero_idx, zero_idx), row_shape
        )
        limit = jnp.max(query_pos) // block_rows + 1
        return (row_start, seq_index, query_rows, query_pos, limit)

    def block_scores(query_rows, row_pos, key_index, seq_index):
        key_start = key_index * block_rows
        slot = (key_start, seq_index, zero_idx, zero_idx)
        key_rows = lax.dynamic_slice(key_h, slot, (block_rows, 1, local_heads, HD))
        value_rows = lax.dynamic_slice(value_h, slot, (block_rows, 1, local_heads, HD))
        scores = (
            jnp.einsum("qshd,kshd->shqk", query_rows, key_rows, preferred_element_type=single)
            * scale_factor
        )
        key_ids = key_start + jnp.arange(block_rows, dtype=jnp.int32)
        allowed = (key_ids[None, :] <= row_pos[:, None])[None, None]
        return (jnp.where(allowed, scores, -jnp.inf), key_rows, value_rows, slot)

    def forward_block(step_index):
        row_start, seq_index, query_rows, row_pos, limit = select(step_index)

        def total_step(key_index, carry):
            running_max, running_sum = carry
            masked, key_rows, value_rows, slot = block_scores(
                query_rows, row_pos, key_index, seq_index
            )
            new_max = jnp.maximum(running_max, jnp.max(masked, axis=-1))
            new_sum = running_sum * jnp.exp(running_max - new_max) + jnp.sum(
                jnp.exp(masked - new_max[..., None]), axis=-1
            )
            return (new_max, new_sum)

        start_max = jnp.full((1, local_heads, block_rows), -jnp.inf, single)
        start_sum = jnp.zeros((1, local_heads, block_rows), single)
        final_max, final_sum = lax.fori_loop(zero_idx, limit, total_step, (start_max, start_sum))
        log_total = final_max + jnp.log(final_sum)

        def value_step(key_index, acc):
            masked, key_rows, value_rows, slot = block_scores(
                query_rows, row_pos, key_index, seq_index
            )
            weights_b = jnp.exp(masked - log_total[..., None]).astype(half_type)
            return acc + jnp.einsum(
                "shqk,kshd->qshd", weights_b, value_rows, preferred_element_type=single
            )

        result = lax.fori_loop(zero_idx, limit, value_step, jnp.zeros(row_shape, single)).astype(
            half_type
        )
        return (result[:, 0], log_total)

    results, log_totals = lax.map(forward_block, step_ids)
    attn_h = jnp.transpose(
        results.reshape(n_blocks, seq_count, block_rows, local_heads, HD), (0, 2, 1, 3, 4)
    ).reshape(local_rows, seq_count, local_heads, HD)
    attn_seq = lax.all_to_all(
        attn_h.reshape(local_rows, seq_count, features),
        ULY,
        split_axis=0,
        concat_axis=2,
        tiled=True,
    )
    proj_out = jnp.einsum(
        "tsd,de->tse", attn_seq, w_dense, preferred_element_type=single
    ) + b_dense.astype(single)
    pre_act = jnp.einsum("tsd,df->tsf", act_two, w_up, preferred_element_type=single) + b_up.astype(
        single
    )
    gelu_out = gelu_value(pre_act).astype(half_type)
    mlp_out = jnp.einsum(
        "tsf,fd->tsd", gelu_out, w_down, preferred_element_type=single
    ) + b_down.astype(single)
    output = (inputs_f + proj_out + mlp_out).astype(half_type)
    back_params = (
        lax.all_gather(qkv_weight, AXES, axis=0, tiled=True),
        lax.all_gather(qkv_bias, AXES, axis=0, tiled=True),
        lax.all_gather(dense_weight, AXES, axis=0, tiled=True),
        lax.all_gather(dense_bias, AXES, axis=0, tiled=True),
        lax.all_gather(norm1_gain, AXES, axis=0, tiled=True),
        lax.all_gather(norm1_bias, AXES, axis=0, tiled=True),
        lax.all_gather(norm2_gain, AXES, axis=0, tiled=True),
        lax.all_gather(norm2_bias, AXES, axis=0, tiled=True),
        lax.all_gather(up_weight, AXES, axis=0, tiled=True),
        lax.all_gather(up_bias, AXES, axis=0, tiled=True),
        lax.all_gather(down_weight, AXES, axis=0, tiled=True),
        lax.all_gather(down_bias, AXES, axis=0, tiled=True),
    )
    back_qkv = back_params[0]
    back_dense = back_params[2]
    back_gain_one = back_params[4].astype(single)
    back_gain_two = back_params[6].astype(single)
    back_up = back_params[8]
    back_down = back_params[10]
    grad_f = cotangent.astype(single)
    bias_sum = jnp.sum(grad_f, axis=(0, 1))
    down_w_grad = jnp.einsum("tsf,tsd->fd", gelu_out, cotangent, preferred_element_type=single)
    gelu_grad = jnp.einsum("tsd,fd->tsf", cotangent, back_down, preferred_element_type=single)
    pre_grad = (gelu_grad * gelu_slope(pre_act)).astype(half_type)
    up_w_grad = jnp.einsum("tsd,tsf->df", act_two, pre_grad, preferred_element_type=single)
    up_b_grad = jnp.sum(pre_grad.astype(single), axis=(0, 1))
    act_two_grad = jnp.einsum("tsf,df->tsd", pre_grad, back_up, preferred_element_type=single)
    gain_two_grad = jnp.sum(act_two_grad * normed, axis=(0, 1))
    shift_two_grad = jnp.sum(act_two_grad, axis=(0, 1))
    dense_w_grad = jnp.einsum("tsd,tse->de", attn_seq, cotangent, preferred_element_type=single)
    attn_grad = jnp.einsum(
        "tse,de->tsd", cotangent, back_dense, preferred_element_type=single
    ).astype(half_type)
    grad_loc = lax.all_to_all(attn_grad, ULY, split_axis=2, concat_axis=0, tiled=True)
    grad_h = grad_loc.reshape(local_rows, seq_count, local_heads, HD)

    def backward_block(acc_pair, step_index):
        row_start, seq_index, query_rows, row_pos, limit = select(step_index)
        own_slot = (row_start, seq_index, zero_idx, zero_idx)
        out_rows = lax.dynamic_slice(attn_h, own_slot, row_shape)
        grad_rows = lax.dynamic_slice(grad_h, own_slot, row_shape)
        log_total = log_totals[step_index]
        delta_row = jnp.transpose(
            jnp.sum(grad_rows.astype(single) * out_rows.astype(single), axis=-1), (1, 2, 0)
        )

        def grad_step(key_index, carry):
            key_acc, value_acc, query_acc = carry
            masked, key_rows, value_rows, slot = block_scores(
                query_rows, row_pos, key_index, seq_index
            )
            probs_f = jnp.exp(masked - log_total[..., None])
            value_part = jnp.einsum(
                "shqk,qshd->kshd",
                probs_f.astype(half_type),
                grad_rows,
                preferred_element_type=single,
            )
            grad_prob = jnp.einsum(
                "qshd,kshd->shqk", grad_rows, value_rows, preferred_element_type=single
            )
            grad_score = (probs_f * (grad_prob - delta_row[..., None]) * scale_factor).astype(
                half_type
            )
            query_acc = query_acc + jnp.einsum(
                "shqk,kshd->qshd", grad_score, key_rows, preferred_element_type=single
            )
            key_part = jnp.einsum(
                "shqk,qshd->kshd", grad_score, query_rows, preferred_element_type=single
            )
            key_acc = lax.dynamic_update_slice(
                key_acc, lax.dynamic_slice(key_acc, slot, key_part.shape) + key_part, slot
            )
            value_acc = lax.dynamic_update_slice(
                value_acc, lax.dynamic_slice(value_acc, slot, value_part.shape) + value_part, slot
            )
            return (key_acc, value_acc, query_acc)

        key_acc, value_acc, query_acc = lax.fori_loop(
            zero_idx, limit, grad_step, (acc_pair[0], acc_pair[1], jnp.zeros(row_shape, single))
        )
        return ((key_acc, value_acc), query_acc[:, 0])

    acc_zero = jnp.zeros((total_rows, seq_count, local_heads, HD), single)
    acc_final, query_parts = lax.scan(backward_block, (acc_zero, acc_zero), step_ids)
    query_grad = jnp.transpose(
        query_parts.reshape(n_blocks, seq_count, block_rows, local_heads, HD), (0, 2, 1, 3, 4)
    ).reshape(local_rows, seq_count, local_heads, HD)
    key_terms = jnp.transpose(
        acc_final[0].reshape(uly_size, blk_size, tok_rows, seq_count, features), (1, 0, 2, 3, 4)
    ).reshape(total_rows, seq_count, features)
    value_terms = jnp.transpose(
        acc_final[1].reshape(uly_size, blk_size, tok_rows, seq_count, features), (1, 0, 2, 3, 4)
    ).reshape(total_rows, seq_count, features)
    key_back, value_back = (
        lax.psum_scatter(key_terms, BLK, scatter_dimension=0, tiled=True),
        lax.psum_scatter(value_terms, BLK, scatter_dimension=0, tiled=True),
    )
    cos_h, sin_h = rotary_tables(query_pos, rotary)
    query_send = (
        rotate_back(query_grad, cos_h, sin_h, rotary)
        .reshape(local_rows, seq_count, features)
        .astype(half_type)
    )
    key_send = (
        rotate_back(key_back.reshape(local_rows, seq_count, local_heads, HD), cos_h, sin_h, rotary)
        .reshape(local_rows, seq_count, features)
        .astype(half_type)
    )
    value_send = value_back.astype(half_type)
    query_ret, key_ret, value_ret = (
        lax.all_to_all(query_send, ULY, split_axis=0, concat_axis=2, tiled=True),
        lax.all_to_all(key_send, ULY, split_axis=0, concat_axis=2, tiled=True),
        lax.all_to_all(value_send, ULY, split_axis=0, concat_axis=2, tiled=True),
    )
    qkv_grad = jnp.concatenate([query_ret, key_ret, value_ret], axis=-1)
    qkv_w_grad = jnp.einsum("tsd,tsf->df", act_one, qkv_grad, preferred_element_type=single)
    qkv_b_grad = jnp.sum(qkv_grad.astype(single), axis=(0, 1))
    act_one_grad = jnp.einsum("tsf,df->tsd", qkv_grad, back_qkv, preferred_element_type=single)
    gain_one_grad = jnp.sum(act_one_grad * normed, axis=(0, 1))
    shift_one_grad = jnp.sum(act_one_grad, axis=(0, 1))
    input_grad = (
        grad_f
        + norm_back(act_one_grad, normed, inverse, back_gain_one)
        + norm_back(act_two_grad, normed, inverse, back_gain_two)
    )
    summed = (
        lax.psum_scatter(qkv_w_grad, AXES, scatter_dimension=0, tiled=True),
        lax.psum_scatter(qkv_b_grad, AXES, scatter_dimension=0, tiled=True),
        lax.psum_scatter(
            dense_w_grad, AXES, scatter_dimension=0, tiled=True
        ),
        lax.psum_scatter(bias_sum, AXES, scatter_dimension=0, tiled=True),
        lax.psum_scatter(
            gain_one_grad, AXES, scatter_dimension=0, tiled=True
        ),
        lax.psum_scatter(
            shift_one_grad, AXES, scatter_dimension=0, tiled=True
        ),
        lax.psum_scatter(
            gain_two_grad, AXES, scatter_dimension=0, tiled=True
        ),
        lax.psum_scatter(
            shift_two_grad, AXES, scatter_dimension=0, tiled=True
        ),
        lax.psum_scatter(up_w_grad, AXES, scatter_dimension=0, tiled=True),
        lax.psum_scatter(up_b_grad, AXES, scatter_dimension=0, tiled=True),
        lax.psum_scatter(down_w_grad, AXES, scatter_dimension=0, tiled=True),
        lax.psum_scatter(bias_sum, AXES, scatter_dimension=0, tiled=True),
    )
    return (
        output,
        input_grad,
        summed[0],
        summed[1],
        summed[2],
        summed[3],
        summed[4],
        summed[5],
        summed[6],
        summed[7],
        summed[8],
        summed[9],
        summed[10],
        summed[11],
    )


MESH = pl.DeviceIdType.MESH


class Place:
    def __init__(self, planes):
        self.planes = planes
        self.b = lax.axis_index(BATCH)
        self.u = lax.axis_index(ULY)
        k = lax.axis_index(BLK)
        self.y, self.c = k // 2, k % 2
        self.t = self.u * 4 + k
        self.xn, self.yn, self.pn = self.peer(4), self.peer(2), self.peer(1)

    def rank(self, d):
        u = 1 - self.u if d & 4 else self.u
        y = 1 - self.y if d & 2 else self.y
        c = 1 - self.c if d & 1 else self.c
        return u * 4 + y * 2 + c

    def chip(self, d):
        return self.rank(d) // 2

    def peer(self, d):
        u = 1 - self.u if d & 4 else self.u
        y = 1 - self.y if d & 2 else self.y
        c = 1 - self.c if d & 1 else self.c
        return {BATCH: self.b, ULY: u, BLK: y * 2 + c}

    def along(self, step):
        return {BATCH: self.b + step, ULY: self.u, BLK: self.y * 2 + self.c}

    def barrier(self):
        sem = pltpu.get_barrier_semaphore()
        for d in range(1, 8):
            pl.semaphore_signal(sem, inc=1, device_id=self.peer(d), device_id_type=MESH)

        @pl.when(self.b > 0)
        def _():
            pl.semaphore_signal(sem, inc=1, device_id=self.along(-1), device_id_type=MESH)

        @pl.when(self.b < self.planes - 1)
        def _():
            pl.semaphore_signal(sem, inc=1, device_id=self.along(1), device_id_type=MESH)

        below = (self.b > 0).astype(jnp.int32)
        above = (self.b < self.planes - 1).astype(jnp.int32)
        pl.semaphore_wait(sem, 7 + below + above)


class Mail:
    def __init__(self, send, recv):
        self.send, self.recv, self.used, self.open = send, recv, 0, []

    def slots(self, n):
        first = self.used
        self.used += n
        return first

    def copy(self, src, dst, slot, device, recv_slot=None):
        return pltpu.make_async_remote_copy(
            src_ref=src,
            dst_ref=dst,
            send_sem=self.send.at[slot],
            recv_sem=self.recv.at[slot if recv_slot is None else recv_slot],
            device_id=device,
            device_id_type=MESH,
        )

    def post(self, src, dst, slot, device):
        made = self.copy(src, dst, slot, device)
        made.start()
        self.open.append(made)

    def arrived(self, dst, slot, device):
        self.copy(dst, dst, slot, device).wait_recv()

    def close(self):
        for made in self.open:
            made.wait_send()


class PlaneGather:
    def __init__(self, at, mail, shard, whole):
        self.at, self.mail, self.shard, self.whole = at, mail, shard, whole
        self.rows = shard.shape[1]
        self.base = mail.slots(8)

    def block(self, d, half=None):
        rows = pl.ds(pl.multiple_of(self.at.rank(d) * self.rows, self.rows), self.rows)
        halves = self.shard.shape[0] // 2
        if half is None:
            return self.whole.at[:, rows, :]
        return self.whole.at[pl.ds(half * halves, halves), rows, :]

    def start(self):
        at, mail, s = self.at, self.mail, self.base
        mine = self.block(0)
        mail.post(self.shard, mine, s, at.xn)
        mail.post(self.shard, mine, s + 1, at.yn)
        mail.post(self.shard, mine, s + 2, at.pn)
        mine[...] = self.shard[...]

    def relay(self):
        at, mail, s = self.at, self.mail, self.base
        mail.arrived(self.block(2), s + 1, at.yn)
        mail.post(self.block(2, 0), self.block(2, 0), s + 3, at.xn)
        mail.arrived(self.block(4), s, at.xn)
        mail.post(self.block(4, 1), self.block(4, 1), s + 4, at.yn)
        mail.post(self.block(2), self.block(2), s + 5, at.pn)
        mail.post(self.block(4), self.block(4), s + 6, at.pn)

    def finish(self):
        at, mail, s = self.at, self.mail, self.base
        mail.arrived(self.block(6, 0), s + 3, at.xn)
        mail.arrived(self.block(6, 1), s + 4, at.yn)
        mail.post(self.block(6), self.block(6), s + 7, at.pn)
        mail.arrived(self.block(1), s + 2, at.pn)
        mail.arrived(self.block(3), s + 5, at.pn)
        mail.arrived(self.block(5), s + 6, at.pn)
        mail.arrived(self.block(7), s + 7, at.pn)


class LineGather:
    def __init__(self, at, mail, held):
        self.at, self.mail, self.held = at, mail, held
        self.up, self.down = mail.slots(at.planes), mail.slots(at.planes)

    def pass_on(self, slot, src=None):
        at = self.at
        part = self.held.at[slot]
        src = part if src is None else src

        @pl.when((slot <= at.b) & (at.b < at.planes - 1))
        def _():
            self.mail.copy(src, part, self.up + slot, at.along(1)).start()

        @pl.when((slot >= at.b) & (at.b > 0))
        def _():
            self.mail.copy(src, part, self.down + slot, at.along(-1)).start()

    def start(self, src=None):
        self.pass_on(self.at.b, src)

    def take(self, distance):
        at = self.at

        @pl.when(at.b >= distance)
        def _():
            slot = at.b - distance
            self.mail.arrived(self.held.at[slot], self.up + slot, at.along(-1))
            self.pass_on(slot)

        @pl.when(at.b + distance < at.planes)
        def _():
            slot = at.b + distance
            self.mail.arrived(self.held.at[slot], self.down + slot, at.along(1))
            self.pass_on(slot)

    def close(self):
        at = self.at
        for slot in range(at.planes):
            part = self.held.at[slot]

            @pl.when((slot <= at.b) & (at.b < at.planes - 1))
            def _():
                self.mail.copy(part, part, self.up + slot, at.along(1)).wait_send()

            @pl.when((slot >= at.b) & (at.b > 0))
            def _():
                self.mail.copy(part, part, self.down + slot, at.along(-1)).wait_send()


class PlaneExchange:
    def __init__(self, at, mail, piece, landing):
        self.at, self.mail, self.piece, self.landing = at, mail, piece, landing
        self.base = mail.slots(8)

    def start(self):
        at = self.at
        for d in range(1, 8):
            self.mail.post(
                self.piece(at.rank(d)), self.landing(at.t), self.base + d, at.peer(d)
            )
        self.landing(at.t)[...] = self.piece(at.t)[...]

    def finish(self):
        at = self.at
        for d in range(1, 8):
            self.mail.arrived(self.landing(at.rank(d)), self.base + d, at.peer(d))


class PairExchange:
    def __init__(self, at, mail, src, dst, landed):
        self.at, self.mail, self.src, self.dst, self.landed = at, mail, src, dst, landed
        self.base = mail.slots(1)

    def start(self):
        self.mail.post(self.src, self.dst, self.base, self.at.pn)

    def finish(self):
        self.mail.arrived(self.landed, self.base, self.at.pn)


class PlaneReduce:
    def __init__(self, at, mail, terms, pairs, sums, side):
        self.at, self.mail, self.terms = at, mail, terms
        self.pairs, self.sums, self.side = pairs, sums, side
        self.base = mail.slots(8)
        self.order = (6, 4, 2, 0)
        self.halves = terms.shape[0] // 2

    def start(self):
        at = self.at
        for i, d in enumerate(self.order):
            chip = at.chip(d)
            self.mail.post(
                self.terms.at[:, chip, 1 - at.c], self.pairs.at[:, chip], self.base + i, at.pn
            )

    def half(self, ref, i):
        return ref.at[pl.ds(i * self.halves, self.halves)]

    def fold(self):
        at, mail, s = self.at, self.mail, self.base
        for i, d in enumerate(self.order):
            chip = at.chip(d)
            mail.arrived(self.pairs.at[:, chip], s + i, at.pn)
            total = self.terms[:, chip, at.c].astype(jnp.float32) + self.pairs[:, chip].astype(
                jnp.float32
            )
            self.sums[:, chip] = total.astype(self.sums.dtype)
            if d == 6:
                far = self.sums.at[:, chip]
                mail.post(self.half(far, 0), self.half(self.side.at[0], 0), s + 4, at.xn)
                mail.post(self.half(far, 1), self.half(self.side.at[0], 1), s + 5, at.yn)

    def turn(self):
        at, mail, s = self.at, self.mail, self.base
        for i, d, other, slot, nbr in ((1, 4, at.yn, 5, at.xn), (0, 2, at.xn, 4, at.yn)):
            chip = at.chip(d)
            landed = self.half(self.side.at[0], i)
            mail.arrived(landed, s + slot, other)
            part = self.half(self.sums.at[:, chip], i)
            part[...] = (part[...].astype(jnp.float32) + landed[...].astype(jnp.float32)).astype(
                self.sums.dtype
            )
            whole = self.sums.at[:, chip]
            mail.post(whole, self.side.at[2 - i], s + 6 + i, nbr)

    def finish(self):
        at, mail, s = self.at, self.mail, self.base
        mail.arrived(self.side.at[1], s + 7, at.xn)
        mail.arrived(self.side.at[2], s + 6, at.yn)
        return (
            self.sums[:, at.chip(0)].astype(jnp.float32)
            + self.side[1].astype(jnp.float32)
            + self.side[2].astype(jnp.float32)
        )


class LineReduce:
    def __init__(self, at, mail, terms, above, below):
        self.at, self.mail, self.terms = at, mail, terms
        self.above, self.below = above, below
        self.up, self.down = mail.slots(at.planes), mail.slots(at.planes)

    def edges(self):
        at, last = self.at, self.at.planes - 1

        @pl.when(at.b == 0)
        def _():
            for slot in range(last, 0, -1):
                self.mail.copy(
                    self.terms.at[slot], self.below.at[slot], self.up + slot, at.along(1)
                ).start()

        @pl.when(at.b == last)
        def _():
            for slot in range(last):
                self.mail.copy(
                    self.terms.at[slot], self.above.at[slot], self.down + slot, at.along(-1)
                ).start()

    def hop(self, hop, rank):
        last = self.at.planes - 1
        if last - rank > hop:
            self._forward(last - rank, self.below, self.up, 1, self.at.b == hop)
            self._forward(rank, self.above, self.down, -1, self.at.b == last - hop)

    def _forward(self, slot, held, base, step, here):
        at, mail = self.at, self.mail
        part = held.at[slot]

        @pl.when(here)
        def _():
            mail.arrived(part, base + slot, at.along(-step))
            total = self.terms[slot].astype(jnp.float32) + part[...].astype(jnp.float32)
            part[...] = total.astype(part.dtype)
            mail.copy(part, part, base + slot, at.along(step)).start()

    def finish(self, out):
        at, mail = self.at, self.mail
        b = at.b
        kind = out.dtype

        @pl.when(b == 0)
        def _():
            mail.arrived(self.above.at[b], self.down + b, at.along(1))
            out[...] = (
                self.terms[b].astype(jnp.float32) + self.above[b].astype(jnp.float32)
            ).astype(kind)

        @pl.when(b == at.planes - 1)
        def _():
            mail.arrived(self.below.at[b], self.up + b, at.along(-1))
            out[...] = (
                self.terms[b].astype(jnp.float32) + self.below[b].astype(jnp.float32)
            ).astype(kind)

        @pl.when((b > 0) & (b < at.planes - 1))
        def _():
            mail.arrived(self.below.at[b], self.up + b, at.along(-1))
            mail.arrived(self.above.at[b], self.down + b, at.along(1))
            out[...] = (
                self.terms[b].astype(jnp.float32)
                + self.below[b].astype(jnp.float32)
                + self.above[b].astype(jnp.float32)
            ).astype(kind)

    def close(self):
        at = self.at
        for slot in range(at.planes):
            part = self.terms.at[slot]

            @pl.when(at.b < slot)
            def _():
                self.mail.copy(part, part, self.up + slot, at.along(1)).wait_send()

            @pl.when(at.b > slot)
            def _():
                self.mail.copy(part, part, self.down + slot, at.along(-1)).wait_send()


TILE = 256
LANES = 128


def dot_nn(a, b):
    return lax.dot_general(a, b, (((1,), (0,)), ((), ())), preferred_element_type=jnp.float32)


def dot_nt(a, b):
    return lax.dot_general(a, b, (((1,), (1,)), ((), ())), preferred_element_type=jnp.float32)


def dot_tn(a, b):
    return lax.dot_general(a, b, (((0,), (0,)), ((), ())), preferred_element_type=jnp.float32)


def turn(value, tables, rows, sign):
    straight, early, late = (table[rows, :] for table in tables)
    ahead = pltpu.roll(value, LANES - HD // 8, 1)
    behind = pltpu.roll(value, HD // 8, 1)
    return value * straight + sign * (ahead * early + behind * late)


def of_head(value, head):
    lane = lax.broadcasted_iota(jnp.int32, value.shape, 1)
    return jnp.where(lane // HD == head, value, jnp.zeros_like(value))


def total_rows(value):
    return jnp.sum(value, axis=0, keepdims=True)


class Layer:
    def __init__(self, refs):
        self.__dict__.update(refs)
        self.seqs, self.length, self.width = self.xa.shape
        self.per_seq = self.length // TILE
        self.tiles = self.seqs * self.per_seq
        self.heads = LANES // HD

    def rows(self, tile):
        return pl.ds(pl.multiple_of(tile * TILE, TILE), TILE)

    def in_seq(self, ref, tile):
        rows = pl.ds(pl.multiple_of(tile % self.per_seq * TILE, TILE), TILE)
        return ref[tile // self.per_seq, rows, :]

    def loop(self, count, step):
        def run(i, carry):
            step(i)
            return carry

        lax.fori_loop(0, count, run, 0)

    def wide(self, row):
        planes = self.va.shape[0]
        return jnp.concatenate(
            [self.va[b, pl.ds(2 * row + a, 1), :] for b in range(planes) for a in range(2)], axis=1
        )

    def statistics(self):
        def step(i):
            x = self.in_seq(self.xa, i).astype(jnp.float32)
            center = jnp.mean(x, axis=1, keepdims=True)
            shifted = x - center
            spread = jnp.mean(shifted * shifted, axis=1, keepdims=True)
            self.center[self.rows(i), :] = center
            self.inverse[self.rows(i), :] = lax.rsqrt(spread + EPSILON)

        self.loop(self.tiles, step)

    def normed(self, i):
        x = self.in_seq(self.xa, i).astype(jnp.float32)
        return (x - self.center[self.rows(i), :]) * self.inverse[self.rows(i), :]

    def activations(self):
        gain_one, shift_one, gain_two, shift_two = (self.wide(j) for j in (1, 2, 3, 4))

        def step(i):
            normed = self.normed(i)
            self.act_one[self.rows(i), :] = (normed * gain_one + shift_one).astype(jnp.bfloat16)
            self.act_two[self.rows(i), :] = (normed * gain_two + shift_two).astype(jnp.bfloat16)

        self.loop(self.tiles, step)

    def bias(self, first, count):
        rows = sum(self.va[b, pl.ds(first, count), :] for b in range(self.va.shape[0]))
        return jnp.concatenate([rows[i : i + 1] for i in range(count)], axis=1)

    def project(self):
        bias = self.bias(12, 3)

        def step(i):
            weight = self.wq[...].reshape(self.width, 3 * LANES)
            qkv = dot_nn(self.act_one[self.rows(i), :], weight) + bias
            rows = pl.ds(pl.multiple_of(i % self.per_seq * TILE, TILE), TILE)
            query = turn(qkv[:, :LANES], self.tables, rows, 1.0).astype(jnp.bfloat16)
            self.query[self.rows(i), :] = query * jnp.asarray(1.0 / math.sqrt(HD), jnp.bfloat16)
            self.key[self.rows(i), :] = turn(
                qkv[:, LANES : 2 * LANES], self.tables, rows, 1.0
            ).astype(jnp.bfloat16)
            self.value[self.rows(i), :] = qkv[:, 2 * LANES :].astype(jnp.bfloat16)

        self.loop(self.tiles, step)

    def keys(self, seq, block):
        start = pl.multiple_of(seq * self.length, TILE)
        return pl.ds(start, (block + 1) * TILE)

    def attend(self):
        def step(seq):
            for block in range(self.per_seq):
                rows = self.rows(seq * self.per_seq + block)
                keys = self.keys(seq, block)
                key, value, query = self.key[keys, :], self.value[keys, :], self.query[rows, :]
                out = None
                for head in range(self.heads):
                    scores = dot_nt(of_head(query, head), key)
                    at = lax.broadcasted_iota(jnp.int32, scores.shape, 0) + block * TILE
                    to = lax.broadcasted_iota(jnp.int32, scores.shape, 1)
                    scores = jnp.where(to <= at, scores, -jnp.inf)
                    top = jnp.max(scores, axis=1, keepdims=True)
                    weight = jnp.exp(scores - top)
                    weight = weight * (1.0 / jnp.sum(weight, axis=1, keepdims=True))
                    self.probs[block][seq * self.heads + head] = weight
                    part = dot_nn(weight.astype(jnp.bfloat16), value)
                    out = of_head(part, head) if out is None else out + of_head(part, head)
                self.attn[rows, :] = out.astype(jnp.bfloat16)

        self.loop(self.seqs, step)

    def attend_out_grad(self):
        def step(i):
            weight = self.wo2[...].reshape(LANES, self.width)
            self.attn_grad[self.rows(i), :] = dot_nt(self.in_seq(self.ca, i), weight).astype(
                jnp.bfloat16
            )

        self.loop(self.tiles, step)

    def attend_grad(self, seq):
        key_grad, value_grad = [None] * self.per_seq, [None] * self.per_seq
        start = seq * self.per_seq
        for block in range(self.per_seq):
            rows = self.rows(start + block)
            keys = self.keys(seq, block)
            key, value, query = self.key[keys, :], self.value[keys, :], self.query[rows, :]
            grad = self.attn_grad[rows, :]
            inner = grad.astype(jnp.float32) * self.attn[rows, :].astype(jnp.float32)
            query_grad = None
            for head in range(self.heads):
                own_grad = of_head(grad, head)
                delta = jnp.sum(of_head(inner, head), axis=1, keepdims=True)
                probs = self.probs[block][seq * self.heads + head]
                grad_prob = dot_nt(own_grad, value)
                grad_score = (probs * (grad_prob - delta)).astype(jnp.bfloat16)
                part = dot_nn(grad_score, of_head(key, head))
                query_grad = part if query_grad is None else query_grad + part
                key_part = dot_tn(grad_score, of_head(query, head))
                value_part = dot_tn(probs.astype(jnp.bfloat16), own_grad)
                for b in range(block + 1):
                    cut = slice(b * TILE, (b + 1) * TILE)
                    key_grad[b] = key_part[cut] if key_grad[b] is None else key_grad[b] + key_part[cut]
                    value_grad[b] = (
                        value_part[cut] if value_grad[b] is None else value_grad[b] + value_part[cut]
                    )
            back = pl.ds(block * TILE, TILE)
            self.qkv_grad[rows, :LANES] = turn(
                query_grad * (1.0 / math.sqrt(HD)), self.tables, back, -1.0
            ).astype(jnp.bfloat16)
        for block in range(self.per_seq):
            rows = self.rows(start + block)
            back = pl.ds(block * TILE, TILE)
            self.qkv_grad[rows, LANES : 2 * LANES] = turn(
                key_grad[block], self.tables, back, -1.0
            ).astype(jnp.bfloat16)
            self.qkv_grad[rows, 2 * LANES :] = value_grad[block].astype(jnp.bfloat16)

    def attend_grads(self):
        self.loop(self.seqs, self.attend_grad)

    def cot_flat(self):
        return self.ca[...].reshape(self.seqs * self.length, self.width)

    def qkv_weight_grad(self):
        def step(i):
            rows = self.gq.shape[1]
            act = self.act_one[:, pl.ds(pl.multiple_of(i * rows, rows), rows)]
            self.gq[i] = dot_tn(act, self.qkv_grad[...]).astype(jnp.bfloat16)

        self.loop(self.gq.shape[0], step)

    def dense_weight_grad(self):
        self.go[...] = (
            dot_tn(self.attn[...], self.cot_flat()).astype(jnp.bfloat16).reshape(self.go.shape)
        )

    def expand(self):
        bias = self.bias(16, 4)

        def step(i):
            weight = self.wu[...].reshape(self.width, self.hidden)
            pre = dot_nn(self.act_two[self.rows(i), :], weight) + bias
            cdf = 0.5 * (1.0 + lax.erf(pre * INV_ROOT_TWO))
            self.gelu[self.rows(i), :] = (pre * cdf).astype(jnp.bfloat16)
            self.slope[self.rows(i), :] = cdf + pre * jnp.exp(-0.5 * pre * pre) * INV_ROOT_TWO_PI

        self.loop(self.tiles, step)

    def down_weight_grad(self):
        def step(i):
            depth = self.gd.shape[1]
            part = self.gelu[:, pl.ds(pl.multiple_of(i * depth, depth), depth)]
            self.gd[i] = dot_tn(part, self.cot_flat()).astype(jnp.bfloat16)

        self.loop(self.gd.shape[0], step)

    def hidden_grad(self):
        def step(i):
            weight = self.wd[...].reshape(self.hidden, self.width)
            grad = dot_nt(self.in_seq(self.ca, i), weight)
            self.pre_grad[self.rows(i), :] = (grad * self.slope[self.rows(i), :]).astype(
                jnp.bfloat16
            )

        self.loop(self.tiles, step)

    def up_weight_grad(self):
        def step(i):
            rows = self.gu.shape[1]
            act = self.act_two[:, pl.ds(pl.multiple_of(i * rows, rows), rows)]
            self.gu[i] = dot_tn(act, self.pre_grad[...]).astype(jnp.bfloat16)

        self.loop(self.gu.shape[0], step)

    def put_terms(self, terms, i, value):
        seq, chips, cores, rows, width = terms.shape
        n = TILE // (cores * rows)
        terms[i // self.per_seq, pl.ds(i % self.per_seq * n, n)] = value.astype(
            jnp.bfloat16
        ).reshape(n, cores, rows, width)

    def out_terms(self):
        def step(i):
            dense = self.wo2[...].reshape(LANES, self.width)
            down = self.wd[...].reshape(self.hidden, self.width)
            self.put_terms(
                self.po,
                i,
                dot_nn(self.attn[self.rows(i), :], dense) + dot_nn(self.gelu[self.rows(i), :], down),
            )

        self.loop(self.tiles, step)

    def in_terms(self):
        gain_one, gain_two = self.wide(1), self.wide(3)
        self.sums[...] = jnp.zeros_like(self.sums)

        def step(i):
            normed = self.normed(i)
            weight = self.wq[...].reshape(self.width, 3 * LANES)
            one = dot_nt(self.qkv_grad[self.rows(i), :], weight)
            weight = self.wu[...].reshape(self.width, self.hidden)
            two = dot_nt(self.pre_grad[self.rows(i), :], weight)
            self.put_terms(self.pg, i, one * gain_one + two * gain_two)
            for j, value in enumerate((one * normed, one, two * normed, two)):
                self.sums[j : j + 1, :] += total_rows(value)

        self.loop(self.tiles, step)

    def small_terms(self):
        ranks = self.sm.shape[0]
        cot = total_rows(jnp.sum(self.cot_own[...].astype(jnp.float32), axis=0))
        for rank in range(ranks):
            cut = slice(rank * LANES, (rank + 1) * LANES)
            self.sm[rank, 0:1, :] = cot[:, cut]
            self.sm[rank, 1:5, :] = self.sums[0:4, cut]

    def small_plane(self, slot):
        total = jnp.sum(self.sm_in[...], axis=0)
        self.vz[slot, 0:8, :] = total
        qkv = total_rows(self.qkv_grad[...].astype(jnp.float32))
        pre = total_rows(self.pre_grad[...].astype(jnp.float32))
        for j in range(3):
            self.vz[slot, 8 + j : 9 + j, :] = qkv[:, j * LANES : (j + 1) * LANES]
        for j in range(self.hidden // LANES):
            self.vz[slot, 12 + j : 13 + j, :] = pre[:, j * LANES : (j + 1) * LANES]

    def result(self, out_sum, in_sum, out, in_grad):
        x = self.x_own[...].astype(jnp.float32)
        center = jnp.mean(x, axis=2, keepdims=True)
        shifted = x - center
        inverse = lax.rsqrt(jnp.mean(shifted * shifted, axis=2, keepdims=True) + EPSILON)
        normed = shifted * inverse
        bias = (self.wide(0) + self.wide(5))[None]
        out[...] = (x + out_sum + bias).astype(jnp.bfloat16)
        in_grad[...] = self.cot_own[...].astype(jnp.float32) + inverse * (
            in_sum
            - jnp.mean(in_sum, axis=2, keepdims=True)
            - normed * jnp.mean(in_sum * normed, axis=2, keepdims=True)
        )


LAYER_SLOTS = 4 * 8 + 10 * 8 + 7 * 8 + 2


def layer_kernel(names, planes, *refs):
    refs = dict(zip(names, refs))
    send, recv = refs.pop(names[-2]), refs.pop(names[-1])
    refs.update(
        tables=tuple(refs["table"].at[i] for i in range(3)),
        probs=tuple(refs[name] for name in names if name.startswith("probs")),
        hidden=refs["gelu"].shape[1],
    )
    do = Layer(refs)
    at = Place(planes)
    mail = Mail(send, recv)
    b, c = at.b, at.c
    rows = do.wq_s.shape[1]
    pair = planes // 2

    def strip(whole):
        return lambda rank: whole.at[b, pl.ds(pl.multiple_of(rank * rows, rows), rows), :]

    def band(whole):
        return lambda rank: whole.at[pl.ds(pl.multiple_of(rank * rows, rows), rows), :]

    gather_x = PlaneGather(at, mail, do.x_own, do.xa)
    gather_c = PlaneGather(at, mail, do.cot_own, do.ca)
    line_v, line_o = LineGather(at, mail, do.va), LineGather(at, mail, do.wo)
    line_q, line_u = LineGather(at, mail, do.wq), LineGather(at, mail, do.wu)
    line_d = LineGather(at, mail, do.wd)
    ex_v = PlaneExchange(at, mail, lambda rank: do.vec_s.at[rank], lambda rank: do.vec_in.at[rank])
    ex_q = PlaneExchange(at, mail, lambda rank: do.wq_s.at[rank], strip(do.wq))
    ex_u = PlaneExchange(at, mail, lambda rank: do.wu_s.at[rank], strip(do.wu))
    mine = do.wo2.at[:, c]
    swap_w = PairExchange(
        at, mail, do.wo.at[pl.ds(pair * (1 - c), pair)], mine, do.wo2.at[:, 1 - c]
    )
    sum_o = LineReduce(at, mail, do.go4, do.above_o, do.below_o)
    sum_q = LineReduce(at, mail, do.gq, do.above_q, do.below_q)
    sum_u = LineReduce(at, mail, do.gu, do.above_u, do.below_u)
    sum_d = LineReduce(at, mail, do.gd, do.above_d, do.below_d)
    swap_g = PairExchange(
        at,
        mail,
        do.go.at[:, 1 - c],
        do.go4.at[pl.ds(pair * c, pair)],
        do.go4.at[pl.ds(pair * (1 - c), pair)],
    )
    back_q = PlaneExchange(at, mail, band(do.fq), lambda rank: do.dq.at[rank])
    back_u = PlaneExchange(at, mail, band(do.fu), lambda rank: do.du.at[rank])
    fold_v = PlaneExchange(at, mail, lambda rank: do.sm.at[rank], lambda rank: do.sm_in.at[rank])
    line_s = LineGather(at, mail, do.vz)
    share_v = PlaneExchange(at, mail, lambda rank: do.vt, lambda rank: do.dv.at[rank])
    plane_o = PlaneReduce(at, mail, do.po, do.pairs_o, do.sums_o, do.side_o)
    plane_g = PlaneReduce(at, mail, do.pg, do.pairs_g, do.sums_g, do.side_g)

    at.barrier()
    ex_v.start()
    ex_q.start()
    gather_x.start()
    line_o.start(do.wo_s)
    do.wo[b] = do.wo_s[...]
    ex_u.start()
    gather_c.start()
    do.wd[b] = do.wd_s[...]
    ex_v.finish()
    do.va[b] = jnp.sum(do.vec_in[...], axis=0)
    line_v.start()
    ex_q.finish()
    line_q.start()
    gather_x.relay()
    line_v.take(1)
    line_o.take(1)
    gather_x.finish()
    line_q.take(1)
    do.statistics()
    line_v.take(2)
    line_o.take(2)
    line_q.take(2)
    gather_c.relay()
    ex_u.finish()
    line_v.take(3)
    do.activations()
    line_o.take(3)
    line_q.take(3)
    line_u.start()
    line_d.start(do.wd_s)
    swap_w.start()
    mine[...] = do.wo[pl.ds(pair * c, pair)]
    do.project()
    gather_c.finish()
    do.attend()
    line_u.take(1)
    swap_w.finish()
    do.attend_out_grad()
    line_d.take(1)
    do.attend_grads()
    line_u.take(2)
    do.dense_weight_grad()
    swap_g.start()
    do.go4[pl.ds(pair * c, pair)] = do.go[:, c]
    do.qkv_weight_grad()
    sum_q.edges()
    swap_g.finish()
    sum_o.edges()
    line_d.take(2)
    line_u.take(3)
    do.expand()
    sum_q.hop(1, 0)
    sum_o.hop(1, 0)
    do.down_weight_grad()
    sum_d.edges()
    sum_q.hop(1, 1)
    sum_o.hop(1, 1)
    sum_q.hop(2, 0)
    sum_o.hop(2, 0)
    line_d.take(3)
    do.hidden_grad()
    sum_d.hop(1, 0)
    do.up_weight_grad()
    sum_u.edges()
    sum_d.hop(1, 1)
    do.out_terms()
    plane_o.start()
    sum_d.hop(2, 0)
    sum_q.finish(do.fq)
    back_q.start()
    do.in_terms()
    plane_g.start()
    do.small_terms()
    fold_v.start()
    plane_o.fold()
    sum_u.hop(1, 0)
    plane_g.fold()
    fold_v.finish()
    do.small_plane(b)
    line_s.start()
    plane_o.turn()
    plane_g.turn()
    sum_u.hop(1, 1)
    line_s.take(1)
    line_s.take(2)
    sum_u.hop(2, 0)
    line_s.take(3)
    do.vt[...] = jnp.sum(do.vz[...], axis=0)
    share_v.start()
    do.result(plane_o.finish(), plane_g.finish(), do.out, do.in_grad)
    sum_o.finish(do.dd_o)
    sum_d.finish(do.dd)
    sum_u.finish(do.fu)
    back_u.start()
    back_q.finish()
    share_v.finish()
    back_u.finish()
    mail.close()
    for line in (line_v, line_o, line_q, line_u, line_d, line_s, sum_o, sum_q, sum_u, sum_d):
        line.close()


VMEM = pl.BlockSpec(memory_space=pltpu.VMEM)


def rotary_rows(length):
    half = HD // 8
    frequency = 1.0 / 10000.0 ** (np.arange(half) * (1.0 / half))
    angles = np.arange(length)[:, None] * frequency[None, :]
    table = np.zeros((3, length, HD))
    table[0] = 1.0
    table[0, :, :half] = table[0, :, half : 2 * half] = np.cos(angles)
    table[1, :, :half] = -np.sin(angles)
    table[2, :, half : 2 * half] = np.sin(angles)
    return np.tile(table, (1, 1, LANES // HD)).astype(np.float32)


def body(shape, *operands):
    residual_in, qkv_weight, down_weight = operands[0], operands[1], operands[11]
    planes = shape[BATCH]
    ranks = shape[ULY] * shape[BLK]
    tok_rows, seqs, width = residual_in.shape
    fits = (
        (shape[ULY], shape[BLK]) == (2, 4)
        and planes == 4
        and seqs % 2 == 0
        and 2 * qkv_weight.shape[0] == HD
        and width == ranks * LANES
        and ranks * tok_rows % TILE == 0
        and TILE % (2 * tok_rows) == 0
        and down_weight.shape[0] == LANES
    )
    return fast_body(planes, *operands) if fits else general_body(*operands)


def fast_body(
    planes,
    residual_in,
    qkv_weight,
    qkv_bias,
    dense_weight,
    dense_bias,
    norm1_gain,
    norm1_bias,
    norm2_gain,
    norm2_bias,
    up_weight,
    up_bias,
    down_weight,
    down_bias,
    cotangent,
):
    single = jnp.float32
    half_type = jnp.bfloat16
    tok_rows, seqs, width = residual_in.shape
    ranks = width // LANES
    rows = qkv_weight.shape[0]
    depth = down_weight.shape[0]
    hidden = planes * depth
    pair = planes // 2
    length = ranks * tok_rows
    tokens = seqs * length
    rank = lax.axis_index(ULY) * lax.axis_size(BLK) + lax.axis_index(BLK)
    owner = lax.axis_index(BATCH) * ranks + rank

    x_own = jnp.transpose(residual_in, (1, 0, 2))
    cot_own = jnp.transpose(cotangent, (1, 0, 2))
    wq_send = jnp.transpose(
        qkv_weight.reshape(rows, 3, 2, pair, ranks // 2, HD), (4, 2, 0, 1, 3, 5)
    ).reshape(ranks, rows, 3 * LANES)
    wu_send = jnp.transpose(
        up_weight.reshape(rows, planes, ranks, depth), (2, 0, 1, 3)
    ).reshape(ranks, rows, hidden)
    at_rank = (jnp.arange(ranks) == rank).astype(single)[:, None]
    at_owner = (jnp.arange(ranks * planes) == owner).astype(single)[:, None]
    placed = [
        (at_rank * v.astype(single)[None]).reshape(1, 2, LANES)
        for v in (dense_bias, norm1_gain, norm1_bias, norm2_gain, norm2_bias, down_bias)
    ]
    placed_qkv = jnp.transpose(
        (at_owner * qkv_bias.astype(single)[None]).reshape(3, 2, pair, ranks // 2, HD),
        (3, 1, 0, 2, 4),
    ).reshape(ranks, 3, LANES)
    placed_up = jnp.transpose(
        (at_owner * up_bias.astype(single)[None]).reshape(planes, ranks, LANES), (1, 0, 2)
    )
    vec_send = jnp.concatenate(
        [jnp.broadcast_to(p, (ranks, 2, LANES)) for p in placed]
        + [
            placed_qkv,
            jnp.zeros((ranks, 1, LANES), single),
            placed_up,
            jnp.zeros((ranks, 4, LANES), single),
        ],
        axis=1,
    )
    table = jnp.asarray(rotary_rows(length))
    inputs = dict(
        x_own=x_own,
        cot_own=cot_own,
        wq_s=wq_send,
        wu_s=wu_send,
        wd_s=down_weight,
        wo_s=dense_weight,
        vec_s=vec_send,
        table=table,
    )
    shard = (seqs, tok_rows, width)
    lanes_in = vec_send.shape[1]
    outputs = dict(
        out=(shard, half_type),
        in_grad=(shard, single),
        dq=((ranks, rows, 3 * LANES), half_type),
        du=((ranks, rows, hidden), half_type),
        dd=((depth, width), single),
        dd_o=((rows, width), single),
        dv=((ranks, 16, LANES), single),
    )
    q_shape = (planes, ranks * rows, 3 * LANES)
    u_shape = (planes, ranks * rows, hidden)
    d_shape = (planes, depth, width)
    o_shape = (planes, rows, width)
    chips = ranks // 2
    scratch = dict(
        xa=((seqs, length, width), half_type),
        ca=((seqs, length, width), half_type),
        wq=(q_shape, half_type),
        wu=(u_shape, half_type),
        wd=(d_shape, half_type),
        wo=(o_shape, half_type),
        wo2=((pair, 2, rows, width), half_type),
        vec_in=((ranks, lanes_in, LANES), single),
        va=((planes, lanes_in, LANES), single),
        center=((tokens, 1), single),
        inverse=((tokens, 1), single),
        act_one=((tokens, width), half_type),
        act_two=((tokens, width), half_type),
        query=((tokens, LANES), half_type),
        key=((tokens, LANES), half_type),
        value=((tokens, LANES), half_type),
        attn=((tokens, LANES), half_type),
        attn_grad=((tokens, LANES), half_type),
        qkv_grad=((tokens, 3 * LANES), half_type),
        gelu=((tokens, hidden), half_type),
        slope=((tokens, hidden), single),
        pre_grad=((tokens, hidden), half_type),
        gq=(q_shape, half_type),
        gu=(u_shape, half_type),
        gd=(d_shape, half_type),
        go=((pair, 2, rows, width), half_type),
        go4=(o_shape, half_type),
        above_q=(q_shape, half_type),
        below_q=(q_shape, half_type),
        above_u=(u_shape, half_type),
        below_u=(u_shape, half_type),
        above_d=(d_shape, half_type),
        below_d=(d_shape, half_type),
        above_o=(o_shape, half_type),
        below_o=(o_shape, half_type),
        fq=(q_shape[1:], half_type),
        fu=(u_shape[1:], half_type),
        po=((seqs, chips, 2, tok_rows, width), half_type),
        pg=((seqs, chips, 2, tok_rows, width), half_type),
        pairs_o=((seqs, chips, tok_rows, width), half_type),
        pairs_g=((seqs, chips, tok_rows, width), half_type),
        sums_o=((seqs, chips, tok_rows, width), half_type),
        sums_g=((seqs, chips, tok_rows, width), half_type),
        side_o=((3,) + shard, half_type),
        side_g=((3,) + shard, half_type),
        sums=((8, width), single),
        sm=((ranks, 8, LANES), single),
        sm_in=((ranks, 8, LANES), single),
        vz=((planes, 16, LANES), single),
        vt=((16, LANES), single),
    )
    for block in range(length // TILE):
        scratch["probs%d" % block] = ((seqs * LANES // HD, TILE, (block + 1) * TILE), single)
    names = tuple(inputs) + tuple(outputs) + tuple(scratch) + ("send", "recv")
    out, in_grad, dq, du, dd, dd_o, dv = pl.pallas_call(
        functools.partial(layer_kernel, names, planes),
        out_shape=[jax.ShapeDtypeStruct(*what) for what in outputs.values()],
        in_specs=[VMEM] * len(inputs),
        out_specs=[VMEM] * len(outputs),
        scratch_shapes=[pltpu.VMEM(*what) for what in scratch.values()]
        + [pltpu.SemaphoreType.DMA((LAYER_SLOTS,))] * 2,
        compiler_params=pltpu.CompilerParams(
            collective_id=0, has_side_effects=True, vmem_limit_bytes=60 * 2**20
        ),
    )(*inputs.values())

    output = jnp.transpose(out, (1, 0, 2))
    input_grad = jnp.transpose(in_grad, (1, 0, 2))
    qkv_grad_out = jnp.transpose(
        dq.reshape(ranks // 2, 2, rows, 3, pair, HD), (2, 3, 1, 4, 0, 5)
    ).reshape(qkv_weight.shape).astype(single)
    up_grad_out = jnp.transpose(
        du.reshape(ranks, rows, planes, depth), (1, 2, 0, 3)
    ).reshape(up_weight.shape).astype(single)
    wide = [
        lax.dynamic_slice(dv[:, j].reshape(width), (owner * rows,), (rows,)) for j in range(5)
    ]
    qkv_bias_grad = lax.dynamic_slice(
        jnp.transpose(
            dv[:, 8:11].reshape(ranks // 2, 2, 3, pair, HD), (2, 1, 3, 0, 4)
        ).reshape(3 * width),
        (owner * qkv_bias.shape[0],),
        qkv_bias.shape,
    )
    up_bias_grad = lax.dynamic_slice(
        dv, (rank, 12 + lax.axis_index(BATCH), 0), (1, 1, LANES)
    ).reshape(up_bias.shape)
    return (
        output,
        input_grad,
        qkv_grad_out,
        qkv_bias_grad,
        dd_o,
        wide[0],
        wide[1],
        wide[2],
        wide[3],
        wide[4],
        up_grad_out,
        up_bias_grad,
        dd,
        wide[0],
    )


def solution(mesh):
    placed = (
        P(TOKENS, BATCH, None),
        P(AXES, None),
        P(AXES),
        P(AXES, None),
        P(AXES),
        P(AXES),
        P(AXES),
        P(AXES),
        P(AXES),
        P(AXES, None),
        P(AXES),
        P(AXES, None),
        P(AXES),
        P(TOKENS, BATCH, None),
    )
    return jax.shard_map(
        functools.partial(body, dict(mesh.shape)),
        mesh=mesh,
        in_specs=placed,
        out_specs=(
            P(TOKENS, BATCH, None),
            P(TOKENS, BATCH, None),
            P(AXES, None),
            P(AXES),
            P(AXES, None),
            P(AXES),
            P(AXES),
            P(AXES),
            P(AXES),
            P(AXES),
            P(AXES, None),
            P(AXES),
            P(AXES, None),
            P(AXES),
        ),
        check_vma=False,
    )
```

```python
import functools
import math

import jax
import jax.numpy as jnp
import numpy as np
from jax import lax
from jax.experimental import pallas as pl
from jax.experimental.pallas import tpu as pltpu
from jax.sharding import PartitionSpec as P

HD = 64
BATCH, ULY, BLK = "batch", "ulysses", "blk"
AXES = (BATCH, ULY, BLK)
TOKENS = (ULY, BLK)


EPSILON = 1e-05
INV_ROOT_TWO = 0.7071067811865476
INV_ROOT_TWO_PI = 0.3989422804014327


def layer_norm(values):
    center = jnp.mean(values, axis=-1, keepdims=True)
    shifted = values - center
    inverse = lax.rsqrt(jnp.mean(shifted * shifted, axis=-1, keepdims=True) + EPSILON)
    return (shifted * inverse, inverse)


def norm_back(gradient, normed, inverse, gain_vec):
    scaled = gradient * gain_vec
    return inverse * (
        scaled
        - jnp.mean(scaled, axis=-1, keepdims=True)
        - normed * jnp.mean(scaled * normed, axis=-1, keepdims=True)
    )


def gelu_value(pre_values):
    return 0.5 * pre_values * (1.0 + jax.scipy.special.erf(pre_values * INV_ROOT_TWO))


def gelu_slope(pre_values):
    normal_cdf = 0.5 * (1.0 + jax.scipy.special.erf(pre_values * INV_ROOT_TWO))
    return normal_cdf + pre_values * jnp.exp(-0.5 * pre_values * pre_values) * INV_ROOT_TWO_PI


def rotary_tables(positions, rotary):
    half_rot = rotary // 2
    frequency = 1.0 / 10000.0 ** (jnp.arange(half_rot, dtype=jnp.float32) * (2.0 / rotary))
    angles = positions.astype(jnp.float32)[:, None] * frequency[None, :]
    cosine = jnp.concatenate([jnp.cos(angles), jnp.cos(angles)], axis=-1)
    sine_table = jnp.concatenate([jnp.sin(angles), jnp.sin(angles)], axis=-1)
    return (cosine, sine_table)


def expand_table(table, tensor):
    extra_dims = (1,) * (tensor.ndim - 2)
    return table.reshape((table.shape[0],) + extra_dims + (table.shape[1],))


def rotate_fwd(tensor, cosine, sine_table, rotary):
    half_rot = rotary // 2
    cos_full = expand_table(cosine, tensor)
    sin_full = expand_table(sine_table, tensor)
    rot_part = tensor[..., :rotary]
    turned = jnp.concatenate([-rot_part[..., half_rot:], rot_part[..., :half_rot]], axis=-1)
    return jnp.concatenate([rot_part * cos_full + turned * sin_full, tensor[..., rotary:]], axis=-1)


def rotate_back(tensor, cosine, sine_table, rotary):
    half_rot = rotary // 2
    cos_full = expand_table(cosine, tensor)
    sin_full = expand_table(sine_table, tensor)
    rot_part = tensor[..., :rotary]
    weighted = rot_part * sin_full
    turned = jnp.concatenate([weighted[..., half_rot:], -weighted[..., :half_rot]], axis=-1)
    return jnp.concatenate([rot_part * cos_full + turned, tensor[..., rotary:]], axis=-1)


def general_body(
    residual_in,
    qkv_weight,
    qkv_bias,
    dense_weight,
    dense_bias,
    norm1_gain,
    norm1_bias,
    norm2_gain,
    norm2_bias,
    up_weight,
    up_bias,
    down_weight,
    down_bias,
    cotangent,
):
    single = jnp.float32
    half_type = jnp.bfloat16
    gathered = (
        lax.all_gather(qkv_weight, AXES, axis=0, tiled=True),
        lax.all_gather(qkv_bias, AXES, axis=0, tiled=True),
        lax.all_gather(dense_weight, AXES, axis=0, tiled=True),
        lax.all_gather(dense_bias, AXES, axis=0, tiled=True),
        lax.all_gather(norm1_gain, AXES, axis=0, tiled=True),
        lax.all_gather(norm1_bias, AXES, axis=0, tiled=True),
        lax.all_gather(norm2_gain, AXES, axis=0, tiled=True),
        lax.all_gather(norm2_bias, AXES, axis=0, tiled=True),
        lax.all_gather(up_weight, AXES, axis=0, tiled=True),
        lax.all_gather(up_bias, AXES, axis=0, tiled=True),
        lax.all_gather(down_weight, AXES, axis=0, tiled=True),
        lax.all_gather(down_bias, AXES, axis=0, tiled=True),
    )
    (
        w_qkv,
        b_qkv,
        w_dense,
        b_dense,
        gain_one,
        shift_one,
        gain_two,
        shift_two,
        w_up,
        b_up,
        w_down,
        b_down,
    ) = gathered
    tok_rows = residual_in.shape[0]
    seq_count = residual_in.shape[1]
    model_width = residual_in.shape[2]
    head_count = model_width // HD
    rotary = HD // 4
    scale_factor = 1.0 / math.sqrt(HD)
    blk_size = lax.axis_size(BLK)
    uly_size = lax.axis_size(ULY)
    blk_index = lax.axis_index(BLK)
    block_id = lax.axis_index(ULY) * blk_size + blk_index
    seq_pos = block_id * tok_rows + jnp.arange(tok_rows, dtype=jnp.int32)
    inputs_f = residual_in.astype(single)
    normed, inverse = layer_norm(inputs_f)
    act_one = (normed * gain_one.astype(single) + shift_one.astype(single)).astype(half_type)
    act_two = (normed * gain_two.astype(single) + shift_two.astype(single)).astype(half_type)
    qkv_full = jnp.einsum(
        "tsd,df->tsf", act_one, w_qkv, preferred_element_type=single
    ) + b_qkv.astype(single)
    cos_seq, sin_seq = rotary_tables(seq_pos, rotary)
    head_shape = (tok_rows, seq_count, head_count, HD)
    query_seq = (
        rotate_fwd(qkv_full[..., :model_width].reshape(head_shape), cos_seq, sin_seq, rotary)
        .reshape(tok_rows, seq_count, model_width)
        .astype(half_type)
    )
    key_seq = (
        rotate_fwd(
            qkv_full[..., model_width : 2 * model_width].reshape(head_shape),
            cos_seq,
            sin_seq,
            rotary,
        )
        .reshape(tok_rows, seq_count, model_width)
        .astype(half_type)
    )
    value_seq = qkv_full[..., 2 * model_width :].astype(half_type)
    query_loc, key_loc, value_loc = (
        lax.all_to_all(query_seq, ULY, split_axis=2, concat_axis=0, tiled=True),
        lax.all_to_all(key_seq, ULY, split_axis=2, concat_axis=0, tiled=True),
        lax.all_to_all(value_seq, ULY, split_axis=2, concat_axis=0, tiled=True),
    )
    local_rows = query_loc.shape[0]
    features = query_loc.shape[2]
    local_heads = features // HD
    key_all, value_all = (
        lax.all_gather(key_loc, BLK, axis=0, tiled=True),
        lax.all_gather(value_loc, BLK, axis=0, tiled=True),
    )
    total_rows = key_all.shape[0]
    row_ids = jnp.arange(local_rows, dtype=jnp.int32)
    query_pos = (row_ids // tok_rows * blk_size + blk_index) * tok_rows + row_ids % tok_rows
    block_rows = math.gcd(512, local_rows)
    n_blocks = local_rows // block_rows
    query_h = query_loc.reshape(local_rows, seq_count, local_heads, HD)
    key_h = jnp.transpose(
        key_all.reshape(blk_size, uly_size, tok_rows, seq_count, features), (1, 0, 2, 3, 4)
    ).reshape(total_rows, seq_count, local_heads, HD)
    value_h = jnp.transpose(
        value_all.reshape(blk_size, uly_size, tok_rows, seq_count, features), (1, 0, 2, 3, 4)
    ).reshape(total_rows, seq_count, local_heads, HD)
    zero_idx = jnp.zeros((), jnp.int32)
    step_ids = jnp.arange(n_blocks * seq_count, dtype=jnp.int32)
    row_shape = (block_rows, 1, local_heads, HD)

    def select(step_index):
        row_start = step_index // seq_count * block_rows
        seq_index = step_index % seq_count
        query_rows = lax.dynamic_slice(
            query_h, (row_start, seq_index, zero_idx, zero_idx), row_shape
        )
        limit = jnp.max(query_pos) // block_rows + 1
        return (row_start, seq_index, query_rows, query_pos, limit)

    def block_scores(query_rows, row_pos, key_index, seq_index):
        key_start = key_index * block_rows
        slot = (key_start, seq_index, zero_idx, zero_idx)
        key_rows = lax.dynamic_slice(key_h, slot, (block_rows, 1, local_heads, HD))
        value_rows = lax.dynamic_slice(value_h, slot, (block_rows, 1, local_heads, HD))
        scores = (
            jnp.einsum("qshd,kshd->shqk", query_rows, key_rows, preferred_element_type=single)
            * scale_factor
        )
        key_ids = key_start + jnp.arange(block_rows, dtype=jnp.int32)
        allowed = (key_ids[None, :] <= row_pos[:, None])[None, None]
        return (jnp.where(allowed, scores, -jnp.inf), key_rows, value_rows, slot)

    def forward_block(step_index):
        row_start, seq_index, query_rows, row_pos, limit = select(step_index)

        def total_step(key_index, carry):
            running_max, running_sum = carry
            masked, key_rows, value_rows, slot = block_scores(
                query_rows, row_pos, key_index, seq_index
            )
            new_max = jnp.maximum(running_max, jnp.max(masked, axis=-1))
            new_sum = running_sum * jnp.exp(running_max - new_max) + jnp.sum(
                jnp.exp(masked - new_max[..., None]), axis=-1
            )
            return (new_max, new_sum)

        start_max = jnp.full((1, local_heads, block_rows), -jnp.inf, single)
        start_sum = jnp.zeros((1, local_heads, block_rows), single)
        final_max, final_sum = lax.fori_loop(zero_idx, limit, total_step, (start_max, start_sum))
        log_total = final_max + jnp.log(final_sum)

        def value_step(key_index, acc):
            masked, key_rows, value_rows, slot = block_scores(
                query_rows, row_pos, key_index, seq_index
            )
            weights_b = jnp.exp(masked - log_total[..., None]).astype(half_type)
            return acc + jnp.einsum(
                "shqk,kshd->qshd", weights_b, value_rows, preferred_element_type=single
            )

        result = lax.fori_loop(zero_idx, limit, value_step, jnp.zeros(row_shape, single)).astype(
            half_type
        )
        return (result[:, 0], log_total)

    results, log_totals = lax.map(forward_block, step_ids)
    attn_h = jnp.transpose(
        results.reshape(n_blocks, seq_count, block_rows, local_heads, HD), (0, 2, 1, 3, 4)
    ).reshape(local_rows, seq_count, local_heads, HD)
    attn_seq = lax.all_to_all(
        attn_h.reshape(local_rows, seq_count, features),
        ULY,
        split_axis=0,
        concat_axis=2,
        tiled=True,
    )
    proj_out = jnp.einsum(
        "tsd,de->tse", attn_seq, w_dense, preferred_element_type=single
    ) + b_dense.astype(single)
    pre_act = jnp.einsum("tsd,df->tsf", act_two, w_up, preferred_element_type=single) + b_up.astype(
        single
    )
    gelu_out = gelu_value(pre_act).astype(half_type)
    mlp_out = jnp.einsum(
        "tsf,fd->tsd", gelu_out, w_down, preferred_element_type=single
    ) + b_down.astype(single)
    output = (inputs_f + proj_out + mlp_out).astype(half_type)
    back_params = (
        lax.all_gather(qkv_weight, AXES, axis=0, tiled=True),
        lax.all_gather(qkv_bias, AXES, axis=0, tiled=True),
        lax.all_gather(dense_weight, AXES, axis=0, tiled=True),
        lax.all_gather(dense_bias, AXES, axis=0, tiled=True),
        lax.all_gather(norm1_gain, AXES, axis=0, tiled=True),
        lax.all_gather(norm1_bias, AXES, axis=0, tiled=True),
        lax.all_gather(norm2_gain, AXES, axis=0, tiled=True),
        lax.all_gather(norm2_bias, AXES, axis=0, tiled=True),
        lax.all_gather(up_weight, AXES, axis=0, tiled=True),
        lax.all_gather(up_bias, AXES, axis=0, tiled=True),
        lax.all_gather(down_weight, AXES, axis=0, tiled=True),
        lax.all_gather(down_bias, AXES, axis=0, tiled=True),
    )
    back_qkv = back_params[0]
    back_dense = back_params[2]
    back_gain_one = back_params[4].astype(single)
    back_gain_two = back_params[6].astype(single)
    back_up = back_params[8]
    back_down = back_params[10]
    grad_f = cotangent.astype(single)
    bias_sum = jnp.sum(grad_f, axis=(0, 1))
    down_w_grad = jnp.einsum("tsf,tsd->fd", gelu_out, cotangent, preferred_element_type=single)
    gelu_grad = jnp.einsum("tsd,fd->tsf", cotangent, back_down, preferred_element_type=single)
    pre_grad = (gelu_grad * gelu_slope(pre_act)).astype(half_type)
    up_w_grad = jnp.einsum("tsd,tsf->df", act_two, pre_grad, preferred_element_type=single)
    up_b_grad = jnp.sum(pre_grad.astype(single), axis=(0, 1))
    act_two_grad = jnp.einsum("tsf,df->tsd", pre_grad, back_up, preferred_element_type=single)
    gain_two_grad = jnp.sum(act_two_grad * normed, axis=(0, 1))
    shift_two_grad = jnp.sum(act_two_grad, axis=(0, 1))
    dense_w_grad = jnp.einsum("tsd,tse->de", attn_seq, cotangent, preferred_element_type=single)
    attn_grad = jnp.einsum(
        "tse,de->tsd", cotangent, back_dense, preferred_element_type=single
    ).astype(half_type)
    grad_loc = lax.all_to_all(attn_grad, ULY, split_axis=2, concat_axis=0, tiled=True)
    grad_h = grad_loc.reshape(local_rows, seq_count, local_heads, HD)

    def backward_block(acc_pair, step_index):
        row_start, seq_index, query_rows, row_pos, limit = select(step_index)
        own_slot = (row_start, seq_index, zero_idx, zero_idx)
        out_rows = lax.dynamic_slice(attn_h, own_slot, row_shape)
        grad_rows = lax.dynamic_slice(grad_h, own_slot, row_shape)
        log_total = log_totals[step_index]
        delta_row = jnp.transpose(
            jnp.sum(grad_rows.astype(single) * out_rows.astype(single), axis=-1), (1, 2, 0)
        )

        def grad_step(key_index, carry):
            key_acc, value_acc, query_acc = carry
            masked, key_rows, value_rows, slot = block_scores(
                query_rows, row_pos, key_index, seq_index
            )
            probs_f = jnp.exp(masked - log_total[..., None])
            value_part = jnp.einsum(
                "shqk,qshd->kshd",
                probs_f.astype(half_type),
                grad_rows,
                preferred_element_type=single,
            )
            grad_prob = jnp.einsum(
                "qshd,kshd->shqk", grad_rows, value_rows, preferred_element_type=single
            )
            grad_score = (probs_f * (grad_prob - delta_row[..., None]) * scale_factor).astype(
                half_type
            )
            query_acc = query_acc + jnp.einsum(
                "shqk,kshd->qshd", grad_score, key_rows, preferred_element_type=single
            )
            key_part = jnp.einsum(
                "shqk,qshd->kshd", grad_score, query_rows, preferred_element_type=single
            )
            key_acc = lax.dynamic_update_slice(
                key_acc, lax.dynamic_slice(key_acc, slot, key_part.shape) + key_part, slot
            )
            value_acc = lax.dynamic_update_slice(
                value_acc, lax.dynamic_slice(value_acc, slot, value_part.shape) + value_part, slot
            )
            return (key_acc, value_acc, query_acc)

        key_acc, value_acc, query_acc = lax.fori_loop(
            zero_idx, limit, grad_step, (acc_pair[0], acc_pair[1], jnp.zeros(row_shape, single))
        )
        return ((key_acc, value_acc), query_acc[:, 0])

    acc_zero = jnp.zeros((total_rows, seq_count, local_heads, HD), single)
    acc_final, query_parts = lax.scan(backward_block, (acc_zero, acc_zero), step_ids)
    query_grad = jnp.transpose(
        query_parts.reshape(n_blocks, seq_count, block_rows, local_heads, HD), (0, 2, 1, 3, 4)
    ).reshape(local_rows, seq_count, local_heads, HD)
    key_terms = jnp.transpose(
        acc_final[0].reshape(uly_size, blk_size, tok_rows, seq_count, features), (1, 0, 2, 3, 4)
    ).reshape(total_rows, seq_count, features)
    value_terms = jnp.transpose(
        acc_final[1].reshape(uly_size, blk_size, tok_rows, seq_count, features), (1, 0, 2, 3, 4)
    ).reshape(total_rows, seq_count, features)
    key_back, value_back = (
        lax.psum_scatter(key_terms, BLK, scatter_dimension=0, tiled=True),
        lax.psum_scatter(value_terms, BLK, scatter_dimension=0, tiled=True),
    )
    cos_h, sin_h = rotary_tables(query_pos, rotary)
    query_send = (
        rotate_back(query_grad, cos_h, sin_h, rotary)
        .reshape(local_rows, seq_count, features)
        .astype(half_type)
    )
    key_send = (
        rotate_back(key_back.reshape(local_rows, seq_count, local_heads, HD), cos_h, sin_h, rotary)
        .reshape(local_rows, seq_count, features)
        .astype(half_type)
    )
    value_send = value_back.astype(half_type)
    query_ret, key_ret, value_ret = (
        lax.all_to_all(query_send, ULY, split_axis=0, concat_axis=2, tiled=True),
        lax.all_to_all(key_send, ULY, split_axis=0, concat_axis=2, tiled=True),
        lax.all_to_all(value_send, ULY, split_axis=0, concat_axis=2, tiled=True),
    )
    qkv_grad = jnp.concatenate([query_ret, key_ret, value_ret], axis=-1)
    qkv_w_grad = jnp.einsum("tsd,tsf->df", act_one, qkv_grad, preferred_element_type=single)
    qkv_b_grad = jnp.sum(qkv_grad.astype(single), axis=(0, 1))
    act_one_grad = jnp.einsum("tsf,df->tsd", qkv_grad, back_qkv, preferred_element_type=single)
    gain_one_grad = jnp.sum(act_one_grad * normed, axis=(0, 1))
    shift_one_grad = jnp.sum(act_one_grad, axis=(0, 1))
    input_grad = (
        grad_f
        + norm_back(act_one_grad, normed, inverse, back_gain_one)
        + norm_back(act_two_grad, normed, inverse, back_gain_two)
    )
    summed = (
        lax.psum_scatter(qkv_w_grad, AXES, scatter_dimension=0, tiled=True),
        lax.psum_scatter(qkv_b_grad, AXES, scatter_dimension=0, tiled=True),
        lax.psum_scatter(
            dense_w_grad, AXES, scatter_dimension=0, tiled=True
        ),
        lax.psum_scatter(bias_sum, AXES, scatter_dimension=0, tiled=True),
        lax.psum_scatter(
            gain_one_grad, AXES, scatter_dimension=0, tiled=True
        ),
        lax.psum_scatter(
            shift_one_grad, AXES, scatter_dimension=0, tiled=True
        ),
        lax.psum_scatter(
            gain_two_grad, AXES, scatter_dimension=0, tiled=True
        ),
        lax.psum_scatter(
            shift_two_grad, AXES, scatter_dimension=0, tiled=True
        ),
        lax.psum_scatter(up_w_grad, AXES, scatter_dimension=0, tiled=True),
        lax.psum_scatter(up_b_grad, AXES, scatter_dimension=0, tiled=True),
        lax.psum_scatter(down_w_grad, AXES, scatter_dimension=0, tiled=True),
        lax.psum_scatter(bias_sum, AXES, scatter_dimension=0, tiled=True),
    )
    return (
        output,
        input_grad,
        summed[0],
        summed[1],
        summed[2],
        summed[3],
        summed[4],
        summed[5],
        summed[6],
        summed[7],
        summed[8],
        summed[9],
        summed[10],
        summed[11],
    )


MESH = pl.DeviceIdType.MESH


class Place:
    def __init__(self, planes):
        self.planes = planes
        self.b = lax.axis_index(BATCH)
        self.u = lax.axis_index(ULY)
        k = lax.axis_index(BLK)
        self.y, self.c = k // 2, k % 2
        self.t = self.u * 4 + k
        self.xn, self.yn, self.pn = self.peer(4), self.peer(2), self.peer(1)

    def rank(self, d):
        u = 1 - self.u if d & 4 else self.u
        y = 1 - self.y if d & 2 else self.y
        c = 1 - self.c if d & 1 else self.c
        return u * 4 + y * 2 + c

    def chip(self, d):
        return self.rank(d) // 2

    def peer(self, d):
        u = 1 - self.u if d & 4 else self.u
        y = 1 - self.y if d & 2 else self.y
        c = 1 - self.c if d & 1 else self.c
        return {BATCH: self.b, ULY: u, BLK: y * 2 + c}

    def along(self, step):
        return {BATCH: self.b + step, ULY: self.u, BLK: self.y * 2 + self.c}

    def barrier(self):
        sem = pltpu.get_barrier_semaphore()
        for d in range(1, 8):
            pl.semaphore_signal(sem, inc=1, device_id=self.peer(d), device_id_type=MESH)

        @pl.when(self.b > 0)
        def _():
            pl.semaphore_signal(sem, inc=1, device_id=self.along(-1), device_id_type=MESH)

        @pl.when(self.b < self.planes - 1)
        def _():
            pl.semaphore_signal(sem, inc=1, device_id=self.along(1), device_id_type=MESH)

        below = (self.b > 0).astype(jnp.int32)
        above = (self.b < self.planes - 1).astype(jnp.int32)
        pl.semaphore_wait(sem, 7 + below + above)


class Mail:
    def __init__(self, send, recv):
        self.send, self.recv, self.used, self.open = send, recv, 0, []

    def slots(self, n):
        first = self.used
        self.used += n
        return first

    def copy(self, src, dst, slot, device, recv_slot=None):
        return pltpu.make_async_remote_copy(
            src_ref=src,
            dst_ref=dst,
            send_sem=self.send.at[slot],
            recv_sem=self.recv.at[slot if recv_slot is None else recv_slot],
            device_id=device,
            device_id_type=MESH,
        )

    def post(self, src, dst, slot, device):
        made = self.copy(src, dst, slot, device)
        made.start()
        self.open.append(made)

    def arrived(self, dst, slot, device):
        self.copy(dst, dst, slot, device).wait_recv()

    def close(self):
        for made in self.open:
            made.wait_send()


class PlaneGather:
    def __init__(self, at, mail, shard, whole):
        self.at, self.mail, self.shard, self.whole = at, mail, shard, whole
        self.rows = shard.shape[1]
        self.base = mail.slots(8)

    def block(self, d, half=None):
        rows = pl.ds(pl.multiple_of(self.at.rank(d) * self.rows, self.rows), self.rows)
        halves = self.shard.shape[0] // 2
        if half is None:
            return self.whole.at[:, rows, :]
        return self.whole.at[pl.ds(half * halves, halves), rows, :]

    def start(self):
        at, mail, s = self.at, self.mail, self.base
        mine = self.block(0)
        mail.post(self.shard, mine, s, at.xn)
        mail.post(self.shard, mine, s + 1, at.yn)
        mail.post(self.shard, mine, s + 2, at.pn)
        mine[...] = self.shard[...]

    def relay_y(self):
        at, mail, s = self.at, self.mail, self.base
        mail.arrived(self.block(2), s + 1, at.yn)
        mail.post(self.block(2, 0), self.block(2, 0), s + 3, at.xn)
        mail.post(self.block(2), self.block(2), s + 5, at.pn)

    def relay_x(self):
        at, mail, s = self.at, self.mail, self.base
        mail.arrived(self.block(4), s, at.xn)
        mail.post(self.block(4, 1), self.block(4, 1), s + 4, at.yn)
        mail.post(self.block(4), self.block(4), s + 6, at.pn)

    def far(self):
        at, mail, s = self.at, self.mail, self.base
        mail.arrived(self.block(6, 0), s + 3, at.xn)
        mail.arrived(self.block(6, 1), s + 4, at.yn)
        mail.post(self.block(6), self.block(6), s + 7, at.pn)

    def finish(self):
        at, mail, s = self.at, self.mail, self.base
        mail.arrived(self.block(1), s + 2, at.pn)
        mail.arrived(self.block(3), s + 5, at.pn)
        mail.arrived(self.block(5), s + 6, at.pn)
        mail.arrived(self.block(7), s + 7, at.pn)


class LineGather:
    def __init__(self, at, mail, held, first=0, count=None):
        self.at, self.mail, self.held = at, mail, held
        self.rows = pl.ds(first, held.shape[1] - first if count is None else count)
        self.up, self.down = mail.slots(at.planes), mail.slots(at.planes)

    def part(self, slot):
        return self.held.at[slot, self.rows]

    def pass_on(self, slot, src=None):
        at = self.at
        part = self.part(slot)
        src = part if src is None else src.at[self.rows]

        @pl.when((slot <= at.b) & (at.b < at.planes - 1))
        def _():
            self.mail.copy(src, part, self.up + slot, at.along(1)).start()

        @pl.when((slot >= at.b) & (at.b > 0))
        def _():
            self.mail.copy(src, part, self.down + slot, at.along(-1)).start()

    def start(self, src=None):
        self.pass_on(self.at.b, src)

    def take(self, distance):
        at = self.at

        @pl.when(at.b >= distance)
        def _():
            slot = at.b - distance
            self.mail.arrived(self.part(slot), self.up + slot, at.along(-1))
            self.pass_on(slot)

        @pl.when(at.b + distance < at.planes)
        def _():
            slot = at.b + distance
            self.mail.arrived(self.part(slot), self.down + slot, at.along(1))
            self.pass_on(slot)

    def close(self):
        at = self.at
        for slot in range(at.planes):
            part = self.part(slot)

            @pl.when((slot <= at.b) & (at.b < at.planes - 1))
            def _():
                self.mail.copy(part, part, self.up + slot, at.along(1)).wait_send()

            @pl.when((slot >= at.b) & (at.b > 0))
            def _():
                self.mail.copy(part, part, self.down + slot, at.along(-1)).wait_send()


class PlaneExchange:
    def __init__(self, at, mail, piece, landing):
        self.at, self.mail, self.piece, self.landing = at, mail, piece, landing
        self.base = mail.slots(8)

    def start(self):
        at = self.at
        for d in range(1, 8):
            self.mail.post(
                self.piece(at.rank(d)), self.landing(at.t), self.base + d, at.peer(d)
            )
        self.landing(at.t)[...] = self.piece(at.t)[...]

    def finish(self):
        at = self.at
        for d in range(1, 8):
            self.mail.arrived(self.landing(at.rank(d)), self.base + d, at.peer(d))


class PairExchange:
    def __init__(self, at, mail, src, dst, landed):
        self.at, self.mail, self.src, self.dst, self.landed = at, mail, src, dst, landed
        self.base = mail.slots(1)

    def start(self):
        self.mail.post(self.src, self.dst, self.base, self.at.pn)

    def finish(self):
        self.mail.arrived(self.landed, self.base, self.at.pn)


class PlaneReduce:
    def __init__(self, at, mail, terms, pairs, sums, side):
        self.at, self.mail, self.terms = at, mail, terms
        self.pairs, self.sums, self.side = pairs, sums, side
        self.base = mail.slots(8)
        self.order = (6, 4, 2, 0)
        self.halves = terms.shape[0] // 2

    def start(self):
        at = self.at
        for i, d in enumerate(self.order):
            chip = at.chip(d)
            self.mail.post(
                self.terms.at[:, chip, 1 - at.c], self.pairs.at[:, chip], self.base + i, at.pn
            )

    def half(self, ref, i):
        return ref.at[pl.ds(i * self.halves, self.halves)]

    def fold(self):
        at, mail, s = self.at, self.mail, self.base
        for i, d in enumerate(self.order):
            chip = at.chip(d)
            mail.arrived(self.pairs.at[:, chip], s + i, at.pn)
            total = self.terms[:, chip, at.c].astype(jnp.float32) + self.pairs[:, chip].astype(
                jnp.float32
            )
            self.sums[:, chip] = total.astype(self.sums.dtype)
            if d == 6:
                far = self.sums.at[:, chip]
                mail.post(self.half(far, 0), self.half(self.side.at[0], 0), s + 4, at.xn)
                mail.post(self.half(far, 1), self.half(self.side.at[0], 1), s + 5, at.yn)

    def turn(self):
        at, mail, s = self.at, self.mail, self.base
        for i, d, other, slot, nbr in ((1, 4, at.yn, 5, at.xn), (0, 2, at.xn, 4, at.yn)):
            chip = at.chip(d)
            landed = self.half(self.side.at[0], i)
            mail.arrived(landed, s + slot, other)
            part = self.half(self.sums.at[:, chip], i)
            part[...] = (part[...].astype(jnp.float32) + landed[...].astype(jnp.float32)).astype(
                self.sums.dtype
            )
            whole = self.sums.at[:, chip]
            mail.post(whole, self.side.at[2 - i], s + 6 + i, nbr)

    def finish(self):
        at, mail, s = self.at, self.mail, self.base
        mail.arrived(self.side.at[1], s + 7, at.xn)
        mail.arrived(self.side.at[2], s + 6, at.yn)
        return (
            self.sums[:, at.chip(0)].astype(jnp.float32)
            + self.side[1].astype(jnp.float32)
            + self.side[2].astype(jnp.float32)
        )


class LineReduce:
    def __init__(self, at, mail, terms, above, below):
        self.at, self.mail, self.terms = at, mail, terms
        self.above, self.below = above, below
        self.up, self.down = mail.slots(at.planes), mail.slots(at.planes)

    def edge(self, slot):
        at, last = self.at, self.at.planes - 1

        @pl.when((at.b == 0) & (slot > 0))
        def _():
            self.mail.copy(
                self.terms.at[slot], self.below.at[slot], self.up + slot, at.along(1)
            ).start()

        @pl.when((at.b == last) & (slot < last))
        def _():
            self.mail.copy(
                self.terms.at[slot], self.above.at[slot], self.down + slot, at.along(-1)
            ).start()

    def hop(self, hop, rank):
        last = self.at.planes - 1
        if last - rank > hop:
            self._forward(last - rank, self.below, self.up, 1, self.at.b == hop)
            self._forward(rank, self.above, self.down, -1, self.at.b == last - hop)

    def _forward(self, slot, held, base, step, here):
        at, mail = self.at, self.mail
        part = held.at[slot]

        @pl.when(here)
        def _():
            mail.arrived(part, base + slot, at.along(-step))
            total = self.terms[slot].astype(jnp.float32) + part[...].astype(jnp.float32)
            part[...] = total.astype(part.dtype)
            mail.copy(part, part, base + slot, at.along(step)).start()

    def finish(self, out):
        at, mail = self.at, self.mail
        b = at.b
        kind = out.dtype

        @pl.when(b == 0)
        def _():
            mail.arrived(self.above.at[b], self.down + b, at.along(1))
            out[...] = (
                self.terms[b].astype(jnp.float32) + self.above[b].astype(jnp.float32)
            ).astype(kind)

        @pl.when(b == at.planes - 1)
        def _():
            mail.arrived(self.below.at[b], self.up + b, at.along(-1))
            out[...] = (
                self.terms[b].astype(jnp.float32) + self.below[b].astype(jnp.float32)
            ).astype(kind)

        @pl.when((b > 0) & (b < at.planes - 1))
        def _():
            mail.arrived(self.below.at[b], self.up + b, at.along(-1))
            mail.arrived(self.above.at[b], self.down + b, at.along(1))
            out[...] = (
                self.terms[b].astype(jnp.float32)
                + self.below[b].astype(jnp.float32)
                + self.above[b].astype(jnp.float32)
            ).astype(kind)

    def close(self):
        at = self.at
        for slot in range(at.planes):
            part = self.terms.at[slot]

            @pl.when(at.b < slot)
            def _():
                self.mail.copy(part, part, self.up + slot, at.along(1)).wait_send()

            @pl.when(at.b > slot)
            def _():
                self.mail.copy(part, part, self.down + slot, at.along(-1)).wait_send()


TILE = 256
LANES = 128


def dot_nn(a, b):
    return lax.dot_general(a, b, (((1,), (0,)), ((), ())), preferred_element_type=jnp.float32)


def dot_nt(a, b):
    return lax.dot_general(a, b, (((1,), (1,)), ((), ())), preferred_element_type=jnp.float32)


def dot_tn(a, b):
    return lax.dot_general(a, b, (((0,), (0,)), ((), ())), preferred_element_type=jnp.float32)


def turn(value, tables, rows, sign):
    straight, early, late = (table[rows, :] for table in tables)
    ahead = pltpu.roll(value, LANES - HD // 8, 1)
    behind = pltpu.roll(value, HD // 8, 1)
    return value * straight + sign * (ahead * early + behind * late)


def of_head(value, head):
    lane = lax.broadcasted_iota(jnp.int32, value.shape, 1)
    return jnp.where(lane // HD == head, value, jnp.zeros_like(value))


def total_rows(value):
    return jnp.sum(value, axis=0, keepdims=True)


class Layer:
    def __init__(self, refs):
        self.__dict__.update(refs)
        self.heads = LANES // HD
        if "xa" in refs:
            self.seqs, self.length, self.width = self.xa.shape
            self.per_seq = self.length // TILE
            self.tiles = self.seqs * self.per_seq

    def rows(self, tile):
        return pl.ds(pl.multiple_of(tile * TILE, TILE), TILE)

    def in_seq(self, ref, tile):
        rows = pl.ds(pl.multiple_of(tile % self.per_seq * TILE, TILE), TILE)
        return ref[tile // self.per_seq, rows, :]

    def loop(self, count, step):
        def run(i, carry):
            step(i)
            return carry

        lax.fori_loop(0, count, run, 0)

    def wide(self, row):
        planes = self.va.shape[0]
        return jnp.concatenate(
            [self.va[b, pl.ds(2 * row + a, 1), :] for b in range(planes) for a in range(2)], axis=1
        )

    def statistics(self):
        def step(i):
            x = self.in_seq(self.xa, i).astype(jnp.float32)
            center = jnp.mean(x, axis=1, keepdims=True)
            shifted = x - center
            spread = jnp.mean(shifted * shifted, axis=1, keepdims=True)
            self.center[self.rows(i), :] = center
            self.inverse[self.rows(i), :] = lax.rsqrt(spread + EPSILON)

        self.loop(self.tiles, step)

    def normed(self, i):
        x = self.in_seq(self.xa, i).astype(jnp.float32)
        return (x - self.center[self.rows(i), :]) * self.inverse[self.rows(i), :]

    def activations(self):
        gain_one, shift_one, gain_two, shift_two = (self.wide(j) for j in (1, 2, 3, 4))

        def step(i):
            normed = self.normed(i)
            self.act_one[self.rows(i), :] = (normed * gain_one + shift_one).astype(jnp.bfloat16)
            self.act_two[self.rows(i), :] = (normed * gain_two + shift_two).astype(jnp.bfloat16)

        self.loop(self.tiles, step)

    def bias(self, first, count):
        rows = sum(self.va[b, pl.ds(first, count), :] for b in range(self.va.shape[0]))
        return jnp.concatenate([rows[i : i + 1] for i in range(count)], axis=1)

    def project(self):
        bias = self.bias(12, 3)

        def step(i):
            weight = self.wq[...].reshape(self.width, 3 * LANES)
            qkv = dot_nn(self.act_one[self.rows(i), :], weight) + bias
            rows = pl.ds(pl.multiple_of(i % self.per_seq * TILE, TILE), TILE)
            query = turn(qkv[:, :LANES], self.tables, rows, 1.0).astype(jnp.bfloat16)
            self.query[self.rows(i), :] = query * jnp.asarray(1.0 / math.sqrt(HD), jnp.bfloat16)
            self.key[self.rows(i), :] = turn(
                qkv[:, LANES : 2 * LANES], self.tables, rows, 1.0
            ).astype(jnp.bfloat16)
            self.value[self.rows(i), :] = qkv[:, 2 * LANES :].astype(jnp.bfloat16)

        self.loop(self.tiles, step)

    def keys(self, seq, block):
        start = pl.multiple_of(seq * self.length, TILE)
        return pl.ds(start, (block + 1) * TILE)

    def attend(self):
        def step(seq):
            for block in range(self.per_seq):
                rows = self.rows(seq * self.per_seq + block)
                keys = self.keys(seq, block)
                key, value, query = self.key[keys, :], self.value[keys, :], self.query[rows, :]
                out = None
                for head in range(self.heads):
                    scores = dot_nt(of_head(query, head), key)
                    at = lax.broadcasted_iota(jnp.int32, scores.shape, 0) + block * TILE
                    to = lax.broadcasted_iota(jnp.int32, scores.shape, 1)
                    scores = jnp.where(to <= at, scores, -jnp.inf)
                    top = jnp.max(scores, axis=1, keepdims=True)
                    weight = jnp.exp(scores - top)
                    weight = weight * (1.0 / jnp.sum(weight, axis=1, keepdims=True))
                    self.probs[block][seq * self.heads + head] = weight
                    part = dot_nn(weight.astype(jnp.bfloat16), value)
                    out = of_head(part, head) if out is None else out + of_head(part, head)
                self.attn[rows, :] = out.astype(jnp.bfloat16)

        self.loop(self.seqs, step)

    def attend_out_grad(self):
        def step(i):
            weight = self.wo2[...].reshape(LANES, self.width)
            self.attn_grad[self.rows(i), :] = dot_nt(self.in_seq(self.ca, i), weight).astype(
                jnp.bfloat16
            )

        self.loop(self.tiles, step)

    def attend_grad(self, seq):
        key_grad, value_grad = [None] * self.per_seq, [None] * self.per_seq
        start = seq * self.per_seq
        for block in range(self.per_seq):
            rows = self.rows(start + block)
            keys = self.keys(seq, block)
            key, value, query = self.key[keys, :], self.value[keys, :], self.query[rows, :]
            grad = self.attn_grad[rows, :]
            inner = grad.astype(jnp.float32) * self.attn[rows, :].astype(jnp.float32)
            query_grad = None
            for head in range(self.heads):
                own_grad = of_head(grad, head)
                delta = jnp.sum(of_head(inner, head), axis=1, keepdims=True)
                probs = self.probs[block][seq * self.heads + head]
                grad_prob = dot_nt(own_grad, value)
                grad_score = (probs * (grad_prob - delta)).astype(jnp.bfloat16)
                part = dot_nn(grad_score, of_head(key, head))
                query_grad = part if query_grad is None else query_grad + part
                key_part = dot_tn(grad_score, of_head(query, head))
                value_part = dot_tn(probs.astype(jnp.bfloat16), own_grad)
                for b in range(block + 1):
                    cut = slice(b * TILE, (b + 1) * TILE)
                    key_grad[b] = key_part[cut] if key_grad[b] is None else key_grad[b] + key_part[cut]
                    value_grad[b] = (
                        value_part[cut] if value_grad[b] is None else value_grad[b] + value_part[cut]
                    )
            back = pl.ds(block * TILE, TILE)
            self.qkv_grad[rows, :LANES] = turn(
                query_grad * (1.0 / math.sqrt(HD)), self.tables, back, -1.0
            ).astype(jnp.bfloat16)
        for block in range(self.per_seq):
            rows = self.rows(start + block)
            back = pl.ds(block * TILE, TILE)
            self.qkv_grad[rows, LANES : 2 * LANES] = turn(
                key_grad[block], self.tables, back, -1.0
            ).astype(jnp.bfloat16)
            self.qkv_grad[rows, 2 * LANES :] = value_grad[block].astype(jnp.bfloat16)

    def attend_grads(self):
        self.loop(self.seqs, self.attend_grad)

    def cot_flat(self):
        return self.ca[...].reshape(self.seqs * self.length, self.width)

    def qkv_weight_grad(self, i):
        rows = self.gq.shape[1]
        act = self.act_one[:, pl.ds(pl.multiple_of(i * rows, rows), rows)]
        self.gq[i] = dot_tn(act, self.qkv_grad[...]).astype(jnp.bfloat16)

    def dense_weight_grad(self):
        self.go[...] = (
            dot_tn(self.attn[...], self.cot_flat()).astype(jnp.bfloat16).reshape(self.go.shape)
        )

    def expand(self):
        bias = self.bias(16, 4)

        def step(i):
            weight = self.wu[...].reshape(self.width, self.hidden)
            pre = dot_nn(self.act_two[self.rows(i), :], weight) + bias
            cdf = 0.5 * (1.0 + lax.erf(pre * INV_ROOT_TWO))
            self.gelu[self.rows(i), :] = (pre * cdf).astype(jnp.bfloat16)
            self.slope[self.rows(i), :] = cdf + pre * jnp.exp(-0.5 * pre * pre) * INV_ROOT_TWO_PI

        self.loop(self.tiles, step)

    def down_weight_grad(self, i):
        depth = self.gd.shape[1]
        part = self.gelu[:, pl.ds(pl.multiple_of(i * depth, depth), depth)]
        self.gd[i] = dot_tn(part, self.cot_flat()).astype(jnp.bfloat16)

    def hidden_grad(self):
        def step(i):
            weight = self.wd[...].reshape(self.hidden, self.width)
            grad = dot_nt(self.in_seq(self.ca, i), weight)
            self.pre_grad[self.rows(i), :] = (grad * self.slope[self.rows(i), :]).astype(
                jnp.bfloat16
            )

        self.loop(self.tiles, step)

    def up_weight_grad(self, i):
        rows = self.gu.shape[1]
        act = self.act_two[:, pl.ds(pl.multiple_of(i * rows, rows), rows)]
        self.gu[i] = dot_tn(act, self.pre_grad[...]).astype(jnp.bfloat16)

    def put_terms(self, terms, i, value):
        seq, chips, cores, rows, width = terms.shape
        n = TILE // (cores * rows)
        terms[i // self.per_seq, pl.ds(i % self.per_seq * n, n)] = value.astype(
            jnp.bfloat16
        ).reshape(n, cores, rows, width)

    def out_terms(self):
        def step(i):
            dense = self.wo2[...].reshape(LANES, self.width)
            down = self.wd[...].reshape(self.hidden, self.width)
            self.put_terms(
                self.po,
                i,
                dot_nn(self.attn[self.rows(i), :], dense) + dot_nn(self.gelu[self.rows(i), :], down),
            )

        self.loop(self.tiles, step)

    def in_terms(self):
        gain_one, gain_two = self.wide(1), self.wide(3)
        self.sums[...] = jnp.zeros_like(self.sums)

        def step(i):
            normed = self.normed(i)
            weight = self.wq[...].reshape(self.width, 3 * LANES)
            one = dot_nt(self.qkv_grad[self.rows(i), :], weight)
            weight = self.wu[...].reshape(self.width, self.hidden)
            two = dot_nt(self.pre_grad[self.rows(i), :], weight)
            self.put_terms(self.pg, i, one * gain_one + two * gain_two)
            for j, value in enumerate((one * normed, one, two * normed, two)):
                self.sums[j : j + 1, :] += total_rows(value)

        self.loop(self.tiles, step)

    def small_terms(self):
        ranks = self.sm.shape[0]
        cot = total_rows(jnp.sum(self.cot_own[...].astype(jnp.float32), axis=0))
        for rank in range(ranks):
            cut = slice(rank * LANES, (rank + 1) * LANES)
            self.sm[rank, 0:1, :] = cot[:, cut]
            self.sm[rank, 1:5, :] = self.sums[0:4, cut]

    def small_plane(self, slot):
        total = jnp.sum(self.sm_in[...], axis=0)
        self.vz[slot, 0:8, :] = total
        qkv = total_rows(self.qkv_grad[...].astype(jnp.float32))
        pre = total_rows(self.pre_grad[...].astype(jnp.float32))
        for j in range(3):
            self.vz[slot, 8 + j : 9 + j, :] = qkv[:, j * LANES : (j + 1) * LANES]
        for j in range(self.hidden // LANES):
            self.vz[slot, 12 + j : 13 + j, :] = pre[:, j * LANES : (j + 1) * LANES]

    def result(self, out_sum, in_sum, out, in_grad):
        x = self.x_own[...].astype(jnp.float32)
        center = jnp.mean(x, axis=2, keepdims=True)
        shifted = x - center
        inverse = lax.rsqrt(jnp.mean(shifted * shifted, axis=2, keepdims=True) + EPSILON)
        normed = shifted * inverse
        bias = (self.wide(0) + self.wide(5))[None]
        out[...] = (x + out_sum + bias).astype(jnp.bfloat16)
        in_grad[...] = self.cot_own[...].astype(jnp.float32) + inverse * (
            in_sum
            - jnp.mean(in_sum, axis=2, keepdims=True)
            - normed * jnp.mean(in_sum * normed, axis=2, keepdims=True)
        )


LAYER_SLOTS = 4 * 8 + 11 * 8 + 7 * 8 + 2


def layer_kernel(names, planes, *refs):
    refs = dict(zip(names, refs))
    send, recv = refs.pop(names[-2]), refs.pop(names[-1])
    refs.update(
        tables=tuple(refs["table"].at[i] for i in range(3)),
        probs=tuple(refs[name] for name in names if name.startswith("probs")),
        hidden=refs["gelu"].shape[1],
    )
    do = Layer(refs)
    at = Place(planes)
    mail = Mail(send, recv)
    b, c = at.b, at.c
    rows = do.wq_s.shape[1]
    pair = planes // 2

    def strip(whole):
        return lambda rank: whole.at[b, pl.ds(pl.multiple_of(rank * rows, rows), rows), :]

    def band(whole):
        return lambda rank: whole.at[pl.ds(pl.multiple_of(rank * rows, rows), rows), :]

    gather_x = PlaneGather(at, mail, do.x_own, do.xa)
    gather_c = PlaneGather(at, mail, do.cot_own, do.ca)
    line_v, line_o = LineGather(at, mail, do.va), LineGather(at, mail, do.wo)
    line_q, line_u = LineGather(at, mail, do.wq), LineGather(at, mail, do.wu)
    half = do.wd.shape[1] // 2
    line_da = LineGather(at, mail, do.wd, 0, half)
    line_db = LineGather(at, mail, do.wd, half, half)
    ex_v = PlaneExchange(at, mail, lambda rank: do.vec_s.at[rank], lambda rank: do.vec_in.at[rank])
    ex_q = PlaneExchange(at, mail, lambda rank: do.wq_s.at[rank], strip(do.wq))
    ex_u = PlaneExchange(at, mail, lambda rank: do.wu_s.at[rank], strip(do.wu))
    mine = do.wo2.at[:, c]
    swap_w = PairExchange(
        at, mail, do.wo.at[pl.ds(pair * (1 - c), pair)], mine, do.wo2.at[:, 1 - c]
    )
    sum_o = LineReduce(at, mail, do.go4, do.above_o, do.below_o)
    sum_q = LineReduce(at, mail, do.gq, do.above_q, do.below_q)
    sum_u = LineReduce(at, mail, do.gu, do.above_u, do.below_u)
    sum_d = LineReduce(at, mail, do.gd, do.above_d, do.below_d)
    swap_g = PairExchange(
        at,
        mail,
        do.go.at[:, 1 - c],
        do.go4.at[pl.ds(pair * c, pair)],
        do.go4.at[pl.ds(pair * (1 - c), pair)],
    )
    back_q = PlaneExchange(at, mail, band(do.fq), lambda rank: do.dq.at[rank])
    back_u = PlaneExchange(at, mail, band(do.fu), lambda rank: do.du.at[rank])
    fold_v = PlaneExchange(at, mail, lambda rank: do.sm.at[rank], lambda rank: do.sm_in.at[rank])
    line_s = LineGather(at, mail, do.vz)
    share_v = PlaneExchange(at, mail, lambda rank: do.vt, lambda rank: do.dv.at[rank])
    plane_o = PlaneReduce(at, mail, do.po, do.pairs_o, do.sums_o, do.side_o)
    plane_g = PlaneReduce(at, mail, do.pg, do.pairs_g, do.sums_g, do.side_g)

    slots = [s + b // pair * (planes - 1 - 2 * s) for s in (3, 0, 2, 1)]

    at.barrier()
    line_da.start(do.wd_s)
    do.wd[b] = do.wd_s[...]
    ex_v.start()
    ex_q.start()
    gather_x.start()
    line_o.start(do.wo_s)
    do.wo[b] = do.wo_s[...]
    ex_v.finish()
    do.va[b] = jnp.sum(do.vec_in[...], axis=0)
    line_v.start()
    line_db.start(do.wd_s)
    line_v.take(1)
    ex_u.start()
    ex_q.finish()
    line_q.start()
    line_o.take(1)
    gather_x.relay_y()
    line_q.take(1)
    gather_x.relay_x()
    gather_c.start()
    line_o.take(2)
    line_v.take(2)
    gather_x.far()
    line_v.take(3)
    line_q.take(2)
    gather_x.finish()
    line_o.take(3)
    do.statistics()
    line_da.take(1)
    do.activations()
    gather_c.relay_y()
    gather_c.relay_x()
    ex_u.finish()
    line_u.start()
    swap_w.start()
    mine[...] = do.wo[pl.ds(pair * c, pair)]
    line_q.take(3)
    do.project()
    swap_w.finish()
    gather_c.far()
    line_da.take(2)
    do.attend()
    gather_c.finish()
    do.dense_weight_grad()
    swap_g.start()
    do.go4[pl.ds(pair * c, pair)] = do.go[:, c]
    do.attend_out_grad()
    swap_g.finish()
    for slot in slots:
        sum_o.edge(slot)
    line_u.take(1)
    do.attend_grads()
    do.qkv_weight_grad(slots[0])
    sum_q.edge(slots[0])
    do.qkv_weight_grad(slots[1])
    sum_q.edge(slots[1])
    do.qkv_weight_grad(slots[2])
    sum_q.edge(slots[2])
    do.qkv_weight_grad(slots[3])
    sum_q.edge(slots[3])
    line_u.take(2)
    line_da.take(3)
    line_u.take(3)
    do.expand()
    do.down_weight_grad(slots[0])
    sum_d.edge(slots[0])
    line_db.take(1)
    sum_o.hop(1, 0)
    sum_q.hop(1, 0)
    line_db.take(2)
    line_db.take(3)
    do.hidden_grad()
    do.up_weight_grad(slots[0])
    sum_u.edge(slots[0])
    sum_q.hop(1, 1)
    do.in_terms()
    plane_g.start()
    sum_q.hop(2, 0)
    do.up_weight_grad(slots[1])
    sum_u.edge(slots[1])
    do.up_weight_grad(slots[2])
    sum_u.edge(slots[2])
    sum_q.finish(do.fq)
    back_q.start()
    do.out_terms()
    plane_o.start()
    plane_g.fold()
    sum_o.hop(2, 0)
    sum_o.hop(1, 1)
    do.up_weight_grad(slots[3])
    sum_u.edge(slots[3])
    sum_u.hop(1, 0)
    do.down_weight_grad(slots[1])
    sum_d.edge(slots[1])
    do.small_terms()
    fold_v.start()
    plane_o.fold()
    plane_g.turn()
    sum_o.finish(do.dd_o)
    fold_v.finish()
    do.small_plane(b)
    line_s.start()
    do.down_weight_grad(slots[2])
    sum_d.edge(slots[2])
    do.down_weight_grad(slots[3])
    sum_d.edge(slots[3])
    sum_d.hop(1, 0)
    plane_o.turn()
    sum_u.hop(2, 0)
    line_s.take(1)
    sum_u.hop(1, 1)
    line_s.take(2)
    back_q.finish()
    line_s.take(3)
    sum_d.hop(1, 1)
    do.vt[...] = jnp.sum(do.vz[...], axis=0)
    share_v.start()
    sum_d.hop(2, 0)
    sum_u.finish(do.fu)
    back_u.start()
    do.result(plane_o.finish(), plane_g.finish(), do.out, do.in_grad)
    share_v.finish()
    sum_d.finish(do.dd)
    back_u.finish()
    mail.close()
    for line in (line_v, line_o, line_q, line_u, line_da, line_db, line_s, sum_o, sum_q, sum_u, sum_d):
        line.close()


def finish_kernel(names, planes, *refs):
    do = Layer(dict(zip(names, refs)))
    at = Place(planes)
    ranks, rows = do.dq.shape[:2]
    lane = lax.broadcasted_iota(jnp.int32, (rows, LANES), 1)
    low = lane < HD
    for part in range(3):
        for core in range(2):
            for pair in range(ranks // 4):
                near, far = (
                    do.dq[2 * (2 * pair + i) + core, :, part * LANES : (part + 1) * LANES].astype(
                        jnp.float32
                    )
                    for i in range(2)
                )
                for j in range(2):
                    both = (
                        jnp.where(low, near, pltpu.roll(far, HD, 1))
                        if j == 0
                        else jnp.where(low, pltpu.roll(near, HD, 1), far)
                    )
                    first = (part * 4 + core * 2 + j) * ranks // 2 * HD + pair * LANES
                    do.qkv_out[:, first : first + LANES] = both
    for rank in range(ranks):
        for b in range(planes):
            first = (b * ranks + rank) * LANES
            do.up_out[:, first : first + LANES] = do.du[
                rank, :, b * LANES : (b + 1) * LANES
            ].astype(jnp.float32)
    do.down_out[...] = do.dd[...]
    do.dense_out[...] = do.dd_o[...]
    for seq in range(do.out.shape[0]):
        do.in_grad_out[:, seq, :] = do.in_grad[seq]
        do.out_out[:, seq, :] = do.out[seq]
    piece = lax.rem(at.t, 4)
    row = (at.b * ranks + at.t) // 4
    values = do.dv[pl.ds(row, 1), 0:8, :].reshape(8, LANES)
    front = jnp.zeros((8, rows), jnp.float32)
    for i in range(4):
        cut = values[:, i * rows : (i + 1) * rows]
        front = front + jnp.where(piece == i, cut, jnp.zeros_like(cut))
    for j, ref in enumerate(
        (do.dense_bias, do.gain_one, do.shift_one, do.gain_two, do.shift_two)
    ):
        ref[...] = front[j].reshape(rows)
    do.down_bias[...] = front[0].reshape(rows)
    do.up_bias[...] = do.dv[pl.ds(at.t, 1), pl.ds(12 + at.b, 1), :].reshape(LANES)
    pieces = []
    for i in range(3):
        index = (at.b * ranks + at.t) * 3 + i
        part, inner = index // 32, lax.rem(index, 32)
        head, half = inner // 2, lax.rem(inner, 2)
        core, j, chip = head // 8, lax.rem(head // 4, 2), lax.rem(head, 4)
        value = do.dv[pl.ds(chip * 2 + core, 1), pl.ds(8 + part, 1), :].reshape(1, LANES)
        spot = 2 * j + half
        total = jnp.zeros((1, rows), jnp.float32)
        for k in range(4):
            cut = value[:, k * rows : (k + 1) * rows]
            total = total + jnp.where(spot == k, cut, jnp.zeros_like(cut))
        pieces.append(total)
    do.qkv_bias[...] = jnp.concatenate(pieces, axis=1).reshape(3 * rows)


VMEM = pl.BlockSpec(memory_space=pltpu.VMEM)


def rotary_rows(length):
    half = HD // 8
    frequency = 1.0 / 10000.0 ** (np.arange(half) * (1.0 / half))
    angles = np.arange(length)[:, None] * frequency[None, :]
    table = np.zeros((3, length, HD))
    table[0] = 1.0
    table[0, :, :half] = table[0, :, half : 2 * half] = np.cos(angles)
    table[1, :, :half] = -np.sin(angles)
    table[2, :, half : 2 * half] = np.sin(angles)
    return np.tile(table, (1, 1, LANES // HD)).astype(np.float32)


def body(shape, *operands):
    residual_in, qkv_weight, down_weight = operands[0], operands[1], operands[11]
    planes = shape[BATCH]
    ranks = shape[ULY] * shape[BLK]
    tok_rows, seqs, width = residual_in.shape
    fits = (
        (shape[ULY], shape[BLK]) == (2, 4)
        and planes == 4
        and seqs % 2 == 0
        and 2 * qkv_weight.shape[0] == HD
        and width == ranks * LANES
        and ranks * tok_rows % TILE == 0
        and TILE % (2 * tok_rows) == 0
        and down_weight.shape[0] == LANES
    )
    return fast_body(planes, *operands) if fits else general_body(*operands)


def fast_body(
    planes,
    residual_in,
    qkv_weight,
    qkv_bias,
    dense_weight,
    dense_bias,
    norm1_gain,
    norm1_bias,
    norm2_gain,
    norm2_bias,
    up_weight,
    up_bias,
    down_weight,
    down_bias,
    cotangent,
):
    single = jnp.float32
    half_type = jnp.bfloat16
    tok_rows, seqs, width = residual_in.shape
    ranks = width // LANES
    rows = qkv_weight.shape[0]
    depth = down_weight.shape[0]
    hidden = planes * depth
    pair = planes // 2
    length = ranks * tok_rows
    tokens = seqs * length
    rank = lax.axis_index(ULY) * lax.axis_size(BLK) + lax.axis_index(BLK)
    owner = lax.axis_index(BATCH) * ranks + rank

    x_own = jnp.transpose(residual_in, (1, 0, 2))
    cot_own = jnp.transpose(cotangent, (1, 0, 2))
    wq_send = jnp.transpose(
        qkv_weight.reshape(rows, 3, 2, pair, ranks // 2, HD), (4, 2, 0, 1, 3, 5)
    ).reshape(ranks, rows, 3 * LANES)
    wu_send = jnp.transpose(
        up_weight.reshape(rows, planes, ranks, depth), (2, 0, 1, 3)
    ).reshape(ranks, rows, hidden)
    at_rank = (jnp.arange(ranks) == rank).astype(single)[:, None]
    at_owner = (jnp.arange(ranks * planes) == owner).astype(single)[:, None]
    placed = [
        (at_rank * v.astype(single)[None]).reshape(1, 2, LANES)
        for v in (dense_bias, norm1_gain, norm1_bias, norm2_gain, norm2_bias, down_bias)
    ]
    placed_qkv = jnp.transpose(
        (at_owner * qkv_bias.astype(single)[None]).reshape(3, 2, pair, ranks // 2, HD),
        (3, 1, 0, 2, 4),
    ).reshape(ranks, 3, LANES)
    placed_up = jnp.transpose(
        (at_owner * up_bias.astype(single)[None]).reshape(planes, ranks, LANES), (1, 0, 2)
    )
    vec_send = jnp.concatenate(
        [jnp.broadcast_to(p, (ranks, 2, LANES)) for p in placed]
        + [
            placed_qkv,
            jnp.zeros((ranks, 1, LANES), single),
            placed_up,
            jnp.zeros((ranks, 4, LANES), single),
        ],
        axis=1,
    )
    table = jnp.asarray(rotary_rows(length))
    inputs = dict(
        x_own=x_own,
        cot_own=cot_own,
        wq_s=wq_send,
        wu_s=wu_send,
        wd_s=down_weight,
        wo_s=dense_weight,
        vec_s=vec_send,
        table=table,
    )
    shard = (seqs, tok_rows, width)
    lanes_in = vec_send.shape[1]
    outputs = dict(
        out=(shard, half_type),
        in_grad=(shard, single),
        dq=((ranks, rows, 3 * LANES), half_type),
        du=((ranks, rows, hidden), half_type),
        dd=((depth, width), single),
        dd_o=((rows, width), single),
        dv=((ranks, 16, LANES), single),
    )
    q_shape = (planes, ranks * rows, 3 * LANES)
    u_shape = (planes, ranks * rows, hidden)
    d_shape = (planes, depth, width)
    o_shape = (planes, rows, width)
    chips = ranks // 2
    scratch = dict(
        xa=((seqs, length, width), half_type),
        ca=((seqs, length, width), half_type),
        wq=(q_shape, half_type),
        wu=(u_shape, half_type),
        wd=(d_shape, half_type),
        wo=(o_shape, half_type),
        wo2=((pair, 2, rows, width), half_type),
        vec_in=((ranks, lanes_in, LANES), single),
        va=((planes, lanes_in, LANES), single),
        center=((tokens, 1), single),
        inverse=((tokens, 1), single),
        act_one=((tokens, width), half_type),
        act_two=((tokens, width), half_type),
        query=((tokens, LANES), half_type),
        key=((tokens, LANES), half_type),
        value=((tokens, LANES), half_type),
        attn=((tokens, LANES), half_type),
        attn_grad=((tokens, LANES), half_type),
        qkv_grad=((tokens, 3 * LANES), half_type),
        gelu=((tokens, hidden), half_type),
        slope=((tokens, hidden), single),
        pre_grad=((tokens, hidden), half_type),
        gq=(q_shape, half_type),
        gu=(u_shape, half_type),
        gd=(d_shape, half_type),
        go=((pair, 2, rows, width), half_type),
        go4=(o_shape, half_type),
        above_q=(q_shape, half_type),
        below_q=(q_shape, half_type),
        above_u=(u_shape, half_type),
        below_u=(u_shape, half_type),
        above_d=(d_shape, half_type),
        below_d=(d_shape, half_type),
        above_o=(o_shape, half_type),
        below_o=(o_shape, half_type),
        fq=(q_shape[1:], half_type),
        fu=(u_shape[1:], half_type),
        po=((seqs, chips, 2, tok_rows, width), half_type),
        pg=((seqs, chips, 2, tok_rows, width), half_type),
        pairs_o=((seqs, chips, tok_rows, width), half_type),
        pairs_g=((seqs, chips, tok_rows, width), half_type),
        sums_o=((seqs, chips, tok_rows, width), half_type),
        sums_g=((seqs, chips, tok_rows, width), half_type),
        side_o=((3,) + shard, half_type),
        side_g=((3,) + shard, half_type),
        sums=((8, width), single),
        sm=((ranks, 8, LANES), single),
        sm_in=((ranks, 8, LANES), single),
        vz=((planes, 16, LANES), single),
        vt=((16, LANES), single),
    )
    for block in range(length // TILE):
        scratch["probs%d" % block] = ((seqs * LANES // HD, TILE, (block + 1) * TILE), single)
    names = tuple(inputs) + tuple(outputs) + tuple(scratch) + ("send", "recv")
    out, in_grad, dq, du, dd, dd_o, dv = pl.pallas_call(
        functools.partial(layer_kernel, names, planes),
        out_shape=[jax.ShapeDtypeStruct(*what) for what in outputs.values()],
        in_specs=[VMEM] * len(inputs),
        out_specs=[VMEM] * len(outputs),
        scratch_shapes=[pltpu.VMEM(*what) for what in scratch.values()]
        + [pltpu.SemaphoreType.DMA((LAYER_SLOTS,))] * 2,
        compiler_params=pltpu.CompilerParams(
            collective_id=0, has_side_effects=True, vmem_limit_bytes=60 * 2**20
        ),
    )(*inputs.values())

    results = dict(
        out_out=(residual_in.shape, half_type),
        in_grad_out=(residual_in.shape, single),
        qkv_out=(qkv_weight.shape, single),
        qkv_bias=(qkv_bias.shape, single),
        dense_out=(dense_weight.shape, single),
        dense_bias=(dense_bias.shape, single),
        gain_one=(norm1_gain.shape, single),
        shift_one=(norm1_bias.shape, single),
        gain_two=(norm2_gain.shape, single),
        shift_two=(norm2_bias.shape, single),
        up_out=(up_weight.shape, single),
        up_bias=(up_bias.shape, single),
        down_out=(down_weight.shape, single),
        down_bias=(down_bias.shape, single),
    )
    return tuple(
        pl.pallas_call(
            functools.partial(finish_kernel, tuple(outputs) + tuple(results), planes),
            out_shape=[jax.ShapeDtypeStruct(*what) for what in results.values()],
            in_specs=[VMEM] * len(outputs),
            out_specs=[VMEM] * len(results),
        )(out, in_grad, dq, du, dd, dd_o, dv)
    )


def solution(mesh):
    placed = (
        P(TOKENS, BATCH, None),
        P(AXES, None),
        P(AXES),
        P(AXES, None),
        P(AXES),
        P(AXES),
        P(AXES),
        P(AXES),
        P(AXES),
        P(AXES, None),
        P(AXES),
        P(AXES, None),
        P(AXES),
        P(TOKENS, BATCH, None),
    )
    return jax.shard_map(
        functools.partial(body, dict(mesh.shape)),
        mesh=mesh,
        in_specs=placed,
        out_specs=(
            P(TOKENS, BATCH, None),
            P(TOKENS, BATCH, None),
            P(AXES, None),
            P(AXES),
            P(AXES, None),
            P(AXES),
            P(AXES),
            P(AXES),
            P(AXES),
            P(AXES),
            P(AXES, None),
            P(AXES),
            P(AXES, None),
            P(AXES),
        ),
        check_vma=False,
    )
```

```python
import functools
import math

import jax
import jax.numpy as jnp
import numpy as np
from jax import lax
from jax.experimental import pallas as pl
from jax.experimental.pallas import tpu as pltpu
from jax.sharding import PartitionSpec as P

HD = 64
BATCH, ULY, BLK = "batch", "ulysses", "blk"
AXES = (BATCH, ULY, BLK)
TOKENS = (ULY, BLK)


EPSILON = 1e-05
INV_ROOT_TWO = 0.7071067811865476
INV_ROOT_TWO_PI = 0.3989422804014327


def layer_norm(values):
    center = jnp.mean(values, axis=-1, keepdims=True)
    shifted = values - center
    inverse = lax.rsqrt(jnp.mean(shifted * shifted, axis=-1, keepdims=True) + EPSILON)
    return (shifted * inverse, inverse)


def norm_back(gradient, normed, inverse, gain_vec):
    scaled = gradient * gain_vec
    return inverse * (
        scaled
        - jnp.mean(scaled, axis=-1, keepdims=True)
        - normed * jnp.mean(scaled * normed, axis=-1, keepdims=True)
    )


def gelu_value(pre_values):
    return 0.5 * pre_values * (1.0 + jax.scipy.special.erf(pre_values * INV_ROOT_TWO))


def gelu_slope(pre_values):
    normal_cdf = 0.5 * (1.0 + jax.scipy.special.erf(pre_values * INV_ROOT_TWO))
    return normal_cdf + pre_values * jnp.exp(-0.5 * pre_values * pre_values) * INV_ROOT_TWO_PI


def rotary_tables(positions, rotary):
    half_rot = rotary // 2
    frequency = 1.0 / 10000.0 ** (jnp.arange(half_rot, dtype=jnp.float32) * (2.0 / rotary))
    angles = positions.astype(jnp.float32)[:, None] * frequency[None, :]
    cosine = jnp.concatenate([jnp.cos(angles), jnp.cos(angles)], axis=-1)
    sine_table = jnp.concatenate([jnp.sin(angles), jnp.sin(angles)], axis=-1)
    return (cosine, sine_table)


def expand_table(table, tensor):
    extra_dims = (1,) * (tensor.ndim - 2)
    return table.reshape((table.shape[0],) + extra_dims + (table.shape[1],))


def rotate_fwd(tensor, cosine, sine_table, rotary):
    half_rot = rotary // 2
    cos_full = expand_table(cosine, tensor)
    sin_full = expand_table(sine_table, tensor)
    rot_part = tensor[..., :rotary]
    turned = jnp.concatenate([-rot_part[..., half_rot:], rot_part[..., :half_rot]], axis=-1)
    return jnp.concatenate([rot_part * cos_full + turned * sin_full, tensor[..., rotary:]], axis=-1)


def rotate_back(tensor, cosine, sine_table, rotary):
    half_rot = rotary // 2
    cos_full = expand_table(cosine, tensor)
    sin_full = expand_table(sine_table, tensor)
    rot_part = tensor[..., :rotary]
    weighted = rot_part * sin_full
    turned = jnp.concatenate([weighted[..., half_rot:], -weighted[..., :half_rot]], axis=-1)
    return jnp.concatenate([rot_part * cos_full + turned, tensor[..., rotary:]], axis=-1)


def general_body(
    residual_in,
    qkv_weight,
    qkv_bias,
    dense_weight,
    dense_bias,
    norm1_gain,
    norm1_bias,
    norm2_gain,
    norm2_bias,
    up_weight,
    up_bias,
    down_weight,
    down_bias,
    cotangent,
):
    single = jnp.float32
    half_type = jnp.bfloat16
    gathered = (
        lax.all_gather(qkv_weight, AXES, axis=0, tiled=True),
        lax.all_gather(qkv_bias, AXES, axis=0, tiled=True),
        lax.all_gather(dense_weight, AXES, axis=0, tiled=True),
        lax.all_gather(dense_bias, AXES, axis=0, tiled=True),
        lax.all_gather(norm1_gain, AXES, axis=0, tiled=True),
        lax.all_gather(norm1_bias, AXES, axis=0, tiled=True),
        lax.all_gather(norm2_gain, AXES, axis=0, tiled=True),
        lax.all_gather(norm2_bias, AXES, axis=0, tiled=True),
        lax.all_gather(up_weight, AXES, axis=0, tiled=True),
        lax.all_gather(up_bias, AXES, axis=0, tiled=True),
        lax.all_gather(down_weight, AXES, axis=0, tiled=True),
        lax.all_gather(down_bias, AXES, axis=0, tiled=True),
    )
    (
        w_qkv,
        b_qkv,
        w_dense,
        b_dense,
        gain_one,
        shift_one,
        gain_two,
        shift_two,
        w_up,
        b_up,
        w_down,
        b_down,
    ) = gathered
    tok_rows = residual_in.shape[0]
    seq_count = residual_in.shape[1]
    model_width = residual_in.shape[2]
    head_count = model_width // HD
    rotary = HD // 4
    scale_factor = 1.0 / math.sqrt(HD)
    blk_size = lax.axis_size(BLK)
    uly_size = lax.axis_size(ULY)
    blk_index = lax.axis_index(BLK)
    block_id = lax.axis_index(ULY) * blk_size + blk_index
    seq_pos = block_id * tok_rows + jnp.arange(tok_rows, dtype=jnp.int32)
    inputs_f = residual_in.astype(single)
    normed, inverse = layer_norm(inputs_f)
    act_one = (normed * gain_one.astype(single) + shift_one.astype(single)).astype(half_type)
    act_two = (normed * gain_two.astype(single) + shift_two.astype(single)).astype(half_type)
    qkv_full = jnp.einsum(
        "tsd,df->tsf", act_one, w_qkv, preferred_element_type=single
    ) + b_qkv.astype(single)
    cos_seq, sin_seq = rotary_tables(seq_pos, rotary)
    head_shape = (tok_rows, seq_count, head_count, HD)
    query_seq = (
        rotate_fwd(qkv_full[..., :model_width].reshape(head_shape), cos_seq, sin_seq, rotary)
        .reshape(tok_rows, seq_count, model_width)
        .astype(half_type)
    )
    key_seq = (
        rotate_fwd(
            qkv_full[..., model_width : 2 * model_width].reshape(head_shape),
            cos_seq,
            sin_seq,
            rotary,
        )
        .reshape(tok_rows, seq_count, model_width)
        .astype(half_type)
    )
    value_seq = qkv_full[..., 2 * model_width :].astype(half_type)
    query_loc, key_loc, value_loc = (
        lax.all_to_all(query_seq, ULY, split_axis=2, concat_axis=0, tiled=True),
        lax.all_to_all(key_seq, ULY, split_axis=2, concat_axis=0, tiled=True),
        lax.all_to_all(value_seq, ULY, split_axis=2, concat_axis=0, tiled=True),
    )
    local_rows = query_loc.shape[0]
    features = query_loc.shape[2]
    local_heads = features // HD
    key_all, value_all = (
        lax.all_gather(key_loc, BLK, axis=0, tiled=True),
        lax.all_gather(value_loc, BLK, axis=0, tiled=True),
    )
    total_rows = key_all.shape[0]
    row_ids = jnp.arange(local_rows, dtype=jnp.int32)
    query_pos = (row_ids // tok_rows * blk_size + blk_index) * tok_rows + row_ids % tok_rows
    block_rows = math.gcd(512, local_rows)
    n_blocks = local_rows // block_rows
    query_h = query_loc.reshape(local_rows, seq_count, local_heads, HD)
    key_h = jnp.transpose(
        key_all.reshape(blk_size, uly_size, tok_rows, seq_count, features), (1, 0, 2, 3, 4)
    ).reshape(total_rows, seq_count, local_heads, HD)
    value_h = jnp.transpose(
        value_all.reshape(blk_size, uly_size, tok_rows, seq_count, features), (1, 0, 2, 3, 4)
    ).reshape(total_rows, seq_count, local_heads, HD)
    zero_idx = jnp.zeros((), jnp.int32)
    step_ids = jnp.arange(n_blocks * seq_count, dtype=jnp.int32)
    row_shape = (block_rows, 1, local_heads, HD)

    def select(step_index):
        row_start = step_index // seq_count * block_rows
        seq_index = step_index % seq_count
        query_rows = lax.dynamic_slice(
            query_h, (row_start, seq_index, zero_idx, zero_idx), row_shape
        )
        limit = jnp.max(query_pos) // block_rows + 1
        return (row_start, seq_index, query_rows, query_pos, limit)

    def block_scores(query_rows, row_pos, key_index, seq_index):
        key_start = key_index * block_rows
        slot = (key_start, seq_index, zero_idx, zero_idx)
        key_rows = lax.dynamic_slice(key_h, slot, (block_rows, 1, local_heads, HD))
        value_rows = lax.dynamic_slice(value_h, slot, (block_rows, 1, local_heads, HD))
        scores = (
            jnp.einsum("qshd,kshd->shqk", query_rows, key_rows, preferred_element_type=single)
            * scale_factor
        )
        key_ids = key_start + jnp.arange(block_rows, dtype=jnp.int32)
        allowed = (key_ids[None, :] <= row_pos[:, None])[None, None]
        return (jnp.where(allowed, scores, -jnp.inf), key_rows, value_rows, slot)

    def forward_block(step_index):
        row_start, seq_index, query_rows, row_pos, limit = select(step_index)

        def total_step(key_index, carry):
            running_max, running_sum = carry
            masked, key_rows, value_rows, slot = block_scores(
                query_rows, row_pos, key_index, seq_index
            )
            new_max = jnp.maximum(running_max, jnp.max(masked, axis=-1))
            new_sum = running_sum * jnp.exp(running_max - new_max) + jnp.sum(
                jnp.exp(masked - new_max[..., None]), axis=-1
            )
            return (new_max, new_sum)

        start_max = jnp.full((1, local_heads, block_rows), -jnp.inf, single)
        start_sum = jnp.zeros((1, local_heads, block_rows), single)
        final_max, final_sum = lax.fori_loop(zero_idx, limit, total_step, (start_max, start_sum))
        log_total = final_max + jnp.log(final_sum)

        def value_step(key_index, acc):
            masked, key_rows, value_rows, slot = block_scores(
                query_rows, row_pos, key_index, seq_index
            )
            weights_b = jnp.exp(masked - log_total[..., None]).astype(half_type)
            return acc + jnp.einsum(
                "shqk,kshd->qshd", weights_b, value_rows, preferred_element_type=single
            )

        result = lax.fori_loop(zero_idx, limit, value_step, jnp.zeros(row_shape, single)).astype(
            half_type
        )
        return (result[:, 0], log_total)

    results, log_totals = lax.map(forward_block, step_ids)
    attn_h = jnp.transpose(
        results.reshape(n_blocks, seq_count, block_rows, local_heads, HD), (0, 2, 1, 3, 4)
    ).reshape(local_rows, seq_count, local_heads, HD)
    attn_seq = lax.all_to_all(
        attn_h.reshape(local_rows, seq_count, features),
        ULY,
        split_axis=0,
        concat_axis=2,
        tiled=True,
    )
    proj_out = jnp.einsum(
        "tsd,de->tse", attn_seq, w_dense, preferred_element_type=single
    ) + b_dense.astype(single)
    pre_act = jnp.einsum("tsd,df->tsf", act_two, w_up, preferred_element_type=single) + b_up.astype(
        single
    )
    gelu_out = gelu_value(pre_act).astype(half_type)
    mlp_out = jnp.einsum(
        "tsf,fd->tsd", gelu_out, w_down, preferred_element_type=single
    ) + b_down.astype(single)
    output = (inputs_f + proj_out + mlp_out).astype(half_type)
    back_params = (
        lax.all_gather(qkv_weight, AXES, axis=0, tiled=True),
        lax.all_gather(qkv_bias, AXES, axis=0, tiled=True),
        lax.all_gather(dense_weight, AXES, axis=0, tiled=True),
        lax.all_gather(dense_bias, AXES, axis=0, tiled=True),
        lax.all_gather(norm1_gain, AXES, axis=0, tiled=True),
        lax.all_gather(norm1_bias, AXES, axis=0, tiled=True),
        lax.all_gather(norm2_gain, AXES, axis=0, tiled=True),
        lax.all_gather(norm2_bias, AXES, axis=0, tiled=True),
        lax.all_gather(up_weight, AXES, axis=0, tiled=True),
        lax.all_gather(up_bias, AXES, axis=0, tiled=True),
        lax.all_gather(down_weight, AXES, axis=0, tiled=True),
        lax.all_gather(down_bias, AXES, axis=0, tiled=True),
    )
    back_qkv = back_params[0]
    back_dense = back_params[2]
    back_gain_one = back_params[4].astype(single)
    back_gain_two = back_params[6].astype(single)
    back_up = back_params[8]
    back_down = back_params[10]
    grad_f = cotangent.astype(single)
    bias_sum = jnp.sum(grad_f, axis=(0, 1))
    down_w_grad = jnp.einsum("tsf,tsd->fd", gelu_out, cotangent, preferred_element_type=single)
    gelu_grad = jnp.einsum("tsd,fd->tsf", cotangent, back_down, preferred_element_type=single)
    pre_grad = (gelu_grad * gelu_slope(pre_act)).astype(half_type)
    up_w_grad = jnp.einsum("tsd,tsf->df", act_two, pre_grad, preferred_element_type=single)
    up_b_grad = jnp.sum(pre_grad.astype(single), axis=(0, 1))
    act_two_grad = jnp.einsum("tsf,df->tsd", pre_grad, back_up, preferred_element_type=single)
    gain_two_grad = jnp.sum(act_two_grad * normed, axis=(0, 1))
    shift_two_grad = jnp.sum(act_two_grad, axis=(0, 1))
    dense_w_grad = jnp.einsum("tsd,tse->de", attn_seq, cotangent, preferred_element_type=single)
    attn_grad = jnp.einsum(
        "tse,de->tsd", cotangent, back_dense, preferred_element_type=single
    ).astype(half_type)
    grad_loc = lax.all_to_all(attn_grad, ULY, split_axis=2, concat_axis=0, tiled=True)
    grad_h = grad_loc.reshape(local_rows, seq_count, local_heads, HD)

    def backward_block(acc_pair, step_index):
        row_start, seq_index, query_rows, row_pos, limit = select(step_index)
        own_slot = (row_start, seq_index, zero_idx, zero_idx)
        out_rows = lax.dynamic_slice(attn_h, own_slot, row_shape)
        grad_rows = lax.dynamic_slice(grad_h, own_slot, row_shape)
        log_total = log_totals[step_index]
        delta_row = jnp.transpose(
            jnp.sum(grad_rows.astype(single) * out_rows.astype(single), axis=-1), (1, 2, 0)
        )

        def grad_step(key_index, carry):
            key_acc, value_acc, query_acc = carry
            masked, key_rows, value_rows, slot = block_scores(
                query_rows, row_pos, key_index, seq_index
            )
            probs_f = jnp.exp(masked - log_total[..., None])
            value_part = jnp.einsum(
                "shqk,qshd->kshd",
                probs_f.astype(half_type),
                grad_rows,
                preferred_element_type=single,
            )
            grad_prob = jnp.einsum(
                "qshd,kshd->shqk", grad_rows, value_rows, preferred_element_type=single
            )
            grad_score = (probs_f * (grad_prob - delta_row[..., None]) * scale_factor).astype(
                half_type
            )
            query_acc = query_acc + jnp.einsum(
                "shqk,kshd->qshd", grad_score, key_rows, preferred_element_type=single
            )
            key_part = jnp.einsum(
                "shqk,qshd->kshd", grad_score, query_rows, preferred_element_type=single
            )
            key_acc = lax.dynamic_update_slice(
                key_acc, lax.dynamic_slice(key_acc, slot, key_part.shape) + key_part, slot
            )
            value_acc = lax.dynamic_update_slice(
                value_acc, lax.dynamic_slice(value_acc, slot, value_part.shape) + value_part, slot
            )
            return (key_acc, value_acc, query_acc)

        key_acc, value_acc, query_acc = lax.fori_loop(
            zero_idx, limit, grad_step, (acc_pair[0], acc_pair[1], jnp.zeros(row_shape, single))
        )
        return ((key_acc, value_acc), query_acc[:, 0])

    acc_zero = jnp.zeros((total_rows, seq_count, local_heads, HD), single)
    acc_final, query_parts = lax.scan(backward_block, (acc_zero, acc_zero), step_ids)
    query_grad = jnp.transpose(
        query_parts.reshape(n_blocks, seq_count, block_rows, local_heads, HD), (0, 2, 1, 3, 4)
    ).reshape(local_rows, seq_count, local_heads, HD)
    key_terms = jnp.transpose(
        acc_final[0].reshape(uly_size, blk_size, tok_rows, seq_count, features), (1, 0, 2, 3, 4)
    ).reshape(total_rows, seq_count, features)
    value_terms = jnp.transpose(
        acc_final[1].reshape(uly_size, blk_size, tok_rows, seq_count, features), (1, 0, 2, 3, 4)
    ).reshape(total_rows, seq_count, features)
    key_back, value_back = (
        lax.psum_scatter(key_terms, BLK, scatter_dimension=0, tiled=True),
        lax.psum_scatter(value_terms, BLK, scatter_dimension=0, tiled=True),
    )
    cos_h, sin_h = rotary_tables(query_pos, rotary)
    query_send = (
        rotate_back(query_grad, cos_h, sin_h, rotary)
        .reshape(local_rows, seq_count, features)
        .astype(half_type)
    )
    key_send = (
        rotate_back(key_back.reshape(local_rows, seq_count, local_heads, HD), cos_h, sin_h, rotary)
        .reshape(local_rows, seq_count, features)
        .astype(half_type)
    )
    value_send = value_back.astype(half_type)
    query_ret, key_ret, value_ret = (
        lax.all_to_all(query_send, ULY, split_axis=0, concat_axis=2, tiled=True),
        lax.all_to_all(key_send, ULY, split_axis=0, concat_axis=2, tiled=True),
        lax.all_to_all(value_send, ULY, split_axis=0, concat_axis=2, tiled=True),
    )
    qkv_grad = jnp.concatenate([query_ret, key_ret, value_ret], axis=-1)
    qkv_w_grad = jnp.einsum("tsd,tsf->df", act_one, qkv_grad, preferred_element_type=single)
    qkv_b_grad = jnp.sum(qkv_grad.astype(single), axis=(0, 1))
    act_one_grad = jnp.einsum("tsf,df->tsd", qkv_grad, back_qkv, preferred_element_type=single)
    gain_one_grad = jnp.sum(act_one_grad * normed, axis=(0, 1))
    shift_one_grad = jnp.sum(act_one_grad, axis=(0, 1))
    input_grad = (
        grad_f
        + norm_back(act_one_grad, normed, inverse, back_gain_one)
        + norm_back(act_two_grad, normed, inverse, back_gain_two)
    )
    summed = (
        lax.psum_scatter(qkv_w_grad, AXES, scatter_dimension=0, tiled=True),
        lax.psum_scatter(qkv_b_grad, AXES, scatter_dimension=0, tiled=True),
        lax.psum_scatter(
            dense_w_grad, AXES, scatter_dimension=0, tiled=True
        ),
        lax.psum_scatter(bias_sum, AXES, scatter_dimension=0, tiled=True),
        lax.psum_scatter(
            gain_one_grad, AXES, scatter_dimension=0, tiled=True
        ),
        lax.psum_scatter(
            shift_one_grad, AXES, scatter_dimension=0, tiled=True
        ),
        lax.psum_scatter(
            gain_two_grad, AXES, scatter_dimension=0, tiled=True
        ),
        lax.psum_scatter(
            shift_two_grad, AXES, scatter_dimension=0, tiled=True
        ),
        lax.psum_scatter(up_w_grad, AXES, scatter_dimension=0, tiled=True),
        lax.psum_scatter(up_b_grad, AXES, scatter_dimension=0, tiled=True),
        lax.psum_scatter(down_w_grad, AXES, scatter_dimension=0, tiled=True),
        lax.psum_scatter(bias_sum, AXES, scatter_dimension=0, tiled=True),
    )
    return (
        output,
        input_grad,
        summed[0],
        summed[1],
        summed[2],
        summed[3],
        summed[4],
        summed[5],
        summed[6],
        summed[7],
        summed[8],
        summed[9],
        summed[10],
        summed[11],
    )


MESH = pl.DeviceIdType.MESH


class Place:
    def __init__(self, planes):
        self.planes = planes
        self.b = lax.axis_index(BATCH)
        self.u = lax.axis_index(ULY)
        k = lax.axis_index(BLK)
        self.y, self.c = k // 2, k % 2
        self.t = self.u * 4 + k
        self.xn, self.yn, self.pn = self.peer(4), self.peer(2), self.peer(1)

    def rank(self, d):
        u = 1 - self.u if d & 4 else self.u
        y = 1 - self.y if d & 2 else self.y
        c = 1 - self.c if d & 1 else self.c
        return u * 4 + y * 2 + c

    def chip(self, d):
        return self.rank(d) // 2

    def peer(self, d):
        u = 1 - self.u if d & 4 else self.u
        y = 1 - self.y if d & 2 else self.y
        c = 1 - self.c if d & 1 else self.c
        return {BATCH: self.b, ULY: u, BLK: y * 2 + c}

    def along(self, step):
        return {BATCH: self.b + step, ULY: self.u, BLK: self.y * 2 + self.c}

    def barrier(self):
        sem = pltpu.get_barrier_semaphore()
        for d in range(1, 8):
            pl.semaphore_signal(sem, inc=1, device_id=self.peer(d), device_id_type=MESH)

        for step in range(1, self.planes):

            @pl.when(self.b >= step)
            def _():
                pl.semaphore_signal(sem, inc=1, device_id=self.along(-step), device_id_type=MESH)

            @pl.when(self.b + step < self.planes)
            def _():
                pl.semaphore_signal(sem, inc=1, device_id=self.along(step), device_id_type=MESH)

        pl.semaphore_wait(sem, 7 + self.planes - 1)


class Mail:
    def __init__(self, send, recv, near):
        self.send, self.recv, self.used, self.open = send, recv, 0, []
        self.near, self.near_used = near, 0

    def bring(self, src, dst):
        made = pltpu.make_async_copy(src, dst, self.near.at[self.near_used])
        self.near_used += 1
        made.start()
        return made

    def slots(self, n):
        first = self.used
        self.used += n
        return first

    def copy(self, src, dst, slot, device, recv_slot=None):
        return pltpu.make_async_remote_copy(
            src_ref=src,
            dst_ref=dst,
            send_sem=self.send.at[slot],
            recv_sem=self.recv.at[slot if recv_slot is None else recv_slot],
            device_id=device,
            device_id_type=MESH,
        )

    def post(self, src, dst, slot, device):
        made = self.copy(src, dst, slot, device)
        made.start()
        self.open.append(made)

    def arrived(self, dst, slot, device):
        self.copy(dst, dst, slot, device).wait_recv()

    def close(self):
        for made in self.open:
            made.wait_send()


class PlaneGather:
    def __init__(self, at, mail, shard, whole):
        self.at, self.mail, self.shard, self.whole = at, mail, shard, whole
        self.rows = shard.shape[1]
        self.halves = shard.shape[0] // 2
        self.base = mail.slots(10)

    def half(self, i):
        return self.shard.at[pl.ds(i * self.halves, self.halves)]

    def block(self, d, half=None):
        rows = pl.ds(pl.multiple_of(self.at.rank(d) * self.rows, self.rows), self.rows)
        if half is None:
            return self.whole.at[:, rows, :]
        return self.whole.at[pl.ds(half * self.halves, self.halves), rows, :]

    def start(self):
        at, mail, s = self.at, self.mail, self.base
        mail.post(self.half(1), self.block(0, 1), s, at.xn)
        mail.post(self.half(0), self.block(0, 0), s + 1, at.yn)
        mail.post(self.half(0), self.block(0, 0), s + 8, at.xn)
        mail.post(self.half(1), self.block(0, 1), s + 9, at.yn)
        mail.post(self.shard, self.block(0), s + 2, at.pn)
        self.own = mail.bring(self.shard, self.block(0))

    def relay_y(self):
        at, mail, s = self.at, self.mail, self.base
        mail.arrived(self.block(2, 0), s + 1, at.yn)
        mail.post(self.block(2, 0), self.block(2, 0), s + 3, at.xn)

    def relay_x(self):
        at, mail, s = self.at, self.mail, self.base
        mail.arrived(self.block(4, 1), s, at.xn)
        mail.post(self.block(4, 1), self.block(4, 1), s + 4, at.yn)

    def share(self):
        at, mail, s = self.at, self.mail, self.base
        mail.arrived(self.block(2, 1), s + 9, at.yn)
        mail.post(self.block(2), self.block(2), s + 5, at.pn)
        mail.arrived(self.block(4, 0), s + 8, at.xn)
        mail.post(self.block(4), self.block(4), s + 6, at.pn)

    def far(self):
        at, mail, s = self.at, self.mail, self.base
        mail.arrived(self.block(6, 0), s + 3, at.xn)
        mail.arrived(self.block(6, 1), s + 4, at.yn)
        mail.post(self.block(6), self.block(6), s + 7, at.pn)

    def finish(self):
        at, mail, s = self.at, self.mail, self.base
        mail.arrived(self.block(1), s + 2, at.pn)
        mail.arrived(self.block(3), s + 5, at.pn)
        mail.arrived(self.block(5), s + 6, at.pn)
        mail.arrived(self.block(7), s + 7, at.pn)
        self.own.wait()


class LineGather:
    def __init__(self, at, mail, held, first=0, count=None):
        self.at, self.mail, self.held = at, mail, held
        self.rows = pl.ds(first, held.shape[1] - first if count is None else count)
        self.up, self.down = mail.slots(at.planes), mail.slots(at.planes)

    def part(self, slot):
        return self.held.at[slot, self.rows]

    def pass_on(self, slot, src=None):
        at = self.at
        part = self.part(slot)
        src = part if src is None else src.at[self.rows]

        @pl.when((slot <= at.b) & (at.b < at.planes - 1))
        def _():
            self.mail.copy(src, part, self.up + slot, at.along(1)).start()

        @pl.when((slot >= at.b) & (at.b > 0))
        def _():
            self.mail.copy(src, part, self.down + slot, at.along(-1)).start()

    def start(self, src=None):
        self.pass_on(self.at.b, src)

    def take(self, distance):
        at = self.at

        @pl.when(at.b >= distance)
        def _():
            slot = at.b - distance
            self.mail.arrived(self.part(slot), self.up + slot, at.along(-1))
            self.pass_on(slot)

        @pl.when(at.b + distance < at.planes)
        def _():
            slot = at.b + distance
            self.mail.arrived(self.part(slot), self.down + slot, at.along(1))
            self.pass_on(slot)

    def close(self):
        at = self.at
        for slot in range(at.planes):
            part = self.part(slot)

            @pl.when((slot <= at.b) & (at.b < at.planes - 1))
            def _():
                self.mail.copy(part, part, self.up + slot, at.along(1)).wait_send()

            @pl.when((slot >= at.b) & (at.b > 0))
            def _():
                self.mail.copy(part, part, self.down + slot, at.along(-1)).wait_send()


class StarGather:
    def __init__(self, at, mail, held):
        self.at, self.mail, self.held = at, mail, held
        self.base = mail.slots(2 * at.planes)

    def each(self, action):
        at = self.at
        for step in range(1, at.planes):

            @pl.when(at.b + step < at.planes)
            def _():
                action(step, self.base + step)

            @pl.when(at.b >= step)
            def _():
                action(-step, self.base + at.planes + step)

    def start(self):
        part = self.held.at[self.at.b]
        self.each(
            lambda step, slot: self.mail.copy(part, part, slot, self.at.along(step)).start()
        )

    def finish(self):
        n = self.at.planes
        for step in range(1, n):

            @pl.when(self.at.b + step < n)
            def _():
                part = self.held.at[self.at.b + step]
                self.mail.arrived(part, self.base + n + step, self.at.along(step))

            @pl.when(self.at.b >= step)
            def _():
                part = self.held.at[self.at.b - step]
                self.mail.arrived(part, self.base + step, self.at.along(-step))

    def close(self):
        part = self.held.at[self.at.b]
        self.each(
            lambda step, slot: self.mail.copy(part, part, slot, self.at.along(step)).wait_send()
        )


class PlaneExchange:
    def __init__(self, at, mail, pieces, landings, parts=1):
        self.at, self.mail, self.parts = at, mail, parts
        self.pieces = (lambda rank: [pieces(rank)]) if parts == 1 else pieces
        self.landings = (lambda rank: [landings(rank)]) if parts == 1 else landings
        self.base = mail.slots(8 * parts)

    def start(self):
        at, n = self.at, self.parts
        for d in range(1, 8):
            for i, (piece, landing) in enumerate(
                zip(self.pieces(at.rank(d)), self.landings(at.t))
            ):
                self.mail.post(piece, landing, self.base + d * n + i, at.peer(d))
        self.own = [
            self.mail.bring(piece, landing)
            for piece, landing in zip(self.pieces(at.t), self.landings(at.t))
        ]

    def finish(self):
        at, n = self.at, self.parts
        for d in range(1, 8):
            for i, landing in enumerate(self.landings(at.rank(d))):
                self.mail.arrived(landing, self.base + d * n + i, at.peer(d))
        for own in self.own:
            own.wait()


class PairExchange:
    def __init__(self, at, mail, src, dst, landed):
        self.at, self.mail, self.src, self.dst, self.landed = at, mail, src, dst, landed
        self.base = mail.slots(1)

    def start(self):
        self.mail.post(self.src, self.dst, self.base, self.at.pn)

    def finish(self):
        self.mail.arrived(self.landed, self.base, self.at.pn)


class PlaneReduce:
    def __init__(self, at, mail, terms, pairs, sums, side):
        self.at, self.mail, self.terms = at, mail, terms
        self.pairs, self.sums, self.side = pairs, sums, side
        self.base = mail.slots(8)
        self.order = (6, 4, 2, 0)
        self.halves = terms.shape[0] // 2

    def start(self):
        at = self.at
        for i, d in enumerate(self.order):
            chip = at.chip(d)
            self.mail.post(
                self.terms.at[:, chip, 1 - at.c], self.pairs.at[:, chip], self.base + i, at.pn
            )

    def half(self, ref, i):
        return ref.at[pl.ds(i * self.halves, self.halves)]

    def fold(self):
        at, mail, s = self.at, self.mail, self.base
        for i, d in enumerate(self.order):
            chip = at.chip(d)
            mail.arrived(self.pairs.at[:, chip], s + i, at.pn)
            total = self.terms[:, chip, at.c].astype(jnp.float32) + self.pairs[:, chip].astype(
                jnp.float32
            )
            self.sums[:, chip] = total.astype(self.sums.dtype)
            if d == 6:
                far = self.sums.at[:, chip]
                mail.post(self.half(far, 0), self.half(self.side.at[0], 0), s + 4, at.xn)
                mail.post(self.half(far, 1), self.half(self.side.at[0], 1), s + 5, at.yn)

    def turn(self):
        at, mail, s = self.at, self.mail, self.base
        for i, d, other, slot, nbr in ((1, 4, at.yn, 5, at.xn), (0, 2, at.xn, 4, at.yn)):
            chip = at.chip(d)
            landed = self.half(self.side.at[0], i)
            mail.arrived(landed, s + slot, other)
            part = self.half(self.sums.at[:, chip], i)
            part[...] = (part[...].astype(jnp.float32) + landed[...].astype(jnp.float32)).astype(
                self.sums.dtype
            )
            whole = self.sums.at[:, chip]
            mail.post(whole, self.side.at[2 - i], s + 6 + i, nbr)

    def finish(self):
        at, mail, s = self.at, self.mail, self.base
        mail.arrived(self.side.at[1], s + 7, at.xn)
        mail.arrived(self.side.at[2], s + 6, at.yn)
        return (
            self.sums[:, at.chip(0)].astype(jnp.float32)
            + self.side[1].astype(jnp.float32)
            + self.side[2].astype(jnp.float32)
        )


class LineReduce:
    def __init__(self, at, mail, terms, above, below):
        self.at, self.mail, self.terms = at, mail, terms
        self.above, self.below = above, below
        self.up, self.down = mail.slots(at.planes), mail.slots(at.planes)

    def edge(self, slot):
        at, last = self.at, self.at.planes - 1

        @pl.when((at.b == 0) & (slot > 0))
        def _():
            self.mail.copy(
                self.terms.at[slot], self.below.at[slot], self.up + slot, at.along(1)
            ).start()

        @pl.when((at.b == last) & (slot < last))
        def _():
            self.mail.copy(
                self.terms.at[slot], self.above.at[slot], self.down + slot, at.along(-1)
            ).start()

    def hop(self, hop, rank):
        last = self.at.planes - 1
        if last - rank > hop:
            self._forward(last - rank, self.below, self.up, 1, self.at.b == hop)
            self._forward(rank, self.above, self.down, -1, self.at.b == last - hop)

    def _forward(self, slot, held, base, step, here):
        at, mail = self.at, self.mail
        part = held.at[slot]

        @pl.when(here)
        def _():
            mail.arrived(part, base + slot, at.along(-step))
            total = self.terms[slot].astype(jnp.float32) + part[...].astype(jnp.float32)
            part[...] = total.astype(part.dtype)
            mail.copy(part, part, base + slot, at.along(step)).start()

    def finish(self, out):
        at, mail = self.at, self.mail
        b = at.b
        kind = out.dtype

        @pl.when(b == 0)
        def _():
            mail.arrived(self.above.at[b], self.down + b, at.along(1))
            out[...] = (
                self.terms[b].astype(jnp.float32) + self.above[b].astype(jnp.float32)
            ).astype(kind)

        @pl.when(b == at.planes - 1)
        def _():
            mail.arrived(self.below.at[b], self.up + b, at.along(-1))
            out[...] = (
                self.terms[b].astype(jnp.float32) + self.below[b].astype(jnp.float32)
            ).astype(kind)

        @pl.when((b > 0) & (b < at.planes - 1))
        def _():
            mail.arrived(self.below.at[b], self.up + b, at.along(-1))
            mail.arrived(self.above.at[b], self.down + b, at.along(1))
            out[...] = (
                self.terms[b].astype(jnp.float32)
                + self.below[b].astype(jnp.float32)
                + self.above[b].astype(jnp.float32)
            ).astype(kind)

    def close(self):
        at = self.at
        for slot in range(at.planes):
            part = self.terms.at[slot]

            @pl.when(at.b < slot)
            def _():
                self.mail.copy(part, part, self.up + slot, at.along(1)).wait_send()

            @pl.when(at.b > slot)
            def _():
                self.mail.copy(part, part, self.down + slot, at.along(-1)).wait_send()


TILE = 256
LANES = 128


def dot_nn(a, b):
    return lax.dot_general(a, b, (((1,), (0,)), ((), ())), preferred_element_type=jnp.float32)


def dot_nt(a, b):
    return lax.dot_general(a, b, (((1,), (1,)), ((), ())), preferred_element_type=jnp.float32)


def dot_tn(a, b):
    return lax.dot_general(a, b, (((0,), (0,)), ((), ())), preferred_element_type=jnp.float32)


def turn(value, tables, rows, sign):
    straight, early, late = (table[rows, :] for table in tables)
    ahead = pltpu.roll(value, LANES - HD // 8, 1)
    behind = pltpu.roll(value, HD // 8, 1)
    return value * straight + sign * (ahead * early + behind * late)


def of_head(value, head):
    lane = lax.broadcasted_iota(jnp.int32, value.shape, 1)
    return jnp.where(lane // HD == head, value, jnp.zeros_like(value))


def total_rows(value):
    return jnp.sum(value, axis=0, keepdims=True)


class Layer:
    def __init__(self, refs):
        self.__dict__.update(refs)
        self.heads = LANES // HD
        if "xa" in refs:
            self.seqs, self.length, self.width = self.xa.shape
            self.per_seq = self.length // TILE
            self.tiles = self.seqs * self.per_seq

    def rows(self, tile):
        return pl.ds(pl.multiple_of(tile * TILE, TILE), TILE)

    def in_seq(self, ref, tile):
        rows = pl.ds(pl.multiple_of(tile % self.per_seq * TILE, TILE), TILE)
        return ref[tile // self.per_seq, rows, :]

    def loop(self, count, step):
        def run(i, carry):
            step(i)
            return carry

        lax.fori_loop(0, count, run, 0)

    def wide(self, row):
        planes = self.va.shape[0]
        return jnp.concatenate(
            [self.va[b, pl.ds(2 * row + a, 1), :] for b in range(planes) for a in range(2)], axis=1
        )

    def own_vectors(self, rank):
        lane = lax.broadcasted_iota(jnp.int32, (2, LANES), 1)
        row = lax.broadcasted_iota(jnp.int32, (2, LANES), 0)
        for j, ref in enumerate(self.vectors):
            piece = ref[...].astype(jnp.float32).reshape(1, ref.shape[0])
            piece = jnp.concatenate([piece] * (LANES // ref.shape[0]), axis=1)
            here = (lane // ref.shape[0] == rank % 4) & (row == rank // 4)
            self.vec_s[2 * j : 2 * j + 2, :] = jnp.where(here, jnp.broadcast_to(piece, here.shape), 0.0)
        bias = self.b_qkv[...].astype(jnp.float32).reshape(1, self.b_qkv.shape[0])
        self.vec_s[12:13, :] = jnp.concatenate(
            [bias, jnp.zeros((1, LANES - bias.shape[1]), jnp.float32)], axis=1
        )
        self.vec_s[13:14, :] = self.b_up[...].astype(jnp.float32).reshape(1, LANES)

    def plane_vectors(self, slot):
        total = jnp.sum(self.vec_in[...], axis=0)
        self.va[slot, 0:16, :] = total
        for rank in range(self.vec_in.shape[0]):
            self.va[slot, 16 + rank : 17 + rank, :] = self.vec_in[rank, 12:13, :]
            self.va[slot, 24 + rank : 25 + rank, :] = self.vec_in[rank, 13:14, :]

    def sort_weight(self):
        rows = self.wq_raw.shape[0]
        low = lax.broadcasted_iota(jnp.int32, (rows, LANES), 1) < HD
        for part in range(3):
            for core in range(2):
                for pair in range(2):
                    first, second = (
                        self.wq_raw[
                            :, pl.ds(part * self.width + (core * 2 + j) * 4 * HD + pair * LANES, LANES)
                        ].astype(jnp.float32)
                        for j in range(2)
                    )
                    cut = slice(part * LANES, (part + 1) * LANES)
                    self.wq_s[4 * pair + core, :, cut] = jnp.where(
                        low, first, pltpu.roll(second, HD, 1)
                    ).astype(jnp.bfloat16)
                    self.wq_s[4 * pair + 2 + core, :, cut] = jnp.where(
                        low, pltpu.roll(first, HD, 1), second
                    ).astype(jnp.bfloat16)

    def statistics(self):
        def step(i):
            x = self.in_seq(self.xa, i).astype(jnp.float32)
            center = jnp.mean(x, axis=1, keepdims=True)
            shifted = x - center
            spread = jnp.mean(shifted * shifted, axis=1, keepdims=True)
            self.center[self.rows(i), :] = center
            self.inverse[self.rows(i), :] = lax.rsqrt(spread + EPSILON)

        self.loop(self.tiles, step)

    def normed(self, i):
        x = self.in_seq(self.xa, i).astype(jnp.float32)
        return (x - self.center[self.rows(i), :]) * self.inverse[self.rows(i), :]

    def activations(self):
        gain_one, shift_one, gain_two, shift_two = (self.wide(j) for j in (1, 2, 3, 4))

        def step(i):
            normed = self.normed(i)
            self.act_one[self.rows(i), :] = (normed * gain_one + shift_one).astype(jnp.bfloat16)
            self.act_two[self.rows(i), :] = (normed * gain_two + shift_two).astype(jnp.bfloat16)

        self.loop(self.tiles, step)

    def qkv_bias(self, rank):
        size = HD // 2
        held = self.b_qkv.shape[0] // size
        ranks = self.vec_in.shape[0]
        pieces = []
        for i in range(3 * LANES // size):
            part, j, half = i // 4, i // 2 % 2, i % 2
            head = (rank % 2 * 2 + j) * 4 + rank // 2
            index = part * (self.width // size) + head * 2 + half
            owner, spot = index // held, index % held
            row = self.va[owner // ranks, pl.ds(16 + owner % ranks, 1), :]
            pieces.append(
                sum(
                    jnp.where(spot == k, row[:, k * size : (k + 1) * size], 0.0)
                    for k in range(held)
                )
            )
        return jnp.concatenate(pieces, axis=1)

    def up_bias(self, rank):
        return jnp.concatenate(
            [self.va[b, pl.ds(24 + rank, 1), :] for b in range(self.va.shape[0])], axis=1
        )

    def project(self, rank):
        bias = self.qkv_bias(rank)

        def step(i):
            weight = self.wq[...].reshape(self.width, 3 * LANES)
            qkv = dot_nn(self.act_one[self.rows(i), :], weight) + bias
            rows = pl.ds(pl.multiple_of(i % self.per_seq * TILE, TILE), TILE)
            query = turn(qkv[:, :LANES], self.tables, rows, 1.0).astype(jnp.bfloat16)
            self.query[self.rows(i), :] = query * jnp.asarray(1.0 / math.sqrt(HD), jnp.bfloat16)
            self.key[self.rows(i), :] = turn(
                qkv[:, LANES : 2 * LANES], self.tables, rows, 1.0
            ).astype(jnp.bfloat16)
            self.value[self.rows(i), :] = qkv[:, 2 * LANES :].astype(jnp.bfloat16)

        self.loop(self.tiles, step)

    def keys(self, seq, block):
        start = pl.multiple_of(seq * self.length, TILE)
        return pl.ds(start, (block + 1) * TILE)

    def attend(self):
        def step(seq):
            for block in range(self.per_seq):
                rows = self.rows(seq * self.per_seq + block)
                keys = self.keys(seq, block)
                key, value, query = self.key[keys, :], self.value[keys, :], self.query[rows, :]
                out = None
                for head in range(self.heads):
                    scores = dot_nt(of_head(query, head), key)
                    at = lax.broadcasted_iota(jnp.int32, scores.shape, 0) + block * TILE
                    to = lax.broadcasted_iota(jnp.int32, scores.shape, 1)
                    scores = jnp.where(to <= at, scores, -jnp.inf)
                    top = jnp.max(scores, axis=1, keepdims=True)
                    weight = jnp.exp(scores - top)
                    weight = weight * (1.0 / jnp.sum(weight, axis=1, keepdims=True))
                    self.probs[block][seq * self.heads + head] = weight
                    part = dot_nn(weight.astype(jnp.bfloat16), value)
                    out = of_head(part, head) if out is None else out + of_head(part, head)
                self.attn[rows, :] = out.astype(jnp.bfloat16)

        self.loop(self.seqs, step)

    def attend_out_grad(self):
        def step(i):
            weight = self.wo2[...].reshape(LANES, self.width)
            self.attn_grad[self.rows(i), :] = dot_nt(self.in_seq(self.ca, i), weight).astype(
                jnp.bfloat16
            )

        self.loop(self.tiles, step)

    def attend_grad(self, seq):
        key_grad, value_grad = [None] * self.per_seq, [None] * self.per_seq
        start = seq * self.per_seq
        for block in range(self.per_seq):
            rows = self.rows(start + block)
            keys = self.keys(seq, block)
            key, value, query = self.key[keys, :], self.value[keys, :], self.query[rows, :]
            grad = self.attn_grad[rows, :]
            inner = grad.astype(jnp.float32) * self.attn[rows, :].astype(jnp.float32)
            query_grad = None
            for head in range(self.heads):
                own_grad = of_head(grad, head)
                delta = jnp.sum(of_head(inner, head), axis=1, keepdims=True)
                probs = self.probs[block][seq * self.heads + head]
                grad_prob = dot_nt(own_grad, value)
                grad_score = (probs * (grad_prob - delta)).astype(jnp.bfloat16)
                part = dot_nn(grad_score, of_head(key, head))
                query_grad = part if query_grad is None else query_grad + part
                key_part = dot_tn(grad_score, of_head(query, head))
                value_part = dot_tn(probs.astype(jnp.bfloat16), own_grad)
                for b in range(block + 1):
                    cut = slice(b * TILE, (b + 1) * TILE)
                    key_grad[b] = key_part[cut] if key_grad[b] is None else key_grad[b] + key_part[cut]
                    value_grad[b] = (
                        value_part[cut] if value_grad[b] is None else value_grad[b] + value_part[cut]
                    )
            back = pl.ds(block * TILE, TILE)
            self.qkv_grad[rows, :LANES] = turn(
                query_grad * (1.0 / math.sqrt(HD)), self.tables, back, -1.0
            ).astype(jnp.bfloat16)
        for block in range(self.per_seq):
            rows = self.rows(start + block)
            back = pl.ds(block * TILE, TILE)
            self.qkv_grad[rows, LANES : 2 * LANES] = turn(
                key_grad[block], self.tables, back, -1.0
            ).astype(jnp.bfloat16)
            self.qkv_grad[rows, 2 * LANES :] = value_grad[block].astype(jnp.bfloat16)

    def attend_grads(self):
        self.loop(self.seqs, self.attend_grad)

    def cot_flat(self):
        return self.ca[...].reshape(self.seqs * self.length, self.width)

    def qkv_weight_grad(self, i):
        rows = self.gq.shape[1]
        act = self.act_one[:, pl.ds(pl.multiple_of(i * rows, rows), rows)]
        self.gq[i] = dot_tn(act, self.qkv_grad[...]).astype(jnp.bfloat16)

    def dense_weight_grad(self):
        self.go[...] = (
            dot_tn(self.attn[...], self.cot_flat()).astype(jnp.bfloat16).reshape(self.go.shape)
        )

    def expand(self, rank):
        bias = self.up_bias(rank)

        def step(i):
            weight = self.wu[...].reshape(self.width, self.hidden)
            pre = dot_nn(self.act_two[self.rows(i), :], weight) + bias
            cdf = 0.5 * (1.0 + lax.erf(pre * INV_ROOT_TWO))
            self.gelu[self.rows(i), :] = (pre * cdf).astype(jnp.bfloat16)
            self.slope[self.rows(i), :] = cdf + pre * jnp.exp(-0.5 * pre * pre) * INV_ROOT_TWO_PI

        self.loop(self.tiles, step)

    def down_weight_grad(self, i):
        depth = self.gd.shape[1]
        part = self.gelu[:, pl.ds(pl.multiple_of(i * depth, depth), depth)]
        self.gd[i] = dot_tn(part, self.cot_flat()).astype(jnp.bfloat16)

    def hidden_grad(self):
        def step(i):
            weight = self.wd[...].reshape(self.hidden, self.width)
            grad = dot_nt(self.in_seq(self.ca, i), weight)
            self.pre_grad[self.rows(i), :] = (grad * self.slope[self.rows(i), :]).astype(
                jnp.bfloat16
            )

        self.loop(self.tiles, step)

    def up_weight_grad(self, i):
        rows = self.gu.shape[1]
        act = self.act_two[:, pl.ds(pl.multiple_of(i * rows, rows), rows)]
        self.gu[i] = dot_tn(act, self.pre_grad[...]).astype(jnp.bfloat16)

    def put_terms(self, terms, i, value):
        seq, chips, cores, rows, width = terms.shape
        n = TILE // (cores * rows)
        terms[i // self.per_seq, pl.ds(i % self.per_seq * n, n)] = value.astype(
            jnp.bfloat16
        ).reshape(n, cores, rows, width)

    def out_terms(self):
        def step(i):
            dense = self.wo2[...].reshape(LANES, self.width)
            down = self.wd[...].reshape(self.hidden, self.width)
            self.put_terms(
                self.po,
                i,
                dot_nn(self.attn[self.rows(i), :], dense) + dot_nn(self.gelu[self.rows(i), :], down),
            )

        self.loop(self.tiles, step)

    def in_terms(self):
        gain_one, gain_two = self.wide(1), self.wide(3)
        self.sums[...] = jnp.zeros_like(self.sums)

        def step(i):
            normed = self.normed(i)
            weight = self.wq[...].reshape(self.width, 3 * LANES)
            one = dot_nt(self.qkv_grad[self.rows(i), :], weight)
            weight = self.wu[...].reshape(self.width, self.hidden)
            two = dot_nt(self.pre_grad[self.rows(i), :], weight)
            self.put_terms(self.pg, i, one * gain_one + two * gain_two)
            for j, value in enumerate((one * normed, one, two * normed, two)):
                self.sums[j : j + 1, :] += total_rows(value)

        self.loop(self.tiles, step)

    def own_rows(self, ref, rank):
        rows = self.out.shape[1]
        return ref[:, pl.ds(pl.multiple_of(rank * rows, rows), rows), :].astype(jnp.float32)

    def small_terms(self, rank):
        ranks = self.sm.shape[0]
        cot = total_rows(jnp.sum(self.own_rows(self.ca, rank), axis=0))
        for to in range(ranks):
            cut = slice(to * LANES, (to + 1) * LANES)
            self.sm[to, 0:1, :] = cot[:, cut]
            self.sm[to, 1:5, :] = self.sums[0:4, cut]

    def small_plane(self, slot):
        total = jnp.sum(self.sm_in[...], axis=0)
        self.vz[slot, 0:8, :] = total
        qkv = total_rows(self.qkv_grad[...].astype(jnp.float32))
        pre = total_rows(self.pre_grad[...].astype(jnp.float32))
        for j in range(3):
            self.vz[slot, 8 + j : 9 + j, :] = qkv[:, j * LANES : (j + 1) * LANES]
        for j in range(self.hidden // LANES):
            self.vz[slot, 12 + j : 13 + j, :] = pre[:, j * LANES : (j + 1) * LANES]

    def result(self, rank, out_sum, in_sum):
        x = self.own_rows(self.xa, rank)
        center = jnp.mean(x, axis=2, keepdims=True)
        shifted = x - center
        inverse = lax.rsqrt(jnp.mean(shifted * shifted, axis=2, keepdims=True) + EPSILON)
        normed = shifted * inverse
        bias = (self.wide(0) + self.wide(5))[None]
        self.out[...] = (x + out_sum + bias).astype(jnp.bfloat16)
        self.in_grad[...] = self.own_rows(self.ca, rank) + inverse * (
            in_sum
            - jnp.mean(in_sum, axis=2, keepdims=True)
            - normed * jnp.mean(in_sum * normed, axis=2, keepdims=True)
        )


LAYER_SLOTS = 4 * 8 + 4 + 12 * 8 + 10 * 8 + 2
NEAR_SLOTS = 24


def layer_kernel(names, planes, *refs):
    refs = dict(zip(names, refs))
    send, recv, near = (refs.pop(name) for name in names[-3:])
    refs.update(
        tables=tuple(refs["table"].at[i] for i in range(3)),
        probs=tuple(refs[name] for name in names if name.startswith("probs")),
        vectors=tuple(refs[name] for name in names if name.startswith("vector")),
        hidden=refs["gelu"].shape[1],
    )
    do = Layer(refs)
    at = Place(planes)
    mail = Mail(send, recv, near)
    b, c = at.b, at.c
    rows = do.wq_s.shape[1]
    pair = planes // 2

    def strip(whole):
        return lambda rank: whole.at[b, pl.ds(pl.multiple_of(rank * rows, rows), rows), :]

    def band(whole):
        return lambda rank: whole.at[pl.ds(pl.multiple_of(rank * rows, rows), rows), :]

    def up_pieces(rank):
        return [
            do.wu_s.at[:, pl.ds(pl.multiple_of((p * 8 + rank) * LANES, LANES), LANES)]
            for p in range(planes)
        ]

    def up_landings(rank):
        strip_rows = pl.ds(pl.multiple_of(rank * rows, rows), rows)
        return [do.wu.at[b, strip_rows, pl.ds(p * LANES, LANES)] for p in range(planes)]

    gather_x = PlaneGather(at, mail, do.x_own, do.xa)
    gather_c = PlaneGather(at, mail, do.cot_own, do.ca)
    line_v, line_o = StarGather(at, mail, do.va), LineGather(at, mail, do.wo)
    line_q = LineGather(at, mail, do.wq)
    half = do.wu.shape[1] // 2
    line_ua = LineGather(at, mail, do.wu, 0, half)
    line_ub = LineGather(at, mail, do.wu, half, half)
    half = do.wd.shape[1] // 2
    line_da = LineGather(at, mail, do.wd, 0, half)
    line_db = LineGather(at, mail, do.wd, half, half)
    ex_v = PlaneExchange(at, mail, lambda rank: do.vec_s, lambda rank: do.vec_in.at[rank])
    ex_q = PlaneExchange(at, mail, lambda rank: do.wq_s.at[rank], strip(do.wq))
    ex_u = PlaneExchange(at, mail, up_pieces, up_landings, planes)
    mine = do.wo2.at[:, c]
    swap_w = PairExchange(
        at, mail, do.wo.at[pl.ds(pair * (1 - c), pair)], mine, do.wo2.at[:, 1 - c]
    )
    sum_o = LineReduce(at, mail, do.go4, do.above_o, do.below_o)
    sum_q = LineReduce(at, mail, do.gq, do.above_q, do.below_q)
    sum_u = LineReduce(at, mail, do.gu, do.above_u, do.below_u)
    sum_d = LineReduce(at, mail, do.gd, do.above_d, do.below_d)
    swap_g = PairExchange(
        at,
        mail,
        do.go.at[:, 1 - c],
        do.go4.at[pl.ds(pair * c, pair)],
        do.go4.at[pl.ds(pair * (1 - c), pair)],
    )
    back_q = PlaneExchange(at, mail, band(do.fq), lambda rank: do.dq.at[rank])
    back_u = PlaneExchange(at, mail, band(do.fu), lambda rank: do.du.at[rank])
    fold_v = PlaneExchange(at, mail, lambda rank: do.sm.at[rank], lambda rank: do.sm_in.at[rank])
    line_s = StarGather(at, mail, do.vz)
    share_v = PlaneExchange(at, mail, lambda rank: do.vt, lambda rank: do.dv.at[rank])
    plane_o = PlaneReduce(at, mail, do.po, do.pairs_o, do.sums_o, do.side_o)
    plane_g = PlaneReduce(at, mail, do.pg, do.pairs_g, do.sums_g, do.side_g)

    slots = [s + b // pair * (planes - 1 - 2 * s) for s in (3, 0, 2, 1)]

    at.barrier()
    line_o.start(do.wo_s)
    own_o = mail.bring(do.wo_s, do.wo.at[b])
    ex_u.start()
    line_da.start(do.wd_s)
    own_d = mail.bring(do.wd_s, do.wd.at[b])
    do.own_vectors(at.t)
    ex_v.start()
    gather_x.start()
    line_o.take(1)
    ex_u.finish()
    line_ua.start()
    ex_v.finish()
    do.plane_vectors(b)
    line_v.start()
    own_raw = mail.bring(do.wq_in, do.wq_raw)
    line_ub.start()
    gather_x.relay_x()
    own_raw.wait()
    do.sort_weight()
    ex_q.start()
    own_o.wait()
    gather_x.relay_y()
    line_ua.take(1)
    gather_x.share()
    gather_c.start()
    line_ub.take(1)
    line_v.finish()
    gather_x.far()
    line_ua.take(2)
    gather_x.finish()
    do.statistics()
    do.activations()
    line_ub.take(2)
    own_table = mail.bring(do.table_in, do.table)
    line_ua.take(3)
    ex_q.finish()
    line_q.start()
    gather_c.relay_y()
    gather_c.relay_x()
    gather_c.share()
    line_ub.take(3)
    do.expand(at.t)
    line_o.take(2)
    gather_c.far()
    gather_c.finish()
    line_q.take(1)
    do.down_weight_grad(slots[0])
    sum_d.edge(slots[0])
    own_table.wait()
    do.down_weight_grad(slots[1])
    sum_d.edge(slots[1])
    line_o.take(3)
    swap_w.start()
    mine[...] = do.wo[pl.ds(pair * c, pair)]
    swap_w.finish()
    do.attend_out_grad()
    line_q.take(2)
    line_db.start(do.wd_s)
    do.down_weight_grad(slots[2])
    sum_d.edge(slots[2])
    do.down_weight_grad(slots[3])
    sum_d.edge(slots[3])
    own_d.wait()
    line_da.take(1)
    line_q.take(3)
    do.project(at.t)
    do.attend()
    do.dense_weight_grad()
    swap_g.start()
    do.go4[pl.ds(pair * c, pair)] = do.go[:, c]
    line_db.take(1)
    do.attend_grads()
    do.qkv_weight_grad(slots[0])
    sum_q.edge(slots[0])
    do.qkv_weight_grad(slots[1])
    sum_q.edge(slots[1])
    line_db.take(2)
    line_db.take(3)
    do.qkv_weight_grad(slots[2])
    sum_q.edge(slots[2])
    sum_d.hop(1, 0)
    line_da.take(2)
    line_da.take(3)
    do.out_terms()
    plane_o.start()
    do.hidden_grad()
    do.up_weight_grad(slots[0])
    sum_u.edge(slots[0])
    plane_o.fold()
    sum_d.hop(1, 1)
    do.up_weight_grad(slots[1])
    sum_u.edge(slots[1])
    do.up_weight_grad(slots[2])
    sum_u.edge(slots[2])
    do.qkv_weight_grad(slots[3])
    sum_q.edge(slots[3])
    do.up_weight_grad(slots[3])
    sum_u.edge(slots[3])
    sum_q.hop(1, 0)
    plane_o.turn()
    do.in_terms()
    plane_g.start()
    sum_q.hop(1, 1)
    sum_d.hop(2, 0)
    sum_u.hop(1, 0)
    sum_q.hop(2, 0)
    plane_g.fold()
    sum_d.finish(do.dd)
    out_d = mail.bring(do.dd, do.dd_to)
    do.small_terms(at.t)
    fold_v.start()
    plane_g.turn()
    sum_u.hop(1, 1)
    sum_u.hop(2, 0)
    fold_v.finish()
    do.small_plane(b)
    line_s.start()
    sum_q.finish(do.fq)
    back_q.start()
    swap_g.finish()
    for slot in slots:
        sum_o.edge(slot)
    sum_u.finish(do.fu)
    back_u.start()
    sum_o.hop(1, 0)
    line_s.finish()
    sum_o.hop(1, 1)
    do.vt[...] = jnp.sum(do.vz[...], axis=0)
    share_v.start()
    back_q.finish()
    sum_o.hop(2, 0)
    do.result(at.t, plane_o.finish(), plane_g.finish())
    out_x = mail.bring(do.out, do.out_to)
    out_g = mail.bring(do.in_grad, do.in_grad_to)
    back_u.finish()
    share_v.finish()
    sum_o.finish(do.dd_o)
    out_o = mail.bring(do.dd_o, do.dd_o_to)
    for copied in (out_o, out_d, out_x, out_g):
        copied.wait()
    mail.close()
    for line in (line_v, line_o, line_q, line_ua, line_ub, line_da, line_db, line_s, sum_o, sum_q, sum_u, sum_d):
        line.close()


def finish_kernel(names, planes, *refs):
    do = Layer(dict(zip(names, refs)))
    at = Place(planes)
    ranks, rows = do.dq.shape[:2]
    lane = lax.broadcasted_iota(jnp.int32, (rows, LANES), 1)
    low = lane < HD
    for part in range(3):
        for core in range(2):
            for pair in range(ranks // 4):
                near, far = (
                    do.dq[2 * (2 * pair + i) + core, :, part * LANES : (part + 1) * LANES].astype(
                        jnp.float32
                    )
                    for i in range(2)
                )
                for j in range(2):
                    both = (
                        jnp.where(low, near, pltpu.roll(far, HD, 1))
                        if j == 0
                        else jnp.where(low, pltpu.roll(near, HD, 1), far)
                    )
                    first = (part * 4 + core * 2 + j) * ranks // 2 * HD + pair * LANES
                    do.qkv_out[:, first : first + LANES] = both
    for rank in range(ranks):
        for b in range(planes):
            first = (b * ranks + rank) * LANES
            do.up_out[:, first : first + LANES] = do.du[
                rank, :, b * LANES : (b + 1) * LANES
            ].astype(jnp.float32)
    do.down_out[...] = do.dd[...]
    do.dense_out[...] = do.dd_o[...]
    for seq in range(do.out.shape[0]):
        do.in_grad_out[:, seq, :] = do.in_grad[seq]
        do.out_out[:, seq, :] = do.out[seq]
    piece = lax.rem(at.t, 4)
    row = (at.b * ranks + at.t) // 4
    values = do.dv[pl.ds(row, 1), 0:8, :].reshape(8, LANES)
    front = jnp.zeros((8, rows), jnp.float32)
    for i in range(4):
        cut = values[:, i * rows : (i + 1) * rows]
        front = front + jnp.where(piece == i, cut, jnp.zeros_like(cut))
    for j, ref in enumerate(
        (do.dense_bias, do.gain_one, do.shift_one, do.gain_two, do.shift_two)
    ):
        ref[...] = front[j].reshape(rows)
    do.down_bias[...] = front[0].reshape(rows)
    do.up_bias[...] = do.dv[pl.ds(at.t, 1), pl.ds(12 + at.b, 1), :].reshape(LANES)
    pieces = []
    for i in range(3):
        index = (at.b * ranks + at.t) * 3 + i
        part, inner = index // 32, lax.rem(index, 32)
        head, half = inner // 2, lax.rem(inner, 2)
        core, j, chip = head // 8, lax.rem(head // 4, 2), lax.rem(head, 4)
        value = do.dv[pl.ds(chip * 2 + core, 1), pl.ds(8 + part, 1), :].reshape(1, LANES)
        spot = 2 * j + half
        total = jnp.zeros((1, rows), jnp.float32)
        for k in range(4):
            cut = value[:, k * rows : (k + 1) * rows]
            total = total + jnp.where(spot == k, cut, jnp.zeros_like(cut))
        pieces.append(total)
    do.qkv_bias[...] = jnp.concatenate(pieces, axis=1).reshape(3 * rows)


VMEM = pl.BlockSpec(memory_space=pltpu.VMEM)


def rotary_rows(length):
    half = HD // 8
    frequency = 1.0 / 10000.0 ** (np.arange(half) * (1.0 / half))
    angles = np.arange(length)[:, None] * frequency[None, :]
    table = np.zeros((3, length, HD))
    table[0] = 1.0
    table[0, :, :half] = table[0, :, half : 2 * half] = np.cos(angles)
    table[1, :, :half] = -np.sin(angles)
    table[2, :, half : 2 * half] = np.sin(angles)
    return np.tile(table, (1, 1, LANES // HD)).astype(np.float32)


def body(shape, *operands):
    residual_in, qkv_weight, down_weight = operands[0], operands[1], operands[11]
    planes = shape[BATCH]
    ranks = shape[ULY] * shape[BLK]
    tok_rows, seqs, width = residual_in.shape
    fits = (
        (shape[ULY], shape[BLK]) == (2, 4)
        and planes == 4
        and seqs % 2 == 0
        and 2 * qkv_weight.shape[0] == HD
        and width == ranks * LANES
        and ranks * tok_rows % TILE == 0
        and TILE % (2 * tok_rows) == 0
        and down_weight.shape[0] == LANES
    )
    return fast_body(planes, *operands) if fits else general_body(*operands)


def fast_body(
    planes,
    residual_in,
    qkv_weight,
    qkv_bias,
    dense_weight,
    dense_bias,
    norm1_gain,
    norm1_bias,
    norm2_gain,
    norm2_bias,
    up_weight,
    up_bias,
    down_weight,
    down_bias,
    cotangent,
):
    single = jnp.float32
    half_type = jnp.bfloat16
    tok_rows, seqs, width = residual_in.shape
    ranks = width // LANES
    rows = qkv_weight.shape[0]
    depth = down_weight.shape[0]
    hidden = planes * depth
    pair = planes // 2
    length = ranks * tok_rows
    tokens = seqs * length
    rank = lax.axis_index(ULY) * lax.axis_size(BLK) + lax.axis_index(BLK)
    owner = lax.axis_index(BATCH) * ranks + rank

    anywhere = pl.BlockSpec(memory_space=pl.ANY)
    inputs = dict(
        x_own=(jnp.transpose(residual_in, (1, 0, 2)), anywhere),
        cot_own=(jnp.transpose(cotangent, (1, 0, 2)), anywhere),
        wq_in=(qkv_weight, anywhere),
        wu_s=(up_weight, anywhere),
        wd_s=(down_weight, anywhere),
        wo_s=(dense_weight, anywhere),
        table_in=(jnp.asarray(rotary_rows(length)), anywhere),
        b_qkv=(qkv_bias, VMEM),
        b_up=(up_bias, VMEM),
    )
    for i, v in enumerate((dense_bias, norm1_gain, norm1_bias, norm2_gain, norm2_bias, down_bias)):
        inputs["vector%d" % i] = (v, VMEM)
    shard = (seqs, tok_rows, width)
    outputs = dict(
        out_to=(shard, half_type),
        in_grad_to=(shard, single),
        dq=((ranks, rows, 3 * LANES), half_type),
        du=((ranks, rows, hidden), half_type),
        dd_to=((depth, width), single),
        dd_o_to=((rows, width), single),
        dv=((ranks, 16, LANES), single),
    )
    q_shape = (planes, ranks * rows, 3 * LANES)
    u_shape = (planes, ranks * rows, hidden)
    d_shape = (planes, depth, width)
    o_shape = (planes, rows, width)
    chips = ranks // 2
    scratch = dict(
        xa=((seqs, length, width), half_type),
        ca=((seqs, length, width), half_type),
        wq=(q_shape, half_type),
        wu=(u_shape, half_type),
        wd=(d_shape, half_type),
        wo=(o_shape, half_type),
        wo2=((pair, 2, rows, width), half_type),
        wq_raw=(qkv_weight.shape, half_type),
        wq_s=((ranks, rows, 3 * LANES), half_type),
        table=((3, length, LANES), single),
        out=(shard, half_type),
        in_grad=(shard, single),
        dd=((depth, width), single),
        dd_o=((rows, width), single),
        vec_s=((16, LANES), single),
        vec_in=((ranks, 16, LANES), single),
        va=((planes, 32, LANES), single),
        center=((tokens, 1), single),
        inverse=((tokens, 1), single),
        act_one=((tokens, width), half_type),
        act_two=((tokens, width), half_type),
        query=((tokens, LANES), half_type),
        key=((tokens, LANES), half_type),
        value=((tokens, LANES), half_type),
        attn=((tokens, LANES), half_type),
        attn_grad=((tokens, LANES), half_type),
        qkv_grad=((tokens, 3 * LANES), half_type),
        gelu=((tokens, hidden), half_type),
        slope=((tokens, hidden), single),
        pre_grad=((tokens, hidden), half_type),
        gq=(q_shape, half_type),
        gu=(u_shape, half_type),
        gd=(d_shape, half_type),
        go=((pair, 2, rows, width), half_type),
        go4=(o_shape, half_type),
        above_q=(q_shape, half_type),
        below_q=(q_shape, half_type),
        above_u=(u_shape, half_type),
        below_u=(u_shape, half_type),
        above_d=(d_shape, half_type),
        below_d=(d_shape, half_type),
        above_o=(o_shape, half_type),
        below_o=(o_shape, half_type),
        fq=(q_shape[1:], half_type),
        fu=(u_shape[1:], half_type),
        po=((seqs, chips, 2, tok_rows, width), half_type),
        pg=((seqs, chips, 2, tok_rows, width), half_type),
        pairs_o=((seqs, chips, tok_rows, width), half_type),
        pairs_g=((seqs, chips, tok_rows, width), half_type),
        sums_o=((seqs, chips, tok_rows, width), half_type),
        sums_g=((seqs, chips, tok_rows, width), half_type),
        side_o=((3,) + shard, half_type),
        side_g=((3,) + shard, half_type),
        sums=((8, width), single),
        sm=((ranks, 8, LANES), single),
        sm_in=((ranks, 8, LANES), single),
        vz=((planes, 16, LANES), single),
        vt=((16, LANES), single),
    )
    for block in range(length // TILE):
        scratch["probs%d" % block] = ((seqs * LANES // HD, TILE, (block + 1) * TILE), single)
    names = tuple(inputs) + tuple(outputs) + tuple(scratch) + ("send", "recv", "near")
    out, in_grad, dq, du, dd, dd_o, dv = pl.pallas_call(
        functools.partial(layer_kernel, names, planes),
        out_shape=[jax.ShapeDtypeStruct(*what) for what in outputs.values()],
        in_specs=[where for _, where in inputs.values()],
        out_specs=[anywhere] * len(outputs),
        scratch_shapes=[pltpu.VMEM(*what) for what in scratch.values()]
        + [pltpu.SemaphoreType.DMA((n,)) for n in (LAYER_SLOTS, LAYER_SLOTS, NEAR_SLOTS)],
        compiler_params=pltpu.CompilerParams(
            collective_id=0, has_side_effects=True, vmem_limit_bytes=60 * 2**20
        ),
    )(*(value for value, _ in inputs.values()))

    results = dict(
        out_out=(residual_in.shape, half_type),
        in_grad_out=(residual_in.shape, single),
        qkv_out=(qkv_weight.shape, single),
        qkv_bias=(qkv_bias.shape, single),
        dense_out=(dense_weight.shape, single),
        dense_bias=(dense_bias.shape, single),
        gain_one=(norm1_gain.shape, single),
        shift_one=(norm1_bias.shape, single),
        gain_two=(norm2_gain.shape, single),
        shift_two=(norm2_bias.shape, single),
        up_out=(up_weight.shape, single),
        up_bias=(up_bias.shape, single),
        down_out=(down_weight.shape, single),
        down_bias=(down_bias.shape, single),
    )
    return tuple(
        pl.pallas_call(
            functools.partial(
                finish_kernel, tuple(n.removesuffix("_to") for n in outputs) + tuple(results), planes
            ),
            out_shape=[jax.ShapeDtypeStruct(*what) for what in results.values()],
            in_specs=[VMEM] * len(outputs),
            out_specs=[VMEM] * len(results),
        )(out, in_grad, dq, du, dd, dd_o, dv)
    )


def solution(mesh):
    placed = (
        P(TOKENS, BATCH, None),
        P(AXES, None),
        P(AXES),
        P(AXES, None),
        P(AXES),
        P(AXES),
        P(AXES),
        P(AXES),
        P(AXES),
        P(AXES, None),
        P(AXES),
        P(AXES, None),
        P(AXES),
        P(TOKENS, BATCH, None),
    )
    return jax.shard_map(
        functools.partial(body, dict(mesh.shape)),
        mesh=mesh,
        in_specs=placed,
        out_specs=(
            P(TOKENS, BATCH, None),
            P(TOKENS, BATCH, None),
            P(AXES, None),
            P(AXES),
            P(AXES, None),
            P(AXES),
            P(AXES),
            P(AXES),
            P(AXES),
            P(AXES),
            P(AXES, None),
            P(AXES),
            P(AXES, None),
            P(AXES),
        ),
        check_vma=False,
    )
```

```python
import functools
import math

import jax
import jax.numpy as jnp
import numpy as np
from jax import lax
from jax.experimental import pallas as pl
from jax.experimental.pallas import tpu as pltpu
from jax.sharding import PartitionSpec as P

HD = 64
BATCH, ULY, BLK = "batch", "ulysses", "blk"
AXES = (BATCH, ULY, BLK)
TOKENS = (ULY, BLK)


EPSILON = 1e-05
INV_ROOT_TWO = 0.7071067811865476
INV_ROOT_TWO_PI = 0.3989422804014327


def layer_norm(values):
    center = jnp.mean(values, axis=-1, keepdims=True)
    shifted = values - center
    inverse = lax.rsqrt(jnp.mean(shifted * shifted, axis=-1, keepdims=True) + EPSILON)
    return (shifted * inverse, inverse)


def norm_back(gradient, normed, inverse, gain_vec):
    scaled = gradient * gain_vec
    return inverse * (
        scaled
        - jnp.mean(scaled, axis=-1, keepdims=True)
        - normed * jnp.mean(scaled * normed, axis=-1, keepdims=True)
    )


def gelu_value(pre_values):
    return 0.5 * pre_values * (1.0 + jax.scipy.special.erf(pre_values * INV_ROOT_TWO))


def gelu_slope(pre_values):
    normal_cdf = 0.5 * (1.0 + jax.scipy.special.erf(pre_values * INV_ROOT_TWO))
    return normal_cdf + pre_values * jnp.exp(-0.5 * pre_values * pre_values) * INV_ROOT_TWO_PI


def rotary_tables(positions, rotary):
    half_rot = rotary // 2
    frequency = 1.0 / 10000.0 ** (jnp.arange(half_rot, dtype=jnp.float32) * (2.0 / rotary))
    angles = positions.astype(jnp.float32)[:, None] * frequency[None, :]
    cosine = jnp.concatenate([jnp.cos(angles), jnp.cos(angles)], axis=-1)
    sine_table = jnp.concatenate([jnp.sin(angles), jnp.sin(angles)], axis=-1)
    return (cosine, sine_table)


def expand_table(table, tensor):
    extra_dims = (1,) * (tensor.ndim - 2)
    return table.reshape((table.shape[0],) + extra_dims + (table.shape[1],))


def rotate_fwd(tensor, cosine, sine_table, rotary):
    half_rot = rotary // 2
    cos_full = expand_table(cosine, tensor)
    sin_full = expand_table(sine_table, tensor)
    rot_part = tensor[..., :rotary]
    turned = jnp.concatenate([-rot_part[..., half_rot:], rot_part[..., :half_rot]], axis=-1)
    return jnp.concatenate([rot_part * cos_full + turned * sin_full, tensor[..., rotary:]], axis=-1)


def rotate_back(tensor, cosine, sine_table, rotary):
    half_rot = rotary // 2
    cos_full = expand_table(cosine, tensor)
    sin_full = expand_table(sine_table, tensor)
    rot_part = tensor[..., :rotary]
    weighted = rot_part * sin_full
    turned = jnp.concatenate([weighted[..., half_rot:], -weighted[..., :half_rot]], axis=-1)
    return jnp.concatenate([rot_part * cos_full + turned, tensor[..., rotary:]], axis=-1)


def general_body(
    residual_in,
    qkv_weight,
    qkv_bias,
    dense_weight,
    dense_bias,
    norm1_gain,
    norm1_bias,
    norm2_gain,
    norm2_bias,
    up_weight,
    up_bias,
    down_weight,
    down_bias,
    cotangent,
):
    single = jnp.float32
    half_type = jnp.bfloat16
    gathered = (
        lax.all_gather(qkv_weight, AXES, axis=0, tiled=True),
        lax.all_gather(qkv_bias, AXES, axis=0, tiled=True),
        lax.all_gather(dense_weight, AXES, axis=0, tiled=True),
        lax.all_gather(dense_bias, AXES, axis=0, tiled=True),
        lax.all_gather(norm1_gain, AXES, axis=0, tiled=True),
        lax.all_gather(norm1_bias, AXES, axis=0, tiled=True),
        lax.all_gather(norm2_gain, AXES, axis=0, tiled=True),
        lax.all_gather(norm2_bias, AXES, axis=0, tiled=True),
        lax.all_gather(up_weight, AXES, axis=0, tiled=True),
        lax.all_gather(up_bias, AXES, axis=0, tiled=True),
        lax.all_gather(down_weight, AXES, axis=0, tiled=True),
        lax.all_gather(down_bias, AXES, axis=0, tiled=True),
    )
    (
        w_qkv,
        b_qkv,
        w_dense,
        b_dense,
        gain_one,
        shift_one,
        gain_two,
        shift_two,
        w_up,
        b_up,
        w_down,
        b_down,
    ) = gathered
    tok_rows = residual_in.shape[0]
    seq_count = residual_in.shape[1]
    model_width = residual_in.shape[2]
    head_count = model_width // HD
    rotary = HD // 4
    scale_factor = 1.0 / math.sqrt(HD)
    blk_size = lax.axis_size(BLK)
    uly_size = lax.axis_size(ULY)
    blk_index = lax.axis_index(BLK)
    block_id = lax.axis_index(ULY) * blk_size + blk_index
    seq_pos = block_id * tok_rows + jnp.arange(tok_rows, dtype=jnp.int32)
    inputs_f = residual_in.astype(single)
    normed, inverse = layer_norm(inputs_f)
    act_one = (normed * gain_one.astype(single) + shift_one.astype(single)).astype(half_type)
    act_two = (normed * gain_two.astype(single) + shift_two.astype(single)).astype(half_type)
    qkv_full = jnp.einsum(
        "tsd,df->tsf", act_one, w_qkv, preferred_element_type=single
    ) + b_qkv.astype(single)
    cos_seq, sin_seq = rotary_tables(seq_pos, rotary)
    head_shape = (tok_rows, seq_count, head_count, HD)
    query_seq = (
        rotate_fwd(qkv_full[..., :model_width].reshape(head_shape), cos_seq, sin_seq, rotary)
        .reshape(tok_rows, seq_count, model_width)
        .astype(half_type)
    )
    key_seq = (
        rotate_fwd(
            qkv_full[..., model_width : 2 * model_width].reshape(head_shape),
            cos_seq,
            sin_seq,
            rotary,
        )
        .reshape(tok_rows, seq_count, model_width)
        .astype(half_type)
    )
    value_seq = qkv_full[..., 2 * model_width :].astype(half_type)
    query_loc, key_loc, value_loc = (
        lax.all_to_all(query_seq, ULY, split_axis=2, concat_axis=0, tiled=True),
        lax.all_to_all(key_seq, ULY, split_axis=2, concat_axis=0, tiled=True),
        lax.all_to_all(value_seq, ULY, split_axis=2, concat_axis=0, tiled=True),
    )
    local_rows = query_loc.shape[0]
    features = query_loc.shape[2]
    local_heads = features // HD
    key_all, value_all = (
        lax.all_gather(key_loc, BLK, axis=0, tiled=True),
        lax.all_gather(value_loc, BLK, axis=0, tiled=True),
    )
    total_rows = key_all.shape[0]
    row_ids = jnp.arange(local_rows, dtype=jnp.int32)
    query_pos = (row_ids // tok_rows * blk_size + blk_index) * tok_rows + row_ids % tok_rows
    block_rows = math.gcd(512, local_rows)
    n_blocks = local_rows // block_rows
    query_h = query_loc.reshape(local_rows, seq_count, local_heads, HD)
    key_h = jnp.transpose(
        key_all.reshape(blk_size, uly_size, tok_rows, seq_count, features), (1, 0, 2, 3, 4)
    ).reshape(total_rows, seq_count, local_heads, HD)
    value_h = jnp.transpose(
        value_all.reshape(blk_size, uly_size, tok_rows, seq_count, features), (1, 0, 2, 3, 4)
    ).reshape(total_rows, seq_count, local_heads, HD)
    zero_idx = jnp.zeros((), jnp.int32)
    step_ids = jnp.arange(n_blocks * seq_count, dtype=jnp.int32)
    row_shape = (block_rows, 1, local_heads, HD)

    def select(step_index):
        row_start = step_index // seq_count * block_rows
        seq_index = step_index % seq_count
        query_rows = lax.dynamic_slice(
            query_h, (row_start, seq_index, zero_idx, zero_idx), row_shape
        )
        limit = jnp.max(query_pos) // block_rows + 1
        return (row_start, seq_index, query_rows, query_pos, limit)

    def block_scores(query_rows, row_pos, key_index, seq_index):
        key_start = key_index * block_rows
        slot = (key_start, seq_index, zero_idx, zero_idx)
        key_rows = lax.dynamic_slice(key_h, slot, (block_rows, 1, local_heads, HD))
        value_rows = lax.dynamic_slice(value_h, slot, (block_rows, 1, local_heads, HD))
        scores = (
            jnp.einsum("qshd,kshd->shqk", query_rows, key_rows, preferred_element_type=single)
            * scale_factor
        )
        key_ids = key_start + jnp.arange(block_rows, dtype=jnp.int32)
        allowed = (key_ids[None, :] <= row_pos[:, None])[None, None]
        return (jnp.where(allowed, scores, -jnp.inf), key_rows, value_rows, slot)

    def forward_block(step_index):
        row_start, seq_index, query_rows, row_pos, limit = select(step_index)

        def total_step(key_index, carry):
            running_max, running_sum = carry
            masked, key_rows, value_rows, slot = block_scores(
                query_rows, row_pos, key_index, seq_index
            )
            new_max = jnp.maximum(running_max, jnp.max(masked, axis=-1))
            new_sum = running_sum * jnp.exp(running_max - new_max) + jnp.sum(
                jnp.exp(masked - new_max[..., None]), axis=-1
            )
            return (new_max, new_sum)

        start_max = jnp.full((1, local_heads, block_rows), -jnp.inf, single)
        start_sum = jnp.zeros((1, local_heads, block_rows), single)
        final_max, final_sum = lax.fori_loop(zero_idx, limit, total_step, (start_max, start_sum))
        log_total = final_max + jnp.log(final_sum)

        def value_step(key_index, acc):
            masked, key_rows, value_rows, slot = block_scores(
                query_rows, row_pos, key_index, seq_index
            )
            weights_b = jnp.exp(masked - log_total[..., None]).astype(half_type)
            return acc + jnp.einsum(
                "shqk,kshd->qshd", weights_b, value_rows, preferred_element_type=single
            )

        result = lax.fori_loop(zero_idx, limit, value_step, jnp.zeros(row_shape, single)).astype(
            half_type
        )
        return (result[:, 0], log_total)

    results, log_totals = lax.map(forward_block, step_ids)
    attn_h = jnp.transpose(
        results.reshape(n_blocks, seq_count, block_rows, local_heads, HD), (0, 2, 1, 3, 4)
    ).reshape(local_rows, seq_count, local_heads, HD)
    attn_seq = lax.all_to_all(
        attn_h.reshape(local_rows, seq_count, features),
        ULY,
        split_axis=0,
        concat_axis=2,
        tiled=True,
    )
    proj_out = jnp.einsum(
        "tsd,de->tse", attn_seq, w_dense, preferred_element_type=single
    ) + b_dense.astype(single)
    pre_act = jnp.einsum("tsd,df->tsf", act_two, w_up, preferred_element_type=single) + b_up.astype(
        single
    )
    gelu_out = gelu_value(pre_act).astype(half_type)
    mlp_out = jnp.einsum(
        "tsf,fd->tsd", gelu_out, w_down, preferred_element_type=single
    ) + b_down.astype(single)
    output = (inputs_f + proj_out + mlp_out).astype(half_type)
    back_params = (
        lax.all_gather(qkv_weight, AXES, axis=0, tiled=True),
        lax.all_gather(qkv_bias, AXES, axis=0, tiled=True),
        lax.all_gather(dense_weight, AXES, axis=0, tiled=True),
        lax.all_gather(dense_bias, AXES, axis=0, tiled=True),
        lax.all_gather(norm1_gain, AXES, axis=0, tiled=True),
        lax.all_gather(norm1_bias, AXES, axis=0, tiled=True),
        lax.all_gather(norm2_gain, AXES, axis=0, tiled=True),
        lax.all_gather(norm2_bias, AXES, axis=0, tiled=True),
        lax.all_gather(up_weight, AXES, axis=0, tiled=True),
        lax.all_gather(up_bias, AXES, axis=0, tiled=True),
        lax.all_gather(down_weight, AXES, axis=0, tiled=True),
        lax.all_gather(down_bias, AXES, axis=0, tiled=True),
    )
    back_qkv = back_params[0]
    back_dense = back_params[2]
    back_gain_one = back_params[4].astype(single)
    back_gain_two = back_params[6].astype(single)
    back_up = back_params[8]
    back_down = back_params[10]
    grad_f = cotangent.astype(single)
    bias_sum = jnp.sum(grad_f, axis=(0, 1))
    down_w_grad = jnp.einsum("tsf,tsd->fd", gelu_out, cotangent, preferred_element_type=single)
    gelu_grad = jnp.einsum("tsd,fd->tsf", cotangent, back_down, preferred_element_type=single)
    pre_grad = (gelu_grad * gelu_slope(pre_act)).astype(half_type)
    up_w_grad = jnp.einsum("tsd,tsf->df", act_two, pre_grad, preferred_element_type=single)
    up_b_grad = jnp.sum(pre_grad.astype(single), axis=(0, 1))
    act_two_grad = jnp.einsum("tsf,df->tsd", pre_grad, back_up, preferred_element_type=single)
    gain_two_grad = jnp.sum(act_two_grad * normed, axis=(0, 1))
    shift_two_grad = jnp.sum(act_two_grad, axis=(0, 1))
    dense_w_grad = jnp.einsum("tsd,tse->de", attn_seq, cotangent, preferred_element_type=single)
    attn_grad = jnp.einsum(
        "tse,de->tsd", cotangent, back_dense, preferred_element_type=single
    ).astype(half_type)
    grad_loc = lax.all_to_all(attn_grad, ULY, split_axis=2, concat_axis=0, tiled=True)
    grad_h = grad_loc.reshape(local_rows, seq_count, local_heads, HD)

    def backward_block(acc_pair, step_index):
        row_start, seq_index, query_rows, row_pos, limit = select(step_index)
        own_slot = (row_start, seq_index, zero_idx, zero_idx)
        out_rows = lax.dynamic_slice(attn_h, own_slot, row_shape)
        grad_rows = lax.dynamic_slice(grad_h, own_slot, row_shape)
        log_total = log_totals[step_index]
        delta_row = jnp.transpose(
            jnp.sum(grad_rows.astype(single) * out_rows.astype(single), axis=-1), (1, 2, 0)
        )

        def grad_step(key_index, carry):
            key_acc, value_acc, query_acc = carry
            masked, key_rows, value_rows, slot = block_scores(
                query_rows, row_pos, key_index, seq_index
            )
            probs_f = jnp.exp(masked - log_total[..., None])
            value_part = jnp.einsum(
                "shqk,qshd->kshd",
                probs_f.astype(half_type),
                grad_rows,
                preferred_element_type=single,
            )
            grad_prob = jnp.einsum(
                "qshd,kshd->shqk", grad_rows, value_rows, preferred_element_type=single
            )
            grad_score = (probs_f * (grad_prob - delta_row[..., None]) * scale_factor).astype(
                half_type
            )
            query_acc = query_acc + jnp.einsum(
                "shqk,kshd->qshd", grad_score, key_rows, preferred_element_type=single
            )
            key_part = jnp.einsum(
                "shqk,qshd->kshd", grad_score, query_rows, preferred_element_type=single
            )
            key_acc = lax.dynamic_update_slice(
                key_acc, lax.dynamic_slice(key_acc, slot, key_part.shape) + key_part, slot
            )
            value_acc = lax.dynamic_update_slice(
                value_acc, lax.dynamic_slice(value_acc, slot, value_part.shape) + value_part, slot
            )
            return (key_acc, value_acc, query_acc)

        key_acc, value_acc, query_acc = lax.fori_loop(
            zero_idx, limit, grad_step, (acc_pair[0], acc_pair[1], jnp.zeros(row_shape, single))
        )
        return ((key_acc, value_acc), query_acc[:, 0])

    acc_zero = jnp.zeros((total_rows, seq_count, local_heads, HD), single)
    acc_final, query_parts = lax.scan(backward_block, (acc_zero, acc_zero), step_ids)
    query_grad = jnp.transpose(
        query_parts.reshape(n_blocks, seq_count, block_rows, local_heads, HD), (0, 2, 1, 3, 4)
    ).reshape(local_rows, seq_count, local_heads, HD)
    key_terms = jnp.transpose(
        acc_final[0].reshape(uly_size, blk_size, tok_rows, seq_count, features), (1, 0, 2, 3, 4)
    ).reshape(total_rows, seq_count, features)
    value_terms = jnp.transpose(
        acc_final[1].reshape(uly_size, blk_size, tok_rows, seq_count, features), (1, 0, 2, 3, 4)
    ).reshape(total_rows, seq_count, features)
    key_back, value_back = (
        lax.psum_scatter(key_terms, BLK, scatter_dimension=0, tiled=True),
        lax.psum_scatter(value_terms, BLK, scatter_dimension=0, tiled=True),
    )
    cos_h, sin_h = rotary_tables(query_pos, rotary)
    query_send = (
        rotate_back(query_grad, cos_h, sin_h, rotary)
        .reshape(local_rows, seq_count, features)
        .astype(half_type)
    )
    key_send = (
        rotate_back(key_back.reshape(local_rows, seq_count, local_heads, HD), cos_h, sin_h, rotary)
        .reshape(local_rows, seq_count, features)
        .astype(half_type)
    )
    value_send = value_back.astype(half_type)
    query_ret, key_ret, value_ret = (
        lax.all_to_all(query_send, ULY, split_axis=0, concat_axis=2, tiled=True),
        lax.all_to_all(key_send, ULY, split_axis=0, concat_axis=2, tiled=True),
        lax.all_to_all(value_send, ULY, split_axis=0, concat_axis=2, tiled=True),
    )
    qkv_grad = jnp.concatenate([query_ret, key_ret, value_ret], axis=-1)
    qkv_w_grad = jnp.einsum("tsd,tsf->df", act_one, qkv_grad, preferred_element_type=single)
    qkv_b_grad = jnp.sum(qkv_grad.astype(single), axis=(0, 1))
    act_one_grad = jnp.einsum("tsf,df->tsd", qkv_grad, back_qkv, preferred_element_type=single)
    gain_one_grad = jnp.sum(act_one_grad * normed, axis=(0, 1))
    shift_one_grad = jnp.sum(act_one_grad, axis=(0, 1))
    input_grad = (
        grad_f
        + norm_back(act_one_grad, normed, inverse, back_gain_one)
        + norm_back(act_two_grad, normed, inverse, back_gain_two)
    )
    summed = (
        lax.psum_scatter(qkv_w_grad, AXES, scatter_dimension=0, tiled=True),
        lax.psum_scatter(qkv_b_grad, AXES, scatter_dimension=0, tiled=True),
        lax.psum_scatter(
            dense_w_grad, AXES, scatter_dimension=0, tiled=True
        ),
        lax.psum_scatter(bias_sum, AXES, scatter_dimension=0, tiled=True),
        lax.psum_scatter(
            gain_one_grad, AXES, scatter_dimension=0, tiled=True
        ),
        lax.psum_scatter(
            shift_one_grad, AXES, scatter_dimension=0, tiled=True
        ),
        lax.psum_scatter(
            gain_two_grad, AXES, scatter_dimension=0, tiled=True
        ),
        lax.psum_scatter(
            shift_two_grad, AXES, scatter_dimension=0, tiled=True
        ),
        lax.psum_scatter(up_w_grad, AXES, scatter_dimension=0, tiled=True),
        lax.psum_scatter(up_b_grad, AXES, scatter_dimension=0, tiled=True),
        lax.psum_scatter(down_w_grad, AXES, scatter_dimension=0, tiled=True),
        lax.psum_scatter(bias_sum, AXES, scatter_dimension=0, tiled=True),
    )
    return (
        output,
        input_grad,
        summed[0],
        summed[1],
        summed[2],
        summed[3],
        summed[4],
        summed[5],
        summed[6],
        summed[7],
        summed[8],
        summed[9],
        summed[10],
        summed[11],
    )


MESH = pl.DeviceIdType.MESH


class Place:
    def __init__(self, planes):
        self.planes = planes
        self.b = lax.axis_index(BATCH)
        self.u = lax.axis_index(ULY)
        k = lax.axis_index(BLK)
        self.y, self.c = k // 2, k % 2
        self.t = self.u * 4 + k
        self.xn, self.yn, self.pn = self.peer(4), self.peer(2), self.peer(1)

    def rank(self, d):
        u = 1 - self.u if d & 4 else self.u
        y = 1 - self.y if d & 2 else self.y
        c = 1 - self.c if d & 1 else self.c
        return u * 4 + y * 2 + c

    def chip(self, d):
        return self.rank(d) // 2

    def peer(self, d):
        u = 1 - self.u if d & 4 else self.u
        y = 1 - self.y if d & 2 else self.y
        c = 1 - self.c if d & 1 else self.c
        return {BATCH: self.b, ULY: u, BLK: y * 2 + c}

    def along(self, step):
        return {BATCH: self.b + step, ULY: self.u, BLK: self.y * 2 + self.c}

    def barrier(self):
        sem = pltpu.get_barrier_semaphore()
        for d in range(1, 8):
            pl.semaphore_signal(sem, inc=1, device_id=self.peer(d), device_id_type=MESH)

        for step in range(1, self.planes):

            @pl.when(self.b >= step)
            def _():
                pl.semaphore_signal(sem, inc=1, device_id=self.along(-step), device_id_type=MESH)

            @pl.when(self.b + step < self.planes)
            def _():
                pl.semaphore_signal(sem, inc=1, device_id=self.along(step), device_id_type=MESH)

        pl.semaphore_wait(sem, 7 + self.planes - 1)


class Mail:
    def __init__(self, send, recv, near):
        self.send, self.recv, self.used, self.open = send, recv, 0, []
        self.near, self.near_used = near, 0

    def bring(self, src, dst):
        made = pltpu.make_async_copy(src, dst, self.near.at[self.near_used])
        self.near_used += 1
        made.start()
        return made

    def slots(self, n):
        first = self.used
        self.used += n
        return first

    def copy(self, src, dst, slot, device, recv_slot=None):
        return pltpu.make_async_remote_copy(
            src_ref=src,
            dst_ref=dst,
            send_sem=self.send.at[slot],
            recv_sem=self.recv.at[slot if recv_slot is None else recv_slot],
            device_id=device,
            device_id_type=MESH,
        )

    def post(self, src, dst, slot, device):
        made = self.copy(src, dst, slot, device)
        made.start()
        self.open.append(made)

    def arrived(self, dst, slot, device):
        self.copy(dst, dst, slot, device).wait_recv()

    def close(self):
        for made in self.open:
            made.wait_send()


class PlaneGather:
    def __init__(self, at, mail, shard, whole):
        self.at, self.mail, self.shard, self.whole = at, mail, shard, whole
        self.rows = shard.shape[1]
        self.halves = shard.shape[0] // 2
        self.base = mail.slots(10)

    def half(self, i):
        return self.shard.at[pl.ds(i * self.halves, self.halves)]

    def block(self, d, half=None):
        rows = pl.ds(pl.multiple_of(self.at.rank(d) * self.rows, self.rows), self.rows)
        if half is None:
            return self.whole.at[:, rows, :]
        return self.whole.at[pl.ds(half * self.halves, self.halves), rows, :]

    def start(self):
        at, mail, s = self.at, self.mail, self.base
        mail.post(self.half(1), self.block(0, 1), s, at.xn)
        mail.post(self.half(0), self.block(0, 0), s + 1, at.yn)
        mail.post(self.half(0), self.block(0, 0), s + 8, at.xn)
        mail.post(self.half(1), self.block(0, 1), s + 9, at.yn)
        mail.post(self.shard, self.block(0), s + 2, at.pn)
        self.own = mail.bring(self.shard, self.block(0))

    def relay_y(self):
        at, mail, s = self.at, self.mail, self.base
        mail.arrived(self.block(2, 0), s + 1, at.yn)
        mail.post(self.block(2, 0), self.block(2, 0), s + 3, at.xn)

    def relay_x(self):
        at, mail, s = self.at, self.mail, self.base
        mail.arrived(self.block(4, 1), s, at.xn)
        mail.post(self.block(4, 1), self.block(4, 1), s + 4, at.yn)

    def share(self):
        at, mail, s = self.at, self.mail, self.base
        mail.arrived(self.block(2, 1), s + 9, at.yn)
        mail.post(self.block(2), self.block(2), s + 5, at.pn)
        mail.arrived(self.block(4, 0), s + 8, at.xn)
        mail.post(self.block(4), self.block(4), s + 6, at.pn)

    def far(self):
        at, mail, s = self.at, self.mail, self.base
        mail.arrived(self.block(6, 0), s + 3, at.xn)
        mail.arrived(self.block(6, 1), s + 4, at.yn)
        mail.post(self.block(6), self.block(6), s + 7, at.pn)

    def finish(self):
        at, mail, s = self.at, self.mail, self.base
        mail.arrived(self.block(1), s + 2, at.pn)
        mail.arrived(self.block(3), s + 5, at.pn)
        mail.arrived(self.block(5), s + 6, at.pn)
        mail.arrived(self.block(7), s + 7, at.pn)
        self.own.wait()


class LineGather:
    def __init__(self, at, mail, held, first=0, count=None):
        self.at, self.mail, self.held = at, mail, held
        self.rows = pl.ds(first, held.shape[1] - first if count is None else count)
        self.up, self.down = mail.slots(at.planes), mail.slots(at.planes)

    def part(self, slot):
        return self.held.at[slot, self.rows]

    def pass_on(self, slot, src=None):
        at = self.at
        part = self.part(slot)
        src = part if src is None else src.at[self.rows]

        @pl.when((slot <= at.b) & (at.b < at.planes - 1))
        def _():
            self.mail.copy(src, part, self.up + slot, at.along(1)).start()

        @pl.when((slot >= at.b) & (at.b > 0))
        def _():
            self.mail.copy(src, part, self.down + slot, at.along(-1)).start()

    def start(self, src=None):
        self.pass_on(self.at.b, src)

    def take(self, distance):
        at = self.at

        @pl.when(at.b >= distance)
        def _():
            slot = at.b - distance
            self.mail.arrived(self.part(slot), self.up + slot, at.along(-1))
            self.pass_on(slot)

        @pl.when(at.b + distance < at.planes)
        def _():
            slot = at.b + distance
            self.mail.arrived(self.part(slot), self.down + slot, at.along(1))
            self.pass_on(slot)

    def close(self):
        at = self.at
        for slot in range(at.planes):
            part = self.part(slot)

            @pl.when((slot <= at.b) & (at.b < at.planes - 1))
            def _():
                self.mail.copy(part, part, self.up + slot, at.along(1)).wait_send()

            @pl.when((slot >= at.b) & (at.b > 0))
            def _():
                self.mail.copy(part, part, self.down + slot, at.along(-1)).wait_send()


class StarGather:
    def __init__(self, at, mail, held):
        self.at, self.mail, self.held = at, mail, held
        self.base = mail.slots(2 * at.planes)

    def each(self, action):
        at = self.at
        for step in range(1, at.planes):

            @pl.when(at.b + step < at.planes)
            def _():
                action(step, self.base + step)

            @pl.when(at.b >= step)
            def _():
                action(-step, self.base + at.planes + step)

    def start(self):
        part = self.held.at[self.at.b]
        self.each(
            lambda step, slot: self.mail.copy(part, part, slot, self.at.along(step)).start()
        )

    def finish(self):
        n = self.at.planes
        for step in range(1, n):

            @pl.when(self.at.b + step < n)
            def _():
                part = self.held.at[self.at.b + step]
                self.mail.arrived(part, self.base + n + step, self.at.along(step))

            @pl.when(self.at.b >= step)
            def _():
                part = self.held.at[self.at.b - step]
                self.mail.arrived(part, self.base + step, self.at.along(-step))

    def close(self):
        part = self.held.at[self.at.b]
        self.each(
            lambda step, slot: self.mail.copy(part, part, slot, self.at.along(step)).wait_send()
        )


class PlaneExchange:
    def __init__(self, at, mail, pieces, landings, parts=1):
        self.at, self.mail, self.parts = at, mail, parts
        self.pieces = (lambda rank: [pieces(rank)]) if parts == 1 else pieces
        self.landings = (lambda rank: [landings(rank)]) if parts == 1 else landings
        self.base = mail.slots(8 * parts)

    def start(self):
        at, n = self.at, self.parts
        for d in range(1, 8):
            for i, (piece, landing) in enumerate(
                zip(self.pieces(at.rank(d)), self.landings(at.t))
            ):
                self.mail.post(piece, landing, self.base + d * n + i, at.peer(d))
        self.own = [
            self.mail.bring(piece, landing)
            for piece, landing in zip(self.pieces(at.t), self.landings(at.t))
        ]

    def finish(self):
        at, n = self.at, self.parts
        for d in range(1, 8):
            for i, landing in enumerate(self.landings(at.rank(d))):
                self.mail.arrived(landing, self.base + d * n + i, at.peer(d))
        for own in self.own:
            own.wait()


class PairExchange:
    def __init__(self, at, mail, src, dst, landed):
        self.at, self.mail, self.src, self.dst, self.landed = at, mail, src, dst, landed
        self.base = mail.slots(1)

    def start(self):
        self.mail.post(self.src, self.dst, self.base, self.at.pn)

    def finish(self):
        self.mail.arrived(self.landed, self.base, self.at.pn)


class PlaneReduce:
    def __init__(self, at, mail, terms, pairs, sums, side):
        self.at, self.mail, self.terms = at, mail, terms
        self.pairs, self.sums, self.side = pairs, sums, side
        self.base = mail.slots(8)
        self.order = (6, 4, 2, 0)
        self.halves = terms.shape[0] // 2

    def start(self):
        at = self.at
        for i, d in enumerate(self.order):
            chip = at.chip(d)
            self.mail.post(
                self.terms.at[:, chip, 1 - at.c], self.pairs.at[:, chip], self.base + i, at.pn
            )

    def half(self, ref, i):
        return ref.at[pl.ds(i * self.halves, self.halves)]

    def fold(self):
        at, mail, s = self.at, self.mail, self.base
        for i, d in enumerate(self.order):
            chip = at.chip(d)
            mail.arrived(self.pairs.at[:, chip], s + i, at.pn)
            total = self.terms[:, chip, at.c].astype(jnp.float32) + self.pairs[:, chip].astype(
                jnp.float32
            )
            self.sums[:, chip] = total.astype(self.sums.dtype)
            if d == 6:
                far = self.sums.at[:, chip]
                mail.post(self.half(far, 0), self.half(self.side.at[0], 0), s + 4, at.xn)
                mail.post(self.half(far, 1), self.half(self.side.at[0], 1), s + 5, at.yn)

    def turn(self):
        at, mail, s = self.at, self.mail, self.base
        for i, d, other, slot, nbr in ((1, 4, at.yn, 5, at.xn), (0, 2, at.xn, 4, at.yn)):
            chip = at.chip(d)
            landed = self.half(self.side.at[0], i)
            mail.arrived(landed, s + slot, other)
            part = self.half(self.sums.at[:, chip], i)
            part[...] = (part[...].astype(jnp.float32) + landed[...].astype(jnp.float32)).astype(
                self.sums.dtype
            )
            whole = self.sums.at[:, chip]
            mail.post(whole, self.side.at[2 - i], s + 6 + i, nbr)

    def finish(self):
        at, mail, s = self.at, self.mail, self.base
        mail.arrived(self.side.at[1], s + 7, at.xn)
        mail.arrived(self.side.at[2], s + 6, at.yn)
        return (
            self.sums[:, at.chip(0)].astype(jnp.float32)
            + self.side[1].astype(jnp.float32)
            + self.side[2].astype(jnp.float32)
        )


class LineReduce:
    def __init__(self, at, mail, terms, above, below, up_cut=None, down_cut=None):
        self.at, self.mail, self.terms = at, mail, terms
        self.above, self.below = above, below
        whole = pl.ds(0, terms.shape[2])
        self.up_cut, self.down_cut = up_cut or whole, down_cut or whole
        self.up, self.down = mail.slots(at.planes), mail.slots(at.planes)

    def edge(self, slot):
        at, last = self.at, self.at.planes - 1

        @pl.when((at.b == 0) & (slot > 0))
        def _():
            self.mail.copy(
                self.terms.at[slot, :, self.up_cut],
                self.below.at[slot, :, self.up_cut],
                self.up + slot,
                at.along(1),
            ).start()

        @pl.when((at.b == last) & (slot < last))
        def _():
            self.mail.copy(
                self.terms.at[slot, :, self.down_cut],
                self.above.at[slot, :, self.down_cut],
                self.down + slot,
                at.along(-1),
            ).start()

    def hop(self, hop, rank):
        last = self.at.planes - 1
        if last - rank > hop:
            self._forward(last - rank, self.below, self.up_cut, self.up, 1, self.at.b == hop)
            self._forward(rank, self.above, self.down_cut, self.down, -1, self.at.b == last - hop)

    def _forward(self, slot, held, cut, base, step, here):
        at, mail = self.at, self.mail
        part = held.at[slot, :, cut]

        @pl.when(here)
        def _():
            mail.arrived(part, base + slot, at.along(-step))
            total = self.terms[slot, :, cut].astype(jnp.float32) + held[slot, :, cut].astype(
                jnp.float32
            )
            held[slot, :, cut] = total.astype(held.dtype)
            mail.copy(part, part, base + slot, at.along(step)).start()

    def landed(self):
        at, mail = self.at, self.mail

        @pl.when(at.b > 0)
        def _():
            mail.arrived(self.below.at[at.b, :, self.up_cut], self.up + at.b, at.along(-1))

        @pl.when(at.b < at.planes - 1)
        def _():
            mail.arrived(self.above.at[at.b, :, self.down_cut], self.down + at.b, at.along(1))

    def total(self, out):
        at = self.at
        b, last = at.b, at.planes - 1

        def put(*parts):
            value = self.terms[b].astype(jnp.float32)
            for part in parts:
                value = value + part[b].astype(jnp.float32)
            out[...] = value.astype(out.dtype)

        @pl.when(b == 0)
        def _():
            put(self.above)

        @pl.when(b == last)
        def _():
            put(self.below)

        @pl.when((b > 0) & (b < last))
        def _():
            put(self.below, self.above)

    def close(self):
        at = self.at
        for slot in range(at.planes):
            up, down = self.terms.at[slot, :, self.up_cut], self.terms.at[slot, :, self.down_cut]

            @pl.when(at.b < slot)
            def _():
                self.mail.copy(up, up, self.up + slot, at.along(1)).wait_send()

            @pl.when(at.b > slot)
            def _():
                self.mail.copy(down, down, self.down + slot, at.along(-1)).wait_send()


TILE = 256
LANES = 128


def dot_nn(a, b):
    return lax.dot_general(a, b, (((1,), (0,)), ((), ())), preferred_element_type=jnp.float32)


def dot_nt(a, b):
    return lax.dot_general(a, b, (((1,), (1,)), ((), ())), preferred_element_type=jnp.float32)


def dot_tn(a, b):
    return lax.dot_general(a, b, (((0,), (0,)), ((), ())), preferred_element_type=jnp.float32)


def turn(value, tables, rows, sign):
    straight, early, late = (table[rows, :] for table in tables)
    ahead = pltpu.roll(value, LANES - HD // 8, 1)
    behind = pltpu.roll(value, HD // 8, 1)
    return value * straight + sign * (ahead * early + behind * late)


def of_head(value, head):
    lane = lax.broadcasted_iota(jnp.int32, value.shape, 1)
    return jnp.where(lane // HD == head, value, jnp.zeros_like(value))


def total_rows(value):
    return jnp.sum(value, axis=0, keepdims=True)


class Layer:
    def __init__(self, refs):
        self.__dict__.update(refs)
        self.heads = LANES // HD
        if "xa" in refs:
            self.seqs, self.length, self.width = self.xa.shape
            self.per_seq = self.length // TILE
            self.tiles = self.seqs * self.per_seq

    def rows(self, tile):
        return pl.ds(pl.multiple_of(tile * TILE, TILE), TILE)

    def in_seq(self, ref, tile):
        rows = pl.ds(pl.multiple_of(tile % self.per_seq * TILE, TILE), TILE)
        return ref[tile // self.per_seq, rows, :]

    def loop(self, count, step):
        def run(i, carry):
            step(i)
            return carry

        lax.fori_loop(0, count, run, 0)

    def wide(self, row):
        planes = self.va.shape[0]
        return jnp.concatenate(
            [self.va[b, pl.ds(2 * row + a, 1), :] for b in range(planes) for a in range(2)], axis=1
        )

    def own_vectors(self, rank):
        lane = lax.broadcasted_iota(jnp.int32, (2, LANES), 1)
        row = lax.broadcasted_iota(jnp.int32, (2, LANES), 0)
        for j, ref in enumerate(self.vectors):
            piece = ref[...].astype(jnp.float32).reshape(1, ref.shape[0])
            piece = jnp.concatenate([piece] * (LANES // ref.shape[0]), axis=1)
            here = (lane // ref.shape[0] == rank % 4) & (row == rank // 4)
            self.vec_s[2 * j : 2 * j + 2, :] = jnp.where(here, jnp.broadcast_to(piece, here.shape), 0.0)
        bias = self.b_qkv[...].astype(jnp.float32).reshape(1, self.b_qkv.shape[0])
        self.vec_s[12:13, :] = jnp.concatenate(
            [bias, jnp.zeros((1, LANES - bias.shape[1]), jnp.float32)], axis=1
        )
        self.vec_s[13:14, :] = self.b_up[...].astype(jnp.float32).reshape(1, LANES)

    def plane_vectors(self, slot):
        total = jnp.sum(self.vec_in[...], axis=0)
        self.va[slot, 0:16, :] = total
        for rank in range(self.vec_in.shape[0]):
            self.va[slot, 16 + rank : 17 + rank, :] = self.vec_in[rank, 12:13, :]
            self.va[slot, 24 + rank : 25 + rank, :] = self.vec_in[rank, 13:14, :]

    def sort_weight(self):
        rows = self.wq_raw.shape[0]
        low = lax.broadcasted_iota(jnp.int32, (rows, LANES), 1) < HD
        for part in range(3):
            for core in range(2):
                for pair in range(2):
                    first, second = (
                        self.wq_raw[
                            :, pl.ds(part * self.width + (core * 2 + j) * 4 * HD + pair * LANES, LANES)
                        ].astype(jnp.float32)
                        for j in range(2)
                    )
                    cut = slice(part * LANES, (part + 1) * LANES)
                    self.wq_s[4 * pair + core, :, cut] = jnp.where(
                        low, first, pltpu.roll(second, HD, 1)
                    ).astype(jnp.bfloat16)
                    self.wq_s[4 * pair + 2 + core, :, cut] = jnp.where(
                        low, pltpu.roll(first, HD, 1), second
                    ).astype(jnp.bfloat16)

    def statistics(self):
        def step(i):
            x = self.in_seq(self.xa, i).astype(jnp.float32)
            center = jnp.mean(x, axis=1, keepdims=True)
            shifted = x - center
            spread = jnp.mean(shifted * shifted, axis=1, keepdims=True)
            self.center[self.rows(i), :] = center
            self.inverse[self.rows(i), :] = lax.rsqrt(spread + EPSILON)

        self.loop(self.tiles, step)

    def normed(self, i):
        x = self.in_seq(self.xa, i).astype(jnp.float32)
        return (x - self.center[self.rows(i), :]) * self.inverse[self.rows(i), :]

    def activations(self):
        gain_one, shift_one, gain_two, shift_two = (self.wide(j) for j in (1, 2, 3, 4))

        def step(i):
            normed = self.normed(i)
            self.act_one[self.rows(i), :] = (normed * gain_one + shift_one).astype(jnp.bfloat16)
            self.act_two[self.rows(i), :] = (normed * gain_two + shift_two).astype(jnp.bfloat16)

        self.loop(self.tiles, step)

    def qkv_bias(self, rank):
        size = HD // 2
        held = self.b_qkv.shape[0] // size
        ranks = self.vec_in.shape[0]
        pieces = []
        for i in range(3 * LANES // size):
            part, j, half = i // 4, i // 2 % 2, i % 2
            head = (rank % 2 * 2 + j) * 4 + rank // 2
            index = part * (self.width // size) + head * 2 + half
            owner, spot = index // held, index % held
            row = self.va[owner // ranks, pl.ds(16 + owner % ranks, 1), :]
            pieces.append(
                sum(
                    jnp.where(spot == k, row[:, k * size : (k + 1) * size], 0.0)
                    for k in range(held)
                )
            )
        return jnp.concatenate(pieces, axis=1)

    def up_bias(self, rank):
        return jnp.concatenate(
            [self.va[b, pl.ds(24 + rank, 1), :] for b in range(self.va.shape[0])], axis=1
        )

    def near(self, ref, side):
        both = ref[pl.ds(side * 2, 2)]
        return both.reshape(both.shape[0] * both.shape[1], both.shape[2])

    def half_columns(self, side, width):
        return pl.ds(pl.multiple_of(side * (width // 2), width // 2), width // 2)

    def project_near(self, side):
        def step(i):
            cut = self.half_columns(side, self.width)
            self.qkv[self.rows(i), :] = dot_nn(self.act_one[self.rows(i), cut], self.near(self.wq, side))

        self.loop(self.tiles, step)

    def project(self, rank, side):
        bias = self.qkv_bias(rank)

        def step(i):
            cut = self.half_columns(side, self.width)
            qkv = dot_nn(self.act_one[self.rows(i), cut], self.near(self.wq, side))
            qkv = qkv + self.qkv[self.rows(i), :] + bias
            rows = pl.ds(pl.multiple_of(i % self.per_seq * TILE, TILE), TILE)
            query = turn(qkv[:, :LANES], self.tables, rows, 1.0).astype(jnp.bfloat16)
            self.query[self.rows(i), :] = query * jnp.asarray(1.0 / math.sqrt(HD), jnp.bfloat16)
            self.key[self.rows(i), :] = turn(
                qkv[:, LANES : 2 * LANES], self.tables, rows, 1.0
            ).astype(jnp.bfloat16)
            self.value[self.rows(i), :] = qkv[:, 2 * LANES :].astype(jnp.bfloat16)

        self.loop(self.tiles, step)

    def keys(self, seq, block):
        start = pl.multiple_of(seq * self.length, TILE)
        return pl.ds(start, (block + 1) * TILE)

    def attend(self, seq):
        for block in range(self.per_seq):
            rows = self.rows(seq * self.per_seq + block)
            keys = self.keys(seq, block)
            key, value, query = self.key[keys, :], self.value[keys, :], self.query[rows, :]
            out = None
            for head in range(self.heads):
                scores = dot_nt(of_head(query, head), key)
                at = lax.broadcasted_iota(jnp.int32, scores.shape, 0) + block * TILE
                to = lax.broadcasted_iota(jnp.int32, scores.shape, 1)
                scores = jnp.where(to <= at, scores, -jnp.inf)
                top = jnp.max(scores, axis=1, keepdims=True)
                weight = jnp.exp(scores - top)
                weight = weight * (1.0 / jnp.sum(weight, axis=1, keepdims=True))
                self.probs[block][seq * self.heads + head] = weight
                part = dot_nn(weight.astype(jnp.bfloat16), value)
                out = of_head(part, head) if out is None else out + of_head(part, head)
            self.attn[rows, :] = out.astype(jnp.bfloat16)

    def attend_out_grad(self):
        def step(i):
            weight = self.wo2[...].reshape(LANES, self.width)
            self.attn_grad[self.rows(i), :] = dot_nt(self.in_seq(self.ca, i), weight).astype(
                jnp.bfloat16
            )

        self.loop(self.tiles, step)

    def attend_grad(self, seq):
        key_grad, value_grad = [None] * self.per_seq, [None] * self.per_seq
        start = seq * self.per_seq
        for block in range(self.per_seq):
            rows = self.rows(start + block)
            keys = self.keys(seq, block)
            key, value, query = self.key[keys, :], self.value[keys, :], self.query[rows, :]
            grad = self.attn_grad[rows, :]
            inner = grad.astype(jnp.float32) * self.attn[rows, :].astype(jnp.float32)
            query_grad = None
            for head in range(self.heads):
                own_grad = of_head(grad, head)
                delta = jnp.sum(of_head(inner, head), axis=1, keepdims=True)
                probs = self.probs[block][seq * self.heads + head]
                grad_prob = dot_nt(own_grad, value)
                grad_score = (probs * (grad_prob - delta)).astype(jnp.bfloat16)
                part = dot_nn(grad_score, of_head(key, head))
                query_grad = part if query_grad is None else query_grad + part
                key_part = dot_tn(grad_score, of_head(query, head))
                value_part = dot_tn(probs.astype(jnp.bfloat16), own_grad)
                for b in range(block + 1):
                    cut = slice(b * TILE, (b + 1) * TILE)
                    key_grad[b] = key_part[cut] if key_grad[b] is None else key_grad[b] + key_part[cut]
                    value_grad[b] = (
                        value_part[cut] if value_grad[b] is None else value_grad[b] + value_part[cut]
                    )
            back = pl.ds(block * TILE, TILE)
            self.qkv_grad[rows, :LANES] = turn(
                query_grad * (1.0 / math.sqrt(HD)), self.tables, back, -1.0
            ).astype(jnp.bfloat16)
        for block in range(self.per_seq):
            rows = self.rows(start + block)
            back = pl.ds(block * TILE, TILE)
            self.qkv_grad[rows, LANES : 2 * LANES] = turn(
                key_grad[block], self.tables, back, -1.0
            ).astype(jnp.bfloat16)
            self.qkv_grad[rows, 2 * LANES :] = value_grad[block].astype(jnp.bfloat16)

    def cot_flat(self):
        return self.ca[...].reshape(self.seqs * self.length, self.width)

    def qkv_weight_grad(self, i):
        rows = self.gq.shape[1]
        act = self.act_one[:, pl.ds(pl.multiple_of(i * rows, rows), rows)]
        self.gq[i] = dot_tn(act, self.qkv_grad[...]).astype(jnp.bfloat16)

    def dense_weight_grad(self):
        self.go[...] = (
            dot_tn(self.attn[...], self.cot_flat()).astype(jnp.bfloat16).reshape(self.go.shape)
        )

    def expand_near(self, side):
        def step(i):
            cut = self.half_columns(side, self.width)
            self.slope[self.rows(i), :] = dot_nn(
                self.act_two[self.rows(i), cut], self.near(self.wu, side)
            )

        self.loop(self.tiles, step)

    def expand(self, rank, side):
        bias = self.up_bias(rank)

        def step(i):
            cut = self.half_columns(side, self.width)
            pre = dot_nn(self.act_two[self.rows(i), cut], self.near(self.wu, side))
            pre = pre + self.slope[self.rows(i), :] + bias
            cdf = 0.5 * (1.0 + lax.erf(pre * INV_ROOT_TWO))
            self.gelu[self.rows(i), :] = (pre * cdf).astype(jnp.bfloat16)
            self.slope[self.rows(i), :] = cdf + pre * jnp.exp(-0.5 * pre * pre) * INV_ROOT_TWO_PI

        self.loop(self.tiles, step)

    def down_weight_grad(self, i):
        depth = self.gd.shape[1]
        part = self.gelu[:, pl.ds(pl.multiple_of(i * depth, depth), depth)]
        self.gd[i] = dot_tn(part, self.cot_flat()).astype(jnp.bfloat16)

    def hidden_grad(self, side):
        def step(i):
            cut = self.half_columns(side, self.hidden)
            grad = dot_nt(self.in_seq(self.ca, i), self.near(self.wd, side))
            self.pre_grad[self.rows(i), cut] = (grad * self.slope[self.rows(i), cut]).astype(
                jnp.bfloat16
            )

        self.loop(self.tiles, step)

    def up_weight_grad(self, i, side):
        rows = self.gu.shape[1]
        act = self.act_two[:, pl.ds(pl.multiple_of(i * rows, rows), rows)]
        cut = self.half_columns(side, self.hidden)
        self.gu[i, :, cut] = dot_tn(act, self.pre_grad[:, cut]).astype(jnp.bfloat16)

    def put_terms(self, terms, i, value):
        seq, chips, cores, rows, width = terms.shape
        n = TILE // (cores * rows)
        terms[i // self.per_seq, pl.ds(i % self.per_seq * n, n)] = value.astype(
            jnp.bfloat16
        ).reshape(n, cores, rows, width)

    def out_terms(self, i):
        dense = self.wo2[...].reshape(LANES, self.width)
        down = self.wd[...].reshape(self.hidden, self.width)
        self.put_terms(
            self.po,
            i,
            dot_nn(self.attn[self.rows(i), :], dense) + dot_nn(self.gelu[self.rows(i), :], down),
        )

    def in_terms(self, i):
        gain_one, gain_two = self.wide(1), self.wide(3)
        normed = self.normed(i)
        weight = self.wq[...].reshape(self.width, 3 * LANES)
        one = dot_nt(self.qkv_grad[self.rows(i), :], weight)
        weight = self.wu[...].reshape(self.width, self.hidden)
        two = dot_nt(self.pre_grad[self.rows(i), :], weight)
        self.put_terms(self.pg, i, one * gain_one + two * gain_two)
        for j, value in enumerate((one * normed, one, two * normed, two)):
            if i == 0:
                self.sums[j : j + 1, :] = total_rows(value)
            else:
                self.sums[j : j + 1, :] += total_rows(value)

    def split(self, raw, own):
        for seq in range(own.shape[0]):
            own[seq] = raw[:, seq, :]

    def own_rows(self, ref, rank):
        rows = self.out.shape[1]
        return ref[:, pl.ds(pl.multiple_of(rank * rows, rows), rows), :].astype(jnp.float32)

    def small_terms(self, rank):
        ranks = self.sm.shape[0]
        cot = total_rows(jnp.sum(self.own_rows(self.ca, rank), axis=0))
        for to in range(ranks):
            cut = slice(to * LANES, (to + 1) * LANES)
            self.sm[to, 0:1, :] = cot[:, cut]
            self.sm[to, 1:5, :] = self.sums[0:4, cut]

    def small_plane(self, slot):
        total = jnp.sum(self.sm_in[...], axis=0)
        self.vz[slot, 0:8, :] = total
        qkv = total_rows(self.qkv_grad[...].astype(jnp.float32))
        pre = total_rows(self.pre_grad[...].astype(jnp.float32))
        for j in range(3):
            self.vz[slot, 8 + j : 9 + j, :] = qkv[:, j * LANES : (j + 1) * LANES]
        for j in range(self.hidden // LANES):
            self.vz[slot, 12 + j : 13 + j, :] = pre[:, j * LANES : (j + 1) * LANES]

    def result(self, rank, out_sum, in_sum):
        x = self.own_rows(self.xa, rank)
        center = jnp.mean(x, axis=2, keepdims=True)
        shifted = x - center
        inverse = lax.rsqrt(jnp.mean(shifted * shifted, axis=2, keepdims=True) + EPSILON)
        normed = shifted * inverse
        bias = (self.wide(0) + self.wide(5))[None]
        self.out[...] = (x + out_sum + bias).astype(jnp.bfloat16)
        self.in_grad[...] = self.own_rows(self.ca, rank) + inverse * (
            in_sum
            - jnp.mean(in_sum, axis=2, keepdims=True)
            - normed * jnp.mean(in_sum * normed, axis=2, keepdims=True)
        )


LAYER_SLOTS = 5 * 8 + 4 + 12 * 8 + 10 * 8 + 2
NEAR_SLOTS = 24


def layer_kernel(names, planes, *refs):
    refs = dict(zip(names, refs))
    send, recv, near = (refs.pop(name) for name in names[-3:])
    refs.update(
        tables=tuple(refs["table"].at[i] for i in range(3)),
        probs=tuple(refs[name] for name in names if name.startswith("probs")),
        vectors=tuple(refs[name] for name in names if name.startswith("vector")),
        hidden=refs["gelu"].shape[1],
    )
    do = Layer(refs)
    at = Place(planes)
    mail = Mail(send, recv, near)
    b, c = at.b, at.c
    rows = do.wq_s.shape[1]
    pair = planes // 2

    def strip(whole):
        return lambda rank: whole.at[b, pl.ds(pl.multiple_of(rank * rows, rows), rows), :]

    def band(whole):
        return lambda rank: whole.at[pl.ds(pl.multiple_of(rank * rows, rows), rows), :]

    def up_pieces(rank):
        return [
            do.wu_s.at[:, pl.ds(pl.multiple_of((p * 8 + rank) * LANES, LANES), LANES)]
            for p in range(planes)
        ]

    def up_landings(rank):
        strip_rows = pl.ds(pl.multiple_of(rank * rows, rows), rows)
        return [do.wu.at[b, strip_rows, pl.ds(p * LANES, LANES)] for p in range(planes)]

    gather_x = PlaneGather(at, mail, do.x_own, do.xa)
    gather_c = PlaneGather(at, mail, do.cot_own, do.ca)
    line_v, line_o = StarGather(at, mail, do.va), LineGather(at, mail, do.wo)
    line_q = LineGather(at, mail, do.wq)
    half = do.wu.shape[1] // 2
    line_ua = LineGather(at, mail, do.wu, 0, half)
    line_ub = LineGather(at, mail, do.wu, half, half)
    half = do.wd.shape[1] // 2
    line_da = LineGather(at, mail, do.wd, 0, half)
    line_db = LineGather(at, mail, do.wd, half, half)
    ex_v = PlaneExchange(at, mail, lambda rank: do.vec_s, lambda rank: do.vec_in.at[rank])
    ex_q = PlaneExchange(at, mail, lambda rank: do.wq_s.at[rank], strip(do.wq))
    ex_u = PlaneExchange(at, mail, up_pieces, up_landings, planes)
    mine = do.wo2.at[:, c]
    swap_w = PairExchange(
        at, mail, do.wo.at[pl.ds(pair * (1 - c), pair)], mine, do.wo2.at[:, 1 - c]
    )
    sum_o = LineReduce(at, mail, do.go4, do.above_o, do.below_o)
    sum_q = LineReduce(at, mail, do.gq, do.above_q, do.below_q)
    first, second = (pl.ds(i * do.hidden // 2, do.hidden // 2) for i in range(2))
    sum_un = LineReduce(at, mail, do.gu, do.above_u, do.below_u, first, second)
    sum_uf = LineReduce(at, mail, do.gu, do.above_u, do.below_u, second, first)
    near_side = b // pair
    far_side = 1 - near_side
    sum_d = LineReduce(at, mail, do.gd, do.above_d, do.below_d)
    swap_g = PairExchange(
        at,
        mail,
        do.go.at[:, 1 - c],
        do.go4.at[pl.ds(pair * c, pair)],
        do.go4.at[pl.ds(pair * (1 - c), pair)],
    )
    back_q = PlaneExchange(at, mail, band(do.fq), lambda rank: do.dq.at[rank])
    back_u = PlaneExchange(at, mail, band(do.fu), lambda rank: do.du.at[rank])
    fold_v = PlaneExchange(at, mail, lambda rank: do.sm.at[rank], lambda rank: do.sm_in.at[rank])
    line_s = StarGather(at, mail, do.vz)
    share_v = PlaneExchange(at, mail, lambda rank: do.vt, lambda rank: do.dv.at[rank])
    plane_o = PlaneReduce(at, mail, do.po, do.pairs_o, do.sums_o, do.side_o)
    plane_g = PlaneReduce(at, mail, do.pg, do.pairs_g, do.sums_g, do.side_g)

    slots = [s + b // pair * (planes - 1 - 2 * s) for s in (3, 0, 2, 1)]

    at.barrier()
    line_da.start(do.wd_s)
    own_d = mail.bring(do.wd_s, do.wd.at[b])
    raw_x = mail.bring(do.x_in, do.x_raw)
    ex_u.start()
    line_db.start(do.wd_s)
    line_o.start(do.wo_s)
    own_o = mail.bring(do.wo_s, do.wo.at[b])
    raw_x.wait()
    do.split(do.x_raw, do.x_own)
    own_raw = mail.bring(do.wq_in, do.wq_raw)
    gather_x.start()
    own_o.wait()
    ex_u.finish()
    line_ua.start()
    raw_c = mail.bring(do.cot_in, do.cot_raw)
    own_table = mail.bring(do.table_in, do.table)
    do.own_vectors(at.t)
    ex_v.start()
    gather_x.relay_x()
    line_ub.start()
    own_raw.wait()
    do.sort_weight()
    ex_q.start()
    own_table.wait()
    gather_x.relay_y()
    line_ua.take(1)
    raw_c.wait()
    do.split(do.cot_raw, do.cot_own)
    ex_v.finish()
    do.plane_vectors(b)
    line_v.start()
    gather_x.share()
    line_ub.take(1)
    gather_x.far()
    gather_c.start()
    line_ua.take(2)
    own_d.wait()
    gather_x.finish()
    do.statistics()
    line_v.finish()
    do.activations()
    line_ub.take(2)
    gather_c.relay_x()
    do.expand_near(near_side)
    gather_c.relay_y()
    ex_q.finish()
    line_q.start()
    line_o.take(1)
    gather_c.share()
    line_ub.take(3)
    line_ua.take(3)
    gather_c.far()
    do.expand(at.t, far_side)
    gather_c.finish()
    do.down_weight_grad(slots[0])
    sum_d.edge(slots[0])
    line_q.take(1)
    do.down_weight_grad(slots[1])
    sum_d.edge(slots[1])
    do.down_weight_grad(slots[2])
    sum_d.edge(slots[2])
    do.down_weight_grad(slots[3])
    sum_d.edge(slots[3])
    line_o.take(2)
    line_o.take(3)
    swap_w.start()
    mine[...] = do.wo[pl.ds(pair * c, pair)]
    do.project_near(near_side)
    swap_w.finish()
    do.attend_out_grad()
    line_q.take(2)
    line_db.take(1)
    line_da.take(1)
    do.hidden_grad(near_side)
    do.up_weight_grad(slots[0], near_side)
    sum_un.edge(slots[0])
    line_q.take(3)
    do.project(at.t, far_side)
    do.attend(0)
    do.attend(1)
    do.dense_weight_grad()
    swap_g.start()
    do.go4[pl.ds(pair * c, pair)] = do.go[:, c]
    line_da.take(2)
    do.up_weight_grad(slots[1], near_side)
    sum_un.edge(slots[1])
    do.up_weight_grad(slots[2], near_side)
    sum_un.edge(slots[2])
    do.attend_grad(0)
    do.attend_grad(1)
    do.qkv_weight_grad(slots[0])
    sum_q.edge(slots[0])
    do.up_weight_grad(slots[3], near_side)
    sum_un.edge(slots[3])
    line_da.take(3)
    line_db.take(2)
    line_db.take(3)
    sum_d.hop(1, 0)
    do.out_terms(0)
    do.out_terms(1)
    do.out_terms(2)
    do.out_terms(3)
    plane_o.start()
    do.hidden_grad(far_side)
    do.up_weight_grad(slots[0], far_side)
    sum_uf.edge(slots[0])
    do.up_weight_grad(slots[1], far_side)
    sum_uf.edge(slots[1])
    do.up_weight_grad(slots[2], far_side)
    sum_uf.edge(slots[2])
    do.up_weight_grad(slots[3], far_side)
    sum_uf.edge(slots[3])
    sum_d.hop(1, 1)
    plane_o.fold()
    do.qkv_weight_grad(slots[1])
    sum_q.edge(slots[1])
    do.qkv_weight_grad(slots[2])
    sum_q.edge(slots[2])
    do.qkv_weight_grad(slots[3])
    sum_q.edge(slots[3])
    do.in_terms(0)
    sum_q.hop(1, 0)
    plane_o.turn()
    do.in_terms(1)
    do.in_terms(2)
    do.in_terms(3)
    plane_g.start()
    sum_un.hop(1, 0)
    sum_d.hop(2, 0)
    plane_g.fold()
    sum_uf.hop(1, 0)
    sum_un.hop(2, 0)
    sum_uf.hop(1, 1)
    do.small_terms(at.t)
    fold_v.start()
    sum_un.hop(1, 1)
    sum_uf.hop(2, 0)
    plane_g.turn()
    fold_v.finish()
    do.small_plane(b)
    line_s.start()
    sum_q.hop(1, 1)
    swap_g.finish()
    for slot in slots:
        sum_o.edge(slot)
    sum_q.hop(2, 0)
    sum_un.landed()
    sum_uf.landed()
    sum_un.total(do.fu)
    back_u.start()
    do.result(at.t, plane_o.finish(), plane_g.finish())
    out_x = mail.bring(do.out, do.out_to)
    out_g = mail.bring(do.in_grad, do.in_grad_to)
    line_s.finish()
    sum_o.hop(1, 0)
    do.vt[...] = jnp.sum(do.vz[...], axis=0)
    share_v.start()
    sum_q.landed()
    sum_q.total(do.fq)
    back_q.start()
    sum_o.hop(1, 1)
    sum_d.landed()
    sum_d.total(do.dd)
    out_d = mail.bring(do.dd, do.dd_to)
    sum_o.hop(2, 0)
    back_u.finish()
    share_v.finish()
    sum_o.landed()
    sum_o.total(do.dd_o)
    out_o = mail.bring(do.dd_o, do.dd_o_to)
    back_q.finish()
    for copied in (out_o, out_d, out_x, out_g):
        copied.wait()
    mail.close()
    for line in (line_v, line_o, line_q, line_ua, line_ub, line_da, line_db, line_s, sum_o, sum_q, sum_un, sum_uf, sum_d):
        line.close()


def finish_kernel(names, planes, *refs):
    do = Layer(dict(zip(names, refs)))
    at = Place(planes)
    ranks, rows = do.dq.shape[:2]
    lane = lax.broadcasted_iota(jnp.int32, (rows, LANES), 1)
    low = lane < HD
    for part in range(3):
        for core in range(2):
            for pair in range(ranks // 4):
                near, far = (
                    do.dq[2 * (2 * pair + i) + core, :, part * LANES : (part + 1) * LANES].astype(
                        jnp.float32
                    )
                    for i in range(2)
                )
                for j in range(2):
                    both = (
                        jnp.where(low, near, pltpu.roll(far, HD, 1))
                        if j == 0
                        else jnp.where(low, pltpu.roll(near, HD, 1), far)
                    )
                    first = (part * 4 + core * 2 + j) * ranks // 2 * HD + pair * LANES
                    do.qkv_out[:, first : first + LANES] = both
    for rank in range(ranks):
        for b in range(planes):
            first = (b * ranks + rank) * LANES
            do.up_out[:, first : first + LANES] = do.du[
                rank, :, b * LANES : (b + 1) * LANES
            ].astype(jnp.float32)
    do.down_out[...] = do.dd[...]
    do.dense_out[...] = do.dd_o[...]
    for seq in range(do.out.shape[0]):
        do.in_grad_out[:, seq, :] = do.in_grad[seq]
        do.out_out[:, seq, :] = do.out[seq]
    piece = lax.rem(at.t, 4)
    row = (at.b * ranks + at.t) // 4
    values = do.dv[pl.ds(row, 1), 0:8, :].reshape(8, LANES)
    front = jnp.zeros((8, rows), jnp.float32)
    for i in range(4):
        cut = values[:, i * rows : (i + 1) * rows]
        front = front + jnp.where(piece == i, cut, jnp.zeros_like(cut))
    for j, ref in enumerate(
        (do.dense_bias, do.gain_one, do.shift_one, do.gain_two, do.shift_two)
    ):
        ref[...] = front[j].reshape(rows)
    do.down_bias[...] = front[0].reshape(rows)
    do.up_bias[...] = do.dv[pl.ds(at.t, 1), pl.ds(12 + at.b, 1), :].reshape(LANES)
    pieces = []
    for i in range(3):
        index = (at.b * ranks + at.t) * 3 + i
        part, inner = index // 32, lax.rem(index, 32)
        head, half = inner // 2, lax.rem(inner, 2)
        core, j, chip = head // 8, lax.rem(head // 4, 2), lax.rem(head, 4)
        value = do.dv[pl.ds(chip * 2 + core, 1), pl.ds(8 + part, 1), :].reshape(1, LANES)
        spot = 2 * j + half
        total = jnp.zeros((1, rows), jnp.float32)
        for k in range(4):
            cut = value[:, k * rows : (k + 1) * rows]
            total = total + jnp.where(spot == k, cut, jnp.zeros_like(cut))
        pieces.append(total)
    do.qkv_bias[...] = jnp.concatenate(pieces, axis=1).reshape(3 * rows)


VMEM = pl.BlockSpec(memory_space=pltpu.VMEM)


def rotary_rows(length):
    half = HD // 8
    frequency = 1.0 / 10000.0 ** (np.arange(half) * (1.0 / half))
    angles = np.arange(length)[:, None] * frequency[None, :]
    table = np.zeros((3, length, HD))
    table[0] = 1.0
    table[0, :, :half] = table[0, :, half : 2 * half] = np.cos(angles)
    table[1, :, :half] = -np.sin(angles)
    table[2, :, half : 2 * half] = np.sin(angles)
    return np.tile(table, (1, 1, LANES // HD)).astype(np.float32)


def body(shape, *operands):
    residual_in, qkv_weight, down_weight = operands[0], operands[1], operands[11]
    planes = shape[BATCH]
    ranks = shape[ULY] * shape[BLK]
    tok_rows, seqs, width = residual_in.shape
    fits = (
        (shape[ULY], shape[BLK]) == (2, 4)
        and planes == 4
        and seqs % 2 == 0
        and 2 * qkv_weight.shape[0] == HD
        and width == ranks * LANES
        and ranks * tok_rows % TILE == 0
        and TILE % (2 * tok_rows) == 0
        and down_weight.shape[0] == LANES
    )
    return fast_body(planes, *operands) if fits else general_body(*operands)


def fast_body(
    planes,
    residual_in,
    qkv_weight,
    qkv_bias,
    dense_weight,
    dense_bias,
    norm1_gain,
    norm1_bias,
    norm2_gain,
    norm2_bias,
    up_weight,
    up_bias,
    down_weight,
    down_bias,
    cotangent,
):
    single = jnp.float32
    half_type = jnp.bfloat16
    tok_rows, seqs, width = residual_in.shape
    ranks = width // LANES
    rows = qkv_weight.shape[0]
    depth = down_weight.shape[0]
    hidden = planes * depth
    pair = planes // 2
    length = ranks * tok_rows
    tokens = seqs * length
    rank = lax.axis_index(ULY) * lax.axis_size(BLK) + lax.axis_index(BLK)
    owner = lax.axis_index(BATCH) * ranks + rank

    anywhere = pl.BlockSpec(memory_space=pl.ANY)
    inputs = dict(
        x_in=(residual_in, anywhere),
        cot_in=(cotangent, anywhere),
        wq_in=(qkv_weight, anywhere),
        wu_s=(up_weight, anywhere),
        wd_s=(down_weight, anywhere),
        wo_s=(dense_weight, anywhere),
        table_in=(jnp.asarray(rotary_rows(length)), anywhere),
        b_qkv=(qkv_bias, VMEM),
        b_up=(up_bias, VMEM),
    )
    for i, v in enumerate((dense_bias, norm1_gain, norm1_bias, norm2_gain, norm2_bias, down_bias)):
        inputs["vector%d" % i] = (v, VMEM)
    shard = (seqs, tok_rows, width)
    outputs = dict(
        out_to=(shard, half_type),
        in_grad_to=(shard, single),
        dq=((ranks, rows, 3 * LANES), half_type),
        du=((ranks, rows, hidden), half_type),
        dd_to=((depth, width), single),
        dd_o_to=((rows, width), single),
        dv=((ranks, 16, LANES), single),
    )
    q_shape = (planes, ranks * rows, 3 * LANES)
    u_shape = (planes, ranks * rows, hidden)
    d_shape = (planes, depth, width)
    o_shape = (planes, rows, width)
    chips = ranks // 2
    scratch = dict(
        xa=((seqs, length, width), half_type),
        ca=((seqs, length, width), half_type),
        wq=(q_shape, half_type),
        wu=(u_shape, half_type),
        wd=(d_shape, half_type),
        wo=(o_shape, half_type),
        wo2=((pair, 2, rows, width), half_type),
        x_raw=(residual_in.shape, half_type),
        cot_raw=(residual_in.shape, half_type),
        x_own=(shard, half_type),
        cot_own=(shard, half_type),
        qkv=((tokens, 3 * LANES), single),
        wq_raw=(qkv_weight.shape, half_type),
        wq_s=((ranks, rows, 3 * LANES), half_type),
        table=((3, length, LANES), single),
        out=(shard, half_type),
        in_grad=(shard, single),
        dd=((depth, width), single),
        dd_o=((rows, width), single),
        vec_s=((16, LANES), single),
        vec_in=((ranks, 16, LANES), single),
        va=((planes, 32, LANES), single),
        center=((tokens, 1), single),
        inverse=((tokens, 1), single),
        act_one=((tokens, width), half_type),
        act_two=((tokens, width), half_type),
        query=((tokens, LANES), half_type),
        key=((tokens, LANES), half_type),
        value=((tokens, LANES), half_type),
        attn=((tokens, LANES), half_type),
        attn_grad=((tokens, LANES), half_type),
        qkv_grad=((tokens, 3 * LANES), half_type),
        gelu=((tokens, hidden), half_type),
        slope=((tokens, hidden), single),
        pre_grad=((tokens, hidden), half_type),
        gq=(q_shape, half_type),
        gu=(u_shape, half_type),
        gd=(d_shape, half_type),
        go=((pair, 2, rows, width), half_type),
        go4=(o_shape, half_type),
        above_q=(q_shape, half_type),
        below_q=(q_shape, half_type),
        above_u=(u_shape, half_type),
        below_u=(u_shape, half_type),
        above_d=(d_shape, half_type),
        below_d=(d_shape, half_type),
        above_o=(o_shape, half_type),
        below_o=(o_shape, half_type),
        fq=(q_shape[1:], half_type),
        fu=(u_shape[1:], half_type),
        po=((seqs, chips, 2, tok_rows, width), half_type),
        pg=((seqs, chips, 2, tok_rows, width), half_type),
        pairs_o=((seqs, chips, tok_rows, width), half_type),
        pairs_g=((seqs, chips, tok_rows, width), half_type),
        sums_o=((seqs, chips, tok_rows, width), half_type),
        sums_g=((seqs, chips, tok_rows, width), half_type),
        side_o=((3,) + shard, half_type),
        side_g=((3,) + shard, half_type),
        sums=((8, width), single),
        sm=((ranks, 8, LANES), single),
        sm_in=((ranks, 8, LANES), single),
        vz=((planes, 16, LANES), single),
        vt=((16, LANES), single),
    )
    for block in range(length // TILE):
        scratch["probs%d" % block] = ((seqs * LANES // HD, TILE, (block + 1) * TILE), single)
    names = tuple(inputs) + tuple(outputs) + tuple(scratch) + ("send", "recv", "near")
    out, in_grad, dq, du, dd, dd_o, dv = pl.pallas_call(
        functools.partial(layer_kernel, names, planes),
        out_shape=[jax.ShapeDtypeStruct(*what) for what in outputs.values()],
        in_specs=[where for _, where in inputs.values()],
        out_specs=[anywhere] * len(outputs),
        scratch_shapes=[pltpu.VMEM(*what) for what in scratch.values()]
        + [pltpu.SemaphoreType.DMA((n,)) for n in (LAYER_SLOTS, LAYER_SLOTS, NEAR_SLOTS)],
        compiler_params=pltpu.CompilerParams(
            collective_id=0, has_side_effects=True, vmem_limit_bytes=60 * 2**20
        ),
    )(*(value for value, _ in inputs.values()))

    results = dict(
        out_out=(residual_in.shape, half_type),
        in_grad_out=(residual_in.shape, single),
        qkv_out=(qkv_weight.shape, single),
        qkv_bias=(qkv_bias.shape, single),
        dense_out=(dense_weight.shape, single),
        dense_bias=(dense_bias.shape, single),
        gain_one=(norm1_gain.shape, single),
        shift_one=(norm1_bias.shape, single),
        gain_two=(norm2_gain.shape, single),
        shift_two=(norm2_bias.shape, single),
        up_out=(up_weight.shape, single),
        up_bias=(up_bias.shape, single),
        down_out=(down_weight.shape, single),
        down_bias=(down_bias.shape, single),
    )
    return tuple(
        pl.pallas_call(
            functools.partial(
                finish_kernel, tuple(n.removesuffix("_to") for n in outputs) + tuple(results), planes
            ),
            out_shape=[jax.ShapeDtypeStruct(*what) for what in results.values()],
            in_specs=[VMEM] * len(outputs),
            out_specs=[VMEM] * len(results),
        )(out, in_grad, dq, du, dd, dd_o, dv)
    )


def solution(mesh):
    placed = (
        P(TOKENS, BATCH, None),
        P(AXES, None),
        P(AXES),
        P(AXES, None),
        P(AXES),
        P(AXES),
        P(AXES),
        P(AXES),
        P(AXES),
        P(AXES, None),
        P(AXES),
        P(AXES, None),
        P(AXES),
        P(TOKENS, BATCH, None),
    )
    return jax.shard_map(
        functools.partial(body, dict(mesh.shape)),
        mesh=mesh,
        in_specs=placed,
        out_specs=(
            P(TOKENS, BATCH, None),
            P(TOKENS, BATCH, None),
            P(AXES, None),
            P(AXES),
            P(AXES, None),
            P(AXES),
            P(AXES),
            P(AXES),
            P(AXES),
            P(AXES),
            P(AXES, None),
            P(AXES),
            P(AXES, None),
            P(AXES),
        ),
        check_vma=False,
    )
```

```python
import functools
import math

import jax
import jax.numpy as jnp
import numpy as np
from jax import lax
from jax.experimental import pallas as pl
from jax.experimental.pallas import tpu as pltpu
from jax.sharding import PartitionSpec as P

HD = 64
BATCH, ULY, BLK = "batch", "ulysses", "blk"
AXES = (BATCH, ULY, BLK)
TOKENS = (ULY, BLK)


EPSILON = 1e-05
INV_ROOT_TWO = 0.7071067811865476
INV_ROOT_TWO_PI = 0.3989422804014327


def layer_norm(values):
    center = jnp.mean(values, axis=-1, keepdims=True)
    shifted = values - center
    inverse = lax.rsqrt(jnp.mean(shifted * shifted, axis=-1, keepdims=True) + EPSILON)
    return (shifted * inverse, inverse)


def norm_back(gradient, normed, inverse, gain_vec):
    scaled = gradient * gain_vec
    return inverse * (
        scaled
        - jnp.mean(scaled, axis=-1, keepdims=True)
        - normed * jnp.mean(scaled * normed, axis=-1, keepdims=True)
    )


def gelu_value(pre_values):
    return 0.5 * pre_values * (1.0 + jax.scipy.special.erf(pre_values * INV_ROOT_TWO))


def gelu_slope(pre_values):
    normal_cdf = 0.5 * (1.0 + jax.scipy.special.erf(pre_values * INV_ROOT_TWO))
    return normal_cdf + pre_values * jnp.exp(-0.5 * pre_values * pre_values) * INV_ROOT_TWO_PI


def rotary_tables(positions, rotary):
    half_rot = rotary // 2
    frequency = 1.0 / 10000.0 ** (jnp.arange(half_rot, dtype=jnp.float32) * (2.0 / rotary))
    angles = positions.astype(jnp.float32)[:, None] * frequency[None, :]
    cosine = jnp.concatenate([jnp.cos(angles), jnp.cos(angles)], axis=-1)
    sine_table = jnp.concatenate([jnp.sin(angles), jnp.sin(angles)], axis=-1)
    return (cosine, sine_table)


def expand_table(table, tensor):
    extra_dims = (1,) * (tensor.ndim - 2)
    return table.reshape((table.shape[0],) + extra_dims + (table.shape[1],))


def rotate_fwd(tensor, cosine, sine_table, rotary):
    half_rot = rotary // 2
    cos_full = expand_table(cosine, tensor)
    sin_full = expand_table(sine_table, tensor)
    rot_part = tensor[..., :rotary]
    turned = jnp.concatenate([-rot_part[..., half_rot:], rot_part[..., :half_rot]], axis=-1)
    return jnp.concatenate([rot_part * cos_full + turned * sin_full, tensor[..., rotary:]], axis=-1)


def rotate_back(tensor, cosine, sine_table, rotary):
    half_rot = rotary // 2
    cos_full = expand_table(cosine, tensor)
    sin_full = expand_table(sine_table, tensor)
    rot_part = tensor[..., :rotary]
    weighted = rot_part * sin_full
    turned = jnp.concatenate([weighted[..., half_rot:], -weighted[..., :half_rot]], axis=-1)
    return jnp.concatenate([rot_part * cos_full + turned, tensor[..., rotary:]], axis=-1)


def general_body(
    residual_in,
    qkv_weight,
    qkv_bias,
    dense_weight,
    dense_bias,
    norm1_gain,
    norm1_bias,
    norm2_gain,
    norm2_bias,
    up_weight,
    up_bias,
    down_weight,
    down_bias,
    cotangent,
):
    single = jnp.float32
    half_type = jnp.bfloat16
    gathered = (
        lax.all_gather(qkv_weight, AXES, axis=0, tiled=True),
        lax.all_gather(qkv_bias, AXES, axis=0, tiled=True),
        lax.all_gather(dense_weight, AXES, axis=0, tiled=True),
        lax.all_gather(dense_bias, AXES, axis=0, tiled=True),
        lax.all_gather(norm1_gain, AXES, axis=0, tiled=True),
        lax.all_gather(norm1_bias, AXES, axis=0, tiled=True),
        lax.all_gather(norm2_gain, AXES, axis=0, tiled=True),
        lax.all_gather(norm2_bias, AXES, axis=0, tiled=True),
        lax.all_gather(up_weight, AXES, axis=0, tiled=True),
        lax.all_gather(up_bias, AXES, axis=0, tiled=True),
        lax.all_gather(down_weight, AXES, axis=0, tiled=True),
        lax.all_gather(down_bias, AXES, axis=0, tiled=True),
    )
    (
        w_qkv,
        b_qkv,
        w_dense,
        b_dense,
        gain_one,
        shift_one,
        gain_two,
        shift_two,
        w_up,
        b_up,
        w_down,
        b_down,
    ) = gathered
    tok_rows = residual_in.shape[0]
    seq_count = residual_in.shape[1]
    model_width = residual_in.shape[2]
    head_count = model_width // HD
    rotary = HD // 4
    scale_factor = 1.0 / math.sqrt(HD)
    blk_size = lax.axis_size(BLK)
    uly_size = lax.axis_size(ULY)
    blk_index = lax.axis_index(BLK)
    block_id = lax.axis_index(ULY) * blk_size + blk_index
    seq_pos = block_id * tok_rows + jnp.arange(tok_rows, dtype=jnp.int32)
    inputs_f = residual_in.astype(single)
    normed, inverse = layer_norm(inputs_f)
    act_one = (normed * gain_one.astype(single) + shift_one.astype(single)).astype(half_type)
    act_two = (normed * gain_two.astype(single) + shift_two.astype(single)).astype(half_type)
    qkv_full = jnp.einsum(
        "tsd,df->tsf", act_one, w_qkv, preferred_element_type=single
    ) + b_qkv.astype(single)
    cos_seq, sin_seq = rotary_tables(seq_pos, rotary)
    head_shape = (tok_rows, seq_count, head_count, HD)
    query_seq = (
        rotate_fwd(qkv_full[..., :model_width].reshape(head_shape), cos_seq, sin_seq, rotary)
        .reshape(tok_rows, seq_count, model_width)
        .astype(half_type)
    )
    key_seq = (
        rotate_fwd(
            qkv_full[..., model_width : 2 * model_width].reshape(head_shape),
            cos_seq,
            sin_seq,
            rotary,
        )
        .reshape(tok_rows, seq_count, model_width)
        .astype(half_type)
    )
    value_seq = qkv_full[..., 2 * model_width :].astype(half_type)
    query_loc, key_loc, value_loc = (
        lax.all_to_all(query_seq, ULY, split_axis=2, concat_axis=0, tiled=True),
        lax.all_to_all(key_seq, ULY, split_axis=2, concat_axis=0, tiled=True),
        lax.all_to_all(value_seq, ULY, split_axis=2, concat_axis=0, tiled=True),
    )
    local_rows = query_loc.shape[0]
    features = query_loc.shape[2]
    local_heads = features // HD
    key_all, value_all = (
        lax.all_gather(key_loc, BLK, axis=0, tiled=True),
        lax.all_gather(value_loc, BLK, axis=0, tiled=True),
    )
    total_rows = key_all.shape[0]
    row_ids = jnp.arange(local_rows, dtype=jnp.int32)
    query_pos = (row_ids // tok_rows * blk_size + blk_index) * tok_rows + row_ids % tok_rows
    block_rows = math.gcd(512, local_rows)
    n_blocks = local_rows // block_rows
    query_h = query_loc.reshape(local_rows, seq_count, local_heads, HD)
    key_h = jnp.transpose(
        key_all.reshape(blk_size, uly_size, tok_rows, seq_count, features), (1, 0, 2, 3, 4)
    ).reshape(total_rows, seq_count, local_heads, HD)
    value_h = jnp.transpose(
        value_all.reshape(blk_size, uly_size, tok_rows, seq_count, features), (1, 0, 2, 3, 4)
    ).reshape(total_rows, seq_count, local_heads, HD)
    zero_idx = jnp.zeros((), jnp.int32)
    step_ids = jnp.arange(n_blocks * seq_count, dtype=jnp.int32)
    row_shape = (block_rows, 1, local_heads, HD)

    def select(step_index):
        row_start = step_index // seq_count * block_rows
        seq_index = step_index % seq_count
        query_rows = lax.dynamic_slice(
            query_h, (row_start, seq_index, zero_idx, zero_idx), row_shape
        )
        limit = jnp.max(query_pos) // block_rows + 1
        return (row_start, seq_index, query_rows, query_pos, limit)

    def block_scores(query_rows, row_pos, key_index, seq_index):
        key_start = key_index * block_rows
        slot = (key_start, seq_index, zero_idx, zero_idx)
        key_rows = lax.dynamic_slice(key_h, slot, (block_rows, 1, local_heads, HD))
        value_rows = lax.dynamic_slice(value_h, slot, (block_rows, 1, local_heads, HD))
        scores = (
            jnp.einsum("qshd,kshd->shqk", query_rows, key_rows, preferred_element_type=single)
            * scale_factor
        )
        key_ids = key_start + jnp.arange(block_rows, dtype=jnp.int32)
        allowed = (key_ids[None, :] <= row_pos[:, None])[None, None]
        return (jnp.where(allowed, scores, -jnp.inf), key_rows, value_rows, slot)

    def forward_block(step_index):
        row_start, seq_index, query_rows, row_pos, limit = select(step_index)

        def total_step(key_index, carry):
            running_max, running_sum = carry
            masked, key_rows, value_rows, slot = block_scores(
                query_rows, row_pos, key_index, seq_index
            )
            new_max = jnp.maximum(running_max, jnp.max(masked, axis=-1))
            new_sum = running_sum * jnp.exp(running_max - new_max) + jnp.sum(
                jnp.exp(masked - new_max[..., None]), axis=-1
            )
            return (new_max, new_sum)

        start_max = jnp.full((1, local_heads, block_rows), -jnp.inf, single)
        start_sum = jnp.zeros((1, local_heads, block_rows), single)
        final_max, final_sum = lax.fori_loop(zero_idx, limit, total_step, (start_max, start_sum))
        log_total = final_max + jnp.log(final_sum)

        def value_step(key_index, acc):
            masked, key_rows, value_rows, slot = block_scores(
                query_rows, row_pos, key_index, seq_index
            )
            weights_b = jnp.exp(masked - log_total[..., None]).astype(half_type)
            return acc + jnp.einsum(
                "shqk,kshd->qshd", weights_b, value_rows, preferred_element_type=single
            )

        result = lax.fori_loop(zero_idx, limit, value_step, jnp.zeros(row_shape, single)).astype(
            half_type
        )
        return (result[:, 0], log_total)

    results, log_totals = lax.map(forward_block, step_ids)
    attn_h = jnp.transpose(
        results.reshape(n_blocks, seq_count, block_rows, local_heads, HD), (0, 2, 1, 3, 4)
    ).reshape(local_rows, seq_count, local_heads, HD)
    attn_seq = lax.all_to_all(
        attn_h.reshape(local_rows, seq_count, features),
        ULY,
        split_axis=0,
        concat_axis=2,
        tiled=True,
    )
    proj_out = jnp.einsum(
        "tsd,de->tse", attn_seq, w_dense, preferred_element_type=single
    ) + b_dense.astype(single)
    pre_act = jnp.einsum("tsd,df->tsf", act_two, w_up, preferred_element_type=single) + b_up.astype(
        single
    )
    gelu_out = gelu_value(pre_act).astype(half_type)
    mlp_out = jnp.einsum(
        "tsf,fd->tsd", gelu_out, w_down, preferred_element_type=single
    ) + b_down.astype(single)
    output = (inputs_f + proj_out + mlp_out).astype(half_type)
    back_params = (
        lax.all_gather(qkv_weight, AXES, axis=0, tiled=True),
        lax.all_gather(qkv_bias, AXES, axis=0, tiled=True),
        lax.all_gather(dense_weight, AXES, axis=0, tiled=True),
        lax.all_gather(dense_bias, AXES, axis=0, tiled=True),
        lax.all_gather(norm1_gain, AXES, axis=0, tiled=True),
        lax.all_gather(norm1_bias, AXES, axis=0, tiled=True),
        lax.all_gather(norm2_gain, AXES, axis=0, tiled=True),
        lax.all_gather(norm2_bias, AXES, axis=0, tiled=True),
        lax.all_gather(up_weight, AXES, axis=0, tiled=True),
        lax.all_gather(up_bias, AXES, axis=0, tiled=True),
        lax.all_gather(down_weight, AXES, axis=0, tiled=True),
        lax.all_gather(down_bias, AXES, axis=0, tiled=True),
    )
    back_qkv = back_params[0]
    back_dense = back_params[2]
    back_gain_one = back_params[4].astype(single)
    back_gain_two = back_params[6].astype(single)
    back_up = back_params[8]
    back_down = back_params[10]
    grad_f = cotangent.astype(single)
    bias_sum = jnp.sum(grad_f, axis=(0, 1))
    down_w_grad = jnp.einsum("tsf,tsd->fd", gelu_out, cotangent, preferred_element_type=single)
    gelu_grad = jnp.einsum("tsd,fd->tsf", cotangent, back_down, preferred_element_type=single)
    pre_grad = (gelu_grad * gelu_slope(pre_act)).astype(half_type)
    up_w_grad = jnp.einsum("tsd,tsf->df", act_two, pre_grad, preferred_element_type=single)
    up_b_grad = jnp.sum(pre_grad.astype(single), axis=(0, 1))
    act_two_grad = jnp.einsum("tsf,df->tsd", pre_grad, back_up, preferred_element_type=single)
    gain_two_grad = jnp.sum(act_two_grad * normed, axis=(0, 1))
    shift_two_grad = jnp.sum(act_two_grad, axis=(0, 1))
    dense_w_grad = jnp.einsum("tsd,tse->de", attn_seq, cotangent, preferred_element_type=single)
    attn_grad = jnp.einsum(
        "tse,de->tsd", cotangent, back_dense, preferred_element_type=single
    ).astype(half_type)
    grad_loc = lax.all_to_all(attn_grad, ULY, split_axis=2, concat_axis=0, tiled=True)
    grad_h = grad_loc.reshape(local_rows, seq_count, local_heads, HD)

    def backward_block(acc_pair, step_index):
        row_start, seq_index, query_rows, row_pos, limit = select(step_index)
        own_slot = (row_start, seq_index, zero_idx, zero_idx)
        out_rows = lax.dynamic_slice(attn_h, own_slot, row_shape)
        grad_rows = lax.dynamic_slice(grad_h, own_slot, row_shape)
        log_total = log_totals[step_index]
        delta_row = jnp.transpose(
            jnp.sum(grad_rows.astype(single) * out_rows.astype(single), axis=-1), (1, 2, 0)
        )

        def grad_step(key_index, carry):
            key_acc, value_acc, query_acc = carry
            masked, key_rows, value_rows, slot = block_scores(
                query_rows, row_pos, key_index, seq_index
            )
            probs_f = jnp.exp(masked - log_total[..., None])
            value_part = jnp.einsum(
                "shqk,qshd->kshd",
                probs_f.astype(half_type),
                grad_rows,
                preferred_element_type=single,
            )
            grad_prob = jnp.einsum(
                "qshd,kshd->shqk", grad_rows, value_rows, preferred_element_type=single
            )
            grad_score = (probs_f * (grad_prob - delta_row[..., None]) * scale_factor).astype(
                half_type
            )
            query_acc = query_acc + jnp.einsum(
                "shqk,kshd->qshd", grad_score, key_rows, preferred_element_type=single
            )
            key_part = jnp.einsum(
                "shqk,qshd->kshd", grad_score, query_rows, preferred_element_type=single
            )
            key_acc = lax.dynamic_update_slice(
                key_acc, lax.dynamic_slice(key_acc, slot, key_part.shape) + key_part, slot
            )
            value_acc = lax.dynamic_update_slice(
                value_acc, lax.dynamic_slice(value_acc, slot, value_part.shape) + value_part, slot
            )
            return (key_acc, value_acc, query_acc)

        key_acc, value_acc, query_acc = lax.fori_loop(
            zero_idx, limit, grad_step, (acc_pair[0], acc_pair[1], jnp.zeros(row_shape, single))
        )
        return ((key_acc, value_acc), query_acc[:, 0])

    acc_zero = jnp.zeros((total_rows, seq_count, local_heads, HD), single)
    acc_final, query_parts = lax.scan(backward_block, (acc_zero, acc_zero), step_ids)
    query_grad = jnp.transpose(
        query_parts.reshape(n_blocks, seq_count, block_rows, local_heads, HD), (0, 2, 1, 3, 4)
    ).reshape(local_rows, seq_count, local_heads, HD)
    key_terms = jnp.transpose(
        acc_final[0].reshape(uly_size, blk_size, tok_rows, seq_count, features), (1, 0, 2, 3, 4)
    ).reshape(total_rows, seq_count, features)
    value_terms = jnp.transpose(
        acc_final[1].reshape(uly_size, blk_size, tok_rows, seq_count, features), (1, 0, 2, 3, 4)
    ).reshape(total_rows, seq_count, features)
    key_back, value_back = (
        lax.psum_scatter(key_terms, BLK, scatter_dimension=0, tiled=True),
        lax.psum_scatter(value_terms, BLK, scatter_dimension=0, tiled=True),
    )
    cos_h, sin_h = rotary_tables(query_pos, rotary)
    query_send = (
        rotate_back(query_grad, cos_h, sin_h, rotary)
        .reshape(local_rows, seq_count, features)
        .astype(half_type)
    )
    key_send = (
        rotate_back(key_back.reshape(local_rows, seq_count, local_heads, HD), cos_h, sin_h, rotary)
        .reshape(local_rows, seq_count, features)
        .astype(half_type)
    )
    value_send = value_back.astype(half_type)
    query_ret, key_ret, value_ret = (
        lax.all_to_all(query_send, ULY, split_axis=0, concat_axis=2, tiled=True),
        lax.all_to_all(key_send, ULY, split_axis=0, concat_axis=2, tiled=True),
        lax.all_to_all(value_send, ULY, split_axis=0, concat_axis=2, tiled=True),
    )
    qkv_grad = jnp.concatenate([query_ret, key_ret, value_ret], axis=-1)
    qkv_w_grad = jnp.einsum("tsd,tsf->df", act_one, qkv_grad, preferred_element_type=single)
    qkv_b_grad = jnp.sum(qkv_grad.astype(single), axis=(0, 1))
    act_one_grad = jnp.einsum("tsf,df->tsd", qkv_grad, back_qkv, preferred_element_type=single)
    gain_one_grad = jnp.sum(act_one_grad * normed, axis=(0, 1))
    shift_one_grad = jnp.sum(act_one_grad, axis=(0, 1))
    input_grad = (
        grad_f
        + norm_back(act_one_grad, normed, inverse, back_gain_one)
        + norm_back(act_two_grad, normed, inverse, back_gain_two)
    )
    summed = (
        lax.psum_scatter(qkv_w_grad, AXES, scatter_dimension=0, tiled=True),
        lax.psum_scatter(qkv_b_grad, AXES, scatter_dimension=0, tiled=True),
        lax.psum_scatter(
            dense_w_grad, AXES, scatter_dimension=0, tiled=True
        ),
        lax.psum_scatter(bias_sum, AXES, scatter_dimension=0, tiled=True),
        lax.psum_scatter(
            gain_one_grad, AXES, scatter_dimension=0, tiled=True
        ),
        lax.psum_scatter(
            shift_one_grad, AXES, scatter_dimension=0, tiled=True
        ),
        lax.psum_scatter(
            gain_two_grad, AXES, scatter_dimension=0, tiled=True
        ),
        lax.psum_scatter(
            shift_two_grad, AXES, scatter_dimension=0, tiled=True
        ),
        lax.psum_scatter(up_w_grad, AXES, scatter_dimension=0, tiled=True),
        lax.psum_scatter(up_b_grad, AXES, scatter_dimension=0, tiled=True),
        lax.psum_scatter(down_w_grad, AXES, scatter_dimension=0, tiled=True),
        lax.psum_scatter(bias_sum, AXES, scatter_dimension=0, tiled=True),
    )
    return (
        output,
        input_grad,
        summed[0],
        summed[1],
        summed[2],
        summed[3],
        summed[4],
        summed[5],
        summed[6],
        summed[7],
        summed[8],
        summed[9],
        summed[10],
        summed[11],
    )


MESH = pl.DeviceIdType.MESH


class Place:
    def __init__(self, planes):
        self.planes = planes
        self.b = lax.axis_index(BATCH)
        self.u = lax.axis_index(ULY)
        k = lax.axis_index(BLK)
        self.y, self.c = k // 2, k % 2
        self.t = self.u * 4 + k
        self.xn, self.yn, self.pn = self.peer(4), self.peer(2), self.peer(1)

    def rank(self, d):
        u = 1 - self.u if d & 4 else self.u
        y = 1 - self.y if d & 2 else self.y
        c = 1 - self.c if d & 1 else self.c
        return u * 4 + y * 2 + c

    def chip(self, d):
        return self.rank(d) // 2

    def peer(self, d):
        u = 1 - self.u if d & 4 else self.u
        y = 1 - self.y if d & 2 else self.y
        c = 1 - self.c if d & 1 else self.c
        return {BATCH: self.b, ULY: u, BLK: y * 2 + c}

    def along(self, step):
        return {BATCH: self.b + step, ULY: self.u, BLK: self.y * 2 + self.c}

    def barrier(self):
        sem = pltpu.get_barrier_semaphore()
        for d in range(1, 8):
            pl.semaphore_signal(sem, inc=1, device_id=self.peer(d), device_id_type=MESH)
        self.to_neighbours(
            lambda step: pl.semaphore_signal(
                sem, inc=1, device_id=self.along(step), device_id_type=MESH
            )
        )
        below = (self.b > 0).astype(jnp.int32)
        above = (self.b < self.planes - 1).astype(jnp.int32)
        pl.semaphore_wait(sem, 7 + below + above)

    def to_neighbours(self, action):
        for step in (-1, 1):

            @pl.when(self.b > 0 if step < 0 else self.b < self.planes - 1)
            def _():
                action(step)

    def reach(self, second, third):
        b, last = self.b, self.planes - 1

        @pl.when((b > 0) & (b < last))
        def _():
            for step in (-1, 1):
                pl.semaphore_signal(
                    second, inc=1, device_id=self.along(step), device_id_type=MESH
                )

        pl.semaphore_wait(second, (b >= 2).astype(jnp.int32) + (b <= last - 2).astype(jnp.int32))
        for middle, step in ((1, -1), (2, 1)):

            @pl.when(b == middle)
            def _():
                pl.semaphore_signal(third, inc=1, device_id=self.along(step), device_id_type=MESH)

        @pl.when((b == 0) | (b == last))
        def _():
            pl.semaphore_wait(third, 1)


class Mail:
    def __init__(self, send, recv, near):
        self.send, self.recv, self.near = send, recv, near
        self.sends = self.recvs = self.nears = 0

    def send_slots(self, n=1):
        self.sends += n
        return self.sends - n

    def recv_slots(self, n=1):
        self.recvs += n
        return self.recvs - n

    def bring(self, src, dst):
        made = pltpu.make_async_copy(src, dst, self.near.at[self.nears])
        self.nears += 1
        made.start()
        return made

    def copy(self, src, dst, send, recv, device):
        return pltpu.make_async_remote_copy(
            src_ref=src,
            dst_ref=dst,
            send_sem=self.send.at[send],
            recv_sem=self.recv.at[recv],
            device_id=device,
            device_id_type=MESH,
        )

    def arrived(self, bulk, recv, device):
        self.copy(bulk, bulk, 0, recv, device).wait_recv()

    def gone(self, bulk, send, device):
        self.copy(bulk, bulk, send, 0, device).wait_send()


class PlaneGather:
    def __init__(self, at, mail, shard, whole):
        self.at, self.mail, self.shard, self.whole = at, mail, shard, whole
        self.rows = shard.shape[1]
        self.halves = shard.shape[0] // 2
        self.send, self.recv = mail.send_slots(), mail.recv_slots(5)

    def half(self, i):
        return self.shard.at[pl.ds(i * self.halves, self.halves)]

    def block(self, d, half=None):
        rows = pl.ds(pl.multiple_of(self.at.rank(d) * self.rows, self.rows), self.rows)
        if half is None:
            return self.whole.at[:, rows, :]
        return self.whole.at[pl.ds(half * self.halves, self.halves), rows, :]

    def bulk(self, shards):
        return self.whole.at[:, pl.ds(0, shards * self.rows), :]

    def post(self, src, dst, recv, device):
        self.mail.copy(src, dst, self.send, self.recv + recv, device).start()

    def arrived(self, bulk, recv, device):
        self.mail.arrived(bulk, self.recv + recv, device)

    def start(self):
        at = self.at
        self.post(self.half(1), self.block(0, 1), 0, at.xn)
        self.post(self.half(0), self.block(0, 0), 1, at.yn)
        self.post(self.half(0), self.block(0, 0), 2, at.xn)
        self.post(self.half(1), self.block(0, 1), 2, at.yn)
        self.post(self.shard, self.block(0), 4, at.pn)
        self.own = self.mail.bring(self.shard, self.block(0))

    def relay_y(self):
        self.arrived(self.block(2, 0), 1, self.at.yn)
        self.post(self.block(2, 0), self.block(2, 0), 3, self.at.xn)

    def relay_x(self):
        self.arrived(self.block(4, 1), 0, self.at.xn)
        self.post(self.block(4, 1), self.block(4, 1), 3, self.at.yn)

    def share(self):
        self.arrived(self.bulk(1), 2, self.at.xn)
        self.post(self.block(2), self.block(2), 4, self.at.pn)
        self.post(self.block(4), self.block(4), 4, self.at.pn)

    def far(self):
        self.arrived(self.block(6), 3, self.at.xn)
        self.post(self.block(6), self.block(6), 4, self.at.pn)

    def finish(self):
        self.arrived(self.bulk(4), 4, self.at.pn)
        self.own.wait()

    def close(self):
        self.mail.gone(self.bulk(7), self.send, self.at.pn)


class LineGather:
    def __init__(self, at, mail, held, first=0, count=None):
        self.at, self.mail, self.held = at, mail, held
        self.rows = pl.ds(first, held.shape[1] - first if count is None else count)
        self.send, self.recv = mail.send_slots(2), mail.recv_slots(at.planes)

    def part(self, slot):
        return self.held.at[slot, self.rows]

    def pass_on(self, slot, src=None):
        at = self.at
        part = self.part(slot)
        src = part if src is None else src.at[self.rows]

        @pl.when((slot <= at.b) & (at.b < at.planes - 1))
        def _():
            self.mail.copy(src, part, self.send, self.recv + slot, at.along(1)).start()

        @pl.when((slot >= at.b) & (at.b > 0))
        def _():
            self.mail.copy(src, part, self.send + 1, self.recv + slot, at.along(-1)).start()

    def start(self, src=None):
        self.pass_on(self.at.b, src)

    def take(self, distance):
        at = self.at

        @pl.when(at.b >= distance)
        def _():
            slot = at.b - distance
            self.mail.arrived(self.part(slot), self.recv + slot, at.along(-1))
            self.pass_on(slot)

        @pl.when(at.b + distance < at.planes)
        def _():
            slot = at.b + distance
            self.mail.arrived(self.part(slot), self.recv + slot, at.along(1))
            self.pass_on(slot)

    def close(self):
        at = self.at
        for b in range(at.planes):

            @pl.when(at.b == b)
            def _():
                if b < at.planes - 1:
                    bulk = self.held.at[pl.ds(0, b + 1), self.rows]
                    self.mail.gone(bulk, self.send, at.along(1))
                if b > 0:
                    bulk = self.held.at[pl.ds(0, at.planes - b), self.rows]
                    self.mail.gone(bulk, self.send + 1, at.along(-1))


class StarGather:
    def __init__(self, at, mail, held):
        self.at, self.mail, self.held = at, mail, held
        self.send, self.recv = mail.send_slots(), mail.recv_slots()

    def start(self):
        at = self.at
        part = self.held.at[at.b]
        for step in range(1, at.planes):

            @pl.when(at.b + step < at.planes)
            def _():
                self.mail.copy(part, part, self.send, self.recv, at.along(step)).start()

            @pl.when(at.b >= step)
            def _():
                self.mail.copy(part, part, self.send, self.recv, at.along(-step)).start()

    def bulk(self):
        return self.held.at[pl.ds(0, self.at.planes - 1)]

    def finish(self):
        self.mail.arrived(self.bulk(), self.recv, self.at.pn)

    def close(self):
        self.mail.gone(self.bulk(), self.send, self.at.pn)


class PlaneExchange:
    def __init__(self, at, mail, pieces, landings, bulk):
        self.at, self.mail, self.bulk = at, mail, bulk
        self.pieces, self.landings = pieces, landings
        self.send, self.recv = mail.send_slots(), mail.recv_slots()

    def start(self):
        at = self.at
        for d in range(1, 8):
            for piece, landing in zip(self.pieces(at.rank(d)), self.landings(at.t)):
                self.mail.copy(piece, landing, self.send, self.recv, at.peer(d)).start()
        self.own = [
            self.mail.bring(piece, landing)
            for piece, landing in zip(self.pieces(at.t), self.landings(at.t))
        ]

    def finish(self):
        self.mail.arrived(self.bulk, self.recv, self.at.pn)
        for own in self.own:
            own.wait()

    def close(self):
        self.mail.gone(self.bulk, self.send, self.at.pn)


class PairExchange:
    def __init__(self, at, mail, src, dst, landed):
        self.at, self.mail, self.src, self.dst, self.landed = at, mail, src, dst, landed
        self.send, self.recv = mail.send_slots(), mail.recv_slots()

    def start(self):
        self.mail.copy(self.src, self.dst, self.send, self.recv, self.at.pn).start()

    def finish(self):
        self.mail.arrived(self.landed, self.recv, self.at.pn)

    def close(self):
        self.mail.gone(self.src, self.send, self.at.pn)


class PlaneReduce:
    def __init__(self, at, mail, terms, pairs, sums, side, bulk):
        self.at, self.mail, self.terms, self.bulk = at, mail, terms, bulk
        self.pairs, self.sums, self.side = pairs, sums, side
        self.send, self.recv = mail.send_slots(), mail.recv_slots(5)
        self.halves = terms.shape[0] // 2

    def post(self, src, dst, recv, device):
        self.mail.copy(src, dst, self.send, self.recv + recv, device).start()

    def start(self):
        at = self.at
        for d in (6, 4, 2, 0):
            chip = at.chip(d)
            self.post(
                self.terms.at[:, chip, 1 - at.c], self.pairs.at[:, chip], 0 if d == 6 else 1, at.pn
            )

    def half(self, ref, i):
        return ref.at[pl.ds(i * self.halves, self.halves)]

    def add_pair(self, d):
        chip = self.at.chip(d)
        total = self.terms[:, chip, self.at.c].astype(jnp.float32) + self.pairs[:, chip].astype(
            jnp.float32
        )
        self.sums[:, chip] = total.astype(self.sums.dtype)

    def fold(self):
        at = self.at
        far = self.sums.at[:, at.chip(6)]
        self.mail.arrived(self.bulk(1), self.recv, at.pn)
        self.add_pair(6)
        self.post(self.half(far, 0), self.half(self.side.at[0], 0), 2, at.xn)
        self.post(self.half(far, 1), self.half(self.side.at[0], 1), 3, at.yn)
        self.mail.arrived(self.bulk(3), self.recv + 1, at.pn)
        for d in (4, 2, 0):
            self.add_pair(d)

    def turn(self):
        at = self.at
        for i, d, other, recv, nbr in ((1, 4, at.yn, 3, at.xn), (0, 2, at.xn, 2, at.yn)):
            landed = self.half(self.side.at[0], i)
            self.mail.arrived(landed, self.recv + recv, other)
            whole = self.sums.at[:, at.chip(d)]
            part = self.half(whole, i)
            part[...] = (part[...].astype(jnp.float32) + landed[...].astype(jnp.float32)).astype(
                self.sums.dtype
            )
            self.post(whole, self.side.at[2 - i], 4, nbr)

    def finish(self):
        self.mail.arrived(self.bulk(2), self.recv + 4, self.at.xn)
        return (
            self.sums[:, self.at.chip(0)].astype(jnp.float32)
            + self.side[1].astype(jnp.float32)
            + self.side[2].astype(jnp.float32)
        )

    def close(self):
        self.mail.gone(self.bulk(7), self.send, self.at.pn)


class LineReduce:
    def __init__(self, at, mail, terms, above, below, up_cut=None, down_cut=None):
        self.at, self.mail, self.terms = at, mail, terms
        self.above, self.below = above, below
        whole = pl.ds(0, terms.shape[2])
        self.up_cut, self.down_cut = up_cut or whole, down_cut or whole
        self.send, self.recv = mail.send_slots(2), mail.recv_slots(at.planes + 1)

    def upward(self, src, slot):
        return self.mail.copy(
            src.at[slot, :, self.up_cut],
            self.below.at[slot, :, self.up_cut],
            self.send,
            self.recv + slot,
            self.at.along(1),
        )

    def downward(self, src, slot, last_step):
        return self.mail.copy(
            src.at[slot, :, self.down_cut],
            self.above.at[slot, :, self.down_cut],
            self.send + 1,
            self.recv + (self.at.planes if last_step else slot),
            self.at.along(-1),
        )

    def edge(self, slot):
        at, last = self.at, self.at.planes - 1
        if slot == 0:
            return

        @pl.when(at.b == 0)
        def _():
            self.upward(self.terms, slot).start()

        @pl.when(at.b == last)
        def _():
            self.downward(self.terms, last - slot, slot == 1).start()

    def hop(self, hop, rank):
        at, mail, last = self.at, self.mail, self.at.planes - 1
        slot = last - rank
        if slot <= hop:
            return

        @pl.when(at.b == hop)
        def _():
            cut = self.up_cut
            mail.arrived(self.below.at[slot, :, cut], self.recv + slot, at.along(-1))
            self.add(self.below, slot, cut)
            self.upward(self.below, slot).start()

        @pl.when(at.b == last - hop)
        def _():
            cut = self.down_cut
            mail.arrived(self.above.at[rank, :, cut], self.recv + rank, at.along(1))
            self.add(self.above, rank, cut)
            self.downward(self.above, rank, rank == last - hop - 1).start()

    def add(self, held, slot, cut):
        total = self.terms[slot, :, cut].astype(jnp.float32) + held[slot, :, cut].astype(
            jnp.float32
        )
        held[slot, :, cut] = total.astype(held.dtype)

    def landed(self):
        at, mail = self.at, self.mail

        @pl.when(at.b > 0)
        def _():
            mail.arrived(self.below.at[at.b, :, self.up_cut], self.recv + at.b, at.along(-1))

        @pl.when(at.b < at.planes - 1)
        def _():
            bulk = self.above.at[at.b, :, self.down_cut]
            mail.arrived(bulk, self.recv + at.planes, at.along(1))

    def total(self, out):
        b, last = self.at.b, self.at.planes - 1

        def put(*parts):
            value = self.terms[b].astype(jnp.float32)
            for part in parts:
                value = value + part[b].astype(jnp.float32)
            out[...] = value.astype(out.dtype)

        @pl.when(b == 0)
        def _():
            put(self.above)

        @pl.when(b == last)
        def _():
            put(self.below)

        @pl.when((b > 0) & (b < last))
        def _():
            put(self.below, self.above)

    def close(self):
        at, last = self.at, self.at.planes - 1
        for b in range(at.planes):

            @pl.when(at.b == b)
            def _():
                if b < last:
                    bulk = self.terms.at[pl.ds(0, last - b), :, self.up_cut]
                    self.mail.gone(bulk, self.send, at.along(1))
                if b > 0:
                    bulk = self.terms.at[pl.ds(0, b), :, self.down_cut]
                    self.mail.gone(bulk, self.send + 1, at.along(-1))


TILE = 256
LANES = 128


def dot_nn(a, b):
    return lax.dot_general(a, b, (((1,), (0,)), ((), ())), preferred_element_type=jnp.float32)


def dot_nt(a, b):
    return lax.dot_general(a, b, (((1,), (1,)), ((), ())), preferred_element_type=jnp.float32)


def dot_tn(a, b):
    return lax.dot_general(a, b, (((0,), (0,)), ((), ())), preferred_element_type=jnp.float32)


def turn(value, tables, rows, sign):
    straight, early, late = (table[rows, :] for table in tables)
    ahead = pltpu.roll(value, LANES - HD // 8, 1)
    behind = pltpu.roll(value, HD // 8, 1)
    return value * straight + sign * (ahead * early + behind * late)


def of_head(value, head):
    lane = lax.broadcasted_iota(jnp.int32, value.shape, 1)
    return jnp.where(lane // HD == head, value, jnp.zeros_like(value))


def total_rows(value):
    return jnp.sum(value, axis=0, keepdims=True)


class Layer:
    def __init__(self, refs):
        self.__dict__.update(refs)
        self.heads = LANES // HD
        if "xa" in refs:
            self.seqs, self.length, self.width = self.xa.shape
            self.per_seq = self.length // TILE
            self.tiles = self.seqs * self.per_seq

    def rows(self, tile):
        return pl.ds(pl.multiple_of(tile * TILE, TILE), TILE)

    def in_seq(self, ref, tile):
        rows = pl.ds(pl.multiple_of(tile % self.per_seq * TILE, TILE), TILE)
        return ref[tile // self.per_seq, rows, :]

    def loop(self, count, step):
        def run(i, carry):
            step(i)
            return carry

        lax.fori_loop(0, count, run, 0)

    def wide(self, row):
        planes = self.va.shape[0]
        return jnp.concatenate(
            [self.va[b, pl.ds(2 * row + a, 1), :] for b in range(planes) for a in range(2)], axis=1
        )

    def own_vectors(self, rank):
        lane = lax.broadcasted_iota(jnp.int32, (2, LANES), 1)
        row = lax.broadcasted_iota(jnp.int32, (2, LANES), 0)
        for j, ref in enumerate(self.vectors):
            piece = ref[...].astype(jnp.float32).reshape(1, ref.shape[0])
            piece = jnp.concatenate([piece] * (LANES // ref.shape[0]), axis=1)
            here = (lane // ref.shape[0] == rank % 4) & (row == rank // 4)
            self.vec_s[2 * j : 2 * j + 2, :] = jnp.where(here, jnp.broadcast_to(piece, here.shape), 0.0)
        bias = self.b_qkv[...].astype(jnp.float32).reshape(1, self.b_qkv.shape[0])
        self.vec_s[12:13, :] = jnp.concatenate(
            [bias, jnp.zeros((1, LANES - bias.shape[1]), jnp.float32)], axis=1
        )
        self.vec_s[13:14, :] = self.b_up[...].astype(jnp.float32).reshape(1, LANES)

    def plane_vectors(self, slot):
        total = jnp.sum(self.vec_in[...], axis=0)
        self.va[slot, 0:16, :] = total
        for rank in range(self.vec_in.shape[0]):
            self.va[slot, 16 + rank : 17 + rank, :] = self.vec_in[rank, 12:13, :]
            self.va[slot, 24 + rank : 25 + rank, :] = self.vec_in[rank, 13:14, :]

    def sort_weight(self):
        rows = self.wq_raw.shape[0]
        low = lax.broadcasted_iota(jnp.int32, (rows, LANES), 1) < HD
        for part in range(3):
            for core in range(2):
                for pair in range(2):
                    first, second = (
                        self.wq_raw[
                            :, pl.ds(part * self.width + (core * 2 + j) * 4 * HD + pair * LANES, LANES)
                        ].astype(jnp.float32)
                        for j in range(2)
                    )
                    cut = slice(part * LANES, (part + 1) * LANES)
                    self.wq_s[4 * pair + core, :, cut] = jnp.where(
                        low, first, pltpu.roll(second, HD, 1)
                    ).astype(jnp.bfloat16)
                    self.wq_s[4 * pair + 2 + core, :, cut] = jnp.where(
                        low, pltpu.roll(first, HD, 1), second
                    ).astype(jnp.bfloat16)

    def statistics(self):
        def step(i):
            x = self.in_seq(self.xa, i).astype(jnp.float32)
            center = jnp.mean(x, axis=1, keepdims=True)
            shifted = x - center
            spread = jnp.mean(shifted * shifted, axis=1, keepdims=True)
            self.center[self.rows(i), :] = center
            self.inverse[self.rows(i), :] = lax.rsqrt(spread + EPSILON)

        self.loop(self.tiles, step)

    def normed(self, i):
        x = self.in_seq(self.xa, i).astype(jnp.float32)
        return (x - self.center[self.rows(i), :]) * self.inverse[self.rows(i), :]

    def activations(self):
        gain_one, shift_one, gain_two, shift_two = (self.wide(j) for j in (1, 2, 3, 4))

        def step(i):
            normed = self.normed(i)
            self.act_one[self.rows(i), :] = (normed * gain_one + shift_one).astype(jnp.bfloat16)
            self.act_two[self.rows(i), :] = (normed * gain_two + shift_two).astype(jnp.bfloat16)

        self.loop(self.tiles, step)

    def qkv_bias(self, rank):
        size = HD // 2
        held = self.b_qkv.shape[0] // size
        ranks = self.vec_in.shape[0]
        pieces = []
        for i in range(3 * LANES // size):
            part, j, half = i // 4, i // 2 % 2, i % 2
            head = (rank % 2 * 2 + j) * 4 + rank // 2
            index = part * (self.width // size) + head * 2 + half
            owner, spot = index // held, index % held
            row = self.va[owner // ranks, pl.ds(16 + owner % ranks, 1), :]
            pieces.append(
                sum(
                    jnp.where(spot == k, row[:, k * size : (k + 1) * size], 0.0)
                    for k in range(held)
                )
            )
        return jnp.concatenate(pieces, axis=1)

    def up_bias(self, rank):
        return jnp.concatenate(
            [self.va[b, pl.ds(24 + rank, 1), :] for b in range(self.va.shape[0])], axis=1
        )

    def near(self, ref, side):
        both = ref[pl.ds(side * 2, 2)]
        return both.reshape(both.shape[0] * both.shape[1], both.shape[2])

    def half_columns(self, side, width):
        return pl.ds(pl.multiple_of(side * (width // 2), width // 2), width // 2)

    def project_near(self, side):
        def step(i):
            cut = self.half_columns(side, self.width)
            self.qkv[self.rows(i), :] = dot_nn(self.act_one[self.rows(i), cut], self.near(self.wq, side))

        self.loop(self.tiles, step)

    def project(self, rank, side):
        bias = self.qkv_bias(rank)

        def step(i):
            cut = self.half_columns(side, self.width)
            qkv = dot_nn(self.act_one[self.rows(i), cut], self.near(self.wq, side))
            qkv = qkv + self.qkv[self.rows(i), :] + bias
            rows = pl.ds(pl.multiple_of(i % self.per_seq * TILE, TILE), TILE)
            query = turn(qkv[:, :LANES], self.tables, rows, 1.0).astype(jnp.bfloat16)
            self.query[self.rows(i), :] = query * jnp.asarray(1.0 / math.sqrt(HD), jnp.bfloat16)
            self.key[self.rows(i), :] = turn(
                qkv[:, LANES : 2 * LANES], self.tables, rows, 1.0
            ).astype(jnp.bfloat16)
            self.value[self.rows(i), :] = qkv[:, 2 * LANES :].astype(jnp.bfloat16)

        self.loop(self.tiles, step)

    def keys(self, seq, block):
        start = pl.multiple_of(seq * self.length, TILE)
        return pl.ds(start, (block + 1) * TILE)

    def attend(self, seq):
        for block in range(self.per_seq):
            rows = self.rows(seq * self.per_seq + block)
            keys = self.keys(seq, block)
            key, value, query = self.key[keys, :], self.value[keys, :], self.query[rows, :]
            out = None
            for head in range(self.heads):
                scores = dot_nt(of_head(query, head), key)
                at = lax.broadcasted_iota(jnp.int32, scores.shape, 0) + block * TILE
                to = lax.broadcasted_iota(jnp.int32, scores.shape, 1)
                scores = jnp.where(to <= at, scores, -jnp.inf)
                top = jnp.max(scores, axis=1, keepdims=True)
                weight = jnp.exp(scores - top)
                weight = weight * (1.0 / jnp.sum(weight, axis=1, keepdims=True))
                self.probs[block][seq * self.heads + head] = weight
                part = dot_nn(weight.astype(jnp.bfloat16), value)
                out = of_head(part, head) if out is None else out + of_head(part, head)
            self.attn[rows, :] = out.astype(jnp.bfloat16)

    def attend_out_grad(self):
        def step(i):
            weight = self.wo2[...].reshape(LANES, self.width)
            self.attn_grad[self.rows(i), :] = dot_nt(self.in_seq(self.ca, i), weight).astype(
                jnp.bfloat16
            )

        self.loop(self.tiles, step)

    def attend_grad(self, seq):
        key_grad, value_grad = [None] * self.per_seq, [None] * self.per_seq
        start = seq * self.per_seq
        for block in range(self.per_seq):
            rows = self.rows(start + block)
            keys = self.keys(seq, block)
            key, value, query = self.key[keys, :], self.value[keys, :], self.query[rows, :]
            grad = self.attn_grad[rows, :]
            inner = grad.astype(jnp.float32) * self.attn[rows, :].astype(jnp.float32)
            query_grad = None
            for head in range(self.heads):
                own_grad = of_head(grad, head)
                delta = jnp.sum(of_head(inner, head), axis=1, keepdims=True)
                probs = self.probs[block][seq * self.heads + head]
                grad_prob = dot_nt(own_grad, value)
                grad_score = (probs * (grad_prob - delta)).astype(jnp.bfloat16)
                part = dot_nn(grad_score, of_head(key, head))
                query_grad = part if query_grad is None else query_grad + part
                key_part = dot_tn(grad_score, of_head(query, head))
                value_part = dot_tn(probs.astype(jnp.bfloat16), own_grad)
                for b in range(block + 1):
                    cut = slice(b * TILE, (b + 1) * TILE)
                    key_grad[b] = key_part[cut] if key_grad[b] is None else key_grad[b] + key_part[cut]
                    value_grad[b] = (
                        value_part[cut] if value_grad[b] is None else value_grad[b] + value_part[cut]
                    )
            back = pl.ds(block * TILE, TILE)
            self.qkv_grad[rows, :LANES] = turn(
                query_grad * (1.0 / math.sqrt(HD)), self.tables, back, -1.0
            ).astype(jnp.bfloat16)
        for block in range(self.per_seq):
            rows = self.rows(start + block)
            back = pl.ds(block * TILE, TILE)
            self.qkv_grad[rows, LANES : 2 * LANES] = turn(
                key_grad[block], self.tables, back, -1.0
            ).astype(jnp.bfloat16)
            self.qkv_grad[rows, 2 * LANES :] = value_grad[block].astype(jnp.bfloat16)

    def cot_flat(self):
        return self.ca[...].reshape(self.seqs * self.length, self.width)

    def qkv_weight_grad(self, i):
        rows = self.gq.shape[1]
        act = self.act_one[:, pl.ds(pl.multiple_of(i * rows, rows), rows)]
        self.gq[i] = dot_tn(act, self.qkv_grad[...]).astype(jnp.bfloat16)

    def dense_weight_grad(self):
        self.go[...] = (
            dot_tn(self.attn[...], self.cot_flat()).astype(jnp.bfloat16).reshape(self.go.shape)
        )

    def expand_near(self, side):
        def step(i):
            cut = self.half_columns(side, self.width)
            self.slope[self.rows(i), :] = dot_nn(
                self.act_two[self.rows(i), cut], self.near(self.wu, side)
            )

        self.loop(self.tiles, step)

    def expand(self, rank, side):
        bias = self.up_bias(rank)

        def step(i):
            cut = self.half_columns(side, self.width)
            pre = dot_nn(self.act_two[self.rows(i), cut], self.near(self.wu, side))
            pre = pre + self.slope[self.rows(i), :] + bias
            cdf = 0.5 * (1.0 + lax.erf(pre * INV_ROOT_TWO))
            self.gelu[self.rows(i), :] = (pre * cdf).astype(jnp.bfloat16)
            self.slope[self.rows(i), :] = cdf + pre * jnp.exp(-0.5 * pre * pre) * INV_ROOT_TWO_PI

        self.loop(self.tiles, step)

    def down_weight_grad(self, i):
        depth = self.gd.shape[1]
        part = self.gelu[:, pl.ds(pl.multiple_of(i * depth, depth), depth)]
        self.gd[i] = dot_tn(part, self.cot_flat()).astype(jnp.bfloat16)

    def hidden_grad(self, side):
        def step(i):
            cut = self.half_columns(side, self.hidden)
            grad = dot_nt(self.in_seq(self.ca, i), self.near(self.wd, side))
            self.pre_grad[self.rows(i), cut] = (grad * self.slope[self.rows(i), cut]).astype(
                jnp.bfloat16
            )

        self.loop(self.tiles, step)

    def up_weight_grad(self, i, side):
        rows = self.gu.shape[1]
        act = self.act_two[:, pl.ds(pl.multiple_of(i * rows, rows), rows)]
        cut = self.half_columns(side, self.hidden)
        self.gu[i, :, cut] = dot_tn(act, self.pre_grad[:, cut]).astype(jnp.bfloat16)

    def put_terms(self, terms, i, value):
        seq, chips, cores, rows, width = terms.shape
        n = TILE // (cores * rows)
        terms[i // self.per_seq, pl.ds(i % self.per_seq * n, n)] = value.astype(
            jnp.bfloat16
        ).reshape(n, cores, rows, width)

    def out_terms(self, i):
        dense = self.wo2[...].reshape(LANES, self.width)
        down = self.wd[...].reshape(self.hidden, self.width)
        self.put_terms(
            self.po,
            i,
            dot_nn(self.attn[self.rows(i), :], dense) + dot_nn(self.gelu[self.rows(i), :], down),
        )

    def in_terms(self, i):
        gain_one, gain_two = self.wide(1), self.wide(3)
        normed = self.normed(i)
        weight = self.wq[...].reshape(self.width, 3 * LANES)
        one = dot_nt(self.qkv_grad[self.rows(i), :], weight)
        weight = self.wu[...].reshape(self.width, self.hidden)
        two = dot_nt(self.pre_grad[self.rows(i), :], weight)
        self.put_terms(self.pg, i, one * gain_one + two * gain_two)
        for j, value in enumerate((one * normed, one, two * normed, two)):
            if i == 0:
                self.sums[j : j + 1, :] = total_rows(value)
            else:
                self.sums[j : j + 1, :] += total_rows(value)

    def split(self, raw, own):
        for seq in range(own.shape[0]):
            own[seq] = raw[:, seq, :]

    def own_rows(self, ref, rank):
        rows = self.out.shape[0]
        return ref[:, pl.ds(pl.multiple_of(rank * rows, rows), rows), :].astype(jnp.float32)

    def small_terms(self, rank):
        ranks = self.sm.shape[0]
        cot = total_rows(jnp.sum(self.own_rows(self.ca, rank), axis=0))
        for to in range(ranks):
            cut = slice(to * LANES, (to + 1) * LANES)
            self.sm[to, 0:1, :] = cot[:, cut]
            self.sm[to, 1:5, :] = self.sums[0:4, cut]

    def small_plane(self, slot):
        total = jnp.sum(self.sm_in[...], axis=0)
        self.vz[slot, 0:8, :] = total
        qkv = total_rows(self.qkv_grad[...].astype(jnp.float32))
        pre = total_rows(self.pre_grad[...].astype(jnp.float32))
        for j in range(3):
            self.vz[slot, 8 + j : 9 + j, :] = qkv[:, j * LANES : (j + 1) * LANES]
        for j in range(self.hidden // LANES):
            self.vz[slot, 12 + j : 13 + j, :] = pre[:, j * LANES : (j + 1) * LANES]

    def result(self, rank, out_sum, in_sum):
        x = self.own_rows(self.xa, rank)
        center = jnp.mean(x, axis=2, keepdims=True)
        shifted = x - center
        inverse = lax.rsqrt(jnp.mean(shifted * shifted, axis=2, keepdims=True) + EPSILON)
        normed = shifted * inverse
        bias = (self.wide(0) + self.wide(5))[None]
        value = (x + out_sum + bias).astype(jnp.bfloat16)
        grad = self.own_rows(self.ca, rank) + inverse * (
            in_sum
            - jnp.mean(in_sum, axis=2, keepdims=True)
            - normed * jnp.mean(in_sum * normed, axis=2, keepdims=True)
        )
        for seq in range(x.shape[0]):
            self.out[:, seq, :] = value[seq]
            self.in_grad[:, seq, :] = grad[seq]


SEND_SLOTS, RECV_SLOTS, NEAR_SLOTS = 37, 80, 22


def layer_kernel(names, planes, *refs):
    refs = dict(zip(names, refs))
    send, recv, near, second, third = (refs.pop(name) for name in names[-5:])
    refs.update(
        tables=tuple(refs["table"].at[i] for i in range(3)),
        probs=tuple(refs[name] for name in names if name.startswith("probs")),
        vectors=tuple(refs[name] for name in names if name.startswith("vector")),
        hidden=refs["gelu"].shape[1],
    )
    do = Layer(refs)
    at = Place(planes)
    mail = Mail(send, recv, near)
    b, c = at.b, at.c
    rows = do.wq_s.shape[1]
    pair = planes // 2
    others = pl.ds(0, 7)

    def shards(n):
        return do.xa.at[:, pl.ds(0, n * do.x_own.shape[1]), :]

    def strip(whole):
        return lambda rank: [whole.at[b, pl.ds(pl.multiple_of(rank * rows, rows), rows), :]]

    def band(whole):
        return lambda rank: [whole.at[pl.ds(pl.multiple_of(rank * rows, rows), rows), :]]

    def up_pieces(rank):
        return [
            do.wu_s.at[:, pl.ds(pl.multiple_of((p * 8 + rank) * LANES, LANES), LANES)]
            for p in range(planes)
        ]

    def up_landings(rank):
        strip_rows = pl.ds(pl.multiple_of(rank * rows, rows), rows)
        return [do.wu.at[b, strip_rows, pl.ds(p * LANES, LANES)] for p in range(planes)]

    gather_x = PlaneGather(at, mail, do.x_own, do.xa)
    gather_c = PlaneGather(at, mail, do.cot_own, do.ca)
    line_v, line_o = StarGather(at, mail, do.va), LineGather(at, mail, do.wo)
    line_q = LineGather(at, mail, do.wq)
    half = do.wu.shape[1] // 2
    line_ua = LineGather(at, mail, do.wu, 0, half)
    line_ub = LineGather(at, mail, do.wu, half, half)
    half = do.wd.shape[1] // 2
    line_da = LineGather(at, mail, do.wd, 0, half)
    line_db = LineGather(at, mail, do.wd, half, half)
    ex_v = PlaneExchange(at, mail, lambda rank: [do.vec_s], lambda rank: [do.vec_in.at[rank]], do.vec_in.at[others])
    ex_q = PlaneExchange(
        at, mail, lambda rank: [do.wq_s.at[rank]], strip(do.wq), do.wq_s.at[others]
    )
    ex_u = PlaneExchange(at, mail, up_pieces, up_landings, do.wu.at[0, pl.ds(0, 7 * rows)])
    mine = do.wo2.at[:, c]
    swap_w = PairExchange(
        at, mail, do.wo.at[pl.ds(pair * (1 - c), pair)], mine, do.wo2.at[:, 1 - c]
    )
    sum_o = LineReduce(at, mail, do.go4, do.above_o, do.below_o)
    sum_q = LineReduce(at, mail, do.gq, do.above_q, do.below_q)
    low, high = (pl.ds(i * do.hidden // 2, do.hidden // 2) for i in range(2))
    sum_un = LineReduce(at, mail, do.gu, do.above_u, do.below_u, low, high)
    sum_uf = LineReduce(at, mail, do.gu, do.above_u, do.below_u, high, low)
    near_side = b // pair
    far_side = 1 - near_side
    sum_d = LineReduce(at, mail, do.gd, do.above_d, do.below_d)
    swap_g = PairExchange(
        at,
        mail,
        do.go.at[:, 1 - c],
        do.go4.at[pl.ds(pair * c, pair)],
        do.go4.at[pl.ds(pair * (1 - c), pair)],
    )
    back_q = PlaneExchange(
        at, mail, band(do.fq), lambda rank: [do.dq.at[rank]], do.fq.at[pl.ds(0, 7 * rows)]
    )
    back_u = PlaneExchange(
        at, mail, band(do.fu), lambda rank: [do.du.at[rank]], do.fu.at[pl.ds(0, 7 * rows)]
    )
    fold_v = PlaneExchange(
        at, mail, lambda rank: [do.sm.at[rank]], lambda rank: [do.sm_in.at[rank]], do.sm.at[others]
    )
    line_s = StarGather(at, mail, do.vz)
    share_v = PlaneExchange(
        at, mail, lambda rank: [do.vt], lambda rank: [do.dv.at[rank]], do.dv.at[others]
    )
    plane_o = PlaneReduce(at, mail, do.po, do.pairs_o, do.sums_o, do.side_o, shards)
    plane_g = PlaneReduce(at, mail, do.pg, do.pairs_g, do.sums_g, do.side_g, shards)

    slots = [s + b // pair * (planes - 1 - 2 * s) for s in (3, 0, 2, 1)]

    at.barrier()
    at.reach(second, third)
    line_da.start(do.wd_s)
    own_d = mail.bring(do.wd_s, do.wd.at[b])
    ex_u.start()
    raw_x = mail.bring(do.x_in, do.x_raw)
    own_raw = mail.bring(do.wq_in, do.wq_raw)
    line_db.start(do.wd_s)
    raw_c = mail.bring(do.cot_in, do.cot_raw)
    do.own_vectors(at.t)
    ex_v.start()
    raw_x.wait()
    do.split(do.x_raw, do.x_own)
    line_o.start(do.wo_s)
    own_o = mail.bring(do.wo_s, do.wo.at[b])
    gather_x.start()
    ex_u.finish()
    line_ua.start()
    gather_x.relay_x()
    line_ub.start()
    own_raw.wait()
    do.sort_weight()
    ex_q.start()
    gather_x.relay_y()
    line_ua.take(1)
    raw_c.wait()
    do.split(do.cot_raw, do.cot_own)
    own_table = mail.bring(do.table_in, do.table)
    ex_v.finish()
    do.plane_vectors(b)
    line_v.start()
    gather_c.start()
    line_ub.take(1)
    gather_x.share()
    gather_x.far()
    line_ua.take(2)
    gather_x.finish()
    do.statistics()
    gather_c.relay_x()
    line_ub.take(2)
    line_v.finish()
    ex_q.finish()
    line_q.start()
    gather_c.relay_y()
    do.activations()
    line_o.take(1)
    gather_c.share()
    do.expand_near(near_side)
    line_ub.take(3)
    line_ua.take(3)
    gather_c.far()
    do.expand(at.t, far_side)
    gather_c.finish()
    do.down_weight_grad(slots[0])
    sum_d.edge(3)
    own_o.wait()
    line_o.take(2)
    line_q.take(1)
    do.down_weight_grad(slots[1])
    sum_d.edge(0)
    own_d.wait()
    line_o.take(3)
    swap_w.start()
    mine[...] = do.wo[pl.ds(pair * c, pair)]
    do.down_weight_grad(slots[2])
    sum_d.edge(2)
    swap_w.finish()
    do.project_near(near_side)
    do.attend_out_grad()
    line_q.take(2)
    own_table.wait()
    line_da.take(1)
    line_db.take(1)
    do.hidden_grad(near_side)
    do.up_weight_grad(slots[0], near_side)
    sum_un.edge(3)
    do.down_weight_grad(slots[3])
    sum_d.edge(1)
    do.up_weight_grad(slots[1], near_side)
    sum_un.edge(0)
    sum_d.hop(1, 0)
    line_q.take(3)
    do.project(at.t, far_side)
    do.up_weight_grad(slots[2], near_side)
    sum_un.edge(2)
    do.attend(0)
    do.attend_grad(0)
    line_da.take(2)
    line_db.take(2)
    do.attend(1)
    do.up_weight_grad(slots[3], near_side)
    sum_un.edge(1)
    line_da.take(3)
    sum_un.hop(1, 0)
    do.attend_grad(1)
    do.qkv_weight_grad(slots[0])
    sum_q.edge(3)
    do.qkv_weight_grad(slots[1])
    sum_q.edge(0)
    line_db.take(3)
    do.out_terms(0)
    do.out_terms(1)
    sum_d.hop(1, 1)
    do.out_terms(2)
    do.out_terms(3)
    plane_o.start()
    do.hidden_grad(far_side)
    do.up_weight_grad(slots[0], far_side)
    sum_uf.edge(3)
    sum_d.hop(2, 0)
    do.up_weight_grad(slots[1], far_side)
    sum_uf.edge(0)
    do.up_weight_grad(slots[2], far_side)
    sum_uf.edge(2)
    plane_o.fold()
    do.in_terms(0)
    do.in_terms(1)
    plane_o.turn()
    do.qkv_weight_grad(slots[2])
    sum_q.edge(2)
    sum_un.hop(1, 1)
    do.in_terms(2)
    do.in_terms(3)
    plane_g.start()
    do.up_weight_grad(slots[3], far_side)
    sum_uf.edge(1)
    sum_uf.hop(1, 0)
    do.qkv_weight_grad(slots[3])
    sum_q.edge(1)
    sum_q.hop(1, 0)
    plane_g.fold()
    do.small_terms(at.t)
    fold_v.start()
    sum_uf.hop(2, 0)
    sum_uf.hop(1, 1)
    sum_un.hop(2, 0)
    plane_g.turn()
    do.dense_weight_grad()
    swap_g.start()
    do.go4[pl.ds(pair * c, pair)] = do.go[:, c]
    sum_q.hop(2, 0)
    fold_v.finish()
    do.small_plane(b)
    line_s.start()
    swap_g.finish()
    sum_o.edge(3)
    sum_o.edge(2)
    sum_o.edge(1)
    sum_d.landed()
    sum_d.total(do.dd)
    out_d = mail.bring(do.dd, do.dd_to)
    sum_q.hop(1, 1)
    sum_un.landed()
    sum_uf.landed()
    sum_un.total(do.fu)
    back_u.start()
    do.result(at.t, plane_o.finish(), plane_g.finish())
    out_x = mail.bring(do.out, do.out_to)
    out_g = mail.bring(do.in_grad, do.in_grad_to)
    line_s.finish()
    sum_o.hop(1, 0)
    do.vt[...] = jnp.sum(do.vz[...], axis=0)
    share_v.start()
    sum_q.landed()
    sum_q.total(do.fq)
    back_q.start()
    sum_o.hop(1, 1)
    back_u.finish()
    sum_o.hop(2, 0)
    sum_o.landed()
    sum_o.total(do.dd_o)
    out_o = mail.bring(do.dd_o, do.dd_o_to)
    share_v.finish()
    back_q.finish()
    for copied in (out_o, out_d, out_x, out_g):
        copied.wait()
    for line in (gather_x, gather_c, line_v, line_o, line_q, line_ua, line_ub, line_da, line_db, line_s, ex_v, ex_q, ex_u, back_q, back_u, fold_v, share_v, swap_w, swap_g, plane_o, plane_g, sum_o, sum_q, sum_un, sum_uf, sum_d):
        line.close()


def finish_kernel(names, planes, *refs):
    refs = dict(zip(names, refs))
    near = refs.pop(names[-1])
    do = Layer(refs)
    at = Place(planes)
    ranks, rows = do.dq.shape[:2]
    moves = []

    def move(src, dst):
        moves.append(pltpu.make_async_copy(src, dst, near.at[len(moves)]))
        moves[-1].start()

    move(do.in_grad, do.in_grad_out)
    move(do.dd, do.down_out)
    move(do.out, do.out_out)
    move(do.dd_o, do.dense_out)
    for rank in range(ranks):
        for b in range(planes):
            first = (b * ranks + rank) * LANES
            do.up_v[:, first : first + LANES] = do.du[
                rank, :, b * LANES : (b + 1) * LANES
            ].astype(jnp.float32)
    move(do.up_v, do.up_out)
    low = lax.broadcasted_iota(jnp.int32, (rows, LANES), 1) < HD
    for part in range(3):
        for core in range(2):
            for pair in range(ranks // 4):
                first, second = (
                    do.dq[2 * (2 * pair + i) + core, :, part * LANES : (part + 1) * LANES].astype(
                        jnp.float32
                    )
                    for i in range(2)
                )
                for j in range(2):
                    both = (
                        jnp.where(low, first, pltpu.roll(second, HD, 1))
                        if j == 0
                        else jnp.where(low, pltpu.roll(first, HD, 1), second)
                    )
                    start = (part * 4 + core * 2 + j) * ranks // 2 * HD + pair * LANES
                    do.qkv_v[:, start : start + LANES] = both
    move(do.qkv_v, do.qkv_out)
    piece = lax.rem(at.t, 4)
    row = (at.b * ranks + at.t) // 4
    values = do.dv[pl.ds(row, 1), 0:8, :].reshape(8, LANES)
    front = jnp.zeros((8, rows), jnp.float32)
    for i in range(4):
        cut = values[:, i * rows : (i + 1) * rows]
        front = front + jnp.where(piece == i, cut, jnp.zeros_like(cut))
    for j, ref in enumerate(
        (do.dense_bias, do.gain_one, do.shift_one, do.gain_two, do.shift_two)
    ):
        ref[...] = front[j].reshape(rows)
    do.down_bias[...] = front[0].reshape(rows)
    do.up_bias[...] = do.dv[pl.ds(at.t, 1), pl.ds(12 + at.b, 1), :].reshape(LANES)
    pieces = []
    for i in range(3):
        index = (at.b * ranks + at.t) * 3 + i
        part, inner = index // 32, lax.rem(index, 32)
        head, half = inner // 2, lax.rem(inner, 2)
        core, j, chip = head // 8, lax.rem(head // 4, 2), lax.rem(head, 4)
        value = do.dv[pl.ds(chip * 2 + core, 1), pl.ds(8 + part, 1), :].reshape(1, LANES)
        spot = 2 * j + half
        total = jnp.zeros((1, rows), jnp.float32)
        for k in range(4):
            cut = value[:, k * rows : (k + 1) * rows]
            total = total + jnp.where(spot == k, cut, jnp.zeros_like(cut))
        pieces.append(total)
    do.qkv_bias[...] = jnp.concatenate(pieces, axis=1).reshape(3 * rows)
    for made in moves:
        made.wait()


VMEM = pl.BlockSpec(memory_space=pltpu.VMEM)


def rotary_rows(length):
    half = HD // 8
    frequency = 1.0 / 10000.0 ** (np.arange(half) * (1.0 / half))
    angles = np.arange(length)[:, None] * frequency[None, :]
    table = np.zeros((3, length, HD))
    table[0] = 1.0
    table[0, :, :half] = table[0, :, half : 2 * half] = np.cos(angles)
    table[1, :, :half] = -np.sin(angles)
    table[2, :, half : 2 * half] = np.sin(angles)
    return np.tile(table, (1, 1, LANES // HD)).astype(np.float32)


def body(shape, *operands):
    residual_in, qkv_weight, down_weight = operands[0], operands[1], operands[11]
    planes = shape[BATCH]
    ranks = shape[ULY] * shape[BLK]
    tok_rows, seqs, width = residual_in.shape
    fits = (
        (shape[ULY], shape[BLK]) == (2, 4)
        and planes == 4
        and seqs % 2 == 0
        and 2 * qkv_weight.shape[0] == HD
        and width == ranks * LANES
        and ranks * tok_rows % TILE == 0
        and TILE % (2 * tok_rows) == 0
        and down_weight.shape[0] == LANES
    )
    return fast_body(planes, *operands) if fits else general_body(*operands)


def fast_body(
    planes,
    residual_in,
    qkv_weight,
    qkv_bias,
    dense_weight,
    dense_bias,
    norm1_gain,
    norm1_bias,
    norm2_gain,
    norm2_bias,
    up_weight,
    up_bias,
    down_weight,
    down_bias,
    cotangent,
):
    single = jnp.float32
    half_type = jnp.bfloat16
    tok_rows, seqs, width = residual_in.shape
    ranks = width // LANES
    rows = qkv_weight.shape[0]
    depth = down_weight.shape[0]
    hidden = planes * depth
    pair = planes // 2
    length = ranks * tok_rows
    tokens = seqs * length
    rank = lax.axis_index(ULY) * lax.axis_size(BLK) + lax.axis_index(BLK)
    owner = lax.axis_index(BATCH) * ranks + rank

    anywhere = pl.BlockSpec(memory_space=pl.ANY)
    in_hbm = pl.BlockSpec(memory_space=pltpu.HBM)
    inputs = dict(
        x_in=(residual_in, in_hbm),
        cot_in=(cotangent, in_hbm),
        wq_in=(qkv_weight, in_hbm),
        wu_s=(up_weight, in_hbm),
        wd_s=(down_weight, in_hbm),
        wo_s=(dense_weight, in_hbm),
        table_in=(jnp.asarray(rotary_rows(length)), in_hbm),
        b_qkv=(qkv_bias, VMEM),
        b_up=(up_bias, VMEM),
    )
    for i, v in enumerate((dense_bias, norm1_gain, norm1_bias, norm2_gain, norm2_bias, down_bias)):
        inputs["vector%d" % i] = (v, VMEM)
    shard = (seqs, tok_rows, width)
    outputs = dict(
        out_to=(residual_in.shape, half_type),
        in_grad_to=(residual_in.shape, single),
        dq=((ranks, rows, 3 * LANES), half_type),
        du=((ranks, rows, hidden), half_type),
        dd_to=((depth, width), single),
        dd_o_to=((rows, width), single),
        dv=((ranks, 16, LANES), single),
    )
    q_shape = (planes, ranks * rows, 3 * LANES)
    u_shape = (planes, ranks * rows, hidden)
    d_shape = (planes, depth, width)
    o_shape = (planes, rows, width)
    chips = ranks // 2
    scratch = dict(
        xa=((seqs, length, width), half_type),
        ca=((seqs, length, width), half_type),
        wq=(q_shape, half_type),
        wu=(u_shape, half_type),
        wd=(d_shape, half_type),
        wo=(o_shape, half_type),
        wo2=((pair, 2, rows, width), half_type),
        x_raw=(residual_in.shape, half_type),
        cot_raw=(residual_in.shape, half_type),
        x_own=(shard, half_type),
        cot_own=(shard, half_type),
        qkv=((tokens, 3 * LANES), single),
        wq_raw=(qkv_weight.shape, half_type),
        wq_s=((ranks, rows, 3 * LANES), half_type),
        table=((3, length, LANES), single),
        out=(residual_in.shape, half_type),
        in_grad=(residual_in.shape, single),
        dd=((depth, width), single),
        dd_o=((rows, width), single),
        vec_s=((16, LANES), single),
        vec_in=((ranks, 16, LANES), single),
        va=((planes, 32, LANES), single),
        center=((tokens, 1), single),
        inverse=((tokens, 1), single),
        act_one=((tokens, width), half_type),
        act_two=((tokens, width), half_type),
        query=((tokens, LANES), half_type),
        key=((tokens, LANES), half_type),
        value=((tokens, LANES), half_type),
        attn=((tokens, LANES), half_type),
        attn_grad=((tokens, LANES), half_type),
        qkv_grad=((tokens, 3 * LANES), half_type),
        gelu=((tokens, hidden), half_type),
        slope=((tokens, hidden), single),
        pre_grad=((tokens, hidden), half_type),
        gq=(q_shape, half_type),
        gu=(u_shape, half_type),
        gd=(d_shape, half_type),
        go=((pair, 2, rows, width), half_type),
        go4=(o_shape, half_type),
        above_q=(q_shape, half_type),
        below_q=(q_shape, half_type),
        above_u=(u_shape, half_type),
        below_u=(u_shape, half_type),
        above_d=(d_shape, half_type),
        below_d=(d_shape, half_type),
        above_o=(o_shape, half_type),
        below_o=(o_shape, half_type),
        fq=(q_shape[1:], half_type),
        fu=(u_shape[1:], half_type),
        po=((seqs, chips, 2, tok_rows, width), half_type),
        pg=((seqs, chips, 2, tok_rows, width), half_type),
        pairs_o=((seqs, chips, tok_rows, width), half_type),
        pairs_g=((seqs, chips, tok_rows, width), half_type),
        sums_o=((seqs, chips, tok_rows, width), half_type),
        sums_g=((seqs, chips, tok_rows, width), half_type),
        side_o=((3,) + shard, half_type),
        side_g=((3,) + shard, half_type),
        sums=((8, width), single),
        sm=((ranks, 8, LANES), single),
        sm_in=((ranks, 8, LANES), single),
        vz=((planes, 16, LANES), single),
        vt=((16, LANES), single),
    )
    for block in range(length // TILE):
        scratch["probs%d" % block] = ((seqs * LANES // HD, TILE, (block + 1) * TILE), single)
    names = tuple(inputs) + tuple(outputs) + tuple(scratch) + ("send", "recv", "near", "second", "third")
    out, in_grad, dq, du, dd, dd_o, dv = pl.pallas_call(
        functools.partial(layer_kernel, names, planes),
        out_shape=[jax.ShapeDtypeStruct(*what) for what in outputs.values()],
        in_specs=[where for _, where in inputs.values()],
        out_specs=[anywhere] * len(outputs),
        scratch_shapes=[pltpu.VMEM(*what) for what in scratch.values()]
        + [pltpu.SemaphoreType.DMA((n,)) for n in (SEND_SLOTS, RECV_SLOTS, NEAR_SLOTS)]
        + [pltpu.SemaphoreType.REGULAR] * 2,
        compiler_params=pltpu.CompilerParams(
            collective_id=0, has_side_effects=True, vmem_limit_bytes=52 * 2**20
        ),
    )(
        *(
            pltpu.with_memory_space_constraint(value, pltpu.HBM) for value, _ in inputs.values()
        )
    )

    results = dict(
        out_out=(residual_in.shape, half_type),
        in_grad_out=(residual_in.shape, single),
        qkv_out=(qkv_weight.shape, single),
        qkv_bias=(qkv_bias.shape, single),
        dense_out=(dense_weight.shape, single),
        dense_bias=(dense_bias.shape, single),
        gain_one=(norm1_gain.shape, single),
        shift_one=(norm1_bias.shape, single),
        gain_two=(norm2_gain.shape, single),
        shift_two=(norm2_bias.shape, single),
        up_out=(up_weight.shape, single),
        up_bias=(up_bias.shape, single),
        down_out=(down_weight.shape, single),
        down_bias=(down_bias.shape, single),
    )
    given = tuple(n.removesuffix("_to") for n in outputs)
    staged = dict(up_v=results["up_out"], qkv_v=results["qkv_out"])
    return tuple(
        pl.pallas_call(
            functools.partial(
                finish_kernel, given + tuple(results) + tuple(staged) + ("near",), planes
            ),
            out_shape=[jax.ShapeDtypeStruct(*what) for what in results.values()],
            in_specs=[VMEM] * len(given),
            out_specs=[anywhere if len(what[0]) > 1 else VMEM for what in results.values()],
            scratch_shapes=[pltpu.VMEM(*what) for what in staged.values()]
            + [pltpu.SemaphoreType.DMA((8,))],
            compiler_params=pltpu.CompilerParams(vmem_limit_bytes=8 * 2**20),
        )(out, in_grad, dq, du, dd, dd_o, dv)
    )


def solution(mesh):
    placed = (
        P(TOKENS, BATCH, None),
        P(AXES, None),
        P(AXES),
        P(AXES, None),
        P(AXES),
        P(AXES),
        P(AXES),
        P(AXES),
        P(AXES),
        P(AXES, None),
        P(AXES),
        P(AXES, None),
        P(AXES),
        P(TOKENS, BATCH, None),
    )
    return jax.shard_map(
        functools.partial(body, dict(mesh.shape)),
        mesh=mesh,
        in_specs=placed,
        out_specs=(
            P(TOKENS, BATCH, None),
            P(TOKENS, BATCH, None),
            P(AXES, None),
            P(AXES),
            P(AXES, None),
            P(AXES),
            P(AXES),
            P(AXES),
            P(AXES),
            P(AXES),
            P(AXES, None),
            P(AXES),
            P(AXES, None),
            P(AXES),
        ),
        check_vma=False,
    )
```

```python
import functools
import math

import jax
import jax.numpy as jnp
import numpy as np
from jax import lax
from jax.experimental import pallas as pl
from jax.experimental.pallas import tpu as pltpu
from jax.sharding import PartitionSpec as P

HD = 64
BATCH, ULY, BLK = "batch", "ulysses", "blk"
AXES = (BATCH, ULY, BLK)
TOKENS = (ULY, BLK)


EPSILON = 1e-05
INV_ROOT_TWO = 0.7071067811865476
INV_ROOT_TWO_PI = 0.3989422804014327


def layer_norm(values):
    center = jnp.mean(values, axis=-1, keepdims=True)
    shifted = values - center
    inverse = lax.rsqrt(jnp.mean(shifted * shifted, axis=-1, keepdims=True) + EPSILON)
    return (shifted * inverse, inverse)


def norm_back(gradient, normed, inverse, gain_vec):
    scaled = gradient * gain_vec
    return inverse * (
        scaled
        - jnp.mean(scaled, axis=-1, keepdims=True)
        - normed * jnp.mean(scaled * normed, axis=-1, keepdims=True)
    )


def gelu_value(pre_values):
    return 0.5 * pre_values * (1.0 + jax.scipy.special.erf(pre_values * INV_ROOT_TWO))


def gelu_slope(pre_values):
    normal_cdf = 0.5 * (1.0 + jax.scipy.special.erf(pre_values * INV_ROOT_TWO))
    return normal_cdf + pre_values * jnp.exp(-0.5 * pre_values * pre_values) * INV_ROOT_TWO_PI


def rotary_tables(positions, rotary):
    half_rot = rotary // 2
    frequency = 1.0 / 10000.0 ** (jnp.arange(half_rot, dtype=jnp.float32) * (2.0 / rotary))
    angles = positions.astype(jnp.float32)[:, None] * frequency[None, :]
    cosine = jnp.concatenate([jnp.cos(angles), jnp.cos(angles)], axis=-1)
    sine_table = jnp.concatenate([jnp.sin(angles), jnp.sin(angles)], axis=-1)
    return (cosine, sine_table)


def expand_table(table, tensor):
    extra_dims = (1,) * (tensor.ndim - 2)
    return table.reshape((table.shape[0],) + extra_dims + (table.shape[1],))


def rotate_fwd(tensor, cosine, sine_table, rotary):
    half_rot = rotary // 2
    cos_full = expand_table(cosine, tensor)
    sin_full = expand_table(sine_table, tensor)
    rot_part = tensor[..., :rotary]
    turned = jnp.concatenate([-rot_part[..., half_rot:], rot_part[..., :half_rot]], axis=-1)
    return jnp.concatenate([rot_part * cos_full + turned * sin_full, tensor[..., rotary:]], axis=-1)


def rotate_back(tensor, cosine, sine_table, rotary):
    half_rot = rotary // 2
    cos_full = expand_table(cosine, tensor)
    sin_full = expand_table(sine_table, tensor)
    rot_part = tensor[..., :rotary]
    weighted = rot_part * sin_full
    turned = jnp.concatenate([weighted[..., half_rot:], -weighted[..., :half_rot]], axis=-1)
    return jnp.concatenate([rot_part * cos_full + turned, tensor[..., rotary:]], axis=-1)


def general_body(
    residual_in,
    qkv_weight,
    qkv_bias,
    dense_weight,
    dense_bias,
    norm1_gain,
    norm1_bias,
    norm2_gain,
    norm2_bias,
    up_weight,
    up_bias,
    down_weight,
    down_bias,
    cotangent,
):
    single = jnp.float32
    half_type = jnp.bfloat16
    gathered = (
        lax.all_gather(qkv_weight, AXES, axis=0, tiled=True),
        lax.all_gather(qkv_bias, AXES, axis=0, tiled=True),
        lax.all_gather(dense_weight, AXES, axis=0, tiled=True),
        lax.all_gather(dense_bias, AXES, axis=0, tiled=True),
        lax.all_gather(norm1_gain, AXES, axis=0, tiled=True),
        lax.all_gather(norm1_bias, AXES, axis=0, tiled=True),
        lax.all_gather(norm2_gain, AXES, axis=0, tiled=True),
        lax.all_gather(norm2_bias, AXES, axis=0, tiled=True),
        lax.all_gather(up_weight, AXES, axis=0, tiled=True),
        lax.all_gather(up_bias, AXES, axis=0, tiled=True),
        lax.all_gather(down_weight, AXES, axis=0, tiled=True),
        lax.all_gather(down_bias, AXES, axis=0, tiled=True),
    )
    (
        w_qkv,
        b_qkv,
        w_dense,
        b_dense,
        gain_one,
        shift_one,
        gain_two,
        shift_two,
        w_up,
        b_up,
        w_down,
        b_down,
    ) = gathered
    tok_rows = residual_in.shape[0]
    seq_count = residual_in.shape[1]
    model_width = residual_in.shape[2]
    head_count = model_width // HD
    rotary = HD // 4
    scale_factor = 1.0 / math.sqrt(HD)
    blk_size = lax.axis_size(BLK)
    uly_size = lax.axis_size(ULY)
    blk_index = lax.axis_index(BLK)
    block_id = lax.axis_index(ULY) * blk_size + blk_index
    seq_pos = block_id * tok_rows + jnp.arange(tok_rows, dtype=jnp.int32)
    inputs_f = residual_in.astype(single)
    normed, inverse = layer_norm(inputs_f)
    act_one = (normed * gain_one.astype(single) + shift_one.astype(single)).astype(half_type)
    act_two = (normed * gain_two.astype(single) + shift_two.astype(single)).astype(half_type)
    qkv_full = jnp.einsum(
        "tsd,df->tsf", act_one, w_qkv, preferred_element_type=single
    ) + b_qkv.astype(single)
    cos_seq, sin_seq = rotary_tables(seq_pos, rotary)
    head_shape = (tok_rows, seq_count, head_count, HD)
    query_seq = (
        rotate_fwd(qkv_full[..., :model_width].reshape(head_shape), cos_seq, sin_seq, rotary)
        .reshape(tok_rows, seq_count, model_width)
        .astype(half_type)
    )
    key_seq = (
        rotate_fwd(
            qkv_full[..., model_width : 2 * model_width].reshape(head_shape),
            cos_seq,
            sin_seq,
            rotary,
        )
        .reshape(tok_rows, seq_count, model_width)
        .astype(half_type)
    )
    value_seq = qkv_full[..., 2 * model_width :].astype(half_type)
    query_loc, key_loc, value_loc = (
        lax.all_to_all(query_seq, ULY, split_axis=2, concat_axis=0, tiled=True),
        lax.all_to_all(key_seq, ULY, split_axis=2, concat_axis=0, tiled=True),
        lax.all_to_all(value_seq, ULY, split_axis=2, concat_axis=0, tiled=True),
    )
    local_rows = query_loc.shape[0]
    features = query_loc.shape[2]
    local_heads = features // HD
    key_all, value_all = (
        lax.all_gather(key_loc, BLK, axis=0, tiled=True),
        lax.all_gather(value_loc, BLK, axis=0, tiled=True),
    )
    total_rows = key_all.shape[0]
    row_ids = jnp.arange(local_rows, dtype=jnp.int32)
    query_pos = (row_ids // tok_rows * blk_size + blk_index) * tok_rows + row_ids % tok_rows
    block_rows = math.gcd(512, local_rows)
    n_blocks = local_rows // block_rows
    query_h = query_loc.reshape(local_rows, seq_count, local_heads, HD)
    key_h = jnp.transpose(
        key_all.reshape(blk_size, uly_size, tok_rows, seq_count, features), (1, 0, 2, 3, 4)
    ).reshape(total_rows, seq_count, local_heads, HD)
    value_h = jnp.transpose(
        value_all.reshape(blk_size, uly_size, tok_rows, seq_count, features), (1, 0, 2, 3, 4)
    ).reshape(total_rows, seq_count, local_heads, HD)
    zero_idx = jnp.zeros((), jnp.int32)
    step_ids = jnp.arange(n_blocks * seq_count, dtype=jnp.int32)
    row_shape = (block_rows, 1, local_heads, HD)

    def select(step_index):
        row_start = step_index // seq_count * block_rows
        seq_index = step_index % seq_count
        query_rows = lax.dynamic_slice(
            query_h, (row_start, seq_index, zero_idx, zero_idx), row_shape
        )
        limit = jnp.max(query_pos) // block_rows + 1
        return (row_start, seq_index, query_rows, query_pos, limit)

    def block_scores(query_rows, row_pos, key_index, seq_index):
        key_start = key_index * block_rows
        slot = (key_start, seq_index, zero_idx, zero_idx)
        key_rows = lax.dynamic_slice(key_h, slot, (block_rows, 1, local_heads, HD))
        value_rows = lax.dynamic_slice(value_h, slot, (block_rows, 1, local_heads, HD))
        scores = (
            jnp.einsum("qshd,kshd->shqk", query_rows, key_rows, preferred_element_type=single)
            * scale_factor
        )
        key_ids = key_start + jnp.arange(block_rows, dtype=jnp.int32)
        allowed = (key_ids[None, :] <= row_pos[:, None])[None, None]
        return (jnp.where(allowed, scores, -jnp.inf), key_rows, value_rows, slot)

    def forward_block(step_index):
        row_start, seq_index, query_rows, row_pos, limit = select(step_index)

        def total_step(key_index, carry):
            running_max, running_sum = carry
            masked, key_rows, value_rows, slot = block_scores(
                query_rows, row_pos, key_index, seq_index
            )
            new_max = jnp.maximum(running_max, jnp.max(masked, axis=-1))
            new_sum = running_sum * jnp.exp(running_max - new_max) + jnp.sum(
                jnp.exp(masked - new_max[..., None]), axis=-1
            )
            return (new_max, new_sum)

        start_max = jnp.full((1, local_heads, block_rows), -jnp.inf, single)
        start_sum = jnp.zeros((1, local_heads, block_rows), single)
        final_max, final_sum = lax.fori_loop(zero_idx, limit, total_step, (start_max, start_sum))
        log_total = final_max + jnp.log(final_sum)

        def value_step(key_index, acc):
            masked, key_rows, value_rows, slot = block_scores(
                query_rows, row_pos, key_index, seq_index
            )
            weights_b = jnp.exp(masked - log_total[..., None]).astype(half_type)
            return acc + jnp.einsum(
                "shqk,kshd->qshd", weights_b, value_rows, preferred_element_type=single
            )

        result = lax.fori_loop(zero_idx, limit, value_step, jnp.zeros(row_shape, single)).astype(
            half_type
        )
        return (result[:, 0], log_total)

    results, log_totals = lax.map(forward_block, step_ids)
    attn_h = jnp.transpose(
        results.reshape(n_blocks, seq_count, block_rows, local_heads, HD), (0, 2, 1, 3, 4)
    ).reshape(local_rows, seq_count, local_heads, HD)
    attn_seq = lax.all_to_all(
        attn_h.reshape(local_rows, seq_count, features),
        ULY,
        split_axis=0,
        concat_axis=2,
        tiled=True,
    )
    proj_out = jnp.einsum(
        "tsd,de->tse", attn_seq, w_dense, preferred_element_type=single
    ) + b_dense.astype(single)
    pre_act = jnp.einsum("tsd,df->tsf", act_two, w_up, preferred_element_type=single) + b_up.astype(
        single
    )
    gelu_out = gelu_value(pre_act).astype(half_type)
    mlp_out = jnp.einsum(
        "tsf,fd->tsd", gelu_out, w_down, preferred_element_type=single
    ) + b_down.astype(single)
    output = (inputs_f + proj_out + mlp_out).astype(half_type)
    back_params = (
        lax.all_gather(qkv_weight, AXES, axis=0, tiled=True),
        lax.all_gather(qkv_bias, AXES, axis=0, tiled=True),
        lax.all_gather(dense_weight, AXES, axis=0, tiled=True),
        lax.all_gather(dense_bias, AXES, axis=0, tiled=True),
        lax.all_gather(norm1_gain, AXES, axis=0, tiled=True),
        lax.all_gather(norm1_bias, AXES, axis=0, tiled=True),
        lax.all_gather(norm2_gain, AXES, axis=0, tiled=True),
        lax.all_gather(norm2_bias, AXES, axis=0, tiled=True),
        lax.all_gather(up_weight, AXES, axis=0, tiled=True),
        lax.all_gather(up_bias, AXES, axis=0, tiled=True),
        lax.all_gather(down_weight, AXES, axis=0, tiled=True),
        lax.all_gather(down_bias, AXES, axis=0, tiled=True),
    )
    back_qkv = back_params[0]
    back_dense = back_params[2]
    back_gain_one = back_params[4].astype(single)
    back_gain_two = back_params[6].astype(single)
    back_up = back_params[8]
    back_down = back_params[10]
    grad_f = cotangent.astype(single)
    bias_sum = jnp.sum(grad_f, axis=(0, 1))
    down_w_grad = jnp.einsum("tsf,tsd->fd", gelu_out, cotangent, preferred_element_type=single)
    gelu_grad = jnp.einsum("tsd,fd->tsf", cotangent, back_down, preferred_element_type=single)
    pre_grad = (gelu_grad * gelu_slope(pre_act)).astype(half_type)
    up_w_grad = jnp.einsum("tsd,tsf->df", act_two, pre_grad, preferred_element_type=single)
    up_b_grad = jnp.sum(pre_grad.astype(single), axis=(0, 1))
    act_two_grad = jnp.einsum("tsf,df->tsd", pre_grad, back_up, preferred_element_type=single)
    gain_two_grad = jnp.sum(act_two_grad * normed, axis=(0, 1))
    shift_two_grad = jnp.sum(act_two_grad, axis=(0, 1))
    dense_w_grad = jnp.einsum("tsd,tse->de", attn_seq, cotangent, preferred_element_type=single)
    attn_grad = jnp.einsum(
        "tse,de->tsd", cotangent, back_dense, preferred_element_type=single
    ).astype(half_type)
    grad_loc = lax.all_to_all(attn_grad, ULY, split_axis=2, concat_axis=0, tiled=True)
    grad_h = grad_loc.reshape(local_rows, seq_count, local_heads, HD)

    def backward_block(acc_pair, step_index):
        row_start, seq_index, query_rows, row_pos, limit = select(step_index)
        own_slot = (row_start, seq_index, zero_idx, zero_idx)
        out_rows = lax.dynamic_slice(attn_h, own_slot, row_shape)
        grad_rows = lax.dynamic_slice(grad_h, own_slot, row_shape)
        log_total = log_totals[step_index]
        delta_row = jnp.transpose(
            jnp.sum(grad_rows.astype(single) * out_rows.astype(single), axis=-1), (1, 2, 0)
        )

        def grad_step(key_index, carry):
            key_acc, value_acc, query_acc = carry
            masked, key_rows, value_rows, slot = block_scores(
                query_rows, row_pos, key_index, seq_index
            )
            probs_f = jnp.exp(masked - log_total[..., None])
            value_part = jnp.einsum(
                "shqk,qshd->kshd",
                probs_f.astype(half_type),
                grad_rows,
                preferred_element_type=single,
            )
            grad_prob = jnp.einsum(
                "qshd,kshd->shqk", grad_rows, value_rows, preferred_element_type=single
            )
            grad_score = (probs_f * (grad_prob - delta_row[..., None]) * scale_factor).astype(
                half_type
            )
            query_acc = query_acc + jnp.einsum(
                "shqk,kshd->qshd", grad_score, key_rows, preferred_element_type=single
            )
            key_part = jnp.einsum(
                "shqk,qshd->kshd", grad_score, query_rows, preferred_element_type=single
            )
            key_acc = lax.dynamic_update_slice(
                key_acc, lax.dynamic_slice(key_acc, slot, key_part.shape) + key_part, slot
            )
            value_acc = lax.dynamic_update_slice(
                value_acc, lax.dynamic_slice(value_acc, slot, value_part.shape) + value_part, slot
            )
            return (key_acc, value_acc, query_acc)

        key_acc, value_acc, query_acc = lax.fori_loop(
            zero_idx, limit, grad_step, (acc_pair[0], acc_pair[1], jnp.zeros(row_shape, single))
        )
        return ((key_acc, value_acc), query_acc[:, 0])

    acc_zero = jnp.zeros((total_rows, seq_count, local_heads, HD), single)
    acc_final, query_parts = lax.scan(backward_block, (acc_zero, acc_zero), step_ids)
    query_grad = jnp.transpose(
        query_parts.reshape(n_blocks, seq_count, block_rows, local_heads, HD), (0, 2, 1, 3, 4)
    ).reshape(local_rows, seq_count, local_heads, HD)
    key_terms = jnp.transpose(
        acc_final[0].reshape(uly_size, blk_size, tok_rows, seq_count, features), (1, 0, 2, 3, 4)
    ).reshape(total_rows, seq_count, features)
    value_terms = jnp.transpose(
        acc_final[1].reshape(uly_size, blk_size, tok_rows, seq_count, features), (1, 0, 2, 3, 4)
    ).reshape(total_rows, seq_count, features)
    key_back, value_back = (
        lax.psum_scatter(key_terms, BLK, scatter_dimension=0, tiled=True),
        lax.psum_scatter(value_terms, BLK, scatter_dimension=0, tiled=True),
    )
    cos_h, sin_h = rotary_tables(query_pos, rotary)
    query_send = (
        rotate_back(query_grad, cos_h, sin_h, rotary)
        .reshape(local_rows, seq_count, features)
        .astype(half_type)
    )
    key_send = (
        rotate_back(key_back.reshape(local_rows, seq_count, local_heads, HD), cos_h, sin_h, rotary)
        .reshape(local_rows, seq_count, features)
        .astype(half_type)
    )
    value_send = value_back.astype(half_type)
    query_ret, key_ret, value_ret = (
        lax.all_to_all(query_send, ULY, split_axis=0, concat_axis=2, tiled=True),
        lax.all_to_all(key_send, ULY, split_axis=0, concat_axis=2, tiled=True),
        lax.all_to_all(value_send, ULY, split_axis=0, concat_axis=2, tiled=True),
    )
    qkv_grad = jnp.concatenate([query_ret, key_ret, value_ret], axis=-1)
    qkv_w_grad = jnp.einsum("tsd,tsf->df", act_one, qkv_grad, preferred_element_type=single)
    qkv_b_grad = jnp.sum(qkv_grad.astype(single), axis=(0, 1))
    act_one_grad = jnp.einsum("tsf,df->tsd", qkv_grad, back_qkv, preferred_element_type=single)
    gain_one_grad = jnp.sum(act_one_grad * normed, axis=(0, 1))
    shift_one_grad = jnp.sum(act_one_grad, axis=(0, 1))
    input_grad = (
        grad_f
        + norm_back(act_one_grad, normed, inverse, back_gain_one)
        + norm_back(act_two_grad, normed, inverse, back_gain_two)
    )
    summed = (
        lax.psum_scatter(qkv_w_grad, AXES, scatter_dimension=0, tiled=True),
        lax.psum_scatter(qkv_b_grad, AXES, scatter_dimension=0, tiled=True),
        lax.psum_scatter(
            dense_w_grad, AXES, scatter_dimension=0, tiled=True
        ),
        lax.psum_scatter(bias_sum, AXES, scatter_dimension=0, tiled=True),
        lax.psum_scatter(
            gain_one_grad, AXES, scatter_dimension=0, tiled=True
        ),
        lax.psum_scatter(
            shift_one_grad, AXES, scatter_dimension=0, tiled=True
        ),
        lax.psum_scatter(
            gain_two_grad, AXES, scatter_dimension=0, tiled=True
        ),
        lax.psum_scatter(
            shift_two_grad, AXES, scatter_dimension=0, tiled=True
        ),
        lax.psum_scatter(up_w_grad, AXES, scatter_dimension=0, tiled=True),
        lax.psum_scatter(up_b_grad, AXES, scatter_dimension=0, tiled=True),
        lax.psum_scatter(down_w_grad, AXES, scatter_dimension=0, tiled=True),
        lax.psum_scatter(bias_sum, AXES, scatter_dimension=0, tiled=True),
    )
    return (
        output,
        input_grad,
        summed[0],
        summed[1],
        summed[2],
        summed[3],
        summed[4],
        summed[5],
        summed[6],
        summed[7],
        summed[8],
        summed[9],
        summed[10],
        summed[11],
    )


MESH = pl.DeviceIdType.MESH


class Place:
    def __init__(self, planes):
        self.planes = planes
        self.b = lax.axis_index(BATCH)
        self.u = lax.axis_index(ULY)
        k = lax.axis_index(BLK)
        self.y, self.c = k // 2, k % 2
        self.t = self.u * 4 + k
        self.xn, self.yn, self.pn = self.peer(4), self.peer(2), self.peer(1)

    def rank(self, d):
        u = 1 - self.u if d & 4 else self.u
        y = 1 - self.y if d & 2 else self.y
        c = 1 - self.c if d & 1 else self.c
        return u * 4 + y * 2 + c

    def chip(self, d):
        return self.rank(d) // 2

    def peer(self, d):
        u = 1 - self.u if d & 4 else self.u
        y = 1 - self.y if d & 2 else self.y
        c = 1 - self.c if d & 1 else self.c
        return {BATCH: self.b, ULY: u, BLK: y * 2 + c}

    def along(self, step):
        return {BATCH: self.b + step, ULY: self.u, BLK: self.y * 2 + self.c}

    def barrier(self):
        sem = pltpu.get_barrier_semaphore()
        for d in range(1, 8):
            pl.semaphore_signal(sem, inc=1, device_id=self.peer(d), device_id_type=MESH)
        self.to_neighbours(
            lambda step: pl.semaphore_signal(
                sem, inc=1, device_id=self.along(step), device_id_type=MESH
            )
        )
        below = (self.b > 0).astype(jnp.int32)
        above = (self.b < self.planes - 1).astype(jnp.int32)
        pl.semaphore_wait(sem, 7 + below + above)

    def to_neighbours(self, action):
        for step in (-1, 1):

            @pl.when(self.b > 0 if step < 0 else self.b < self.planes - 1)
            def _():
                action(step)

    def reach(self, second, third):
        b, last = self.b, self.planes - 1

        @pl.when((b > 0) & (b < last))
        def _():
            for step in (-1, 1):
                pl.semaphore_signal(
                    second, inc=1, device_id=self.along(step), device_id_type=MESH
                )

        pl.semaphore_wait(second, (b >= 2).astype(jnp.int32) + (b <= last - 2).astype(jnp.int32))
        for middle, step in ((1, -1), (2, 1)):

            @pl.when(b == middle)
            def _():
                pl.semaphore_signal(third, inc=1, device_id=self.along(step), device_id_type=MESH)

        @pl.when((b == 0) | (b == last))
        def _():
            pl.semaphore_wait(third, 1)


class Mail:
    def __init__(self, send, recv, near):
        self.send, self.recv, self.near = send, recv, near
        self.sends = self.recvs = self.nears = 0

    def send_slots(self, n=1):
        self.sends += n
        return self.sends - n

    def recv_slots(self, n=1):
        self.recvs += n
        return self.recvs - n

    def bring(self, src, dst):
        made = pltpu.make_async_copy(src, dst, self.near.at[self.nears])
        self.nears += 1
        made.start()
        return made

    def copy(self, src, dst, send, recv, device):
        return pltpu.make_async_remote_copy(
            src_ref=src,
            dst_ref=dst,
            send_sem=self.send.at[send],
            recv_sem=self.recv.at[recv],
            device_id=device,
            device_id_type=MESH,
        )

    def arrived(self, bulk, recv, device):
        self.copy(bulk, bulk, 0, recv, device).wait_recv()

    def gone(self, bulk, send, device):
        self.copy(bulk, bulk, send, 0, device).wait_send()


class PlaneGather:
    def __init__(self, at, mail, shard, whole):
        self.at, self.mail, self.shard, self.whole = at, mail, shard, whole
        self.rows = shard.shape[1]
        self.halves = shard.shape[0] // 2
        self.send, self.recv = mail.send_slots(), mail.recv_slots(5)

    def half(self, i):
        return self.shard.at[pl.ds(i * self.halves, self.halves)]

    def block(self, d, half=None):
        rows = pl.ds(pl.multiple_of(self.at.rank(d) * self.rows, self.rows), self.rows)
        if half is None:
            return self.whole.at[:, rows, :]
        return self.whole.at[pl.ds(half * self.halves, self.halves), rows, :]

    def bulk(self, shards):
        return self.whole.at[:, pl.ds(0, shards * self.rows), :]

    def post(self, src, dst, recv, device):
        self.mail.copy(src, dst, self.send, self.recv + recv, device).start()

    def arrived(self, bulk, recv, device):
        self.mail.arrived(bulk, self.recv + recv, device)

    def start(self):
        at = self.at
        self.post(self.half(1), self.block(0, 1), 0, at.xn)
        self.post(self.half(0), self.block(0, 0), 1, at.yn)
        self.post(self.half(0), self.block(0, 0), 2, at.xn)
        self.post(self.half(1), self.block(0, 1), 2, at.yn)
        self.post(self.shard, self.block(0), 4, at.pn)
        self.own = self.mail.bring(self.shard, self.block(0))

    def relay_y(self):
        self.arrived(self.block(2, 0), 1, self.at.yn)
        self.post(self.block(2, 0), self.block(2, 0), 3, self.at.xn)

    def relay_x(self):
        self.arrived(self.block(4, 1), 0, self.at.xn)
        self.post(self.block(4, 1), self.block(4, 1), 3, self.at.yn)

    def share(self):
        self.arrived(self.bulk(1), 2, self.at.xn)
        self.post(self.block(2), self.block(2), 4, self.at.pn)
        self.post(self.block(4), self.block(4), 4, self.at.pn)

    def far(self):
        self.arrived(self.block(6), 3, self.at.xn)
        self.post(self.block(6), self.block(6), 4, self.at.pn)

    def finish(self):
        self.arrived(self.bulk(4), 4, self.at.pn)
        self.own.wait()

    def close(self):
        self.mail.gone(self.bulk(7), self.send, self.at.pn)


class LineGather:
    def __init__(self, at, mail, held, up_cut=None, down_cut=None):
        self.at, self.mail, self.held = at, mail, held
        whole = tuple(pl.ds(0, n) for n in held.shape[1:])
        self.up_cut, self.down_cut = up_cut or whole, down_cut or whole
        self.send, self.recv = mail.send_slots(2), mail.recv_slots(at.planes)

    def upward(self, slot, src):
        part = self.held.at[(slot,) + self.up_cut]
        src = part if src is None else src.at[self.up_cut]
        return self.mail.copy(src, part, self.send, self.recv + slot, self.at.along(1))

    def downward(self, slot, src):
        part = self.held.at[(slot,) + self.down_cut]
        src = part if src is None else src.at[self.down_cut]
        return self.mail.copy(src, part, self.send + 1, self.recv + slot, self.at.along(-1))

    def start(self, src=None):
        at = self.at

        @pl.when(at.b < at.planes - 1)
        def _():
            self.upward(at.b, src).start()

        @pl.when(at.b > 0)
        def _():
            self.downward(at.b, src).start()

    def from_below(self, distance, here):
        at = self.at
        slot = at.b - distance

        @pl.when((slot >= 0) & here)
        def _():
            part = self.held.at[(slot,) + self.up_cut]
            self.mail.arrived(part, self.recv + slot, at.along(-1))

            @pl.when(at.b < at.planes - 1)
            def _():
                self.upward(slot, None).start()

    def from_above(self, distance, here):
        at = self.at
        slot = at.b + distance

        @pl.when((slot < at.planes) & here)
        def _():
            part = self.held.at[(slot,) + self.down_cut]
            self.mail.arrived(part, self.recv + slot, at.along(1))

            @pl.when(at.b > 0)
            def _():
                self.downward(slot, None).start()

    def take(self, distance):
        self.from_below(distance, self.at.b >= 0)
        self.from_above(distance, self.at.b >= 0)

    def inner(self, distance):
        middle = self.at.planes // 2
        self.from_below(distance, self.at.b >= middle)
        self.from_above(distance, self.at.b < middle)

    def outer(self, distance):
        middle = self.at.planes // 2
        self.from_below(distance, self.at.b < middle)
        self.from_above(distance, self.at.b >= middle)

    def close(self):
        at = self.at
        for b in range(at.planes):

            @pl.when(at.b == b)
            def _():
                if b < at.planes - 1:
                    bulk = self.held.at[(pl.ds(0, b + 1),) + self.up_cut]
                    self.mail.gone(bulk, self.send, at.along(1))
                if b > 0:
                    bulk = self.held.at[(pl.ds(0, at.planes - b),) + self.down_cut]
                    self.mail.gone(bulk, self.send + 1, at.along(-1))


class StarGather:
    def __init__(self, at, mail, held):
        self.at, self.mail, self.held = at, mail, held
        self.send, self.recv = mail.send_slots(), mail.recv_slots()

    def start(self):
        at = self.at
        part = self.held.at[at.b]
        for step in range(1, at.planes):

            @pl.when(at.b + step < at.planes)
            def _():
                self.mail.copy(part, part, self.send, self.recv, at.along(step)).start()

            @pl.when(at.b >= step)
            def _():
                self.mail.copy(part, part, self.send, self.recv, at.along(-step)).start()

    def bulk(self):
        return self.held.at[pl.ds(0, self.at.planes - 1)]

    def finish(self):
        self.mail.arrived(self.bulk(), self.recv, self.at.pn)

    def close(self):
        self.mail.gone(self.bulk(), self.send, self.at.pn)


class PlaneExchange:
    def __init__(self, at, mail, pieces, landings, bulk):
        self.at, self.mail, self.bulk = at, mail, bulk
        self.pieces, self.landings = pieces, landings
        self.send, self.recv = mail.send_slots(), mail.recv_slots()

    def start(self):
        at = self.at
        for d in range(1, 8):
            for piece, landing in zip(self.pieces(at.rank(d)), self.landings(at.t)):
                self.mail.copy(piece, landing, self.send, self.recv, at.peer(d)).start()
        self.own = [
            self.mail.bring(piece, landing)
            for piece, landing in zip(self.pieces(at.t), self.landings(at.t))
        ]

    def finish(self):
        self.mail.arrived(self.bulk, self.recv, self.at.pn)
        for own in self.own:
            own.wait()

    def close(self):
        self.mail.gone(self.bulk, self.send, self.at.pn)


class PairExchange:
    def __init__(self, at, mail, src, dst, landed):
        self.at, self.mail, self.src, self.dst, self.landed = at, mail, src, dst, landed
        self.send, self.recv = mail.send_slots(), mail.recv_slots()

    def start(self):
        self.mail.copy(self.src, self.dst, self.send, self.recv, self.at.pn).start()

    def finish(self):
        self.mail.arrived(self.landed, self.recv, self.at.pn)

    def close(self):
        self.mail.gone(self.src, self.send, self.at.pn)


class PlaneReduce:
    def __init__(self, at, mail, terms, pairs, sums, side, bulk):
        self.at, self.mail, self.terms, self.bulk = at, mail, terms, bulk
        self.pairs, self.sums, self.side = pairs, sums, side
        self.send, self.recv = mail.send_slots(), mail.recv_slots(5)
        self.halves = terms.shape[0] // 2

    def post(self, src, dst, recv, device):
        self.mail.copy(src, dst, self.send, self.recv + recv, device).start()

    def start(self):
        at = self.at
        for d in (6, 4, 2, 0):
            chip = at.chip(d)
            self.post(
                self.terms.at[:, chip, 1 - at.c], self.pairs.at[:, chip], 0 if d == 6 else 1, at.pn
            )

    def half(self, ref, i):
        return ref.at[pl.ds(i * self.halves, self.halves)]

    def add_pair(self, d):
        chip = self.at.chip(d)
        total = self.terms[:, chip, self.at.c].astype(jnp.float32) + self.pairs[:, chip].astype(
            jnp.float32
        )
        self.sums[:, chip] = total.astype(self.sums.dtype)

    def fold(self):
        at = self.at
        far = self.sums.at[:, at.chip(6)]
        self.mail.arrived(self.bulk(1), self.recv, at.pn)
        self.add_pair(6)
        self.post(self.half(far, 0), self.half(self.side.at[0], 0), 2, at.xn)
        self.post(self.half(far, 1), self.half(self.side.at[0], 1), 3, at.yn)
        self.mail.arrived(self.bulk(3), self.recv + 1, at.pn)
        for d in (4, 2, 0):
            self.add_pair(d)

    def turn(self):
        at = self.at
        for i, d, other, recv, nbr in ((1, 4, at.yn, 3, at.xn), (0, 2, at.xn, 2, at.yn)):
            landed = self.half(self.side.at[0], i)
            self.mail.arrived(landed, self.recv + recv, other)
            whole = self.sums.at[:, at.chip(d)]
            part = self.half(whole, i)
            part[...] = (part[...].astype(jnp.float32) + landed[...].astype(jnp.float32)).astype(
                self.sums.dtype
            )
            self.post(whole, self.side.at[2 - i], 4, nbr)

    def finish(self):
        self.mail.arrived(self.bulk(2), self.recv + 4, self.at.xn)
        return (
            self.sums[:, self.at.chip(0)].astype(jnp.float32)
            + self.side[1].astype(jnp.float32)
            + self.side[2].astype(jnp.float32)
        )

    def close(self):
        self.mail.gone(self.bulk(7), self.send, self.at.pn)


class LineReduce:
    def __init__(self, at, mail, terms, above, below, up_cut=None, down_cut=None):
        self.at, self.mail, self.terms = at, mail, terms
        self.above, self.below = above, below
        whole = pl.ds(0, terms.shape[2])
        self.up_cut, self.down_cut = up_cut or whole, down_cut or whole
        self.send, self.recv = mail.send_slots(2), mail.recv_slots(at.planes + 1)

    def upward(self, src, slot):
        return self.mail.copy(
            src.at[slot, :, self.up_cut],
            self.below.at[slot, :, self.up_cut],
            self.send,
            self.recv + slot,
            self.at.along(1),
        )

    def downward(self, src, slot, last_step):
        return self.mail.copy(
            src.at[slot, :, self.down_cut],
            self.above.at[slot, :, self.down_cut],
            self.send + 1,
            self.recv + (self.at.planes if last_step else slot),
            self.at.along(-1),
        )

    def edge(self, slot):
        at, last = self.at, self.at.planes - 1
        if slot == 0:
            return

        @pl.when(at.b == 0)
        def _():
            self.upward(self.terms, slot).start()

        @pl.when(at.b == last)
        def _():
            self.downward(self.terms, last - slot, slot == 1).start()

    def hop(self, hop, rank):
        at, mail, last = self.at, self.mail, self.at.planes - 1
        slot = last - rank
        if slot <= hop:
            return

        @pl.when(at.b == hop)
        def _():
            cut = self.up_cut
            mail.arrived(self.below.at[slot, :, cut], self.recv + slot, at.along(-1))
            self.add(self.below, slot, cut)
            self.upward(self.below, slot).start()

        @pl.when(at.b == last - hop)
        def _():
            cut = self.down_cut
            mail.arrived(self.above.at[rank, :, cut], self.recv + rank, at.along(1))
            self.add(self.above, rank, cut)
            self.downward(self.above, rank, rank == last - hop - 1).start()

    def add(self, held, slot, cut):
        total = self.terms[slot, :, cut].astype(jnp.float32) + held[slot, :, cut].astype(
            jnp.float32
        )
        held[slot, :, cut] = total.astype(held.dtype)

    def landed(self):
        at, mail = self.at, self.mail

        @pl.when(at.b > 0)
        def _():
            mail.arrived(self.below.at[at.b, :, self.up_cut], self.recv + at.b, at.along(-1))

        @pl.when(at.b < at.planes - 1)
        def _():
            bulk = self.above.at[at.b, :, self.down_cut]
            mail.arrived(bulk, self.recv + at.planes, at.along(1))

    def total(self, out):
        b, last = self.at.b, self.at.planes - 1

        def put(*parts):
            value = self.terms[b].astype(jnp.float32)
            for part in parts:
                value = value + part[b].astype(jnp.float32)
            out[...] = value.astype(out.dtype)

        @pl.when(b == 0)
        def _():
            put(self.above)

        @pl.when(b == last)
        def _():
            put(self.below)

        @pl.when((b > 0) & (b < last))
        def _():
            put(self.below, self.above)

    def close(self):
        at, last = self.at, self.at.planes - 1
        for b in range(at.planes):

            @pl.when(at.b == b)
            def _():
                if b < last:
                    bulk = self.terms.at[pl.ds(0, last - b), :, self.up_cut]
                    self.mail.gone(bulk, self.send, at.along(1))
                if b > 0:
                    bulk = self.terms.at[pl.ds(0, b), :, self.down_cut]
                    self.mail.gone(bulk, self.send + 1, at.along(-1))


TILE = 256
LANES = 128


def dot_nn(a, b):
    return lax.dot_general(a, b, (((1,), (0,)), ((), ())), preferred_element_type=jnp.float32)


def dot_nt(a, b):
    return lax.dot_general(a, b, (((1,), (1,)), ((), ())), preferred_element_type=jnp.float32)


def dot_tn(a, b):
    return lax.dot_general(a, b, (((0,), (0,)), ((), ())), preferred_element_type=jnp.float32)


def turn(value, tables, rows, sign):
    straight, early, late = (table[rows, :] for table in tables)
    ahead = pltpu.roll(value, LANES - HD // 8, 1)
    behind = pltpu.roll(value, HD // 8, 1)
    return value * straight + sign * (ahead * early + behind * late)


def of_head(value, head):
    lane = lax.broadcasted_iota(jnp.int32, value.shape, 1)
    return jnp.where(lane // HD == head, value, jnp.zeros_like(value))


def total_rows(value):
    return jnp.sum(value, axis=0, keepdims=True)


class Layer:
    def __init__(self, refs):
        self.__dict__.update(refs)
        self.heads = LANES // HD
        if "xa" in refs:
            self.seqs, self.length, self.width = self.xa.shape
            self.per_seq = self.length // TILE
            self.tiles = self.seqs * self.per_seq

    def rows(self, tile):
        return pl.ds(pl.multiple_of(tile * TILE, TILE), TILE)

    def in_seq(self, ref, tile):
        rows = pl.ds(pl.multiple_of(tile % self.per_seq * TILE, TILE), TILE)
        return ref[tile // self.per_seq, rows, :]

    def loop(self, count, step):
        def run(i, carry):
            step(i)
            return carry

        lax.fori_loop(0, count, run, 0)

    def wide(self, row):
        planes = self.va.shape[0]
        return jnp.concatenate(
            [self.va[b, pl.ds(2 * row + a, 1), :] for b in range(planes) for a in range(2)], axis=1
        )

    def own_vectors(self, rank):
        lane = lax.broadcasted_iota(jnp.int32, (2, LANES), 1)
        row = lax.broadcasted_iota(jnp.int32, (2, LANES), 0)
        for j, ref in enumerate(self.vectors):
            piece = ref[...].astype(jnp.float32).reshape(1, ref.shape[0])
            piece = jnp.concatenate([piece] * (LANES // ref.shape[0]), axis=1)
            here = (lane // ref.shape[0] == rank % 4) & (row == rank // 4)
            self.vec_s[2 * j : 2 * j + 2, :] = jnp.where(here, jnp.broadcast_to(piece, here.shape), 0.0)
        bias = self.b_qkv[...].astype(jnp.float32).reshape(1, self.b_qkv.shape[0])
        self.vec_s[12:13, :] = jnp.concatenate(
            [bias, jnp.zeros((1, LANES - bias.shape[1]), jnp.float32)], axis=1
        )
        self.vec_s[13:14, :] = self.b_up[...].astype(jnp.float32).reshape(1, LANES)

    def plane_vectors(self, slot):
        total = jnp.sum(self.vec_in[...], axis=0)
        self.va[slot, 0:16, :] = total
        for rank in range(self.vec_in.shape[0]):
            self.va[slot, 16 + rank : 17 + rank, :] = self.vec_in[rank, 12:13, :]
            self.va[slot, 24 + rank : 25 + rank, :] = self.vec_in[rank, 13:14, :]

    def sort_weight(self):
        rows = self.wq_raw.shape[0]
        low = lax.broadcasted_iota(jnp.int32, (rows, LANES), 1) < HD
        for part in range(3):
            for core in range(2):
                for pair in range(2):
                    first, second = (
                        self.wq_raw[
                            :, pl.ds(part * self.width + (core * 2 + j) * 4 * HD + pair * LANES, LANES)
                        ].astype(jnp.float32)
                        for j in range(2)
                    )
                    cut = slice(part * LANES, (part + 1) * LANES)
                    self.wq_s[4 * pair + core, :, cut] = jnp.where(
                        low, first, pltpu.roll(second, HD, 1)
                    ).astype(jnp.bfloat16)
                    self.wq_s[4 * pair + 2 + core, :, cut] = jnp.where(
                        low, pltpu.roll(first, HD, 1), second
                    ).astype(jnp.bfloat16)

    def statistics(self):
        def step(i):
            x = self.in_seq(self.xa, i).astype(jnp.float32)
            center = jnp.mean(x, axis=1, keepdims=True)
            shifted = x - center
            spread = jnp.mean(shifted * shifted, axis=1, keepdims=True)
            self.center[self.rows(i), :] = center
            self.inverse[self.rows(i), :] = lax.rsqrt(spread + EPSILON)

        self.loop(self.tiles, step)

    def normed(self, i):
        x = self.in_seq(self.xa, i).astype(jnp.float32)
        return (x - self.center[self.rows(i), :]) * self.inverse[self.rows(i), :]

    def activations(self):
        gain_one, shift_one, gain_two, shift_two = (self.wide(j) for j in (1, 2, 3, 4))

        def step(i):
            normed = self.normed(i)
            self.act_one[self.rows(i), :] = (normed * gain_one + shift_one).astype(jnp.bfloat16)
            self.act_two[self.rows(i), :] = (normed * gain_two + shift_two).astype(jnp.bfloat16)

        self.loop(self.tiles, step)

    def qkv_bias(self, rank):
        size = HD // 2
        held = self.b_qkv.shape[0] // size
        ranks = self.vec_in.shape[0]
        pieces = []
        for i in range(3 * LANES // size):
            part, j, half = i // 4, i // 2 % 2, i % 2
            head = (rank % 2 * 2 + j) * 4 + rank // 2
            index = part * (self.width // size) + head * 2 + half
            owner, spot = index // held, index % held
            row = self.va[owner // ranks, pl.ds(16 + owner % ranks, 1), :]
            pieces.append(
                sum(
                    jnp.where(spot == k, row[:, k * size : (k + 1) * size], 0.0)
                    for k in range(held)
                )
            )
        return jnp.concatenate(pieces, axis=1)

    def near(self, ref, side):
        both = ref[pl.ds(side * 2, 2)]
        return both.reshape(both.shape[0] * both.shape[1], both.shape[2])

    def half_columns(self, side, width):
        return pl.ds(pl.multiple_of(side * (width // 2), width // 2), width // 2)

    def project_near(self, side):
        def step(i):
            cut = self.half_columns(side, self.width)
            self.qkv[self.rows(i), :] = dot_nn(self.act_one[self.rows(i), cut], self.near(self.wq, side))

        self.loop(self.tiles, step)

    def project(self, rank, side):
        bias = self.qkv_bias(rank)

        def step(i):
            cut = self.half_columns(side, self.width)
            qkv = dot_nn(self.act_one[self.rows(i), cut], self.near(self.wq, side))
            qkv = qkv + self.qkv[self.rows(i), :] + bias
            rows = pl.ds(pl.multiple_of(i % self.per_seq * TILE, TILE), TILE)
            query = turn(qkv[:, :LANES], self.tables, rows, 1.0).astype(jnp.bfloat16)
            self.query[self.rows(i), :] = query * jnp.asarray(1.0 / math.sqrt(HD), jnp.bfloat16)
            self.key[self.rows(i), :] = turn(
                qkv[:, LANES : 2 * LANES], self.tables, rows, 1.0
            ).astype(jnp.bfloat16)
            self.value[self.rows(i), :] = qkv[:, 2 * LANES :].astype(jnp.bfloat16)

        self.loop(self.tiles, step)

    def keys(self, seq, block):
        start = pl.multiple_of(seq * self.length, TILE)
        return pl.ds(start, (block + 1) * TILE)

    def attend(self, seq):
        for block in range(self.per_seq):
            rows = self.rows(seq * self.per_seq + block)
            keys = self.keys(seq, block)
            key, value, query = self.key[keys, :], self.value[keys, :], self.query[rows, :]
            out = None
            for head in range(self.heads):
                scores = dot_nt(of_head(query, head), key)
                at = lax.broadcasted_iota(jnp.int32, scores.shape, 0) + block * TILE
                to = lax.broadcasted_iota(jnp.int32, scores.shape, 1)
                scores = jnp.where(to <= at, scores, -jnp.inf)
                top = jnp.max(scores, axis=1, keepdims=True)
                weight = jnp.exp(scores - top)
                weight = weight * (1.0 / jnp.sum(weight, axis=1, keepdims=True))
                self.probs[block][seq * self.heads + head] = weight
                part = dot_nn(weight.astype(jnp.bfloat16), value)
                out = of_head(part, head) if out is None else out + of_head(part, head)
            self.attn[rows, :] = out.astype(jnp.bfloat16)

    def attend_out_grad(self):
        def step(i):
            weight = self.wo2[...].reshape(LANES, self.width)
            self.attn_grad[self.rows(i), :] = dot_nt(self.in_seq(self.ca, i), weight).astype(
                jnp.bfloat16
            )

        self.loop(self.tiles, step)

    def attend_grad(self, seq):
        key_grad, value_grad = [None] * self.per_seq, [None] * self.per_seq
        start = seq * self.per_seq
        for block in range(self.per_seq):
            rows = self.rows(start + block)
            keys = self.keys(seq, block)
            key, value, query = self.key[keys, :], self.value[keys, :], self.query[rows, :]
            grad = self.attn_grad[rows, :]
            inner = grad.astype(jnp.float32) * self.attn[rows, :].astype(jnp.float32)
            query_grad = None
            for head in range(self.heads):
                own_grad = of_head(grad, head)
                delta = jnp.sum(of_head(inner, head), axis=1, keepdims=True)
                probs = self.probs[block][seq * self.heads + head]
                grad_prob = dot_nt(own_grad, value)
                grad_score = (probs * (grad_prob - delta)).astype(jnp.bfloat16)
                part = dot_nn(grad_score, of_head(key, head))
                query_grad = part if query_grad is None else query_grad + part
                key_part = dot_tn(grad_score, of_head(query, head))
                value_part = dot_tn(probs.astype(jnp.bfloat16), own_grad)
                for b in range(block + 1):
                    cut = slice(b * TILE, (b + 1) * TILE)
                    key_grad[b] = key_part[cut] if key_grad[b] is None else key_grad[b] + key_part[cut]
                    value_grad[b] = (
                        value_part[cut] if value_grad[b] is None else value_grad[b] + value_part[cut]
                    )
            back = pl.ds(block * TILE, TILE)
            self.qkv_grad[rows, :LANES] = turn(
                query_grad * (1.0 / math.sqrt(HD)), self.tables, back, -1.0
            ).astype(jnp.bfloat16)
        for block in range(self.per_seq):
            rows = self.rows(start + block)
            back = pl.ds(block * TILE, TILE)
            self.qkv_grad[rows, LANES : 2 * LANES] = turn(
                key_grad[block], self.tables, back, -1.0
            ).astype(jnp.bfloat16)
            self.qkv_grad[rows, 2 * LANES :] = value_grad[block].astype(jnp.bfloat16)

    def cot_flat(self):
        return self.ca[...].reshape(self.seqs * self.length, self.width)

    def qkv_weight_grad(self, i):
        rows = self.gq.shape[1]
        act = self.act_one[:, pl.ds(pl.multiple_of(i * rows, rows), rows)]
        self.gq[i] = dot_tn(act, self.qkv_grad[...]).astype(jnp.bfloat16)

    def dense_weight_grad(self):
        self.go[...] = (
            dot_tn(self.attn[...], self.cot_flat()).astype(jnp.bfloat16).reshape(self.go.shape)
        )

    def expand(self, rank, side):
        cut = self.half_columns(side, self.hidden)
        slots = self.va.shape[0] // 2
        bias = jnp.concatenate(
            [self.va[side * slots + i, pl.ds(24 + rank, 1), :] for i in range(slots)], axis=1
        )

        def step(i):
            weight = self.wu[:, :, cut].reshape(self.width, self.hidden // 2)
            pre = dot_nn(self.act_two[self.rows(i), :], weight) + bias
            cdf = 0.5 * (1.0 + lax.erf(pre * INV_ROOT_TWO))
            self.gelu[self.rows(i), cut] = (pre * cdf).astype(jnp.bfloat16)
            self.slope[self.rows(i), cut] = cdf + pre * jnp.exp(-0.5 * pre * pre) * INV_ROOT_TWO_PI

        self.loop(self.tiles, step)

    def down_weight_grad(self, i):
        depth = self.gd.shape[1]
        part = self.gelu[:, pl.ds(pl.multiple_of(i * depth, depth), depth)]
        self.gd[i] = dot_tn(part, self.cot_flat()).astype(jnp.bfloat16)

    def hidden_grad(self, side):
        def step(i):
            cut = self.half_columns(side, self.hidden)
            grad = dot_nt(self.in_seq(self.ca, i), self.near(self.wd, side))
            self.pre_grad[self.rows(i), cut] = (grad * self.slope[self.rows(i), cut]).astype(
                jnp.bfloat16
            )

        self.loop(self.tiles, step)

    def up_weight_grad(self, i, side):
        rows = self.gu.shape[1]
        act = self.act_two[:, pl.ds(pl.multiple_of(i * rows, rows), rows)]
        cut = self.half_columns(side, self.hidden)
        self.gu[i, :, cut] = dot_tn(act, self.pre_grad[:, cut]).astype(jnp.bfloat16)

    def put_terms(self, terms, i, value):
        seq, chips, cores, rows, width = terms.shape
        n = TILE // (cores * rows)
        terms[i // self.per_seq, pl.ds(i % self.per_seq * n, n)] = value.astype(
            jnp.bfloat16
        ).reshape(n, cores, rows, width)

    def out_terms(self, i):
        dense = self.wo2[...].reshape(LANES, self.width)
        down = self.wd[...].reshape(self.hidden, self.width)
        self.put_terms(
            self.po,
            i,
            dot_nn(self.attn[self.rows(i), :], dense) + dot_nn(self.gelu[self.rows(i), :], down),
        )

    def in_terms(self, i):
        gain_one, gain_two = self.wide(1), self.wide(3)
        normed = self.normed(i)
        weight = self.wq[...].reshape(self.width, 3 * LANES)
        one = dot_nt(self.qkv_grad[self.rows(i), :], weight)
        weight = self.wu[...].reshape(self.width, self.hidden)
        two = dot_nt(self.pre_grad[self.rows(i), :], weight)
        self.put_terms(self.pg, i, one * gain_one + two * gain_two)
        for j, value in enumerate((one * normed, one, two * normed, two)):
            if i == 0:
                self.sums[j : j + 1, :] = total_rows(value)
            else:
                self.sums[j : j + 1, :] += total_rows(value)

    def split(self, raw, own):
        for seq in range(own.shape[0]):
            own[seq] = raw[:, seq, :]

    def own_rows(self, ref, rank):
        rows = self.out.shape[0]
        return ref[:, pl.ds(pl.multiple_of(rank * rows, rows), rows), :].astype(jnp.float32)

    def small_terms(self, rank):
        ranks = self.sm.shape[0]
        cot = total_rows(jnp.sum(self.own_rows(self.ca, rank), axis=0))
        for to in range(ranks):
            cut = slice(to * LANES, (to + 1) * LANES)
            self.sm[to, 0:1, :] = cot[:, cut]
            self.sm[to, 1:5, :] = self.sums[0:4, cut]

    def small_plane(self, slot):
        total = jnp.sum(self.sm_in[...], axis=0)
        self.vz[slot, 0:8, :] = total
        qkv = total_rows(self.qkv_grad[...].astype(jnp.float32))
        pre = total_rows(self.pre_grad[...].astype(jnp.float32))
        for j in range(3):
            self.vz[slot, 8 + j : 9 + j, :] = qkv[:, j * LANES : (j + 1) * LANES]
        for j in range(self.hidden // LANES):
            self.vz[slot, 12 + j : 13 + j, :] = pre[:, j * LANES : (j + 1) * LANES]

    def result(self, rank, out_sum, in_sum):
        x = self.own_rows(self.xa, rank)
        center = jnp.mean(x, axis=2, keepdims=True)
        shifted = x - center
        inverse = lax.rsqrt(jnp.mean(shifted * shifted, axis=2, keepdims=True) + EPSILON)
        normed = shifted * inverse
        bias = (self.wide(0) + self.wide(5))[None]
        value = (x + out_sum + bias).astype(jnp.bfloat16)
        grad = self.own_rows(self.ca, rank) + inverse * (
            in_sum
            - jnp.mean(in_sum, axis=2, keepdims=True)
            - normed * jnp.mean(in_sum * normed, axis=2, keepdims=True)
        )
        for seq in range(x.shape[0]):
            self.out[:, seq, :] = value[seq]
            self.in_grad[:, seq, :] = grad[seq]


SEND_SLOTS, RECV_SLOTS, NEAR_SLOTS = 37, 80, 22


def layer_kernel(names, planes, *refs):
    refs = dict(zip(names, refs))
    send, recv, near, second, third = (refs.pop(name) for name in names[-5:])
    refs.update(
        tables=tuple(refs["table"].at[i] for i in range(3)),
        probs=tuple(refs[name] for name in names if name.startswith("probs")),
        vectors=tuple(refs[name] for name in names if name.startswith("vector")),
        hidden=refs["gelu"].shape[1],
    )
    do = Layer(refs)
    at = Place(planes)
    mail = Mail(send, recv, near)
    b, c = at.b, at.c
    rows = do.wq_s.shape[1]
    pair = planes // 2
    others = pl.ds(0, 7)

    def shards(n):
        return do.xa.at[:, pl.ds(0, n * do.x_own.shape[1]), :]

    def strip(whole):
        return lambda rank: [whole.at[b, pl.ds(pl.multiple_of(rank * rows, rows), rows), :]]

    def band(whole):
        return lambda rank: [whole.at[pl.ds(pl.multiple_of(rank * rows, rows), rows), :]]

    def up_pieces(rank):
        return [
            do.wu_s.at[:, pl.ds(pl.multiple_of((p * 8 + rank) * LANES, LANES), LANES)]
            for p in range(planes)
        ]

    def up_landings(rank):
        strip_rows = pl.ds(pl.multiple_of(rank * rows, rows), rows)
        return [do.wu.at[b, strip_rows, pl.ds(p * LANES, LANES)] for p in range(planes)]

    gather_x = PlaneGather(at, mail, do.x_own, do.xa)
    gather_c = PlaneGather(at, mail, do.cot_own, do.ca)
    line_v, line_o = StarGather(at, mail, do.va), LineGather(at, mail, do.wo)
    line_q = LineGather(at, mail, do.wq)
    low, high = (pl.ds(i * do.hidden // 2, do.hidden // 2) for i in range(2))
    all_rows = pl.ds(0, do.wu.shape[1])
    line_ua = LineGather(at, mail, do.wu, (all_rows, low), (all_rows, high))
    line_ub = LineGather(at, mail, do.wu, (all_rows, high), (all_rows, low))
    half = do.wd.shape[1] // 2
    cuts = [(pl.ds(i * half, half), pl.ds(0, do.wd.shape[2])) for i in range(2)]
    line_da = LineGather(at, mail, do.wd, cuts[0], cuts[0])
    line_db = LineGather(at, mail, do.wd, cuts[1], cuts[1])
    ex_v = PlaneExchange(at, mail, lambda rank: [do.vec_s], lambda rank: [do.vec_in.at[rank]], do.vec_in.at[others])
    ex_q = PlaneExchange(
        at, mail, lambda rank: [do.wq_s.at[rank]], strip(do.wq), do.wq_s.at[others]
    )
    ex_u = PlaneExchange(at, mail, up_pieces, up_landings, do.wu.at[0, pl.ds(0, 7 * rows)])
    mine = do.wo2.at[:, c]
    swap_w = PairExchange(
        at, mail, do.wo.at[pl.ds(pair * (1 - c), pair)], mine, do.wo2.at[:, 1 - c]
    )
    sum_o = LineReduce(at, mail, do.go4, do.above_o, do.below_o)
    sum_q = LineReduce(at, mail, do.gq, do.above_q, do.below_q)
    sum_un = LineReduce(at, mail, do.gu, do.above_u, do.below_u, low, high)
    sum_uf = LineReduce(at, mail, do.gu, do.above_u, do.below_u, high, low)
    near_side = b // pair
    far_side = 1 - near_side
    sum_d = LineReduce(at, mail, do.gd, do.above_d, do.below_d)
    swap_g = PairExchange(
        at,
        mail,
        do.go.at[:, 1 - c],
        do.go4.at[pl.ds(pair * c, pair)],
        do.go4.at[pl.ds(pair * (1 - c), pair)],
    )
    back_q = PlaneExchange(
        at, mail, band(do.fq), lambda rank: [do.dq.at[rank]], do.fq.at[pl.ds(0, 7 * rows)]
    )
    back_u = PlaneExchange(
        at, mail, band(do.fu), lambda rank: [do.du.at[rank]], do.fu.at[pl.ds(0, 7 * rows)]
    )
    fold_v = PlaneExchange(
        at, mail, lambda rank: [do.sm.at[rank]], lambda rank: [do.sm_in.at[rank]], do.sm.at[others]
    )
    line_s = StarGather(at, mail, do.vz)
    share_v = PlaneExchange(
        at, mail, lambda rank: [do.vt], lambda rank: [do.dv.at[rank]], do.dv.at[others]
    )
    plane_o = PlaneReduce(at, mail, do.po, do.pairs_o, do.sums_o, do.side_o, shards)
    plane_g = PlaneReduce(at, mail, do.pg, do.pairs_g, do.sums_g, do.side_g, shards)

    slots = [s + b // pair * (planes - 1 - 2 * s) for s in (3, 0, 2, 1)]
    turned = [s + b // pair * (planes - 1 - 2 * s) for s in (3, 2, 1, 0)]

    at.barrier()
    line_da.start(do.wd_s)
    own_d = mail.bring(do.wd_s, do.wd.at[b])
    raw_x = mail.bring(do.x_in, do.x_raw)
    ex_u.start()
    line_db.start(do.wd_s)
    at.reach(second, third)
    do.own_vectors(at.t)
    ex_v.start()
    line_o.start(do.wo_s)
    own_o = mail.bring(do.wo_s, do.wo.at[b])
    raw_x.wait()
    do.split(do.x_raw, do.x_own)
    gather_x.start()
    ex_u.finish()
    line_ua.start()
    gather_x.relay_x()
    gather_x.relay_y()
    own_raw = mail.bring(do.wq_in, do.wq_raw)
    ex_v.finish()
    do.plane_vectors(b)
    line_v.start()
    raw_c = mail.bring(do.cot_in, do.cot_raw)
    line_ub.start()
    own_o.wait()
    own_raw.wait()
    do.sort_weight()
    ex_q.start()
    line_ua.inner(1)
    raw_c.wait()
    do.split(do.cot_raw, do.cot_own)
    gather_x.share()
    line_ua.outer(1)
    line_v.finish()
    gather_x.far()
    gather_c.start()
    own_table = mail.bring(do.table_in, do.table)
    line_ub.outer(1)
    line_ub.inner(1)
    gather_x.finish()
    do.statistics()
    do.activations()
    line_ua.inner(2)
    line_o.take(1)
    gather_c.relay_y()
    own_d.wait()
    line_ub.inner(2)
    gather_c.relay_x()
    ex_q.finish()
    line_q.start()
    gather_c.share()
    line_ua.inner(3)
    do.expand(at.t, far_side)
    gather_c.far()
    own_table.wait()
    line_o.take(2)
    gather_c.finish()
    do.down_weight_grad(turned[0])
    sum_d.edge(3)
    do.down_weight_grad(turned[1])
    sum_d.edge(2)
    line_ub.inner(3)
    line_q.take(1)
    do.expand(at.t, near_side)
    do.down_weight_grad(turned[2])
    sum_d.edge(1)
    do.down_weight_grad(turned[3])
    sum_d.edge(0)
    line_o.take(3)
    swap_w.start()
    mine[...] = do.wo[pl.ds(pair * c, pair)]
    do.project_near(near_side)
    swap_w.finish()
    do.attend_out_grad()
    line_q.take(2)
    line_da.take(1)
    line_db.take(1)
    do.hidden_grad(near_side)
    do.up_weight_grad(slots[0], near_side)
    sum_un.edge(3)
    do.up_weight_grad(slots[1], near_side)
    sum_un.edge(0)
    do.up_weight_grad(slots[2], near_side)
    sum_un.edge(2)
    do.up_weight_grad(slots[3], near_side)
    sum_un.edge(1)
    line_q.take(3)
    do.project(at.t, far_side)
    do.attend(0)
    do.attend(1)
    do.dense_weight_grad()
    swap_g.start()
    do.go4[pl.ds(pair * c, pair)] = do.go[:, c]
    do.attend_grad(0)
    sum_d.hop(1, 0)
    do.attend_grad(1)
    line_da.take(2)
    do.qkv_weight_grad(slots[0])
    sum_q.edge(3)
    do.qkv_weight_grad(slots[1])
    sum_q.edge(0)
    do.qkv_weight_grad(slots[2])
    sum_q.edge(2)
    do.qkv_weight_grad(slots[3])
    sum_q.edge(1)
    line_db.take(2)
    line_da.take(3)
    line_db.take(3)
    do.out_terms(0)
    do.out_terms(1)
    sum_un.hop(1, 0)
    do.out_terms(2)
    do.out_terms(3)
    plane_o.start()
    do.hidden_grad(far_side)
    do.up_weight_grad(slots[0], far_side)
    sum_uf.edge(3)
    sum_d.hop(1, 1)
    do.up_weight_grad(slots[1], far_side)
    sum_uf.edge(0)
    plane_o.fold()
    do.in_terms(0)
    sum_d.hop(2, 0)
    do.up_weight_grad(slots[2], far_side)
    sum_uf.edge(2)
    plane_o.turn()
    sum_q.hop(1, 0)
    do.in_terms(1)
    do.in_terms(2)
    do.in_terms(3)
    plane_g.start()
    do.up_weight_grad(slots[3], far_side)
    sum_uf.edge(1)
    sum_q.hop(1, 1)
    sum_q.hop(2, 0)
    do.small_terms(at.t)
    fold_v.start()
    sum_un.hop(2, 0)
    sum_un.hop(1, 1)
    plane_g.fold()
    sum_uf.hop(1, 0)
    sum_q.landed()
    sum_q.total(do.fq)
    back_q.start()
    plane_g.turn()
    fold_v.finish()
    do.small_plane(b)
    line_s.start()
    sum_uf.hop(1, 1)
    sum_d.landed()
    sum_d.total(do.dd)
    out_d = mail.bring(do.dd, do.dd_to)
    swap_g.finish()
    sum_o.edge(3)
    sum_o.edge(2)
    sum_o.edge(1)
    sum_uf.hop(2, 0)
    back_q.finish()
    sum_o.hop(1, 0)
    sum_un.landed()
    sum_uf.landed()
    sum_un.total(do.fu)
    back_u.start()
    do.result(at.t, plane_o.finish(), plane_g.finish())
    out_x = mail.bring(do.out, do.out_to)
    out_g = mail.bring(do.in_grad, do.in_grad_to)
    sum_o.hop(1, 1)
    sum_o.hop(2, 0)
    line_s.finish()
    do.vt[...] = jnp.sum(do.vz[...], axis=0)
    share_v.start()
    sum_o.landed()
    sum_o.total(do.dd_o)
    out_o = mail.bring(do.dd_o, do.dd_o_to)
    back_u.finish()
    share_v.finish()
    for copied in (out_o, out_d, out_x, out_g):
        copied.wait()
    for line in (gather_x, gather_c, line_v, line_o, line_q, line_ua, line_ub, line_da, line_db, line_s, ex_v, ex_q, ex_u, back_q, back_u, fold_v, share_v, swap_w, swap_g, plane_o, plane_g, sum_o, sum_q, sum_un, sum_uf, sum_d):
        line.close()


def finish_kernel(names, planes, *refs):
    refs = dict(zip(names, refs))
    near = refs.pop(names[-1])
    do = Layer(refs)
    at = Place(planes)
    ranks, rows = do.dq.shape[:2]
    moves = []

    def move(src, dst):
        moves.append(pltpu.make_async_copy(src, dst, near.at[len(moves)]))
        moves[-1].start()

    move(do.in_grad, do.in_grad_out)
    move(do.dd, do.down_out)
    move(do.out, do.out_out)
    move(do.dd_o, do.dense_out)
    for rank in range(ranks):
        for b in range(planes):
            first = (b * ranks + rank) * LANES
            do.up_v[:, first : first + LANES] = do.du[
                rank, :, b * LANES : (b + 1) * LANES
            ].astype(jnp.float32)
    move(do.up_v, do.up_out)
    low = lax.broadcasted_iota(jnp.int32, (rows, LANES), 1) < HD
    for part in range(3):
        for core in range(2):
            for pair in range(ranks // 4):
                first, second = (
                    do.dq[2 * (2 * pair + i) + core, :, part * LANES : (part + 1) * LANES].astype(
                        jnp.float32
                    )
                    for i in range(2)
                )
                for j in range(2):
                    both = (
                        jnp.where(low, first, pltpu.roll(second, HD, 1))
                        if j == 0
                        else jnp.where(low, pltpu.roll(first, HD, 1), second)
                    )
                    start = (part * 4 + core * 2 + j) * ranks // 2 * HD + pair * LANES
                    do.qkv_v[:, start : start + LANES] = both
    move(do.qkv_v, do.qkv_out)
    piece = lax.rem(at.t, 4)
    row = (at.b * ranks + at.t) // 4
    values = do.dv[pl.ds(row, 1), 0:8, :].reshape(8, LANES)
    front = jnp.zeros((8, rows), jnp.float32)
    for i in range(4):
        cut = values[:, i * rows : (i + 1) * rows]
        front = front + jnp.where(piece == i, cut, jnp.zeros_like(cut))
    for j, ref in enumerate(
        (do.dense_bias, do.gain_one, do.shift_one, do.gain_two, do.shift_two)
    ):
        ref[...] = front[j].reshape(rows)
    do.down_bias[...] = front[0].reshape(rows)
    do.up_bias[...] = do.dv[pl.ds(at.t, 1), pl.ds(12 + at.b, 1), :].reshape(LANES)
    pieces = []
    for i in range(3):
        index = (at.b * ranks + at.t) * 3 + i
        part, inner = index // 32, lax.rem(index, 32)
        head, half = inner // 2, lax.rem(inner, 2)
        core, j, chip = head // 8, lax.rem(head // 4, 2), lax.rem(head, 4)
        value = do.dv[pl.ds(chip * 2 + core, 1), pl.ds(8 + part, 1), :].reshape(1, LANES)
        spot = 2 * j + half
        total = jnp.zeros((1, rows), jnp.float32)
        for k in range(4):
            cut = value[:, k * rows : (k + 1) * rows]
            total = total + jnp.where(spot == k, cut, jnp.zeros_like(cut))
        pieces.append(total)
    do.qkv_bias[...] = jnp.concatenate(pieces, axis=1).reshape(3 * rows)
    for made in moves:
        made.wait()


VMEM = pl.BlockSpec(memory_space=pltpu.VMEM)


def rotary_rows(length):
    half = HD // 8
    frequency = 1.0 / 10000.0 ** (np.arange(half) * (1.0 / half))
    angles = np.arange(length)[:, None] * frequency[None, :]
    table = np.zeros((3, length, HD))
    table[0] = 1.0
    table[0, :, :half] = table[0, :, half : 2 * half] = np.cos(angles)
    table[1, :, :half] = -np.sin(angles)
    table[2, :, half : 2 * half] = np.sin(angles)
    return np.tile(table, (1, 1, LANES // HD)).astype(np.float32)


def body(shape, *operands):
    residual_in, qkv_weight, down_weight = operands[0], operands[1], operands[11]
    planes = shape[BATCH]
    ranks = shape[ULY] * shape[BLK]
    tok_rows, seqs, width = residual_in.shape
    fits = (
        (shape[ULY], shape[BLK]) == (2, 4)
        and planes == 4
        and seqs % 2 == 0
        and 2 * qkv_weight.shape[0] == HD
        and width == ranks * LANES
        and ranks * tok_rows % TILE == 0
        and TILE % (2 * tok_rows) == 0
        and down_weight.shape[0] == LANES
    )
    return fast_body(planes, *operands) if fits else general_body(*operands)


def fast_body(
    planes,
    residual_in,
    qkv_weight,
    qkv_bias,
    dense_weight,
    dense_bias,
    norm1_gain,
    norm1_bias,
    norm2_gain,
    norm2_bias,
    up_weight,
    up_bias,
    down_weight,
    down_bias,
    cotangent,
):
    single = jnp.float32
    half_type = jnp.bfloat16
    tok_rows, seqs, width = residual_in.shape
    ranks = width // LANES
    rows = qkv_weight.shape[0]
    depth = down_weight.shape[0]
    hidden = planes * depth
    pair = planes // 2
    length = ranks * tok_rows
    tokens = seqs * length
    rank = lax.axis_index(ULY) * lax.axis_size(BLK) + lax.axis_index(BLK)
    owner = lax.axis_index(BATCH) * ranks + rank

    anywhere = pl.BlockSpec(memory_space=pl.ANY)
    in_hbm = pl.BlockSpec(memory_space=pltpu.HBM)
    inputs = dict(
        x_in=(residual_in, in_hbm),
        cot_in=(cotangent, in_hbm),
        wq_in=(qkv_weight, in_hbm),
        wu_s=(up_weight, in_hbm),
        wd_s=(down_weight, in_hbm),
        wo_s=(dense_weight, in_hbm),
        table_in=(jnp.asarray(rotary_rows(length)), in_hbm),
        b_qkv=(qkv_bias, VMEM),
        b_up=(up_bias, VMEM),
    )
    for i, v in enumerate((dense_bias, norm1_gain, norm1_bias, norm2_gain, norm2_bias, down_bias)):
        inputs["vector%d" % i] = (v, VMEM)
    shard = (seqs, tok_rows, width)
    outputs = dict(
        out_to=(residual_in.shape, half_type),
        in_grad_to=(residual_in.shape, single),
        dq=((ranks, rows, 3 * LANES), half_type),
        du=((ranks, rows, hidden), half_type),
        dd_to=((depth, width), single),
        dd_o_to=((rows, width), single),
        dv=((ranks, 16, LANES), single),
    )
    q_shape = (planes, ranks * rows, 3 * LANES)
    u_shape = (planes, ranks * rows, hidden)
    d_shape = (planes, depth, width)
    o_shape = (planes, rows, width)
    chips = ranks // 2
    scratch = dict(
        xa=((seqs, length, width), half_type),
        ca=((seqs, length, width), half_type),
        wq=(q_shape, half_type),
        wu=(u_shape, half_type),
        wd=(d_shape, half_type),
        wo=(o_shape, half_type),
        wo2=((pair, 2, rows, width), half_type),
        x_raw=(residual_in.shape, half_type),
        cot_raw=(residual_in.shape, half_type),
        x_own=(shard, half_type),
        cot_own=(shard, half_type),
        qkv=((tokens, 3 * LANES), single),
        wq_raw=(qkv_weight.shape, half_type),
        wq_s=((ranks, rows, 3 * LANES), half_type),
        table=((3, length, LANES), single),
        out=(residual_in.shape, half_type),
        in_grad=(residual_in.shape, single),
        dd=((depth, width), single),
        dd_o=((rows, width), single),
        vec_s=((16, LANES), single),
        vec_in=((ranks, 16, LANES), single),
        va=((planes, 32, LANES), single),
        center=((tokens, 1), single),
        inverse=((tokens, 1), single),
        act_one=((tokens, width), half_type),
        act_two=((tokens, width), half_type),
        query=((tokens, LANES), half_type),
        key=((tokens, LANES), half_type),
        value=((tokens, LANES), half_type),
        attn=((tokens, LANES), half_type),
        attn_grad=((tokens, LANES), half_type),
        qkv_grad=((tokens, 3 * LANES), half_type),
        gelu=((tokens, hidden), half_type),
        slope=((tokens, hidden), single),
        pre_grad=((tokens, hidden), half_type),
        gq=(q_shape, half_type),
        gu=(u_shape, half_type),
        gd=(d_shape, half_type),
        go=((pair, 2, rows, width), half_type),
        go4=(o_shape, half_type),
        above_q=(q_shape, half_type),
        below_q=(q_shape, half_type),
        above_u=(u_shape, half_type),
        below_u=(u_shape, half_type),
        above_d=(d_shape, half_type),
        below_d=(d_shape, half_type),
        above_o=(o_shape, half_type),
        below_o=(o_shape, half_type),
        fq=(q_shape[1:], half_type),
        fu=(u_shape[1:], half_type),
        po=((seqs, chips, 2, tok_rows, width), half_type),
        pg=((seqs, chips, 2, tok_rows, width), half_type),
        pairs_o=((seqs, chips, tok_rows, width), half_type),
        pairs_g=((seqs, chips, tok_rows, width), half_type),
        sums_o=((seqs, chips, tok_rows, width), half_type),
        sums_g=((seqs, chips, tok_rows, width), half_type),
        side_o=((3,) + shard, half_type),
        side_g=((3,) + shard, half_type),
        sums=((8, width), single),
        sm=((ranks, 8, LANES), single),
        sm_in=((ranks, 8, LANES), single),
        vz=((planes, 16, LANES), single),
        vt=((16, LANES), single),
    )
    for block in range(length // TILE):
        scratch["probs%d" % block] = ((seqs * LANES // HD, TILE, (block + 1) * TILE), single)
    names = tuple(inputs) + tuple(outputs) + tuple(scratch) + ("send", "recv", "near", "second", "third")
    out, in_grad, dq, du, dd, dd_o, dv = pl.pallas_call(
        functools.partial(layer_kernel, names, planes),
        out_shape=[jax.ShapeDtypeStruct(*what) for what in outputs.values()],
        in_specs=[where for _, where in inputs.values()],
        out_specs=[anywhere] * len(outputs),
        scratch_shapes=[pltpu.VMEM(*what) for what in scratch.values()]
        + [pltpu.SemaphoreType.DMA((n,)) for n in (SEND_SLOTS, RECV_SLOTS, NEAR_SLOTS)]
        + [pltpu.SemaphoreType.REGULAR] * 2,
        compiler_params=pltpu.CompilerParams(
            collective_id=0, has_side_effects=True, vmem_limit_bytes=52 * 2**20
        ),
    )(
        *(
            pltpu.with_memory_space_constraint(value, pltpu.HBM) for value, _ in inputs.values()
        )
    )

    results = dict(
        out_out=(residual_in.shape, half_type),
        in_grad_out=(residual_in.shape, single),
        qkv_out=(qkv_weight.shape, single),
        qkv_bias=(qkv_bias.shape, single),
        dense_out=(dense_weight.shape, single),
        dense_bias=(dense_bias.shape, single),
        gain_one=(norm1_gain.shape, single),
        shift_one=(norm1_bias.shape, single),
        gain_two=(norm2_gain.shape, single),
        shift_two=(norm2_bias.shape, single),
        up_out=(up_weight.shape, single),
        up_bias=(up_bias.shape, single),
        down_out=(down_weight.shape, single),
        down_bias=(down_bias.shape, single),
    )
    given = tuple(n.removesuffix("_to") for n in outputs)
    staged = dict(up_v=results["up_out"], qkv_v=results["qkv_out"])
    return tuple(
        pl.pallas_call(
            functools.partial(
                finish_kernel, given + tuple(results) + tuple(staged) + ("near",), planes
            ),
            out_shape=[jax.ShapeDtypeStruct(*what) for what in results.values()],
            in_specs=[VMEM] * len(given),
            out_specs=[anywhere if len(what[0]) > 1 else VMEM for what in results.values()],
            scratch_shapes=[pltpu.VMEM(*what) for what in staged.values()]
            + [pltpu.SemaphoreType.DMA((8,))],
            compiler_params=pltpu.CompilerParams(vmem_limit_bytes=8 * 2**20),
        )(out, in_grad, dq, du, dd, dd_o, dv)
    )


def solution(mesh):
    placed = (
        P(TOKENS, BATCH, None),
        P(AXES, None),
        P(AXES),
        P(AXES, None),
        P(AXES),
        P(AXES),
        P(AXES),
        P(AXES),
        P(AXES),
        P(AXES, None),
        P(AXES),
        P(AXES, None),
        P(AXES),
        P(TOKENS, BATCH, None),
    )
    return jax.shard_map(
        functools.partial(body, dict(mesh.shape)),
        mesh=mesh,
        in_specs=placed,
        out_specs=(
            P(TOKENS, BATCH, None),
            P(TOKENS, BATCH, None),
            P(AXES, None),
            P(AXES),
            P(AXES, None),
            P(AXES),
            P(AXES),
            P(AXES),
            P(AXES),
            P(AXES),
            P(AXES, None),
            P(AXES),
            P(AXES, None),
            P(AXES),
        ),
        check_vma=False,
    )
```

```python
import functools
import math

import jax
import jax.numpy as jnp
import numpy as np
from jax import lax
from jax.experimental import pallas as pl
from jax.experimental.pallas import tpu as pltpu
from jax.sharding import PartitionSpec as P

HD = 64
BATCH, ULY, BLK = "batch", "ulysses", "blk"
AXES = (BATCH, ULY, BLK)
TOKENS = (ULY, BLK)


EPSILON = 1e-05
INV_ROOT_TWO = 0.7071067811865476
INV_ROOT_TWO_PI = 0.3989422804014327


def layer_norm(values):
    center = jnp.mean(values, axis=-1, keepdims=True)
    shifted = values - center
    inverse = lax.rsqrt(jnp.mean(shifted * shifted, axis=-1, keepdims=True) + EPSILON)
    return (shifted * inverse, inverse)


def norm_back(gradient, normed, inverse, gain_vec):
    scaled = gradient * gain_vec
    return inverse * (
        scaled
        - jnp.mean(scaled, axis=-1, keepdims=True)
        - normed * jnp.mean(scaled * normed, axis=-1, keepdims=True)
    )


def gelu_value(pre_values):
    return 0.5 * pre_values * (1.0 + jax.scipy.special.erf(pre_values * INV_ROOT_TWO))


def gelu_slope(pre_values):
    normal_cdf = 0.5 * (1.0 + jax.scipy.special.erf(pre_values * INV_ROOT_TWO))
    return normal_cdf + pre_values * jnp.exp(-0.5 * pre_values * pre_values) * INV_ROOT_TWO_PI


def rotary_tables(positions, rotary):
    half_rot = rotary // 2
    frequency = 1.0 / 10000.0 ** (jnp.arange(half_rot, dtype=jnp.float32) * (2.0 / rotary))
    angles = positions.astype(jnp.float32)[:, None] * frequency[None, :]
    cosine = jnp.concatenate([jnp.cos(angles), jnp.cos(angles)], axis=-1)
    sine_table = jnp.concatenate([jnp.sin(angles), jnp.sin(angles)], axis=-1)
    return (cosine, sine_table)


def expand_table(table, tensor):
    extra_dims = (1,) * (tensor.ndim - 2)
    return table.reshape((table.shape[0],) + extra_dims + (table.shape[1],))


def rotate_fwd(tensor, cosine, sine_table, rotary):
    half_rot = rotary // 2
    cos_full = expand_table(cosine, tensor)
    sin_full = expand_table(sine_table, tensor)
    rot_part = tensor[..., :rotary]
    turned = jnp.concatenate([-rot_part[..., half_rot:], rot_part[..., :half_rot]], axis=-1)
    return jnp.concatenate([rot_part * cos_full + turned * sin_full, tensor[..., rotary:]], axis=-1)


def rotate_back(tensor, cosine, sine_table, rotary):
    half_rot = rotary // 2
    cos_full = expand_table(cosine, tensor)
    sin_full = expand_table(sine_table, tensor)
    rot_part = tensor[..., :rotary]
    weighted = rot_part * sin_full
    turned = jnp.concatenate([weighted[..., half_rot:], -weighted[..., :half_rot]], axis=-1)
    return jnp.concatenate([rot_part * cos_full + turned, tensor[..., rotary:]], axis=-1)


def general_body(
    residual_in,
    qkv_weight,
    qkv_bias,
    dense_weight,
    dense_bias,
    norm1_gain,
    norm1_bias,
    norm2_gain,
    norm2_bias,
    up_weight,
    up_bias,
    down_weight,
    down_bias,
    cotangent,
):
    single = jnp.float32
    half_type = jnp.bfloat16
    gathered = (
        lax.all_gather(qkv_weight, AXES, axis=0, tiled=True),
        lax.all_gather(qkv_bias, AXES, axis=0, tiled=True),
        lax.all_gather(dense_weight, AXES, axis=0, tiled=True),
        lax.all_gather(dense_bias, AXES, axis=0, tiled=True),
        lax.all_gather(norm1_gain, AXES, axis=0, tiled=True),
        lax.all_gather(norm1_bias, AXES, axis=0, tiled=True),
        lax.all_gather(norm2_gain, AXES, axis=0, tiled=True),
        lax.all_gather(norm2_bias, AXES, axis=0, tiled=True),
        lax.all_gather(up_weight, AXES, axis=0, tiled=True),
        lax.all_gather(up_bias, AXES, axis=0, tiled=True),
        lax.all_gather(down_weight, AXES, axis=0, tiled=True),
        lax.all_gather(down_bias, AXES, axis=0, tiled=True),
    )
    (
        w_qkv,
        b_qkv,
        w_dense,
        b_dense,
        gain_one,
        shift_one,
        gain_two,
        shift_two,
        w_up,
        b_up,
        w_down,
        b_down,
    ) = gathered
    tok_rows = residual_in.shape[0]
    seq_count = residual_in.shape[1]
    model_width = residual_in.shape[2]
    head_count = model_width // HD
    rotary = HD // 4
    scale_factor = 1.0 / math.sqrt(HD)
    blk_size = lax.axis_size(BLK)
    uly_size = lax.axis_size(ULY)
    blk_index = lax.axis_index(BLK)
    block_id = lax.axis_index(ULY) * blk_size + blk_index
    seq_pos = block_id * tok_rows + jnp.arange(tok_rows, dtype=jnp.int32)
    inputs_f = residual_in.astype(single)
    normed, inverse = layer_norm(inputs_f)
    act_one = (normed * gain_one.astype(single) + shift_one.astype(single)).astype(half_type)
    act_two = (normed * gain_two.astype(single) + shift_two.astype(single)).astype(half_type)
    qkv_full = jnp.einsum(
        "tsd,df->tsf", act_one, w_qkv, preferred_element_type=single
    ) + b_qkv.astype(single)
    cos_seq, sin_seq = rotary_tables(seq_pos, rotary)
    head_shape = (tok_rows, seq_count, head_count, HD)
    query_seq = (
        rotate_fwd(qkv_full[..., :model_width].reshape(head_shape), cos_seq, sin_seq, rotary)
        .reshape(tok_rows, seq_count, model_width)
        .astype(half_type)
    )
    key_seq = (
        rotate_fwd(
            qkv_full[..., model_width : 2 * model_width].reshape(head_shape),
            cos_seq,
            sin_seq,
            rotary,
        )
        .reshape(tok_rows, seq_count, model_width)
        .astype(half_type)
    )
    value_seq = qkv_full[..., 2 * model_width :].astype(half_type)
    query_loc, key_loc, value_loc = (
        lax.all_to_all(query_seq, ULY, split_axis=2, concat_axis=0, tiled=True),
        lax.all_to_all(key_seq, ULY, split_axis=2, concat_axis=0, tiled=True),
        lax.all_to_all(value_seq, ULY, split_axis=2, concat_axis=0, tiled=True),
    )
    local_rows = query_loc.shape[0]
    features = query_loc.shape[2]
    local_heads = features // HD
    key_all, value_all = (
        lax.all_gather(key_loc, BLK, axis=0, tiled=True),
        lax.all_gather(value_loc, BLK, axis=0, tiled=True),
    )
    total_rows = key_all.shape[0]
    row_ids = jnp.arange(local_rows, dtype=jnp.int32)
    query_pos = (row_ids // tok_rows * blk_size + blk_index) * tok_rows + row_ids % tok_rows
    block_rows = math.gcd(512, local_rows)
    n_blocks = local_rows // block_rows
    query_h = query_loc.reshape(local_rows, seq_count, local_heads, HD)
    key_h = jnp.transpose(
        key_all.reshape(blk_size, uly_size, tok_rows, seq_count, features), (1, 0, 2, 3, 4)
    ).reshape(total_rows, seq_count, local_heads, HD)
    value_h = jnp.transpose(
        value_all.reshape(blk_size, uly_size, tok_rows, seq_count, features), (1, 0, 2, 3, 4)
    ).reshape(total_rows, seq_count, local_heads, HD)
    zero_idx = jnp.zeros((), jnp.int32)
    step_ids = jnp.arange(n_blocks * seq_count, dtype=jnp.int32)
    row_shape = (block_rows, 1, local_heads, HD)

    def select(step_index):
        row_start = step_index // seq_count * block_rows
        seq_index = step_index % seq_count
        query_rows = lax.dynamic_slice(
            query_h, (row_start, seq_index, zero_idx, zero_idx), row_shape
        )
        limit = jnp.max(query_pos) // block_rows + 1
        return (row_start, seq_index, query_rows, query_pos, limit)

    def block_scores(query_rows, row_pos, key_index, seq_index):
        key_start = key_index * block_rows
        slot = (key_start, seq_index, zero_idx, zero_idx)
        key_rows = lax.dynamic_slice(key_h, slot, (block_rows, 1, local_heads, HD))
        value_rows = lax.dynamic_slice(value_h, slot, (block_rows, 1, local_heads, HD))
        scores = (
            jnp.einsum("qshd,kshd->shqk", query_rows, key_rows, preferred_element_type=single)
            * scale_factor
        )
        key_ids = key_start + jnp.arange(block_rows, dtype=jnp.int32)
        allowed = (key_ids[None, :] <= row_pos[:, None])[None, None]
        return (jnp.where(allowed, scores, -jnp.inf), key_rows, value_rows, slot)

    def forward_block(step_index):
        row_start, seq_index, query_rows, row_pos, limit = select(step_index)

        def total_step(key_index, carry):
            running_max, running_sum = carry
            masked, key_rows, value_rows, slot = block_scores(
                query_rows, row_pos, key_index, seq_index
            )
            new_max = jnp.maximum(running_max, jnp.max(masked, axis=-1))
            new_sum = running_sum * jnp.exp(running_max - new_max) + jnp.sum(
                jnp.exp(masked - new_max[..., None]), axis=-1
            )
            return (new_max, new_sum)

        start_max = jnp.full((1, local_heads, block_rows), -jnp.inf, single)
        start_sum = jnp.zeros((1, local_heads, block_rows), single)
        final_max, final_sum = lax.fori_loop(zero_idx, limit, total_step, (start_max, start_sum))
        log_total = final_max + jnp.log(final_sum)

        def value_step(key_index, acc):
            masked, key_rows, value_rows, slot = block_scores(
                query_rows, row_pos, key_index, seq_index
            )
            weights_b = jnp.exp(masked - log_total[..., None]).astype(half_type)
            return acc + jnp.einsum(
                "shqk,kshd->qshd", weights_b, value_rows, preferred_element_type=single
            )

        result = lax.fori_loop(zero_idx, limit, value_step, jnp.zeros(row_shape, single)).astype(
            half_type
        )
        return (result[:, 0], log_total)

    results, log_totals = lax.map(forward_block, step_ids)
    attn_h = jnp.transpose(
        results.reshape(n_blocks, seq_count, block_rows, local_heads, HD), (0, 2, 1, 3, 4)
    ).reshape(local_rows, seq_count, local_heads, HD)
    attn_seq = lax.all_to_all(
        attn_h.reshape(local_rows, seq_count, features),
        ULY,
        split_axis=0,
        concat_axis=2,
        tiled=True,
    )
    proj_out = jnp.einsum(
        "tsd,de->tse", attn_seq, w_dense, preferred_element_type=single
    ) + b_dense.astype(single)
    pre_act = jnp.einsum("tsd,df->tsf", act_two, w_up, preferred_element_type=single) + b_up.astype(
        single
    )
    gelu_out = gelu_value(pre_act).astype(half_type)
    mlp_out = jnp.einsum(
        "tsf,fd->tsd", gelu_out, w_down, preferred_element_type=single
    ) + b_down.astype(single)
    output = (inputs_f + proj_out + mlp_out).astype(half_type)
    back_params = (
        lax.all_gather(qkv_weight, AXES, axis=0, tiled=True),
        lax.all_gather(qkv_bias, AXES, axis=0, tiled=True),
        lax.all_gather(dense_weight, AXES, axis=0, tiled=True),
        lax.all_gather(dense_bias, AXES, axis=0, tiled=True),
        lax.all_gather(norm1_gain, AXES, axis=0, tiled=True),
        lax.all_gather(norm1_bias, AXES, axis=0, tiled=True),
        lax.all_gather(norm2_gain, AXES, axis=0, tiled=True),
        lax.all_gather(norm2_bias, AXES, axis=0, tiled=True),
        lax.all_gather(up_weight, AXES, axis=0, tiled=True),
        lax.all_gather(up_bias, AXES, axis=0, tiled=True),
        lax.all_gather(down_weight, AXES, axis=0, tiled=True),
        lax.all_gather(down_bias, AXES, axis=0, tiled=True),
    )
    back_qkv = back_params[0]
    back_dense = back_params[2]
    back_gain_one = back_params[4].astype(single)
    back_gain_two = back_params[6].astype(single)
    back_up = back_params[8]
    back_down = back_params[10]
    grad_f = cotangent.astype(single)
    bias_sum = jnp.sum(grad_f, axis=(0, 1))
    down_w_grad = jnp.einsum("tsf,tsd->fd", gelu_out, cotangent, preferred_element_type=single)
    gelu_grad = jnp.einsum("tsd,fd->tsf", cotangent, back_down, preferred_element_type=single)
    pre_grad = (gelu_grad * gelu_slope(pre_act)).astype(half_type)
    up_w_grad = jnp.einsum("tsd,tsf->df", act_two, pre_grad, preferred_element_type=single)
    up_b_grad = jnp.sum(pre_grad.astype(single), axis=(0, 1))
    act_two_grad = jnp.einsum("tsf,df->tsd", pre_grad, back_up, preferred_element_type=single)
    gain_two_grad = jnp.sum(act_two_grad * normed, axis=(0, 1))
    shift_two_grad = jnp.sum(act_two_grad, axis=(0, 1))
    dense_w_grad = jnp.einsum("tsd,tse->de", attn_seq, cotangent, preferred_element_type=single)
    attn_grad = jnp.einsum(
        "tse,de->tsd", cotangent, back_dense, preferred_element_type=single
    ).astype(half_type)
    grad_loc = lax.all_to_all(attn_grad, ULY, split_axis=2, concat_axis=0, tiled=True)
    grad_h = grad_loc.reshape(local_rows, seq_count, local_heads, HD)

    def backward_block(acc_pair, step_index):
        row_start, seq_index, query_rows, row_pos, limit = select(step_index)
        own_slot = (row_start, seq_index, zero_idx, zero_idx)
        out_rows = lax.dynamic_slice(attn_h, own_slot, row_shape)
        grad_rows = lax.dynamic_slice(grad_h, own_slot, row_shape)
        log_total = log_totals[step_index]
        delta_row = jnp.transpose(
            jnp.sum(grad_rows.astype(single) * out_rows.astype(single), axis=-1), (1, 2, 0)
        )

        def grad_step(key_index, carry):
            key_acc, value_acc, query_acc = carry
            masked, key_rows, value_rows, slot = block_scores(
                query_rows, row_pos, key_index, seq_index
            )
            probs_f = jnp.exp(masked - log_total[..., None])
            value_part = jnp.einsum(
                "shqk,qshd->kshd",
                probs_f.astype(half_type),
                grad_rows,
                preferred_element_type=single,
            )
            grad_prob = jnp.einsum(
                "qshd,kshd->shqk", grad_rows, value_rows, preferred_element_type=single
            )
            grad_score = (probs_f * (grad_prob - delta_row[..., None]) * scale_factor).astype(
                half_type
            )
            query_acc = query_acc + jnp.einsum(
                "shqk,kshd->qshd", grad_score, key_rows, preferred_element_type=single
            )
            key_part = jnp.einsum(
                "shqk,qshd->kshd", grad_score, query_rows, preferred_element_type=single
            )
            key_acc = lax.dynamic_update_slice(
                key_acc, lax.dynamic_slice(key_acc, slot, key_part.shape) + key_part, slot
            )
            value_acc = lax.dynamic_update_slice(
                value_acc, lax.dynamic_slice(value_acc, slot, value_part.shape) + value_part, slot
            )
            return (key_acc, value_acc, query_acc)

        key_acc, value_acc, query_acc = lax.fori_loop(
            zero_idx, limit, grad_step, (acc_pair[0], acc_pair[1], jnp.zeros(row_shape, single))
        )
        return ((key_acc, value_acc), query_acc[:, 0])

    acc_zero = jnp.zeros((total_rows, seq_count, local_heads, HD), single)
    acc_final, query_parts = lax.scan(backward_block, (acc_zero, acc_zero), step_ids)
    query_grad = jnp.transpose(
        query_parts.reshape(n_blocks, seq_count, block_rows, local_heads, HD), (0, 2, 1, 3, 4)
    ).reshape(local_rows, seq_count, local_heads, HD)
    key_terms = jnp.transpose(
        acc_final[0].reshape(uly_size, blk_size, tok_rows, seq_count, features), (1, 0, 2, 3, 4)
    ).reshape(total_rows, seq_count, features)
    value_terms = jnp.transpose(
        acc_final[1].reshape(uly_size, blk_size, tok_rows, seq_count, features), (1, 0, 2, 3, 4)
    ).reshape(total_rows, seq_count, features)
    key_back, value_back = (
        lax.psum_scatter(key_terms, BLK, scatter_dimension=0, tiled=True),
        lax.psum_scatter(value_terms, BLK, scatter_dimension=0, tiled=True),
    )
    cos_h, sin_h = rotary_tables(query_pos, rotary)
    query_send = (
        rotate_back(query_grad, cos_h, sin_h, rotary)
        .reshape(local_rows, seq_count, features)
        .astype(half_type)
    )
    key_send = (
        rotate_back(key_back.reshape(local_rows, seq_count, local_heads, HD), cos_h, sin_h, rotary)
        .reshape(local_rows, seq_count, features)
        .astype(half_type)
    )
    value_send = value_back.astype(half_type)
    query_ret, key_ret, value_ret = (
        lax.all_to_all(query_send, ULY, split_axis=0, concat_axis=2, tiled=True),
        lax.all_to_all(key_send, ULY, split_axis=0, concat_axis=2, tiled=True),
        lax.all_to_all(value_send, ULY, split_axis=0, concat_axis=2, tiled=True),
    )
    qkv_grad = jnp.concatenate([query_ret, key_ret, value_ret], axis=-1)
    qkv_w_grad = jnp.einsum("tsd,tsf->df", act_one, qkv_grad, preferred_element_type=single)
    qkv_b_grad = jnp.sum(qkv_grad.astype(single), axis=(0, 1))
    act_one_grad = jnp.einsum("tsf,df->tsd", qkv_grad, back_qkv, preferred_element_type=single)
    gain_one_grad = jnp.sum(act_one_grad * normed, axis=(0, 1))
    shift_one_grad = jnp.sum(act_one_grad, axis=(0, 1))
    input_grad = (
        grad_f
        + norm_back(act_one_grad, normed, inverse, back_gain_one)
        + norm_back(act_two_grad, normed, inverse, back_gain_two)
    )
    summed = (
        lax.psum_scatter(qkv_w_grad, AXES, scatter_dimension=0, tiled=True),
        lax.psum_scatter(qkv_b_grad, AXES, scatter_dimension=0, tiled=True),
        lax.psum_scatter(
            dense_w_grad, AXES, scatter_dimension=0, tiled=True
        ),
        lax.psum_scatter(bias_sum, AXES, scatter_dimension=0, tiled=True),
        lax.psum_scatter(
            gain_one_grad, AXES, scatter_dimension=0, tiled=True
        ),
        lax.psum_scatter(
            shift_one_grad, AXES, scatter_dimension=0, tiled=True
        ),
        lax.psum_scatter(
            gain_two_grad, AXES, scatter_dimension=0, tiled=True
        ),
        lax.psum_scatter(
            shift_two_grad, AXES, scatter_dimension=0, tiled=True
        ),
        lax.psum_scatter(up_w_grad, AXES, scatter_dimension=0, tiled=True),
        lax.psum_scatter(up_b_grad, AXES, scatter_dimension=0, tiled=True),
        lax.psum_scatter(down_w_grad, AXES, scatter_dimension=0, tiled=True),
        lax.psum_scatter(bias_sum, AXES, scatter_dimension=0, tiled=True),
    )
    return (
        output,
        input_grad,
        summed[0],
        summed[1],
        summed[2],
        summed[3],
        summed[4],
        summed[5],
        summed[6],
        summed[7],
        summed[8],
        summed[9],
        summed[10],
        summed[11],
    )


MESH = pl.DeviceIdType.MESH


class Place:
    def __init__(self, planes):
        self.planes = planes
        self.b = lax.axis_index(BATCH)
        self.u = lax.axis_index(ULY)
        k = lax.axis_index(BLK)
        self.y, self.c = k // 2, k % 2
        self.t = self.u * 4 + k
        self.xn, self.yn, self.pn = self.peer(4), self.peer(2), self.peer(1)

    def rank(self, d):
        u = 1 - self.u if d & 4 else self.u
        y = 1 - self.y if d & 2 else self.y
        c = 1 - self.c if d & 1 else self.c
        return u * 4 + y * 2 + c

    def chip(self, d):
        return self.rank(d) // 2

    def peer(self, d):
        u = 1 - self.u if d & 4 else self.u
        y = 1 - self.y if d & 2 else self.y
        c = 1 - self.c if d & 1 else self.c
        return {BATCH: self.b, ULY: u, BLK: y * 2 + c}

    def along(self, step):
        return {BATCH: self.b + step, ULY: self.u, BLK: self.y * 2 + self.c}

    def barrier(self):
        sem = pltpu.get_barrier_semaphore()
        for d in range(1, 8):
            pl.semaphore_signal(sem, inc=1, device_id=self.peer(d), device_id_type=MESH)
        self.to_neighbours(
            lambda step: pl.semaphore_signal(
                sem, inc=1, device_id=self.along(step), device_id_type=MESH
            )
        )
        below = (self.b > 0).astype(jnp.int32)
        above = (self.b < self.planes - 1).astype(jnp.int32)
        pl.semaphore_wait(sem, 7 + below + above)

    def to_neighbours(self, action):
        for step in (-1, 1):

            @pl.when(self.b > 0 if step < 0 else self.b < self.planes - 1)
            def _():
                action(step)

    def reach(self, second, third):
        b, last = self.b, self.planes - 1

        @pl.when((b > 0) & (b < last))
        def _():
            for step in (-1, 1):
                pl.semaphore_signal(
                    second, inc=1, device_id=self.along(step), device_id_type=MESH
                )

        pl.semaphore_wait(second, (b >= 2).astype(jnp.int32) + (b <= last - 2).astype(jnp.int32))
        for middle, step in ((1, -1), (2, 1)):

            @pl.when(b == middle)
            def _():
                pl.semaphore_signal(third, inc=1, device_id=self.along(step), device_id_type=MESH)

        @pl.when((b == 0) | (b == last))
        def _():
            pl.semaphore_wait(third, 1)


class Mail:
    def __init__(self, send, recv, near):
        self.send, self.recv, self.near = send, recv, near
        self.sends = self.recvs = self.nears = 0

    def send_slots(self, n=1):
        self.sends += n
        return self.sends - n

    def recv_slots(self, n=1):
        self.recvs += n
        return self.recvs - n

    def bring(self, src, dst):
        made = pltpu.make_async_copy(src, dst, self.near.at[self.nears])
        self.nears += 1
        made.start()
        return made

    def copy(self, src, dst, send, recv, device):
        return pltpu.make_async_remote_copy(
            src_ref=src,
            dst_ref=dst,
            send_sem=self.send.at[send],
            recv_sem=self.recv.at[recv],
            device_id=device,
            device_id_type=MESH,
        )

    def arrived(self, bulk, recv, device):
        self.copy(bulk, bulk, 0, recv, device).wait_recv()

    def gone(self, bulk, send, device):
        self.copy(bulk, bulk, send, 0, device).wait_send()


class PlaneGather:
    def __init__(self, at, mail, shard, whole):
        self.at, self.mail, self.shard, self.whole = at, mail, shard, whole
        self.rows = shard.shape[1]
        self.halves = shard.shape[0] // 2
        self.send, self.recv = mail.send_slots(), mail.recv_slots(5)

    def half(self, i):
        return self.shard.at[pl.ds(i * self.halves, self.halves)]

    def block(self, d, half=None):
        rows = pl.ds(pl.multiple_of(self.at.rank(d) * self.rows, self.rows), self.rows)
        if half is None:
            return self.whole.at[:, rows, :]
        return self.whole.at[pl.ds(half * self.halves, self.halves), rows, :]

    def bulk(self, shards):
        return self.whole.at[:, pl.ds(0, shards * self.rows), :]

    def post(self, src, dst, recv, device):
        self.mail.copy(src, dst, self.send, self.recv + recv, device).start()

    def arrived(self, bulk, recv, device):
        self.mail.arrived(bulk, self.recv + recv, device)

    def start(self):
        at = self.at
        self.post(self.half(1), self.block(0, 1), 0, at.xn)
        self.post(self.half(0), self.block(0, 0), 1, at.yn)
        self.post(self.half(0), self.block(0, 0), 2, at.xn)
        self.post(self.half(1), self.block(0, 1), 2, at.yn)
        self.post(self.shard, self.block(0), 4, at.pn)
        self.own = self.mail.bring(self.shard, self.block(0))

    def relay_y(self):
        self.arrived(self.block(2, 0), 1, self.at.yn)
        self.post(self.block(2, 0), self.block(2, 0), 3, self.at.xn)

    def relay_x(self):
        self.arrived(self.block(4, 1), 0, self.at.xn)
        self.post(self.block(4, 1), self.block(4, 1), 3, self.at.yn)

    def share(self):
        self.arrived(self.bulk(1), 2, self.at.xn)
        self.post(self.block(2), self.block(2), 4, self.at.pn)
        self.post(self.block(4), self.block(4), 4, self.at.pn)

    def far(self):
        self.arrived(self.block(6), 3, self.at.xn)
        self.post(self.block(6), self.block(6), 4, self.at.pn)

    def finish(self):
        self.arrived(self.bulk(4), 4, self.at.pn)
        self.own.wait()

    def close(self):
        self.mail.gone(self.bulk(7), self.send, self.at.pn)


class LineGather:
    def __init__(self, at, mail, held, up_cut=None, down_cut=None):
        self.at, self.mail, self.held = at, mail, held
        whole = tuple(pl.ds(0, n) for n in held.shape[1:])
        self.up_cut, self.down_cut = up_cut or whole, down_cut or whole
        self.send, self.recv = mail.send_slots(2), mail.recv_slots(at.planes)

    def upward(self, slot, src):
        part = self.held.at[(slot,) + self.up_cut]
        src = part if src is None else src.at[self.up_cut]
        return self.mail.copy(src, part, self.send, self.recv + slot, self.at.along(1))

    def downward(self, slot, src):
        part = self.held.at[(slot,) + self.down_cut]
        src = part if src is None else src.at[self.down_cut]
        return self.mail.copy(src, part, self.send + 1, self.recv + slot, self.at.along(-1))

    def start(self, src=None):
        at = self.at

        @pl.when(at.b < at.planes - 1)
        def _():
            self.upward(at.b, src).start()

        @pl.when(at.b > 0)
        def _():
            self.downward(at.b, src).start()

    def from_below(self, distance, here):
        at = self.at
        slot = at.b - distance

        @pl.when((slot >= 0) & here)
        def _():
            part = self.held.at[(slot,) + self.up_cut]
            self.mail.arrived(part, self.recv + slot, at.along(-1))

            @pl.when(at.b < at.planes - 1)
            def _():
                self.upward(slot, None).start()

    def from_above(self, distance, here):
        at = self.at
        slot = at.b + distance

        @pl.when((slot < at.planes) & here)
        def _():
            part = self.held.at[(slot,) + self.down_cut]
            self.mail.arrived(part, self.recv + slot, at.along(1))

            @pl.when(at.b > 0)
            def _():
                self.downward(slot, None).start()

    def take(self, distance):
        self.from_below(distance, self.at.b >= 0)
        self.from_above(distance, self.at.b >= 0)

    def inner(self, distance):
        middle = self.at.planes // 2
        self.from_below(distance, self.at.b >= middle)
        self.from_above(distance, self.at.b < middle)

    def outer(self, distance):
        middle = self.at.planes // 2
        self.from_below(distance, self.at.b < middle)
        self.from_above(distance, self.at.b >= middle)

    def close(self):
        at = self.at
        for b in range(at.planes):

            @pl.when(at.b == b)
            def _():
                if b < at.planes - 1:
                    bulk = self.held.at[(pl.ds(0, b + 1),) + self.up_cut]
                    self.mail.gone(bulk, self.send, at.along(1))
                if b > 0:
                    bulk = self.held.at[(pl.ds(0, at.planes - b),) + self.down_cut]
                    self.mail.gone(bulk, self.send + 1, at.along(-1))


class StarGather:
    def __init__(self, at, mail, held):
        self.at, self.mail, self.held = at, mail, held
        self.send, self.recv = mail.send_slots(), mail.recv_slots()

    def start(self):
        at = self.at
        part = self.held.at[at.b]
        for step in range(1, at.planes):

            @pl.when(at.b + step < at.planes)
            def _():
                self.mail.copy(part, part, self.send, self.recv, at.along(step)).start()

            @pl.when(at.b >= step)
            def _():
                self.mail.copy(part, part, self.send, self.recv, at.along(-step)).start()

    def bulk(self):
        return self.held.at[pl.ds(0, self.at.planes - 1)]

    def finish(self):
        self.mail.arrived(self.bulk(), self.recv, self.at.pn)

    def close(self):
        self.mail.gone(self.bulk(), self.send, self.at.pn)


class PlaneExchange:
    def __init__(self, at, mail, pieces, landings, bulk):
        self.at, self.mail, self.bulk = at, mail, bulk
        self.pieces, self.landings = pieces, landings
        self.send, self.recv = mail.send_slots(), mail.recv_slots()

    def start(self):
        at = self.at
        for d in range(1, 8):
            for piece, landing in zip(self.pieces(at.rank(d)), self.landings(at.t)):
                self.mail.copy(piece, landing, self.send, self.recv, at.peer(d)).start()
        self.own = [
            self.mail.bring(piece, landing)
            for piece, landing in zip(self.pieces(at.t), self.landings(at.t))
        ]

    def finish(self):
        self.mail.arrived(self.bulk, self.recv, self.at.pn)
        for own in self.own:
            own.wait()

    def close(self):
        self.mail.gone(self.bulk, self.send, self.at.pn)


class PairExchange:
    def __init__(self, at, mail, src, dst, landed):
        self.at, self.mail, self.src, self.dst, self.landed = at, mail, src, dst, landed
        self.send, self.recv = mail.send_slots(), mail.recv_slots()

    def start(self):
        self.mail.copy(self.src, self.dst, self.send, self.recv, self.at.pn).start()

    def finish(self):
        self.mail.arrived(self.landed, self.recv, self.at.pn)

    def close(self):
        self.mail.gone(self.src, self.send, self.at.pn)


class PlaneReduce:
    def __init__(self, at, mail, terms, pairs, sums, side, bulk):
        self.at, self.mail, self.terms, self.bulk = at, mail, terms, bulk
        self.pairs, self.sums, self.side = pairs, sums, side
        self.send, self.recv = mail.send_slots(), mail.recv_slots(6)
        self.halves = terms.shape[0] // 2

    def post(self, src, dst, recv, device):
        self.mail.copy(src, dst, self.send, self.recv + recv, device).start()

    def start(self, *chips):
        at = self.at
        for d in chips:
            chip = at.chip(d)
            recv = {6: 0, 4: 1}.get(d, 5)
            self.post(self.terms.at[:, chip, 1 - at.c], self.pairs.at[:, chip], recv, at.pn)

    def half(self, ref, i):
        return ref.at[pl.ds(i * self.halves, self.halves)]

    def add_pair(self, d):
        chip = self.at.chip(d)
        total = self.terms[:, chip, self.at.c].astype(jnp.float32) + self.pairs[:, chip].astype(
            jnp.float32
        )
        self.sums[:, chip] = total.astype(self.sums.dtype)

    def fold_far(self):
        at = self.at
        far = self.sums.at[:, at.chip(6)]
        self.mail.arrived(self.bulk(1), self.recv, at.pn)
        self.add_pair(6)
        self.post(self.half(far, 0), self.half(self.side.at[0], 0), 2, at.xn)
        self.post(self.half(far, 1), self.half(self.side.at[0], 1), 3, at.yn)

    def fold_x(self):
        self.mail.arrived(self.bulk(1), self.recv + 1, self.at.pn)
        self.add_pair(4)

    def fold_near(self):
        self.mail.arrived(self.bulk(2), self.recv + 5, self.at.pn)
        self.add_pair(2)
        self.add_pair(0)

    def turn_x(self):
        self.turn(1, 4, self.at.yn, 3, self.at.xn)

    def turn_y(self):
        self.turn(0, 2, self.at.xn, 2, self.at.yn)

    def turn(self, i, d, other, recv, nbr):
        landed = self.half(self.side.at[0], i)
        self.mail.arrived(landed, self.recv + recv, other)
        whole = self.sums.at[:, self.at.chip(d)]
        part = self.half(whole, i)
        part[...] = (part[...].astype(jnp.float32) + landed[...].astype(jnp.float32)).astype(
            self.sums.dtype
        )
        self.post(whole, self.side.at[2 - i], 4, nbr)

    def finish(self):
        self.mail.arrived(self.bulk(2), self.recv + 4, self.at.xn)
        return (
            self.sums[:, self.at.chip(0)].astype(jnp.float32)
            + self.side[1].astype(jnp.float32)
            + self.side[2].astype(jnp.float32)
        )

    def close(self):
        self.mail.gone(self.bulk(7), self.send, self.at.pn)


class LineReduce:
    def __init__(self, at, mail, terms, above, below, up_cut=None, down_cut=None):
        self.at, self.mail, self.terms = at, mail, terms
        self.above, self.below = above, below
        whole = pl.ds(0, terms.shape[2])
        self.up_cut, self.down_cut = up_cut or whole, down_cut or whole
        self.send, self.recv = mail.send_slots(2), mail.recv_slots(at.planes + 1)

    def upward(self, src, slot):
        return self.mail.copy(
            src.at[slot, :, self.up_cut],
            self.below.at[slot, :, self.up_cut],
            self.send,
            self.recv + slot,
            self.at.along(1),
        )

    def downward(self, src, slot, last_step):
        return self.mail.copy(
            src.at[slot, :, self.down_cut],
            self.above.at[slot, :, self.down_cut],
            self.send + 1,
            self.recv + (self.at.planes if last_step else slot),
            self.at.along(-1),
        )

    def edge(self, slot):
        at, last = self.at, self.at.planes - 1
        if slot == 0:
            return

        @pl.when(at.b == 0)
        def _():
            self.upward(self.terms, slot).start()

        @pl.when(at.b == last)
        def _():
            self.downward(self.terms, last - slot, slot == 1).start()

    def hop(self, hop, rank):
        at, mail, last = self.at, self.mail, self.at.planes - 1
        slot = last - rank
        if slot <= hop:
            return

        @pl.when(at.b == hop)
        def _():
            cut = self.up_cut
            mail.arrived(self.below.at[slot, :, cut], self.recv + slot, at.along(-1))
            self.add(self.below, slot, cut)
            self.upward(self.below, slot).start()

        @pl.when(at.b == last - hop)
        def _():
            cut = self.down_cut
            mail.arrived(self.above.at[rank, :, cut], self.recv + rank, at.along(1))
            self.add(self.above, rank, cut)
            self.downward(self.above, rank, rank == last - hop - 1).start()

    def add(self, held, slot, cut):
        total = self.terms[slot, :, cut].astype(jnp.float32) + held[slot, :, cut].astype(
            jnp.float32
        )
        held[slot, :, cut] = total.astype(held.dtype)

    def landed(self):
        at, mail = self.at, self.mail

        @pl.when(at.b > 0)
        def _():
            mail.arrived(self.below.at[at.b, :, self.up_cut], self.recv + at.b, at.along(-1))

        @pl.when(at.b < at.planes - 1)
        def _():
            bulk = self.above.at[at.b, :, self.down_cut]
            mail.arrived(bulk, self.recv + at.planes, at.along(1))

    def total(self, out):
        b, last = self.at.b, self.at.planes - 1

        def put(*parts):
            value = self.terms[b].astype(jnp.float32)
            for part in parts:
                value = value + part[b].astype(jnp.float32)
            out[...] = value.astype(out.dtype)

        @pl.when(b == 0)
        def _():
            put(self.above)

        @pl.when(b == last)
        def _():
            put(self.below)

        @pl.when((b > 0) & (b < last))
        def _():
            put(self.below, self.above)

    def close(self):
        at, last = self.at, self.at.planes - 1
        for b in range(at.planes):

            @pl.when(at.b == b)
            def _():
                if b < last:
                    bulk = self.terms.at[pl.ds(0, last - b), :, self.up_cut]
                    self.mail.gone(bulk, self.send, at.along(1))
                if b > 0:
                    bulk = self.terms.at[pl.ds(0, b), :, self.down_cut]
                    self.mail.gone(bulk, self.send + 1, at.along(-1))


TILE = 256
LANES = 128


def dot_nn(a, b):
    return lax.dot_general(a, b, (((1,), (0,)), ((), ())), preferred_element_type=jnp.float32)


def dot_nt(a, b):
    return lax.dot_general(a, b, (((1,), (1,)), ((), ())), preferred_element_type=jnp.float32)


def dot_tn(a, b):
    return lax.dot_general(a, b, (((0,), (0,)), ((), ())), preferred_element_type=jnp.float32)


def turn(value, tables, rows, sign):
    straight, early, late = (table[rows, :] for table in tables)
    ahead = pltpu.roll(value, LANES - HD // 8, 1)
    behind = pltpu.roll(value, HD // 8, 1)
    return value * straight + sign * (ahead * early + behind * late)


def of_head(value, head):
    lane = lax.broadcasted_iota(jnp.int32, value.shape, 1)
    return jnp.where(lane // HD == head, value, jnp.zeros_like(value))


def total_rows(value):
    return jnp.sum(value, axis=0, keepdims=True)


class Layer:
    def __init__(self, refs):
        self.__dict__.update(refs)
        self.heads = LANES // HD
        if "xa" in refs:
            self.seqs, self.length, self.width = self.xa.shape
            self.per_seq = self.length // TILE
            self.tiles = self.seqs * self.per_seq

    def rows(self, tile):
        return pl.ds(pl.multiple_of(tile * TILE, TILE), TILE)

    def in_seq(self, ref, tile):
        rows = pl.ds(pl.multiple_of(tile % self.per_seq * TILE, TILE), TILE)
        return ref[tile // self.per_seq, rows, :]

    def loop(self, count, step):
        def run(i, carry):
            step(i)
            return carry

        lax.fori_loop(0, count, run, 0)

    def wide(self, row):
        planes = self.va.shape[0]
        return jnp.concatenate(
            [self.va[b, pl.ds(2 * row + a, 1), :] for b in range(planes) for a in range(2)], axis=1
        )

    def own_vectors(self, rank):
        lane = lax.broadcasted_iota(jnp.int32, (2, LANES), 1)
        row = lax.broadcasted_iota(jnp.int32, (2, LANES), 0)
        for j, ref in enumerate(self.vectors):
            piece = ref[...].astype(jnp.float32).reshape(1, ref.shape[0])
            piece = jnp.concatenate([piece] * (LANES // ref.shape[0]), axis=1)
            here = (lane // ref.shape[0] == rank % 4) & (row == rank // 4)
            self.vec_s[2 * j : 2 * j + 2, :] = jnp.where(here, jnp.broadcast_to(piece, here.shape), 0.0)
        bias = self.b_qkv[...].astype(jnp.float32).reshape(1, self.b_qkv.shape[0])
        self.vec_s[12:13, :] = jnp.concatenate(
            [bias, jnp.zeros((1, LANES - bias.shape[1]), jnp.float32)], axis=1
        )
        self.vec_s[13:14, :] = self.b_up[...].astype(jnp.float32).reshape(1, LANES)

    def plane_vectors(self, slot):
        total = jnp.sum(self.vec_in[...], axis=0)
        self.va[slot, 0:16, :] = total
        for rank in range(self.vec_in.shape[0]):
            self.va[slot, 16 + rank : 17 + rank, :] = self.vec_in[rank, 12:13, :]
            self.va[slot, 24 + rank : 25 + rank, :] = self.vec_in[rank, 13:14, :]

    def sort_weight(self):
        rows = self.wq_raw.shape[0]
        low = lax.broadcasted_iota(jnp.int32, (rows, LANES), 1) < HD
        for part in range(3):
            for core in range(2):
                for pair in range(2):
                    first, second = (
                        self.wq_raw[
                            :, pl.ds(part * self.width + (core * 2 + j) * 4 * HD + pair * LANES, LANES)
                        ].astype(jnp.float32)
                        for j in range(2)
                    )
                    cut = slice(part * LANES, (part + 1) * LANES)
                    self.wq_s[4 * pair + core, :, cut] = jnp.where(
                        low, first, pltpu.roll(second, HD, 1)
                    ).astype(jnp.bfloat16)
                    self.wq_s[4 * pair + 2 + core, :, cut] = jnp.where(
                        low, pltpu.roll(first, HD, 1), second
                    ).astype(jnp.bfloat16)

    def statistics(self):
        def step(i):
            x = self.in_seq(self.xa, i).astype(jnp.float32)
            center = jnp.mean(x, axis=1, keepdims=True)
            shifted = x - center
            spread = jnp.mean(shifted * shifted, axis=1, keepdims=True)
            self.center[self.rows(i), :] = center
            self.inverse[self.rows(i), :] = lax.rsqrt(spread + EPSILON)

        self.loop(self.tiles, step)

    def normed(self, i):
        x = self.in_seq(self.xa, i).astype(jnp.float32)
        return (x - self.center[self.rows(i), :]) * self.inverse[self.rows(i), :]

    def activations(self):
        gain_one, shift_one, gain_two, shift_two = (self.wide(j) for j in (1, 2, 3, 4))

        def step(i):
            normed = self.normed(i)
            self.act_one[self.rows(i), :] = (normed * gain_one + shift_one).astype(jnp.bfloat16)
            self.act_two[self.rows(i), :] = (normed * gain_two + shift_two).astype(jnp.bfloat16)

        self.loop(self.tiles, step)

    def qkv_bias(self, rank):
        size = HD // 2
        held = self.b_qkv.shape[0] // size
        ranks = self.vec_in.shape[0]
        pieces = []
        for i in range(3 * LANES // size):
            part, j, half = i // 4, i // 2 % 2, i % 2
            head = (rank % 2 * 2 + j) * 4 + rank // 2
            index = part * (self.width // size) + head * 2 + half
            owner, spot = index // held, index % held
            row = self.va[owner // ranks, pl.ds(16 + owner % ranks, 1), :]
            pieces.append(
                sum(
                    jnp.where(spot == k, row[:, k * size : (k + 1) * size], 0.0)
                    for k in range(held)
                )
            )
        return jnp.concatenate(pieces, axis=1)

    def near(self, ref, side):
        both = ref[pl.ds(side * 2, 2)]
        return both.reshape(both.shape[0] * both.shape[1], both.shape[2])

    def half_columns(self, side, width):
        return pl.ds(pl.multiple_of(side * (width // 2), width // 2), width // 2)

    def project_near(self, side):
        def step(i):
            cut = self.half_columns(side, self.width)
            self.qkv[self.rows(i), :] = dot_nn(self.act_one[self.rows(i), cut], self.near(self.wq, side))

        self.loop(self.tiles, step)

    def project(self, rank, side):
        bias = self.qkv_bias(rank)

        def step(i):
            cut = self.half_columns(side, self.width)
            qkv = dot_nn(self.act_one[self.rows(i), cut], self.near(self.wq, side))
            qkv = qkv + self.qkv[self.rows(i), :] + bias
            rows = pl.ds(pl.multiple_of(i % self.per_seq * TILE, TILE), TILE)
            query = turn(qkv[:, :LANES], self.tables, rows, 1.0).astype(jnp.bfloat16)
            self.query[self.rows(i), :] = query * jnp.asarray(1.0 / math.sqrt(HD), jnp.bfloat16)
            self.key[self.rows(i), :] = turn(
                qkv[:, LANES : 2 * LANES], self.tables, rows, 1.0
            ).astype(jnp.bfloat16)
            self.value[self.rows(i), :] = qkv[:, 2 * LANES :].astype(jnp.bfloat16)

        self.loop(self.tiles, step)

    def keys(self, seq, block):
        start = pl.multiple_of(seq * self.length, TILE)
        return pl.ds(start, (block + 1) * TILE)

    def attend(self, seq):
        for block in range(self.per_seq):
            rows = self.rows(seq * self.per_seq + block)
            keys = self.keys(seq, block)
            key, value, query = self.key[keys, :], self.value[keys, :], self.query[rows, :]
            out = None
            for head in range(self.heads):
                scores = dot_nt(of_head(query, head), key)
                at = lax.broadcasted_iota(jnp.int32, scores.shape, 0) + block * TILE
                to = lax.broadcasted_iota(jnp.int32, scores.shape, 1)
                scores = jnp.where(to <= at, scores, -jnp.inf)
                top = jnp.max(scores, axis=1, keepdims=True)
                weight = jnp.exp(scores - top)
                weight = weight * (1.0 / jnp.sum(weight, axis=1, keepdims=True))
                self.probs[block][seq * self.heads + head] = weight
                part = dot_nn(weight.astype(jnp.bfloat16), value)
                out = of_head(part, head) if out is None else out + of_head(part, head)
            self.attn[rows, :] = out.astype(jnp.bfloat16)

    def attend_out_grad(self):
        def step(i):
            weight = self.wo2[...].reshape(LANES, self.width)
            self.attn_grad[self.rows(i), :] = dot_nt(self.in_seq(self.ca, i), weight).astype(
                jnp.bfloat16
            )

        self.loop(self.tiles, step)

    def attend_grad(self, seq):
        key_grad, value_grad = [None] * self.per_seq, [None] * self.per_seq
        start = seq * self.per_seq
        for block in range(self.per_seq):
            rows = self.rows(start + block)
            keys = self.keys(seq, block)
            key, value, query = self.key[keys, :], self.value[keys, :], self.query[rows, :]
            grad = self.attn_grad[rows, :]
            inner = grad.astype(jnp.float32) * self.attn[rows, :].astype(jnp.float32)
            query_grad = None
            for head in range(self.heads):
                own_grad = of_head(grad, head)
                delta = jnp.sum(of_head(inner, head), axis=1, keepdims=True)
                probs = self.probs[block][seq * self.heads + head]
                grad_prob = dot_nt(own_grad, value)
                grad_score = (probs * (grad_prob - delta)).astype(jnp.bfloat16)
                part = dot_nn(grad_score, of_head(key, head))
                query_grad = part if query_grad is None else query_grad + part
                key_part = dot_tn(grad_score, of_head(query, head))
                value_part = dot_tn(probs.astype(jnp.bfloat16), own_grad)
                for b in range(block + 1):
                    cut = slice(b * TILE, (b + 1) * TILE)
                    key_grad[b] = key_part[cut] if key_grad[b] is None else key_grad[b] + key_part[cut]
                    value_grad[b] = (
                        value_part[cut] if value_grad[b] is None else value_grad[b] + value_part[cut]
                    )
            back = pl.ds(block * TILE, TILE)
            self.qkv_grad[rows, :LANES] = turn(
                query_grad * (1.0 / math.sqrt(HD)), self.tables, back, -1.0
            ).astype(jnp.bfloat16)
        for block in range(self.per_seq):
            rows = self.rows(start + block)
            back = pl.ds(block * TILE, TILE)
            self.qkv_grad[rows, LANES : 2 * LANES] = turn(
                key_grad[block], self.tables, back, -1.0
            ).astype(jnp.bfloat16)
            self.qkv_grad[rows, 2 * LANES :] = value_grad[block].astype(jnp.bfloat16)

    def cot_flat(self):
        return self.ca[...].reshape(self.seqs * self.length, self.width)

    def qkv_weight_grad(self, i):
        rows = self.gq.shape[1]
        act = self.act_one[:, pl.ds(pl.multiple_of(i * rows, rows), rows)]
        self.gq[i] = dot_tn(act, self.qkv_grad[...]).astype(jnp.bfloat16)

    def dense_weight_grad(self):
        self.go[...] = (
            dot_tn(self.attn[...], self.cot_flat()).astype(jnp.bfloat16).reshape(self.go.shape)
        )

    def expand(self, rank, side):
        cut = self.half_columns(side, self.hidden)
        slots = self.va.shape[0] // 2
        bias = jnp.concatenate(
            [self.va[side * slots + i, pl.ds(24 + rank, 1), :] for i in range(slots)], axis=1
        )

        def step(i):
            weight = self.wu[:, :, cut].reshape(self.width, self.hidden // 2)
            pre = dot_nn(self.act_two[self.rows(i), :], weight) + bias
            cdf = 0.5 * (1.0 + lax.erf(pre * INV_ROOT_TWO))
            self.gelu[self.rows(i), cut] = (pre * cdf).astype(jnp.bfloat16)
            self.slope[self.rows(i), cut] = cdf + pre * jnp.exp(-0.5 * pre * pre) * INV_ROOT_TWO_PI

        self.loop(self.tiles, step)

    def down_weight_grad(self, i):
        depth = self.gd.shape[1]
        part = self.gelu[:, pl.ds(pl.multiple_of(i * depth, depth), depth)]
        self.gd[i] = dot_tn(part, self.cot_flat()).astype(jnp.bfloat16)

    def hidden_grad(self, side):
        def step(i):
            cut = self.half_columns(side, self.hidden)
            grad = dot_nt(self.in_seq(self.ca, i), self.near(self.wd, side))
            self.pre_grad[self.rows(i), cut] = (grad * self.slope[self.rows(i), cut]).astype(
                jnp.bfloat16
            )

        self.loop(self.tiles, step)

    def up_weight_grad(self, i, side):
        rows = self.gu.shape[1]
        act = self.act_two[:, pl.ds(pl.multiple_of(i * rows, rows), rows)]
        cut = self.half_columns(side, self.hidden)
        self.gu[i, :, cut] = dot_tn(act, self.pre_grad[:, cut]).astype(jnp.bfloat16)

    def put_terms(self, terms, i, value):
        seq, chips, cores, rows, width = terms.shape
        n = TILE // (cores * rows)
        terms[i // self.per_seq, pl.ds(i % self.per_seq * n, n)] = value.astype(
            jnp.bfloat16
        ).reshape(n, cores, rows, width)

    def out_terms(self, i):
        dense = self.wo2[...].reshape(LANES, self.width)
        down = self.wd[...].reshape(self.hidden, self.width)
        self.put_terms(
            self.po,
            i,
            dot_nn(self.attn[self.rows(i), :], dense) + dot_nn(self.gelu[self.rows(i), :], down),
        )

    def in_terms_one(self, i, first):
        gain = self.wide(1)
        weight = self.wq[...].reshape(self.width, 3 * LANES)
        value = dot_nt(self.qkv_grad[self.rows(i), :], weight)
        self.park(i, value * gain)
        self.add_sums(0, value, self.normed(i), first)

    def in_terms_two(self, i, first):
        gain = self.wide(3)
        weight = self.wu[...].reshape(self.width, self.hidden)
        value = dot_nt(self.pre_grad[self.rows(i), :], weight)
        self.put_terms(self.pg, i, self.parked(i) + value * gain)
        self.add_sums(2, value, self.normed(i), first)

    def park(self, i, value):
        quarter = self.width // 4
        self.probs[1][i] = value[:, : 2 * quarter]
        self.probs[0][i] = value[:, 2 * quarter : 3 * quarter]
        self.qkv[self.rows(i), :quarter] = value[:, 3 * quarter :]

    def parked(self, i):
        quarter = self.width // 4
        return jnp.concatenate(
            [self.probs[1][i], self.probs[0][i], self.qkv[self.rows(i), :quarter]], axis=1
        )

    def add_sums(self, row, value, normed, first):
        for j, sums in ((row, total_rows(value * normed)), (row + 1, total_rows(value))):
            if first:
                self.sums[j : j + 1, :] = sums
            else:
                self.sums[j : j + 1, :] += sums

    def split(self, raw, own):
        for seq in range(own.shape[0]):
            own[seq] = raw[:, seq, :]

    def own_rows(self, ref, rank):
        rows = self.out.shape[0]
        return ref[:, pl.ds(pl.multiple_of(rank * rows, rows), rows), :].astype(jnp.float32)

    def small_terms(self, rank):
        ranks = self.sm.shape[0]
        cot = total_rows(jnp.sum(self.own_rows(self.ca, rank), axis=0))
        for to in range(ranks):
            cut = slice(to * LANES, (to + 1) * LANES)
            self.sm[to, 0:1, :] = cot[:, cut]
            self.sm[to, 1:5, :] = self.sums[0:4, cut]

    def small_plane(self, slot):
        total = jnp.sum(self.sm_in[...], axis=0)
        self.vz[slot, 0:8, :] = total
        qkv = total_rows(self.qkv_grad[...].astype(jnp.float32))
        pre = total_rows(self.pre_grad[...].astype(jnp.float32))
        for j in range(3):
            self.vz[slot, 8 + j : 9 + j, :] = qkv[:, j * LANES : (j + 1) * LANES]
        for j in range(self.hidden // LANES):
            self.vz[slot, 12 + j : 13 + j, :] = pre[:, j * LANES : (j + 1) * LANES]

    def result(self, rank, out_sum, in_sum):
        x = self.own_rows(self.xa, rank)
        center = jnp.mean(x, axis=2, keepdims=True)
        shifted = x - center
        inverse = lax.rsqrt(jnp.mean(shifted * shifted, axis=2, keepdims=True) + EPSILON)
        normed = shifted * inverse
        bias = (self.wide(0) + self.wide(5))[None]
        value = (x + out_sum + bias).astype(jnp.bfloat16)
        grad = self.own_rows(self.ca, rank) + inverse * (
            in_sum
            - jnp.mean(in_sum, axis=2, keepdims=True)
            - normed * jnp.mean(in_sum * normed, axis=2, keepdims=True)
        )
        for seq in range(x.shape[0]):
            self.out[:, seq, :] = value[seq]
            self.in_grad[:, seq, :] = grad[seq]


SEND_SLOTS, RECV_SLOTS, NEAR_SLOTS = 37, 82, 30


def layer_kernel(names, planes, *refs):
    refs = dict(zip(names, refs))
    send, recv, near, second, third = (refs.pop(name) for name in names[-5:])
    refs.update(
        tables=tuple(refs["table"].at[i] for i in range(3)),
        probs=tuple(refs[name] for name in names if name.startswith("probs")),
        vectors=tuple(refs[name] for name in names if name.startswith("vector")),
        hidden=refs["gelu"].shape[1],
    )
    given = [refs["in_qkv"], refs["in_up"]]
    given += [refs[name] for name in names if name.startswith("in_vector")]
    do = Layer(refs)
    at = Place(planes)
    mail = Mail(send, recv, near)
    b, c = at.b, at.c
    rows = do.wq_s.shape[1]
    pair = planes // 2
    others = pl.ds(0, 7)

    def shards(n):
        return do.xa.at[:, pl.ds(0, n * do.x_own.shape[1]), :]

    def strip(whole):
        return lambda rank: [whole.at[b, pl.ds(pl.multiple_of(rank * rows, rows), rows), :]]

    def band(whole):
        return lambda rank: [whole.at[pl.ds(pl.multiple_of(rank * rows, rows), rows), :]]

    def up_pieces(rank):
        return [
            do.wu_s.at[:, pl.ds(pl.multiple_of((p * 8 + rank) * LANES, LANES), LANES)]
            for p in range(planes)
        ]

    def up_landings(rank):
        strip_rows = pl.ds(pl.multiple_of(rank * rows, rows), rows)
        return [do.wu.at[b, strip_rows, pl.ds(p * LANES, LANES)] for p in range(planes)]

    gather_x = PlaneGather(at, mail, do.x_own, do.xa)
    gather_c = PlaneGather(at, mail, do.cot_own, do.ca)
    line_v, line_o = StarGather(at, mail, do.va), LineGather(at, mail, do.wo)
    line_q = LineGather(at, mail, do.wq)
    low, high = (pl.ds(i * do.hidden // 2, do.hidden // 2) for i in range(2))
    all_rows = pl.ds(0, do.wu.shape[1])
    line_ua = LineGather(at, mail, do.wu, (all_rows, low), (all_rows, high))
    line_ub = LineGather(at, mail, do.wu, (all_rows, high), (all_rows, low))
    half = do.wd.shape[1] // 2
    cuts = [(pl.ds(i * half, half), pl.ds(0, do.wd.shape[2])) for i in range(2)]
    line_da = LineGather(at, mail, do.wd, cuts[0], cuts[0])
    line_db = LineGather(at, mail, do.wd, cuts[1], cuts[1])
    ex_v = PlaneExchange(at, mail, lambda rank: [do.vec_s], lambda rank: [do.vec_in.at[rank]], do.vec_in.at[others])
    ex_q = PlaneExchange(
        at, mail, lambda rank: [do.wq_s.at[rank]], strip(do.wq), do.wq_s.at[others]
    )
    ex_u = PlaneExchange(at, mail, up_pieces, up_landings, do.wu.at[0, pl.ds(0, 7 * rows)])
    mine = do.wo2.at[:, c]
    swap_w = PairExchange(
        at, mail, do.wo.at[pl.ds(pair * (1 - c), pair)], mine, do.wo2.at[:, 1 - c]
    )
    sum_o = LineReduce(at, mail, do.go4, do.above_o, do.below_o)
    sum_q = LineReduce(at, mail, do.gq, do.above_q, do.below_q)
    sum_un = LineReduce(at, mail, do.gu, do.above_u, do.below_u, low, high)
    sum_uf = LineReduce(at, mail, do.gu, do.above_u, do.below_u, high, low)
    near_side = b // pair
    far_side = 1 - near_side
    sum_d = LineReduce(at, mail, do.gd, do.above_d, do.below_d)
    swap_g = PairExchange(
        at,
        mail,
        do.go.at[:, 1 - c],
        do.go4.at[pl.ds(pair * c, pair)],
        do.go4.at[pl.ds(pair * (1 - c), pair)],
    )
    back_q = PlaneExchange(
        at, mail, band(do.fq), lambda rank: [do.dq.at[rank]], do.fq.at[pl.ds(0, 7 * rows)]
    )
    back_u = PlaneExchange(
        at, mail, band(do.fu), lambda rank: [do.du.at[rank]], do.fu.at[pl.ds(0, 7 * rows)]
    )
    fold_v = PlaneExchange(
        at, mail, lambda rank: [do.sm.at[rank]], lambda rank: [do.sm_in.at[rank]], do.sm.at[others]
    )
    line_s = StarGather(at, mail, do.vz)
    share_v = PlaneExchange(
        at, mail, lambda rank: [do.vt], lambda rank: [do.dv.at[rank]], do.dv.at[others]
    )
    plane_o = PlaneReduce(at, mail, do.po, do.pairs_o, do.sums_o, do.side_o, shards)
    plane_g = PlaneReduce(at, mail, do.pg, do.pairs_g, do.sums_g, do.side_g, shards)

    slots = [s + b // pair * (planes - 1 - 2 * s) for s in (3, 0, 2, 1)]
    tiles = [seq * 2 + half for half in (1 - at.u, at.u) for seq in range(2)]
    turned = [s + b // pair * (planes - 1 - 2 * s) for s in (3, 2, 1, 0)]

    at.barrier()
    own_v = [mail.bring(src, dst) for src, dst in zip(given, [do.b_qkv, do.b_up, *do.vectors])]
    line_da.start(do.wd_s)
    own_d = mail.bring(do.wd_s, do.wd.at[b])
    raw_x = mail.bring(do.x_in, do.x_raw)
    at.reach(second, third)
    ex_u.start()
    line_db.start(do.wd_s)
    raw_x.wait()
    do.split(do.x_raw, do.x_own)
    own_raw = mail.bring(do.wq_in, do.wq_raw)
    line_o.start(do.wo_s)
    own_o = mail.bring(do.wo_s, do.wo.at[b])
    gather_x.start()
    raw_c = mail.bring(do.cot_in, do.cot_raw)
    own_table = mail.bring(do.table_in, do.table)
    ex_u.finish()
    line_ua.start()
    for made in own_v:
        made.wait()
    do.own_vectors(at.t)
    ex_v.start()
    line_o.take(1)
    gather_x.relay_x()
    gather_x.relay_y()
    own_raw.wait()
    do.sort_weight()
    ex_q.start()
    line_ua.outer(1)
    line_ua.inner(1)
    gather_x.share()
    raw_c.wait()
    do.split(do.cot_raw, do.cot_own)
    ex_v.finish()
    do.plane_vectors(b)
    line_v.start()
    line_ub.start()
    gather_x.far()
    gather_c.start()
    line_o.take(2)
    own_table.wait()
    line_ua.inner(2)
    gather_x.finish()
    do.statistics()
    line_v.finish()
    do.activations()
    line_ub.outer(1)
    gather_c.relay_x()
    line_o.take(3)
    gather_c.relay_y()
    line_ub.inner(1)
    ex_q.finish()
    line_q.start()
    own_o.wait()
    swap_w.start()
    mine[...] = do.wo[pl.ds(pair * c, pair)]
    line_ua.inner(3)
    gather_c.share()
    do.expand(at.t, far_side)
    gather_c.far()
    line_ub.inner(2)
    own_d.wait()
    swap_w.finish()
    gather_c.finish()
    do.down_weight_grad(turned[0])
    sum_d.edge(3)
    line_q.take(1)
    do.down_weight_grad(turned[1])
    sum_d.edge(2)
    line_ub.inner(3)
    do.expand(at.t, near_side)
    do.down_weight_grad(turned[2])
    sum_d.edge(1)
    do.down_weight_grad(turned[3])
    sum_d.edge(0)
    do.project_near(near_side)
    do.attend_out_grad()
    line_q.take(2)
    line_db.take(1)
    line_da.take(1)
    do.hidden_grad(near_side)
    do.up_weight_grad(slots[0], near_side)
    sum_un.edge(3)
    do.up_weight_grad(slots[1], near_side)
    sum_un.edge(0)
    do.up_weight_grad(slots[2], near_side)
    sum_un.edge(2)
    do.up_weight_grad(slots[3], near_side)
    sum_un.edge(1)
    line_q.take(3)
    do.project(at.t, far_side)
    do.attend(0)
    do.attend(1)
    do.dense_weight_grad()
    swap_g.start()
    do.go4[pl.ds(pair * c, pair)] = do.go[:, c]
    sum_d.hop(1, 0)
    do.attend_grad(0)
    do.attend_grad(1)
    do.qkv_weight_grad(slots[0])
    sum_q.edge(3)
    line_da.take(2)
    line_da.take(3)
    line_db.take(2)
    do.in_terms_one(tiles[0], True)
    do.in_terms_one(tiles[1], False)
    line_db.take(3)
    do.hidden_grad(far_side)
    do.up_weight_grad(slots[0], far_side)
    sum_uf.edge(3)
    sum_d.hop(1, 1)
    do.out_terms(tiles[0])
    do.out_terms(tiles[1])
    plane_o.start(6, 4)
    do.in_terms_two(tiles[0], True)
    do.in_terms_two(tiles[1], False)
    plane_g.start(6, 4)
    plane_o.fold_far()
    do.up_weight_grad(slots[1], far_side)
    sum_uf.edge(0)
    do.up_weight_grad(slots[2], far_side)
    sum_uf.edge(2)
    do.up_weight_grad(slots[3], far_side)
    sum_uf.edge(1)
    do.out_terms(tiles[2])
    do.out_terms(tiles[3])
    plane_o.start(2, 0)
    sum_un.hop(1, 0)
    plane_g.fold_far()
    do.qkv_weight_grad(slots[1])
    sum_q.edge(0)
    do.qkv_weight_grad(slots[2])
    sum_q.edge(2)
    swap_g.finish()
    sum_o.edge(3)
    do.qkv_weight_grad(slots[3])
    sum_q.edge(1)
    sum_un.hop(1, 1)
    plane_o.fold_x()
    plane_o.turn_x()
    plane_o.fold_near()
    plane_o.turn_y()
    do.in_terms_one(tiles[2], False)
    sum_q.hop(1, 0)
    do.in_terms_two(tiles[2], False)
    do.in_terms_one(tiles[3], False)
    do.in_terms_two(tiles[3], False)
    plane_g.start(2, 0)
    plane_g.fold_x()
    sum_uf.hop(1, 0)
    sum_un.hop(2, 0)
    do.small_terms(at.t)
    fold_v.start()
    sum_uf.hop(1, 1)
    plane_g.turn_x()
    plane_g.fold_near()
    plane_g.turn_y()
    sum_q.hop(2, 0)
    sum_uf.hop(2, 0)
    fold_v.finish()
    do.small_plane(b)
    line_s.start()
    sum_d.hop(2, 0)
    sum_o.edge(2)
    sum_q.hop(1, 1)
    sum_un.landed()
    sum_uf.landed()
    sum_un.total(do.fu)
    back_u.start()
    sum_o.edge(1)
    sum_o.hop(1, 0)
    do.result(at.t, plane_o.finish(), plane_g.finish())
    out_x = mail.bring(do.out, do.out_to)
    out_g = mail.bring(do.in_grad, do.in_grad_to)
    sum_q.landed()
    sum_q.total(do.fq)
    back_q.start()
    sum_o.hop(2, 0)
    line_s.finish()
    sum_o.hop(1, 1)
    do.vt[...] = jnp.sum(do.vz[...], axis=0)
    share_v.start()
    sum_d.landed()
    sum_d.total(do.dd)
    out_d = mail.bring(do.dd, do.dd_to)
    sum_o.landed()
    sum_o.total(do.dd_o)
    out_o = mail.bring(do.dd_o, do.dd_o_to)
    back_q.finish()
    back_u.finish()
    share_v.finish()
    for copied in (out_o, out_d, out_x, out_g):
        copied.wait()
    for line in (gather_x, gather_c, line_v, line_o, line_q, line_ua, line_ub, line_da, line_db, line_s, ex_v, ex_q, ex_u, back_q, back_u, fold_v, share_v, swap_w, swap_g, plane_o, plane_g, sum_o, sum_q, sum_un, sum_uf, sum_d):
        line.close()


def finish_kernel(names, planes, *refs):
    refs = dict(zip(names, refs))
    near = refs.pop(names[-1])
    do = Layer(refs)
    at = Place(planes)
    ranks, rows = do.dq.shape[:2]
    moves = []

    def move(src, dst):
        moves.append(pltpu.make_async_copy(src, dst, near.at[len(moves)]))
        moves[-1].start()

    move(do.in_grad, do.in_grad_out)
    move(do.dd, do.down_out)
    move(do.out, do.out_out)
    move(do.dd_o, do.dense_out)
    for rank in range(ranks):
        for b in range(planes):
            first = (b * ranks + rank) * LANES
            do.up_v[:, first : first + LANES] = do.du[
                rank, :, b * LANES : (b + 1) * LANES
            ].astype(jnp.float32)
    move(do.up_v, do.up_out)
    low = lax.broadcasted_iota(jnp.int32, (rows, LANES), 1) < HD
    for part in range(3):
        for core in range(2):
            for pair in range(ranks // 4):
                first, second = (
                    do.dq[2 * (2 * pair + i) + core, :, part * LANES : (part + 1) * LANES].astype(
                        jnp.float32
                    )
                    for i in range(2)
                )
                for j in range(2):
                    both = (
                        jnp.where(low, first, pltpu.roll(second, HD, 1))
                        if j == 0
                        else jnp.where(low, pltpu.roll(first, HD, 1), second)
                    )
                    start = (part * 4 + core * 2 + j) * ranks // 2 * HD + pair * LANES
                    do.qkv_v[:, start : start + LANES] = both
    move(do.qkv_v, do.qkv_out)
    piece = lax.rem(at.t, 4)
    row = (at.b * ranks + at.t) // 4
    values = do.dv[pl.ds(row, 1), 0:8, :].reshape(8, LANES)
    front = jnp.zeros((8, rows), jnp.float32)
    for i in range(4):
        cut = values[:, i * rows : (i + 1) * rows]
        front = front + jnp.where(piece == i, cut, jnp.zeros_like(cut))
    for j, ref in enumerate(
        (do.dense_bias, do.gain_one, do.shift_one, do.gain_two, do.shift_two)
    ):
        ref[...] = front[j].reshape(rows)
    do.down_bias[...] = front[0].reshape(rows)
    do.up_bias[...] = do.dv[pl.ds(at.t, 1), pl.ds(12 + at.b, 1), :].reshape(LANES)
    pieces = []
    for i in range(3):
        index = (at.b * ranks + at.t) * 3 + i
        part, inner = index // 32, lax.rem(index, 32)
        head, half = inner // 2, lax.rem(inner, 2)
        core, j, chip = head // 8, lax.rem(head // 4, 2), lax.rem(head, 4)
        value = do.dv[pl.ds(chip * 2 + core, 1), pl.ds(8 + part, 1), :].reshape(1, LANES)
        spot = 2 * j + half
        total = jnp.zeros((1, rows), jnp.float32)
        for k in range(4):
            cut = value[:, k * rows : (k + 1) * rows]
            total = total + jnp.where(spot == k, cut, jnp.zeros_like(cut))
        pieces.append(total)
    do.qkv_bias[...] = jnp.concatenate(pieces, axis=1).reshape(3 * rows)
    for made in moves:
        made.wait()


VMEM = pl.BlockSpec(memory_space=pltpu.VMEM)


def rotary_rows(length):
    half = HD // 8
    frequency = 1.0 / 10000.0 ** (np.arange(half) * (1.0 / half))
    angles = np.arange(length)[:, None] * frequency[None, :]
    table = np.zeros((3, length, HD))
    table[0] = 1.0
    table[0, :, :half] = table[0, :, half : 2 * half] = np.cos(angles)
    table[1, :, :half] = -np.sin(angles)
    table[2, :, half : 2 * half] = np.sin(angles)
    return np.tile(table, (1, 1, LANES // HD)).astype(np.float32)


def body(shape, *operands):
    residual_in, qkv_weight, down_weight = operands[0], operands[1], operands[11]
    planes = shape[BATCH]
    ranks = shape[ULY] * shape[BLK]
    tok_rows, seqs, width = residual_in.shape
    fits = (
        (shape[ULY], shape[BLK]) == (2, 4)
        and planes == 4
        and seqs == 2
        and 2 * qkv_weight.shape[0] == HD
        and width == ranks * LANES == 4 * TILE
        and ranks * tok_rows == 2 * TILE
        and TILE % (2 * tok_rows) == 0
        and down_weight.shape[0] == LANES
    )
    return fast_body(planes, *operands) if fits else general_body(*operands)


def fast_body(
    planes,
    residual_in,
    qkv_weight,
    qkv_bias,
    dense_weight,
    dense_bias,
    norm1_gain,
    norm1_bias,
    norm2_gain,
    norm2_bias,
    up_weight,
    up_bias,
    down_weight,
    down_bias,
    cotangent,
):
    single = jnp.float32
    half_type = jnp.bfloat16
    tok_rows, seqs, width = residual_in.shape
    ranks = width // LANES
    rows = qkv_weight.shape[0]
    depth = down_weight.shape[0]
    hidden = planes * depth
    pair = planes // 2
    length = ranks * tok_rows
    tokens = seqs * length
    rank = lax.axis_index(ULY) * lax.axis_size(BLK) + lax.axis_index(BLK)
    owner = lax.axis_index(BATCH) * ranks + rank

    anywhere = pl.BlockSpec(memory_space=pl.ANY)
    in_hbm = pl.BlockSpec(memory_space=pltpu.HBM)
    inputs = dict(
        x_in=(residual_in, in_hbm),
        cot_in=(cotangent, in_hbm),
        wq_in=(qkv_weight, in_hbm),
        wu_s=(up_weight, in_hbm),
        wd_s=(down_weight, in_hbm),
        wo_s=(dense_weight, in_hbm),
        table_in=(jnp.asarray(rotary_rows(length)), in_hbm),
        in_qkv=(qkv_bias, in_hbm),
        in_up=(up_bias, in_hbm),
    )
    for i, v in enumerate((dense_bias, norm1_gain, norm1_bias, norm2_gain, norm2_bias, down_bias)):
        inputs["in_vector%d" % i] = (v, in_hbm)
    shard = (seqs, tok_rows, width)
    outputs = dict(
        out_to=(residual_in.shape, half_type),
        in_grad_to=(residual_in.shape, single),
        dq=((ranks, rows, 3 * LANES), half_type),
        du=((ranks, rows, hidden), half_type),
        dd_to=((depth, width), single),
        dd_o_to=((rows, width), single),
        dv=((ranks, 16, LANES), single),
    )
    q_shape = (planes, ranks * rows, 3 * LANES)
    u_shape = (planes, ranks * rows, hidden)
    d_shape = (planes, depth, width)
    o_shape = (planes, rows, width)
    chips = ranks // 2
    scratch = dict(
        xa=((seqs, length, width), half_type),
        ca=((seqs, length, width), half_type),
        wq=(q_shape, half_type),
        wu=(u_shape, half_type),
        wd=(d_shape, half_type),
        wo=(o_shape, half_type),
        wo2=((pair, 2, rows, width), half_type),
        b_qkv=(qkv_bias.shape, half_type),
        b_up=(up_bias.shape, half_type),
        x_raw=(residual_in.shape, half_type),
        cot_raw=(residual_in.shape, half_type),
        x_own=(shard, half_type),
        cot_own=(shard, half_type),
        qkv=((tokens, 3 * LANES), single),
        wq_raw=(qkv_weight.shape, half_type),
        wq_s=((ranks, rows, 3 * LANES), half_type),
        table=((3, length, LANES), single),
        out=(residual_in.shape, half_type),
        in_grad=(residual_in.shape, single),
        dd=((depth, width), single),
        dd_o=((rows, width), single),
        vec_s=((16, LANES), single),
        vec_in=((ranks, 16, LANES), single),
        va=((planes, 32, LANES), single),
        center=((tokens, 1), single),
        inverse=((tokens, 1), single),
        act_one=((tokens, width), half_type),
        act_two=((tokens, width), half_type),
        query=((tokens, LANES), half_type),
        key=((tokens, LANES), half_type),
        value=((tokens, LANES), half_type),
        attn=((tokens, LANES), half_type),
        attn_grad=((tokens, LANES), half_type),
        qkv_grad=((tokens, 3 * LANES), half_type),
        gelu=((tokens, hidden), half_type),
        slope=((tokens, hidden), single),
        pre_grad=((tokens, hidden), half_type),
        gq=(q_shape, half_type),
        gu=(u_shape, half_type),
        gd=(d_shape, half_type),
        go=((pair, 2, rows, width), half_type),
        go4=(o_shape, half_type),
        above_q=(q_shape, half_type),
        below_q=(q_shape, half_type),
        above_u=(u_shape, half_type),
        below_u=(u_shape, half_type),
        above_d=(d_shape, half_type),
        below_d=(d_shape, half_type),
        above_o=(o_shape, half_type),
        below_o=(o_shape, half_type),
        fq=(q_shape[1:], half_type),
        fu=(u_shape[1:], half_type),
        po=((seqs, chips, 2, tok_rows, width), half_type),
        pg=((seqs, chips, 2, tok_rows, width), half_type),
        pairs_o=((seqs, chips, tok_rows, width), half_type),
        pairs_g=((seqs, chips, tok_rows, width), half_type),
        sums_o=((seqs, chips, tok_rows, width), half_type),
        sums_g=((seqs, chips, tok_rows, width), half_type),
        side_o=((3,) + shard, half_type),
        side_g=((3,) + shard, half_type),
        sums=((8, width), single),
        sm=((ranks, 8, LANES), single),
        sm_in=((ranks, 8, LANES), single),
        vz=((planes, 16, LANES), single),
        vt=((16, LANES), single),
    )
    for i in range(6):
        scratch["vector%d" % i] = (norm1_gain.shape, half_type)
    for block in range(length // TILE):
        scratch["probs%d" % block] = ((seqs * LANES // HD, TILE, (block + 1) * TILE), single)
    names = tuple(inputs) + tuple(outputs) + tuple(scratch) + ("send", "recv", "near", "second", "third")
    out, in_grad, dq, du, dd, dd_o, dv = pl.pallas_call(
        functools.partial(layer_kernel, names, planes),
        out_shape=[jax.ShapeDtypeStruct(*what) for what in outputs.values()],
        in_specs=[where for _, where in inputs.values()],
        out_specs=[anywhere] * len(outputs),
        scratch_shapes=[pltpu.VMEM(*what) for what in scratch.values()]
        + [pltpu.SemaphoreType.DMA((n,)) for n in (SEND_SLOTS, RECV_SLOTS, NEAR_SLOTS)]
        + [pltpu.SemaphoreType.REGULAR] * 2,
        compiler_params=pltpu.CompilerParams(
            collective_id=0, has_side_effects=True, vmem_limit_bytes=52 * 2**20
        ),
    )(
        *(
            pltpu.with_memory_space_constraint(value, pltpu.HBM) for value, _ in inputs.values()
        )
    )

    results = dict(
        out_out=(residual_in.shape, half_type),
        in_grad_out=(residual_in.shape, single),
        qkv_out=(qkv_weight.shape, single),
        qkv_bias=(qkv_bias.shape, single),
        dense_out=(dense_weight.shape, single),
        dense_bias=(dense_bias.shape, single),
        gain_one=(norm1_gain.shape, single),
        shift_one=(norm1_bias.shape, single),
        gain_two=(norm2_gain.shape, single),
        shift_two=(norm2_bias.shape, single),
        up_out=(up_weight.shape, single),
        up_bias=(up_bias.shape, single),
        down_out=(down_weight.shape, single),
        down_bias=(down_bias.shape, single),
    )
    given = tuple(n.removesuffix("_to") for n in outputs)
    staged = dict(up_v=results["up_out"], qkv_v=results["qkv_out"])
    return tuple(
        pl.pallas_call(
            functools.partial(
                finish_kernel, given + tuple(results) + tuple(staged) + ("near",), planes
            ),
            out_shape=[jax.ShapeDtypeStruct(*what) for what in results.values()],
            in_specs=[VMEM] * len(given),
            out_specs=[anywhere if len(what[0]) > 1 else VMEM for what in results.values()],
            scratch_shapes=[pltpu.VMEM(*what) for what in staged.values()]
            + [pltpu.SemaphoreType.DMA((8,))],
            compiler_params=pltpu.CompilerParams(vmem_limit_bytes=8 * 2**20),
        )(out, in_grad, dq, du, dd, dd_o, dv)
    )


def solution(mesh):
    placed = (
        P(TOKENS, BATCH, None),
        P(AXES, None),
        P(AXES),
        P(AXES, None),
        P(AXES),
        P(AXES),
        P(AXES),
        P(AXES),
        P(AXES),
        P(AXES, None),
        P(AXES),
        P(AXES, None),
        P(AXES),
        P(TOKENS, BATCH, None),
    )
    return jax.shard_map(
        functools.partial(body, dict(mesh.shape)),
        mesh=mesh,
        in_specs=placed,
        out_specs=(
            P(TOKENS, BATCH, None),
            P(TOKENS, BATCH, None),
            P(AXES, None),
            P(AXES),
            P(AXES, None),
            P(AXES),
            P(AXES),
            P(AXES),
            P(AXES),
            P(AXES),
            P(AXES, None),
            P(AXES),
            P(AXES, None),
            P(AXES),
        ),
        check_vma=False,
    )
```

```python
import functools
import math

import jax
import jax.numpy as jnp
import numpy as np
from jax import lax
from jax.experimental import pallas as pl
from jax.experimental.pallas import tpu as pltpu
from jax.sharding import PartitionSpec as P

HD = 64
BATCH, ULY, BLK = "batch", "ulysses", "blk"
AXES = (BATCH, ULY, BLK)
TOKENS = (ULY, BLK)


EPSILON = 1e-05
INV_ROOT_TWO = 0.7071067811865476
INV_ROOT_TWO_PI = 0.3989422804014327


def layer_norm(values):
    center = jnp.mean(values, axis=-1, keepdims=True)
    shifted = values - center
    inverse = lax.rsqrt(jnp.mean(shifted * shifted, axis=-1, keepdims=True) + EPSILON)
    return (shifted * inverse, inverse)


def norm_back(gradient, normed, inverse, gain_vec):
    scaled = gradient * gain_vec
    return inverse * (
        scaled
        - jnp.mean(scaled, axis=-1, keepdims=True)
        - normed * jnp.mean(scaled * normed, axis=-1, keepdims=True)
    )


def gelu_value(pre_values):
    return 0.5 * pre_values * (1.0 + jax.scipy.special.erf(pre_values * INV_ROOT_TWO))


def gelu_slope(pre_values):
    normal_cdf = 0.5 * (1.0 + jax.scipy.special.erf(pre_values * INV_ROOT_TWO))
    return normal_cdf + pre_values * jnp.exp(-0.5 * pre_values * pre_values) * INV_ROOT_TWO_PI


def rotary_tables(positions, rotary):
    half_rot = rotary // 2
    frequency = 1.0 / 10000.0 ** (jnp.arange(half_rot, dtype=jnp.float32) * (2.0 / rotary))
    angles = positions.astype(jnp.float32)[:, None] * frequency[None, :]
    cosine = jnp.concatenate([jnp.cos(angles), jnp.cos(angles)], axis=-1)
    sine_table = jnp.concatenate([jnp.sin(angles), jnp.sin(angles)], axis=-1)
    return (cosine, sine_table)


def expand_table(table, tensor):
    extra_dims = (1,) * (tensor.ndim - 2)
    return table.reshape((table.shape[0],) + extra_dims + (table.shape[1],))


def rotate_fwd(tensor, cosine, sine_table, rotary):
    half_rot = rotary // 2
    cos_full = expand_table(cosine, tensor)
    sin_full = expand_table(sine_table, tensor)
    rot_part = tensor[..., :rotary]
    turned = jnp.concatenate([-rot_part[..., half_rot:], rot_part[..., :half_rot]], axis=-1)
    return jnp.concatenate([rot_part * cos_full + turned * sin_full, tensor[..., rotary:]], axis=-1)


def rotate_back(tensor, cosine, sine_table, rotary):
    half_rot = rotary // 2
    cos_full = expand_table(cosine, tensor)
    sin_full = expand_table(sine_table, tensor)
    rot_part = tensor[..., :rotary]
    weighted = rot_part * sin_full
    turned = jnp.concatenate([weighted[..., half_rot:], -weighted[..., :half_rot]], axis=-1)
    return jnp.concatenate([rot_part * cos_full + turned, tensor[..., rotary:]], axis=-1)


def general_body(
    residual_in,
    qkv_weight,
    qkv_bias,
    dense_weight,
    dense_bias,
    norm1_gain,
    norm1_bias,
    norm2_gain,
    norm2_bias,
    up_weight,
    up_bias,
    down_weight,
    down_bias,
    cotangent,
):
    single = jnp.float32
    half_type = jnp.bfloat16
    gathered = (
        lax.all_gather(qkv_weight, AXES, axis=0, tiled=True),
        lax.all_gather(qkv_bias, AXES, axis=0, tiled=True),
        lax.all_gather(dense_weight, AXES, axis=0, tiled=True),
        lax.all_gather(dense_bias, AXES, axis=0, tiled=True),
        lax.all_gather(norm1_gain, AXES, axis=0, tiled=True),
        lax.all_gather(norm1_bias, AXES, axis=0, tiled=True),
        lax.all_gather(norm2_gain, AXES, axis=0, tiled=True),
        lax.all_gather(norm2_bias, AXES, axis=0, tiled=True),
        lax.all_gather(up_weight, AXES, axis=0, tiled=True),
        lax.all_gather(up_bias, AXES, axis=0, tiled=True),
        lax.all_gather(down_weight, AXES, axis=0, tiled=True),
        lax.all_gather(down_bias, AXES, axis=0, tiled=True),
    )
    (
        w_qkv,
        b_qkv,
        w_dense,
        b_dense,
        gain_one,
        shift_one,
        gain_two,
        shift_two,
        w_up,
        b_up,
        w_down,
        b_down,
    ) = gathered
    tok_rows = residual_in.shape[0]
    seq_count = residual_in.shape[1]
    model_width = residual_in.shape[2]
    head_count = model_width // HD
    rotary = HD // 4
    scale_factor = 1.0 / math.sqrt(HD)
    blk_size = lax.axis_size(BLK)
    uly_size = lax.axis_size(ULY)
    blk_index = lax.axis_index(BLK)
    block_id = lax.axis_index(ULY) * blk_size + blk_index
    seq_pos = block_id * tok_rows + jnp.arange(tok_rows, dtype=jnp.int32)
    inputs_f = residual_in.astype(single)
    normed, inverse = layer_norm(inputs_f)
    act_one = (normed * gain_one.astype(single) + shift_one.astype(single)).astype(half_type)
    act_two = (normed * gain_two.astype(single) + shift_two.astype(single)).astype(half_type)
    qkv_full = jnp.einsum(
        "tsd,df->tsf", act_one, w_qkv, preferred_element_type=single
    ) + b_qkv.astype(single)
    cos_seq, sin_seq = rotary_tables(seq_pos, rotary)
    head_shape = (tok_rows, seq_count, head_count, HD)
    query_seq = (
        rotate_fwd(qkv_full[..., :model_width].reshape(head_shape), cos_seq, sin_seq, rotary)
        .reshape(tok_rows, seq_count, model_width)
        .astype(half_type)
    )
    key_seq = (
        rotate_fwd(
            qkv_full[..., model_width : 2 * model_width].reshape(head_shape),
            cos_seq,
            sin_seq,
            rotary,
        )
        .reshape(tok_rows, seq_count, model_width)
        .astype(half_type)
    )
    value_seq = qkv_full[..., 2 * model_width :].astype(half_type)
    query_loc, key_loc, value_loc = (
        lax.all_to_all(query_seq, ULY, split_axis=2, concat_axis=0, tiled=True),
        lax.all_to_all(key_seq, ULY, split_axis=2, concat_axis=0, tiled=True),
        lax.all_to_all(value_seq, ULY, split_axis=2, concat_axis=0, tiled=True),
    )
    local_rows = query_loc.shape[0]
    features = query_loc.shape[2]
    local_heads = features // HD
    key_all, value_all = (
        lax.all_gather(key_loc, BLK, axis=0, tiled=True),
        lax.all_gather(value_loc, BLK, axis=0, tiled=True),
    )
    total_rows = key_all.shape[0]
    row_ids = jnp.arange(local_rows, dtype=jnp.int32)
    query_pos = (row_ids // tok_rows * blk_size + blk_index) * tok_rows + row_ids % tok_rows
    block_rows = math.gcd(512, local_rows)
    n_blocks = local_rows // block_rows
    query_h = query_loc.reshape(local_rows, seq_count, local_heads, HD)
    key_h = jnp.transpose(
        key_all.reshape(blk_size, uly_size, tok_rows, seq_count, features), (1, 0, 2, 3, 4)
    ).reshape(total_rows, seq_count, local_heads, HD)
    value_h = jnp.transpose(
        value_all.reshape(blk_size, uly_size, tok_rows, seq_count, features), (1, 0, 2, 3, 4)
    ).reshape(total_rows, seq_count, local_heads, HD)
    zero_idx = jnp.zeros((), jnp.int32)
    step_ids = jnp.arange(n_blocks * seq_count, dtype=jnp.int32)
    row_shape = (block_rows, 1, local_heads, HD)

    def select(step_index):
        row_start = step_index // seq_count * block_rows
        seq_index = step_index % seq_count
        query_rows = lax.dynamic_slice(
            query_h, (row_start, seq_index, zero_idx, zero_idx), row_shape
        )
        limit = jnp.max(query_pos) // block_rows + 1
        return (row_start, seq_index, query_rows, query_pos, limit)

    def block_scores(query_rows, row_pos, key_index, seq_index):
        key_start = key_index * block_rows
        slot = (key_start, seq_index, zero_idx, zero_idx)
        key_rows = lax.dynamic_slice(key_h, slot, (block_rows, 1, local_heads, HD))
        value_rows = lax.dynamic_slice(value_h, slot, (block_rows, 1, local_heads, HD))
        scores = (
            jnp.einsum("qshd,kshd->shqk", query_rows, key_rows, preferred_element_type=single)
            * scale_factor
        )
        key_ids = key_start + jnp.arange(block_rows, dtype=jnp.int32)
        allowed = (key_ids[None, :] <= row_pos[:, None])[None, None]
        return (jnp.where(allowed, scores, -jnp.inf), key_rows, value_rows, slot)

    def forward_block(step_index):
        row_start, seq_index, query_rows, row_pos, limit = select(step_index)

        def total_step(key_index, carry):
            running_max, running_sum = carry
            masked, key_rows, value_rows, slot = block_scores(
                query_rows, row_pos, key_index, seq_index
            )
            new_max = jnp.maximum(running_max, jnp.max(masked, axis=-1))
            new_sum = running_sum * jnp.exp(running_max - new_max) + jnp.sum(
                jnp.exp(masked - new_max[..., None]), axis=-1
            )
            return (new_max, new_sum)

        start_max = jnp.full((1, local_heads, block_rows), -jnp.inf, single)
        start_sum = jnp.zeros((1, local_heads, block_rows), single)
        final_max, final_sum = lax.fori_loop(zero_idx, limit, total_step, (start_max, start_sum))
        log_total = final_max + jnp.log(final_sum)

        def value_step(key_index, acc):
            masked, key_rows, value_rows, slot = block_scores(
                query_rows, row_pos, key_index, seq_index
            )
            weights_b = jnp.exp(masked - log_total[..., None]).astype(half_type)
            return acc + jnp.einsum(
                "shqk,kshd->qshd", weights_b, value_rows, preferred_element_type=single
            )

        result = lax.fori_loop(zero_idx, limit, value_step, jnp.zeros(row_shape, single)).astype(
            half_type
        )
        return (result[:, 0], log_total)

    results, log_totals = lax.map(forward_block, step_ids)
    attn_h = jnp.transpose(
        results.reshape(n_blocks, seq_count, block_rows, local_heads, HD), (0, 2, 1, 3, 4)
    ).reshape(local_rows, seq_count, local_heads, HD)
    attn_seq = lax.all_to_all(
        attn_h.reshape(local_rows, seq_count, features),
        ULY,
        split_axis=0,
        concat_axis=2,
        tiled=True,
    )
    proj_out = jnp.einsum(
        "tsd,de->tse", attn_seq, w_dense, preferred_element_type=single
    ) + b_dense.astype(single)
    pre_act = jnp.einsum("tsd,df->tsf", act_two, w_up, preferred_element_type=single) + b_up.astype(
        single
    )
    gelu_out = gelu_value(pre_act).astype(half_type)
    mlp_out = jnp.einsum(
        "tsf,fd->tsd", gelu_out, w_down, preferred_element_type=single
    ) + b_down.astype(single)
    output = (inputs_f + proj_out + mlp_out).astype(half_type)
    back_params = (
        lax.all_gather(qkv_weight, AXES, axis=0, tiled=True),
        lax.all_gather(qkv_bias, AXES, axis=0, tiled=True),
        lax.all_gather(dense_weight, AXES, axis=0, tiled=True),
        lax.all_gather(dense_bias, AXES, axis=0, tiled=True),
        lax.all_gather(norm1_gain, AXES, axis=0, tiled=True),
        lax.all_gather(norm1_bias, AXES, axis=0, tiled=True),
        lax.all_gather(norm2_gain, AXES, axis=0, tiled=True),
        lax.all_gather(norm2_bias, AXES, axis=0, tiled=True),
        lax.all_gather(up_weight, AXES, axis=0, tiled=True),
        lax.all_gather(up_bias, AXES, axis=0, tiled=True),
        lax.all_gather(down_weight, AXES, axis=0, tiled=True),
        lax.all_gather(down_bias, AXES, axis=0, tiled=True),
    )
    back_qkv = back_params[0]
    back_dense = back_params[2]
    back_gain_one = back_params[4].astype(single)
    back_gain_two = back_params[6].astype(single)
    back_up = back_params[8]
    back_down = back_params[10]
    grad_f = cotangent.astype(single)
    bias_sum = jnp.sum(grad_f, axis=(0, 1))
    down_w_grad = jnp.einsum("tsf,tsd->fd", gelu_out, cotangent, preferred_element_type=single)
    gelu_grad = jnp.einsum("tsd,fd->tsf", cotangent, back_down, preferred_element_type=single)
    pre_grad = (gelu_grad * gelu_slope(pre_act)).astype(half_type)
    up_w_grad = jnp.einsum("tsd,tsf->df", act_two, pre_grad, preferred_element_type=single)
    up_b_grad = jnp.sum(pre_grad.astype(single), axis=(0, 1))
    act_two_grad = jnp.einsum("tsf,df->tsd", pre_grad, back_up, preferred_element_type=single)
    gain_two_grad = jnp.sum(act_two_grad * normed, axis=(0, 1))
    shift_two_grad = jnp.sum(act_two_grad, axis=(0, 1))
    dense_w_grad = jnp.einsum("tsd,tse->de", attn_seq, cotangent, preferred_element_type=single)
    attn_grad = jnp.einsum(
        "tse,de->tsd", cotangent, back_dense, preferred_element_type=single
    ).astype(half_type)
    grad_loc = lax.all_to_all(attn_grad, ULY, split_axis=2, concat_axis=0, tiled=True)
    grad_h = grad_loc.reshape(local_rows, seq_count, local_heads, HD)

    def backward_block(acc_pair, step_index):
        row_start, seq_index, query_rows, row_pos, limit = select(step_index)
        own_slot = (row_start, seq_index, zero_idx, zero_idx)
        out_rows = lax.dynamic_slice(attn_h, own_slot, row_shape)
        grad_rows = lax.dynamic_slice(grad_h, own_slot, row_shape)
        log_total = log_totals[step_index]
        delta_row = jnp.transpose(
            jnp.sum(grad_rows.astype(single) * out_rows.astype(single), axis=-1), (1, 2, 0)
        )

        def grad_step(key_index, carry):
            key_acc, value_acc, query_acc = carry
            masked, key_rows, value_rows, slot = block_scores(
                query_rows, row_pos, key_index, seq_index
            )
            probs_f = jnp.exp(masked - log_total[..., None])
            value_part = jnp.einsum(
                "shqk,qshd->kshd",
                probs_f.astype(half_type),
                grad_rows,
                preferred_element_type=single,
            )
            grad_prob = jnp.einsum(
                "qshd,kshd->shqk", grad_rows, value_rows, preferred_element_type=single
            )
            grad_score = (probs_f * (grad_prob - delta_row[..., None]) * scale_factor).astype(
                half_type
            )
            query_acc = query_acc + jnp.einsum(
                "shqk,kshd->qshd", grad_score, key_rows, preferred_element_type=single
            )
            key_part = jnp.einsum(
                "shqk,qshd->kshd", grad_score, query_rows, preferred_element_type=single
            )
            key_acc = lax.dynamic_update_slice(
                key_acc, lax.dynamic_slice(key_acc, slot, key_part.shape) + key_part, slot
            )
            value_acc = lax.dynamic_update_slice(
                value_acc, lax.dynamic_slice(value_acc, slot, value_part.shape) + value_part, slot
            )
            return (key_acc, value_acc, query_acc)

        key_acc, value_acc, query_acc = lax.fori_loop(
            zero_idx, limit, grad_step, (acc_pair[0], acc_pair[1], jnp.zeros(row_shape, single))
        )
        return ((key_acc, value_acc), query_acc[:, 0])

    acc_zero = jnp.zeros((total_rows, seq_count, local_heads, HD), single)
    acc_final, query_parts = lax.scan(backward_block, (acc_zero, acc_zero), step_ids)
    query_grad = jnp.transpose(
        query_parts.reshape(n_blocks, seq_count, block_rows, local_heads, HD), (0, 2, 1, 3, 4)
    ).reshape(local_rows, seq_count, local_heads, HD)
    key_terms = jnp.transpose(
        acc_final[0].reshape(uly_size, blk_size, tok_rows, seq_count, features), (1, 0, 2, 3, 4)
    ).reshape(total_rows, seq_count, features)
    value_terms = jnp.transpose(
        acc_final[1].reshape(uly_size, blk_size, tok_rows, seq_count, features), (1, 0, 2, 3, 4)
    ).reshape(total_rows, seq_count, features)
    key_back, value_back = (
        lax.psum_scatter(key_terms, BLK, scatter_dimension=0, tiled=True),
        lax.psum_scatter(value_terms, BLK, scatter_dimension=0, tiled=True),
    )
    cos_h, sin_h = rotary_tables(query_pos, rotary)
    query_send = (
        rotate_back(query_grad, cos_h, sin_h, rotary)
        .reshape(local_rows, seq_count, features)
        .astype(half_type)
    )
    key_send = (
        rotate_back(key_back.reshape(local_rows, seq_count, local_heads, HD), cos_h, sin_h, rotary)
        .reshape(local_rows, seq_count, features)
        .astype(half_type)
    )
    value_send = value_back.astype(half_type)
    query_ret, key_ret, value_ret = (
        lax.all_to_all(query_send, ULY, split_axis=0, concat_axis=2, tiled=True),
        lax.all_to_all(key_send, ULY, split_axis=0, concat_axis=2, tiled=True),
        lax.all_to_all(value_send, ULY, split_axis=0, concat_axis=2, tiled=True),
    )
    qkv_grad = jnp.concatenate([query_ret, key_ret, value_ret], axis=-1)
    qkv_w_grad = jnp.einsum("tsd,tsf->df", act_one, qkv_grad, preferred_element_type=single)
    qkv_b_grad = jnp.sum(qkv_grad.astype(single), axis=(0, 1))
    act_one_grad = jnp.einsum("tsf,df->tsd", qkv_grad, back_qkv, preferred_element_type=single)
    gain_one_grad = jnp.sum(act_one_grad * normed, axis=(0, 1))
    shift_one_grad = jnp.sum(act_one_grad, axis=(0, 1))
    input_grad = (
        grad_f
        + norm_back(act_one_grad, normed, inverse, back_gain_one)
        + norm_back(act_two_grad, normed, inverse, back_gain_two)
    )
    summed = (
        lax.psum_scatter(qkv_w_grad, AXES, scatter_dimension=0, tiled=True),
        lax.psum_scatter(qkv_b_grad, AXES, scatter_dimension=0, tiled=True),
        lax.psum_scatter(
            dense_w_grad, AXES, scatter_dimension=0, tiled=True
        ),
        lax.psum_scatter(bias_sum, AXES, scatter_dimension=0, tiled=True),
        lax.psum_scatter(
            gain_one_grad, AXES, scatter_dimension=0, tiled=True
        ),
        lax.psum_scatter(
            shift_one_grad, AXES, scatter_dimension=0, tiled=True
        ),
        lax.psum_scatter(
            gain_two_grad, AXES, scatter_dimension=0, tiled=True
        ),
        lax.psum_scatter(
            shift_two_grad, AXES, scatter_dimension=0, tiled=True
        ),
        lax.psum_scatter(up_w_grad, AXES, scatter_dimension=0, tiled=True),
        lax.psum_scatter(up_b_grad, AXES, scatter_dimension=0, tiled=True),
        lax.psum_scatter(down_w_grad, AXES, scatter_dimension=0, tiled=True),
        lax.psum_scatter(bias_sum, AXES, scatter_dimension=0, tiled=True),
    )
    return (
        output,
        input_grad,
        summed[0],
        summed[1],
        summed[2],
        summed[3],
        summed[4],
        summed[5],
        summed[6],
        summed[7],
        summed[8],
        summed[9],
        summed[10],
        summed[11],
    )


MESH = pl.DeviceIdType.MESH


class Place:
    def __init__(self, planes):
        self.planes = planes
        self.b = lax.axis_index(BATCH)
        self.u = lax.axis_index(ULY)
        k = lax.axis_index(BLK)
        self.y, self.c = k // 2, k % 2
        self.t = self.u * 4 + k
        self.xn, self.yn, self.pn = self.peer(4), self.peer(2), self.peer(1)

    def rank(self, d):
        u = 1 - self.u if d & 4 else self.u
        y = 1 - self.y if d & 2 else self.y
        c = 1 - self.c if d & 1 else self.c
        return u * 4 + y * 2 + c

    def chip(self, d):
        return self.rank(d) // 2

    def peer(self, d):
        u = 1 - self.u if d & 4 else self.u
        y = 1 - self.y if d & 2 else self.y
        c = 1 - self.c if d & 1 else self.c
        return {BATCH: self.b, ULY: u, BLK: y * 2 + c}

    def along(self, step):
        return {BATCH: self.b + step, ULY: self.u, BLK: self.y * 2 + self.c}

    def barrier(self):
        sem = pltpu.get_barrier_semaphore()
        for d in range(1, 8):
            pl.semaphore_signal(sem, inc=1, device_id=self.peer(d), device_id_type=MESH)
        self.to_neighbours(
            lambda step: pl.semaphore_signal(
                sem, inc=1, device_id=self.along(step), device_id_type=MESH
            )
        )
        below = (self.b > 0).astype(jnp.int32)
        above = (self.b < self.planes - 1).astype(jnp.int32)
        pl.semaphore_wait(sem, 7 + below + above)

    def to_neighbours(self, action):
        for step in (-1, 1):

            @pl.when(self.b > 0 if step < 0 else self.b < self.planes - 1)
            def _():
                action(step)

    def reach(self, second, third):
        b, last = self.b, self.planes - 1

        @pl.when((b > 0) & (b < last))
        def _():
            for step in (-1, 1):
                pl.semaphore_signal(
                    second, inc=1, device_id=self.along(step), device_id_type=MESH
                )

        pl.semaphore_wait(second, (b >= 2).astype(jnp.int32) + (b <= last - 2).astype(jnp.int32))
        for middle, step in ((1, -1), (2, 1)):

            @pl.when(b == middle)
            def _():
                pl.semaphore_signal(third, inc=1, device_id=self.along(step), device_id_type=MESH)

        @pl.when((b == 0) | (b == last))
        def _():
            pl.semaphore_wait(third, 1)


class Mail:
    def __init__(self, send, recv, near):
        self.send, self.recv, self.near = send, recv, near
        self.sends = self.recvs = self.nears = 0

    def send_slots(self, n=1):
        self.sends += n
        return self.sends - n

    def recv_slots(self, n=1):
        self.recvs += n
        return self.recvs - n

    def bring(self, src, dst):
        made = pltpu.make_async_copy(src, dst, self.near.at[self.nears])
        self.nears += 1
        made.start()
        return made

    def copy(self, src, dst, send, recv, device):
        return pltpu.make_async_remote_copy(
            src_ref=src,
            dst_ref=dst,
            send_sem=self.send.at[send],
            recv_sem=self.recv.at[recv],
            device_id=device,
            device_id_type=MESH,
        )

    def arrived(self, bulk, recv, device):
        self.copy(bulk, bulk, 0, recv, device).wait_recv()

    def gone(self, bulk, send, device):
        self.copy(bulk, bulk, send, 0, device).wait_send()


class PlaneGather:
    def __init__(self, at, mail, shard, whole):
        self.at, self.mail, self.shard, self.whole = at, mail, shard, whole
        self.rows = shard.shape[1]
        self.halves = shard.shape[0] // 2
        self.send, self.recv = mail.send_slots(), mail.recv_slots(5)

    def half(self, i):
        return self.shard.at[pl.ds(i * self.halves, self.halves)]

    def block(self, d, half=None):
        rows = pl.ds(pl.multiple_of(self.at.rank(d) * self.rows, self.rows), self.rows)
        if half is None:
            return self.whole.at[:, rows, :]
        return self.whole.at[pl.ds(half * self.halves, self.halves), rows, :]

    def bulk(self, shards):
        return self.whole.at[:, pl.ds(0, shards * self.rows), :]

    def post(self, src, dst, recv, device):
        self.mail.copy(src, dst, self.send, self.recv + recv, device).start()

    def arrived(self, bulk, recv, device):
        self.mail.arrived(bulk, self.recv + recv, device)

    def start(self):
        at = self.at
        self.post(self.half(1), self.block(0, 1), 0, at.xn)
        self.post(self.half(0), self.block(0, 0), 1, at.yn)
        self.post(self.half(0), self.block(0, 0), 2, at.xn)
        self.post(self.half(1), self.block(0, 1), 2, at.yn)
        self.post(self.shard, self.block(0), 4, at.pn)
        self.own = self.mail.bring(self.shard, self.block(0))

    def relay_y(self):
        self.arrived(self.block(2, 0), 1, self.at.yn)
        self.post(self.block(2, 0), self.block(2, 0), 3, self.at.xn)

    def relay_x(self):
        self.arrived(self.block(4, 1), 0, self.at.xn)
        self.post(self.block(4, 1), self.block(4, 1), 3, self.at.yn)

    def share(self):
        self.arrived(self.bulk(1), 2, self.at.xn)
        self.post(self.block(2), self.block(2), 4, self.at.pn)
        self.post(self.block(4), self.block(4), 4, self.at.pn)

    def far(self):
        self.arrived(self.block(6), 3, self.at.xn)
        self.post(self.block(6), self.block(6), 4, self.at.pn)

    def finish(self):
        self.arrived(self.bulk(4), 4, self.at.pn)
        self.own.wait()

    def close(self):
        self.mail.gone(self.bulk(7), self.send, self.at.pn)


class LineGather:
    def __init__(self, at, mail, held, up_cut=None, down_cut=None):
        self.at, self.mail, self.held = at, mail, held
        whole = tuple(pl.ds(0, n) for n in held.shape[1:])
        self.up_cut, self.down_cut = up_cut or whole, down_cut or whole
        self.send, self.recv = mail.send_slots(2), mail.recv_slots(at.planes)

    def upward(self, slot, src):
        part = self.held.at[(slot,) + self.up_cut]
        src = part if src is None else src.at[self.up_cut]
        return self.mail.copy(src, part, self.send, self.recv + slot, self.at.along(1))

    def downward(self, slot, src):
        part = self.held.at[(slot,) + self.down_cut]
        src = part if src is None else src.at[self.down_cut]
        return self.mail.copy(src, part, self.send + 1, self.recv + slot, self.at.along(-1))

    def start(self, src=None):
        at = self.at

        @pl.when(at.b < at.planes - 1)
        def _():
            self.upward(at.b, src).start()

        @pl.when(at.b > 0)
        def _():
            self.downward(at.b, src).start()

    def from_below(self, distance, here):
        at = self.at
        slot = at.b - distance

        @pl.when((slot >= 0) & here)
        def _():
            part = self.held.at[(slot,) + self.up_cut]
            self.mail.arrived(part, self.recv + slot, at.along(-1))

            @pl.when(at.b < at.planes - 1)
            def _():
                self.upward(slot, None).start()

    def from_above(self, distance, here):
        at = self.at
        slot = at.b + distance

        @pl.when((slot < at.planes) & here)
        def _():
            part = self.held.at[(slot,) + self.down_cut]
            self.mail.arrived(part, self.recv + slot, at.along(1))

            @pl.when(at.b > 0)
            def _():
                self.downward(slot, None).start()

    def take(self, distance):
        self.from_below(distance, self.at.b >= 0)
        self.from_above(distance, self.at.b >= 0)

    def inner(self, distance):
        middle = self.at.planes // 2
        self.from_below(distance, self.at.b >= middle)
        self.from_above(distance, self.at.b < middle)

    def outer(self, distance):
        middle = self.at.planes // 2
        self.from_below(distance, self.at.b < middle)
        self.from_above(distance, self.at.b >= middle)

    def close(self):
        at = self.at
        for b in range(at.planes):

            @pl.when(at.b == b)
            def _():
                if b < at.planes - 1:
                    bulk = self.held.at[(pl.ds(0, b + 1),) + self.up_cut]
                    self.mail.gone(bulk, self.send, at.along(1))
                if b > 0:
                    bulk = self.held.at[(pl.ds(0, at.planes - b),) + self.down_cut]
                    self.mail.gone(bulk, self.send + 1, at.along(-1))


class StarGather:
    def __init__(self, at, mail, held):
        self.at, self.mail, self.held = at, mail, held
        self.send, self.recv = mail.send_slots(), mail.recv_slots()

    def start(self):
        at = self.at
        part = self.held.at[at.b]
        for step in range(1, at.planes):

            @pl.when(at.b + step < at.planes)
            def _():
                self.mail.copy(part, part, self.send, self.recv, at.along(step)).start()

            @pl.when(at.b >= step)
            def _():
                self.mail.copy(part, part, self.send, self.recv, at.along(-step)).start()

    def bulk(self):
        return self.held.at[pl.ds(0, self.at.planes - 1)]

    def finish(self):
        self.mail.arrived(self.bulk(), self.recv, self.at.pn)

    def close(self):
        self.mail.gone(self.bulk(), self.send, self.at.pn)


class PlaneExchange:
    def __init__(self, at, mail, pieces, landings, bulk):
        self.at, self.mail, self.bulk = at, mail, bulk
        self.pieces, self.landings = pieces, landings
        self.send, self.recv = mail.send_slots(), mail.recv_slots()

    def start(self):
        at = self.at
        for d in range(1, 8):
            for piece, landing in zip(self.pieces(at.rank(d)), self.landings(at.t)):
                self.mail.copy(piece, landing, self.send, self.recv, at.peer(d)).start()
        self.own = [
            self.mail.bring(piece, landing)
            for piece, landing in zip(self.pieces(at.t), self.landings(at.t))
        ]

    def finish(self):
        self.mail.arrived(self.bulk, self.recv, self.at.pn)
        for own in self.own:
            own.wait()

    def close(self):
        self.mail.gone(self.bulk, self.send, self.at.pn)


class PairExchange:
    def __init__(self, at, mail, src, dst, landed):
        self.at, self.mail, self.src, self.dst, self.landed = at, mail, src, dst, landed
        self.send, self.recv = mail.send_slots(), mail.recv_slots()

    def start(self):
        self.mail.copy(self.src, self.dst, self.send, self.recv, self.at.pn).start()

    def finish(self):
        self.mail.arrived(self.landed, self.recv, self.at.pn)

    def close(self):
        self.mail.gone(self.src, self.send, self.at.pn)


class PlaneReduce:
    def __init__(self, at, mail, terms, pairs, sums, side, bulk):
        self.at, self.mail, self.terms, self.bulk = at, mail, terms, bulk
        self.pairs, self.sums, self.side = pairs, sums, side
        self.send, self.recv = mail.send_slots(), mail.recv_slots(6)
        self.halves = terms.shape[0] // 2

    def post(self, src, dst, recv, device):
        self.mail.copy(src, dst, self.send, self.recv + recv, device).start()

    def start(self, *chips):
        at = self.at
        for d in chips:
            chip = at.chip(d)
            recv = {6: 0, 4: 1}.get(d, 5)
            self.post(self.terms.at[:, chip, 1 - at.c], self.pairs.at[:, chip], recv, at.pn)

    def half(self, ref, i):
        return ref.at[pl.ds(i * self.halves, self.halves)]

    def add_pair(self, d):
        chip = self.at.chip(d)
        total = self.terms[:, chip, self.at.c].astype(jnp.float32) + self.pairs[:, chip].astype(
            jnp.float32
        )
        self.sums[:, chip] = total.astype(self.sums.dtype)

    def fold_far(self):
        at = self.at
        far = self.sums.at[:, at.chip(6)]
        self.mail.arrived(self.bulk(1), self.recv, at.pn)
        self.add_pair(6)
        self.post(self.half(far, 0), self.half(self.side.at[0], 0), 2, at.xn)
        self.post(self.half(far, 1), self.half(self.side.at[0], 1), 3, at.yn)

    def fold_x(self):
        self.mail.arrived(self.bulk(1), self.recv + 1, self.at.pn)
        self.add_pair(4)

    def fold_near(self):
        self.mail.arrived(self.bulk(2), self.recv + 5, self.at.pn)
        self.add_pair(2)
        self.add_pair(0)

    def turn_x(self):
        self.turn(1, 4, self.at.yn, 3, self.at.xn)

    def turn_y(self):
        self.turn(0, 2, self.at.xn, 2, self.at.yn)

    def turn(self, i, d, other, recv, nbr):
        landed = self.half(self.side.at[0], i)
        self.mail.arrived(landed, self.recv + recv, other)
        whole = self.sums.at[:, self.at.chip(d)]
        part = self.half(whole, i)
        part[...] = (part[...].astype(jnp.float32) + landed[...].astype(jnp.float32)).astype(
            self.sums.dtype
        )
        self.post(whole, self.side.at[2 - i], 4, nbr)

    def finish(self):
        self.mail.arrived(self.bulk(2), self.recv + 4, self.at.xn)
        return (
            self.sums[:, self.at.chip(0)].astype(jnp.float32)
            + self.side[1].astype(jnp.float32)
            + self.side[2].astype(jnp.float32)
        )

    def close(self):
        self.mail.gone(self.bulk(7), self.send, self.at.pn)


class LineReduce:
    def __init__(self, at, mail, terms, above, below, up_cut=None, down_cut=None):
        self.at, self.mail, self.terms = at, mail, terms
        self.above, self.below = above, below
        whole = pl.ds(0, terms.shape[2])
        self.up_cut, self.down_cut = up_cut or whole, down_cut or whole
        self.send, self.recv = mail.send_slots(2), mail.recv_slots(at.planes + 1)

    def upward(self, src, slot):
        return self.mail.copy(
            src.at[slot, :, self.up_cut],
            self.below.at[slot, :, self.up_cut],
            self.send,
            self.recv + slot,
            self.at.along(1),
        )

    def downward(self, src, slot, last_step):
        return self.mail.copy(
            src.at[slot, :, self.down_cut],
            self.above.at[slot, :, self.down_cut],
            self.send + 1,
            self.recv + (self.at.planes if last_step else slot),
            self.at.along(-1),
        )

    def edge(self, slot):
        at, last = self.at, self.at.planes - 1
        if slot == 0:
            return

        @pl.when(at.b == 0)
        def _():
            self.upward(self.terms, slot).start()

        @pl.when(at.b == last)
        def _():
            self.downward(self.terms, last - slot, slot == 1).start()

    def hop(self, hop, rank):
        at, mail, last = self.at, self.mail, self.at.planes - 1
        slot = last - rank
        if slot <= hop:
            return

        @pl.when(at.b == hop)
        def _():
            cut = self.up_cut
            mail.arrived(self.below.at[slot, :, cut], self.recv + slot, at.along(-1))
            self.add(self.below, slot, cut)
            self.upward(self.below, slot).start()

        @pl.when(at.b == last - hop)
        def _():
            cut = self.down_cut
            mail.arrived(self.above.at[rank, :, cut], self.recv + rank, at.along(1))
            self.add(self.above, rank, cut)
            self.downward(self.above, rank, rank == last - hop - 1).start()

    def add(self, held, slot, cut):
        total = self.terms[slot, :, cut].astype(jnp.float32) + held[slot, :, cut].astype(
            jnp.float32
        )
        held[slot, :, cut] = total.astype(held.dtype)

    def landed(self):
        at, mail = self.at, self.mail

        @pl.when(at.b > 0)
        def _():
            mail.arrived(self.below.at[at.b, :, self.up_cut], self.recv + at.b, at.along(-1))

        @pl.when(at.b < at.planes - 1)
        def _():
            bulk = self.above.at[at.b, :, self.down_cut]
            mail.arrived(bulk, self.recv + at.planes, at.along(1))

    def total(self, out):
        b, last = self.at.b, self.at.planes - 1

        def put(*parts):
            value = self.terms[b].astype(jnp.float32)
            for part in parts:
                value = value + part[b].astype(jnp.float32)
            out[...] = value.astype(out.dtype)

        @pl.when(b == 0)
        def _():
            put(self.above)

        @pl.when(b == last)
        def _():
            put(self.below)

        @pl.when((b > 0) & (b < last))
        def _():
            put(self.below, self.above)

    def close(self):
        at, last = self.at, self.at.planes - 1
        for b in range(at.planes):

            @pl.when(at.b == b)
            def _():
                if b < last:
                    bulk = self.terms.at[pl.ds(0, last - b), :, self.up_cut]
                    self.mail.gone(bulk, self.send, at.along(1))
                if b > 0:
                    bulk = self.terms.at[pl.ds(0, b), :, self.down_cut]
                    self.mail.gone(bulk, self.send + 1, at.along(-1))


TILE = 256
LANES = 128


def dot_nn(a, b):
    return lax.dot_general(a, b, (((1,), (0,)), ((), ())), preferred_element_type=jnp.float32)


def dot_nt(a, b):
    return lax.dot_general(a, b, (((1,), (1,)), ((), ())), preferred_element_type=jnp.float32)


def dot_tn(a, b):
    return lax.dot_general(a, b, (((0,), (0,)), ((), ())), preferred_element_type=jnp.float32)


def turn(value, tables, rows, sign):
    straight, early, late = (table[rows, :] for table in tables)
    ahead = pltpu.roll(value, LANES - HD // 8, 1)
    behind = pltpu.roll(value, HD // 8, 1)
    return value * straight + sign * (ahead * early + behind * late)


def of_head(value, head):
    lane = lax.broadcasted_iota(jnp.int32, value.shape, 1)
    return jnp.where(lane // HD == head, value, jnp.zeros_like(value))


def total_rows(value):
    return jnp.sum(value, axis=0, keepdims=True)


class Layer:
    def __init__(self, refs):
        self.__dict__.update(refs)
        self.heads = LANES // HD
        if "xa" in refs:
            self.seqs, self.length, self.width = self.xa.shape
            self.per_seq = self.length // TILE
            self.tiles = self.seqs * self.per_seq

    def rows(self, tile):
        return pl.ds(pl.multiple_of(tile * TILE, TILE), TILE)

    def in_seq(self, ref, tile):
        rows = pl.ds(pl.multiple_of(tile % self.per_seq * TILE, TILE), TILE)
        return ref[tile // self.per_seq, rows, :]

    def loop(self, count, step):
        def run(i, carry):
            step(i)
            return carry

        lax.fori_loop(0, count, run, 0)

    def wide(self, row):
        planes = self.va.shape[0]
        return jnp.concatenate(
            [self.va[b, pl.ds(2 * row + a, 1), :] for b in range(planes) for a in range(2)], axis=1
        )

    def own_vectors(self, rank):
        lane = lax.broadcasted_iota(jnp.int32, (2, LANES), 1)
        row = lax.broadcasted_iota(jnp.int32, (2, LANES), 0)
        for j, ref in enumerate(self.vectors):
            piece = ref[...].astype(jnp.float32).reshape(1, ref.shape[0])
            piece = jnp.concatenate([piece] * (LANES // ref.shape[0]), axis=1)
            here = (lane // ref.shape[0] == rank % 4) & (row == rank // 4)
            self.vec_s[2 * j : 2 * j + 2, :] = jnp.where(here, jnp.broadcast_to(piece, here.shape), 0.0)
        bias = self.b_qkv[...].astype(jnp.float32).reshape(1, self.b_qkv.shape[0])
        self.vec_s[12:13, :] = jnp.concatenate(
            [bias, jnp.zeros((1, LANES - bias.shape[1]), jnp.float32)], axis=1
        )
        self.vec_s[13:14, :] = self.b_up[...].astype(jnp.float32).reshape(1, LANES)

    def plane_vectors(self, slot):
        total = jnp.sum(self.vec_in[...], axis=0)
        self.va[slot, 0:16, :] = total
        for rank in range(self.vec_in.shape[0]):
            self.va[slot, 16 + rank : 17 + rank, :] = self.vec_in[rank, 12:13, :]
            self.va[slot, 24 + rank : 25 + rank, :] = self.vec_in[rank, 13:14, :]

    def sort_weight(self):
        rows = self.wq_raw.shape[0]
        low = lax.broadcasted_iota(jnp.int32, (rows, LANES), 1) < HD
        for part in range(3):
            for core in range(2):
                for pair in range(2):
                    first, second = (
                        self.wq_raw[
                            :, pl.ds(part * self.width + (core * 2 + j) * 4 * HD + pair * LANES, LANES)
                        ].astype(jnp.float32)
                        for j in range(2)
                    )
                    cut = slice(part * LANES, (part + 1) * LANES)
                    self.wq_s[4 * pair + core, :, cut] = jnp.where(
                        low, first, pltpu.roll(second, HD, 1)
                    ).astype(jnp.bfloat16)
                    self.wq_s[4 * pair + 2 + core, :, cut] = jnp.where(
                        low, pltpu.roll(first, HD, 1), second
                    ).astype(jnp.bfloat16)

    def statistics(self):
        def step(i):
            x = self.in_seq(self.xa, i).astype(jnp.float32)
            center = jnp.mean(x, axis=1, keepdims=True)
            shifted = x - center
            spread = jnp.mean(shifted * shifted, axis=1, keepdims=True)
            self.center[self.rows(i), :] = center
            self.inverse[self.rows(i), :] = lax.rsqrt(spread + EPSILON)

        self.loop(self.tiles, step)

    def normed(self, i):
        x = self.in_seq(self.xa, i).astype(jnp.float32)
        return (x - self.center[self.rows(i), :]) * self.inverse[self.rows(i), :]

    def activations(self):
        gain_one, shift_one, gain_two, shift_two = (self.wide(j) for j in (1, 2, 3, 4))

        def step(i):
            normed = self.normed(i)
            self.act_one[self.rows(i), :] = (normed * gain_one + shift_one).astype(jnp.bfloat16)
            self.act_two[self.rows(i), :] = (normed * gain_two + shift_two).astype(jnp.bfloat16)

        self.loop(self.tiles, step)

    def qkv_bias(self, rank):
        size = HD // 2
        held = self.b_qkv.shape[0] // size
        ranks = self.vec_in.shape[0]
        pieces = []
        for i in range(3 * LANES // size):
            part, j, half = i // 4, i // 2 % 2, i % 2
            head = (rank % 2 * 2 + j) * 4 + rank // 2
            index = part * (self.width // size) + head * 2 + half
            owner, spot = index // held, index % held
            row = self.va[owner // ranks, pl.ds(16 + owner % ranks, 1), :]
            pieces.append(
                sum(
                    jnp.where(spot == k, row[:, k * size : (k + 1) * size], 0.0)
                    for k in range(held)
                )
            )
        return jnp.concatenate(pieces, axis=1)

    def near(self, ref, side):
        both = ref[pl.ds(side * 2, 2)]
        return both.reshape(both.shape[0] * both.shape[1], both.shape[2])

    def half_columns(self, side, width):
        return pl.ds(pl.multiple_of(side * (width // 2), width // 2), width // 2)

    def project_near(self, side):
        def step(i):
            cut = self.half_columns(side, self.width)
            self.qkv[self.rows(i), :] = dot_nn(self.act_one[self.rows(i), cut], self.near(self.wq, side))

        self.loop(self.tiles, step)

    def project(self, rank, side):
        bias = self.qkv_bias(rank)

        def step(i):
            cut = self.half_columns(side, self.width)
            qkv = dot_nn(self.act_one[self.rows(i), cut], self.near(self.wq, side))
            qkv = qkv + self.qkv[self.rows(i), :] + bias
            rows = pl.ds(pl.multiple_of(i % self.per_seq * TILE, TILE), TILE)
            query = turn(qkv[:, :LANES], self.tables, rows, 1.0).astype(jnp.bfloat16)
            self.query[self.rows(i), :] = query * jnp.asarray(1.0 / math.sqrt(HD), jnp.bfloat16)
            self.key[self.rows(i), :] = turn(
                qkv[:, LANES : 2 * LANES], self.tables, rows, 1.0
            ).astype(jnp.bfloat16)
            self.value[self.rows(i), :] = qkv[:, 2 * LANES :].astype(jnp.bfloat16)

        self.loop(self.tiles, step)

    def keys(self, seq, block):
        start = pl.multiple_of(seq * self.length, TILE)
        return pl.ds(start, (block + 1) * TILE)

    def attend(self, seq):
        for block in range(self.per_seq):
            rows = self.rows(seq * self.per_seq + block)
            keys = self.keys(seq, block)
            key, value, query = self.key[keys, :], self.value[keys, :], self.query[rows, :]
            out = None
            for head in range(self.heads):
                scores = dot_nt(of_head(query, head), key)
                at = lax.broadcasted_iota(jnp.int32, scores.shape, 0) + block * TILE
                to = lax.broadcasted_iota(jnp.int32, scores.shape, 1)
                scores = jnp.where(to <= at, scores, -jnp.inf)
                top = jnp.max(scores, axis=1, keepdims=True)
                weight = jnp.exp(scores - top)
                weight = weight * (1.0 / jnp.sum(weight, axis=1, keepdims=True))
                self.probs[block][seq * self.heads + head] = weight
                part = dot_nn(weight.astype(jnp.bfloat16), value)
                out = of_head(part, head) if out is None else out + of_head(part, head)
            self.attn[rows, :] = out.astype(jnp.bfloat16)

    def attend_out_grad(self):
        def step(i):
            weight = self.wo2[...].reshape(LANES, self.width)
            self.attn_grad[self.rows(i), :] = dot_nt(self.in_seq(self.ca, i), weight).astype(
                jnp.bfloat16
            )

        self.loop(self.tiles, step)

    def attend_grad(self, seq):
        key_grad, value_grad = [None] * self.per_seq, [None] * self.per_seq
        start = seq * self.per_seq
        for block in range(self.per_seq):
            rows = self.rows(start + block)
            keys = self.keys(seq, block)
            key, value, query = self.key[keys, :], self.value[keys, :], self.query[rows, :]
            grad = self.attn_grad[rows, :]
            inner = grad.astype(jnp.float32) * self.attn[rows, :].astype(jnp.float32)
            query_grad = None
            for head in range(self.heads):
                own_grad = of_head(grad, head)
                delta = jnp.sum(of_head(inner, head), axis=1, keepdims=True)
                probs = self.probs[block][seq * self.heads + head]
                grad_prob = dot_nt(own_grad, value)
                grad_score = (probs * (grad_prob - delta)).astype(jnp.bfloat16)
                part = dot_nn(grad_score, of_head(key, head))
                query_grad = part if query_grad is None else query_grad + part
                key_part = dot_tn(grad_score, of_head(query, head))
                value_part = dot_tn(probs.astype(jnp.bfloat16), own_grad)
                for b in range(block + 1):
                    cut = slice(b * TILE, (b + 1) * TILE)
                    key_grad[b] = key_part[cut] if key_grad[b] is None else key_grad[b] + key_part[cut]
                    value_grad[b] = (
                        value_part[cut] if value_grad[b] is None else value_grad[b] + value_part[cut]
                    )
            back = pl.ds(block * TILE, TILE)
            self.qkv_grad[rows, :LANES] = turn(
                query_grad * (1.0 / math.sqrt(HD)), self.tables, back, -1.0
            ).astype(jnp.bfloat16)
        for block in range(self.per_seq):
            rows = self.rows(start + block)
            back = pl.ds(block * TILE, TILE)
            self.qkv_grad[rows, LANES : 2 * LANES] = turn(
                key_grad[block], self.tables, back, -1.0
            ).astype(jnp.bfloat16)
            self.qkv_grad[rows, 2 * LANES :] = value_grad[block].astype(jnp.bfloat16)

    def cot_flat(self):
        return self.ca[...].reshape(self.seqs * self.length, self.width)

    def qkv_weight_grad(self, i):
        rows = self.gq.shape[1]
        act = self.act_one[:, pl.ds(pl.multiple_of(i * rows, rows), rows)]
        self.gq[i] = dot_tn(act, self.qkv_grad[...]).astype(jnp.bfloat16)

    def dense_weight_grad(self):
        self.go[...] = (
            dot_tn(self.attn[...], self.cot_flat()).astype(jnp.bfloat16).reshape(self.go.shape)
        )

    def expand(self, rank, side):
        cut = self.half_columns(side, self.hidden)
        slots = self.va.shape[0] // 2
        bias = jnp.concatenate(
            [self.va[side * slots + i, pl.ds(24 + rank, 1), :] for i in range(slots)], axis=1
        )

        def step(i):
            weight = self.wu[:, :, cut].reshape(self.width, self.hidden // 2)
            pre = dot_nn(self.act_two[self.rows(i), :], weight) + bias
            cdf = 0.5 * (1.0 + lax.erf(pre * INV_ROOT_TWO))
            self.gelu[self.rows(i), cut] = (pre * cdf).astype(jnp.bfloat16)
            self.slope[self.rows(i), cut] = cdf + pre * jnp.exp(-0.5 * pre * pre) * INV_ROOT_TWO_PI

        self.loop(self.tiles, step)

    def down_weight_grad(self, i):
        depth = self.gd.shape[1]
        part = self.gelu[:, pl.ds(pl.multiple_of(i * depth, depth), depth)]
        self.gd[i] = dot_tn(part, self.cot_flat()).astype(jnp.bfloat16)

    def hidden_grad(self, side):
        def step(i):
            cut = self.half_columns(side, self.hidden)
            grad = dot_nt(self.in_seq(self.ca, i), self.near(self.wd, side))
            self.pre_grad[self.rows(i), cut] = (grad * self.slope[self.rows(i), cut]).astype(
                jnp.bfloat16
            )

        self.loop(self.tiles, step)

    def up_weight_grad(self, i, side):
        rows = self.gu.shape[1]
        act = self.act_two[:, pl.ds(pl.multiple_of(i * rows, rows), rows)]
        cut = self.half_columns(side, self.hidden)
        self.gu[i, :, cut] = dot_tn(act, self.pre_grad[:, cut]).astype(jnp.bfloat16)

    def put_terms(self, terms, i, value):
        seq, chips, cores, rows, width = terms.shape
        n = TILE // (cores * rows)
        terms[i // self.per_seq, pl.ds(i % self.per_seq * n, n)] = value.astype(
            jnp.bfloat16
        ).reshape(n, cores, rows, width)

    def out_terms(self, i):
        dense = self.wo2[...].reshape(LANES, self.width)
        down = self.wd[...].reshape(self.hidden, self.width)
        self.put_terms(
            self.po,
            i,
            dot_nn(self.attn[self.rows(i), :], dense) + dot_nn(self.gelu[self.rows(i), :], down),
        )

    def in_terms_one(self, i, first):
        gain = self.wide(1)
        weight = self.wq[...].reshape(self.width, 3 * LANES)
        value = dot_nt(self.qkv_grad[self.rows(i), :], weight)
        self.park(i, value * gain)
        self.add_sums(0, value, self.normed(i), first)

    def in_terms_two(self, i, first):
        gain = self.wide(3)
        weight = self.wu[...].reshape(self.width, self.hidden)
        value = dot_nt(self.pre_grad[self.rows(i), :], weight)
        self.put_terms(self.pg, i, self.parked(i) + value * gain)
        self.add_sums(2, value, self.normed(i), first)

    def park(self, i, value):
        quarter = self.width // 4
        self.probs[1][i] = value[:, : 2 * quarter]
        self.probs[0][i] = value[:, 2 * quarter : 3 * quarter]
        self.qkv[self.rows(i), :quarter] = value[:, 3 * quarter :]

    def parked(self, i):
        quarter = self.width // 4
        return jnp.concatenate(
            [self.probs[1][i], self.probs[0][i], self.qkv[self.rows(i), :quarter]], axis=1
        )

    def add_sums(self, row, value, normed, first):
        for j, sums in ((row, total_rows(value * normed)), (row + 1, total_rows(value))):
            if first:
                self.sums[j : j + 1, :] = sums
            else:
                self.sums[j : j + 1, :] += sums

    def split(self, raw, own):
        for seq in range(own.shape[0]):
            own[seq] = raw[:, seq, :]

    def own_rows(self, ref, rank):
        rows = self.out.shape[0]
        return ref[:, pl.ds(pl.multiple_of(rank * rows, rows), rows), :].astype(jnp.float32)

    def small_terms(self, rank):
        ranks = self.sm.shape[0]
        cot = total_rows(jnp.sum(self.own_rows(self.ca, rank), axis=0))
        for to in range(ranks):
            cut = slice(to * LANES, (to + 1) * LANES)
            self.sm[to, 0:1, :] = cot[:, cut]
            self.sm[to, 1:5, :] = self.sums[0:4, cut]

    def small_plane(self, slot):
        total = jnp.sum(self.sm_in[...], axis=0)
        self.vz[slot, 0:8, :] = total
        qkv = total_rows(self.qkv_grad[...].astype(jnp.float32))
        pre = total_rows(self.pre_grad[...].astype(jnp.float32))
        for j in range(3):
            self.vz[slot, 8 + j : 9 + j, :] = qkv[:, j * LANES : (j + 1) * LANES]
        for j in range(self.hidden // LANES):
            self.vz[slot, 12 + j : 13 + j, :] = pre[:, j * LANES : (j + 1) * LANES]

    def result(self, rank, out_sum, in_sum):
        x = self.own_rows(self.xa, rank)
        center = jnp.mean(x, axis=2, keepdims=True)
        shifted = x - center
        inverse = lax.rsqrt(jnp.mean(shifted * shifted, axis=2, keepdims=True) + EPSILON)
        normed = shifted * inverse
        bias = (self.wide(0) + self.wide(5))[None]
        value = (x + out_sum + bias).astype(jnp.bfloat16)
        grad = self.own_rows(self.ca, rank) + inverse * (
            in_sum
            - jnp.mean(in_sum, axis=2, keepdims=True)
            - normed * jnp.mean(in_sum * normed, axis=2, keepdims=True)
        )
        for seq in range(x.shape[0]):
            self.out[:, seq, :] = value[seq]
            self.in_grad[:, seq, :] = grad[seq]


SEND_SLOTS, RECV_SLOTS, NEAR_SLOTS = 37, 82, 30


def layer_kernel(names, planes, *refs):
    refs = dict(zip(names, refs))
    send, recv, near, second, third = (refs.pop(name) for name in names[-5:])
    refs.update(
        tables=tuple(refs["table"].at[i] for i in range(3)),
        probs=tuple(refs[name] for name in names if name.startswith("probs")),
        vectors=tuple(refs[name] for name in names if name.startswith("vector")),
        hidden=refs["gelu"].shape[1],
    )
    given = [refs["in_qkv"], refs["in_up"]]
    given += [refs[name] for name in names if name.startswith("in_vector")]
    do = Layer(refs)
    at = Place(planes)
    mail = Mail(send, recv, near)
    b, c = at.b, at.c
    rows = do.wq_s.shape[1]
    pair = planes // 2
    others = pl.ds(0, 7)

    def shards(n):
        return do.xa.at[:, pl.ds(0, n * do.x_own.shape[1]), :]

    def strip(whole):
        return lambda rank: [whole.at[b, pl.ds(pl.multiple_of(rank * rows, rows), rows), :]]

    def band(whole):
        return lambda rank: [whole.at[pl.ds(pl.multiple_of(rank * rows, rows), rows), :]]

    def up_pieces(rank):
        return [
            do.wu_s.at[:, pl.ds(pl.multiple_of((p * 8 + rank) * LANES, LANES), LANES)]
            for p in range(planes)
        ]

    def up_landings(rank):
        strip_rows = pl.ds(pl.multiple_of(rank * rows, rows), rows)
        return [do.wu.at[b, strip_rows, pl.ds(p * LANES, LANES)] for p in range(planes)]

    gather_x = PlaneGather(at, mail, do.x_own, do.xa)
    gather_c = PlaneGather(at, mail, do.cot_own, do.ca)
    line_v, line_o = StarGather(at, mail, do.va), LineGather(at, mail, do.wo)
    line_q = LineGather(at, mail, do.wq)
    low, high = (pl.ds(i * do.hidden // 2, do.hidden // 2) for i in range(2))
    all_rows = pl.ds(0, do.wu.shape[1])
    line_ua = LineGather(at, mail, do.wu, (all_rows, low), (all_rows, high))
    line_ub = LineGather(at, mail, do.wu, (all_rows, high), (all_rows, low))
    half = do.wd.shape[1] // 2
    cuts = [(pl.ds(i * half, half), pl.ds(0, do.wd.shape[2])) for i in range(2)]
    line_da = LineGather(at, mail, do.wd, cuts[0], cuts[0])
    line_db = LineGather(at, mail, do.wd, cuts[1], cuts[1])
    ex_v = PlaneExchange(at, mail, lambda rank: [do.vec_s], lambda rank: [do.vec_in.at[rank]], do.vec_in.at[others])
    ex_q = PlaneExchange(
        at, mail, lambda rank: [do.wq_s.at[rank]], strip(do.wq), do.wq_s.at[others]
    )
    ex_u = PlaneExchange(at, mail, up_pieces, up_landings, do.wu.at[0, pl.ds(0, 7 * rows)])
    mine = do.wo2.at[:, c]
    swap_w = PairExchange(
        at, mail, do.wo.at[pl.ds(pair * (1 - c), pair)], mine, do.wo2.at[:, 1 - c]
    )
    sum_o = LineReduce(at, mail, do.go4, do.above_o, do.below_o)
    sum_q = LineReduce(at, mail, do.gq, do.above_q, do.below_q)
    sum_un = LineReduce(at, mail, do.gu, do.above_u, do.below_u, low, high)
    sum_uf = LineReduce(at, mail, do.gu, do.above_u, do.below_u, high, low)
    near_side = b // pair
    far_side = 1 - near_side
    sum_d = LineReduce(at, mail, do.gd, do.above_d, do.below_d)
    swap_g = PairExchange(
        at,
        mail,
        do.go.at[:, 1 - c],
        do.go4.at[pl.ds(pair * c, pair)],
        do.go4.at[pl.ds(pair * (1 - c), pair)],
    )
    back_q = PlaneExchange(
        at, mail, band(do.fq), lambda rank: [do.dq.at[rank]], do.fq.at[pl.ds(0, 7 * rows)]
    )
    back_u = PlaneExchange(
        at, mail, band(do.fu), lambda rank: [do.du.at[rank]], do.fu.at[pl.ds(0, 7 * rows)]
    )
    fold_v = PlaneExchange(
        at, mail, lambda rank: [do.sm.at[rank]], lambda rank: [do.sm_in.at[rank]], do.sm.at[others]
    )
    line_s = StarGather(at, mail, do.vz)
    share_v = PlaneExchange(
        at, mail, lambda rank: [do.vt], lambda rank: [do.dv.at[rank]], do.dv.at[others]
    )
    plane_o = PlaneReduce(at, mail, do.po, do.pairs_o, do.sums_o, do.side_o, shards)
    plane_g = PlaneReduce(at, mail, do.pg, do.pairs_g, do.sums_g, do.side_g, shards)

    slots = [s + b // pair * (planes - 1 - 2 * s) for s in (3, 0, 2, 1)]
    tiles = [seq * 2 + half for half in (1 - at.u, at.u) for seq in range(2)]
    turned = [s + b // pair * (planes - 1 - 2 * s) for s in (3, 2, 1, 0)]

    at.barrier()
    line_da.start(do.wd_s)
    own_d = mail.bring(do.wd_s, do.wd.at[b])
    raw_x = mail.bring(do.x_in, do.x_raw)
    ex_u.start()
    line_o.start(do.wo_s)
    own_o = mail.bring(do.wo_s, do.wo.at[b])
    raw_x.wait()
    do.split(do.x_raw, do.x_own)
    gather_x.start()
    line_db.start(do.wd_s)
    raw_c = mail.bring(do.cot_in, do.cot_raw)
    line_o.take(1)
    ex_u.finish()
    line_ua.start()
    gather_x.relay_x()
    own_v = [mail.bring(src, dst) for src, dst in zip(given, [do.b_qkv, do.b_up, *do.vectors])]
    own_raw = mail.bring(do.wq_in, do.wq_raw)
    gather_x.relay_y()
    line_ub.start()
    for made in own_v:
        made.wait()
    do.own_vectors(at.t)
    ex_v.start()
    gather_x.share()
    own_d.wait()
    raw_c.wait()
    do.split(do.cot_raw, do.cot_own)
    line_ua.outer(1)
    own_raw.wait()
    do.sort_weight()
    ex_q.start()
    at.reach(second, third)
    gather_x.far()
    line_ua.inner(1)
    line_o.take(2)
    gather_c.start()
    gather_x.finish()
    ex_v.finish()
    do.plane_vectors(b)
    line_v.start()
    line_ua.inner(2)
    line_ub.outer(1)
    gather_c.relay_x()
    gather_c.relay_y()
    do.statistics()
    line_ub.inner(1)
    ex_q.finish()
    line_q.start()
    line_o.take(3)
    own_table = mail.bring(do.table_in, do.table)
    line_v.finish()
    do.activations()
    line_ua.inner(3)
    own_o.wait()
    gather_c.share()
    do.expand(at.t, far_side)
    gather_c.far()
    gather_c.finish()
    do.down_weight_grad(turned[0])
    sum_d.edge(3)
    line_ub.inner(2)
    swap_w.start()
    mine[...] = do.wo[pl.ds(pair * c, pair)]
    line_q.take(1)
    own_table.wait()
    do.down_weight_grad(turned[1])
    sum_d.edge(2)
    swap_w.finish()
    do.attend_out_grad()
    do.project_near(near_side)
    line_ub.inner(3)
    do.expand(at.t, near_side)
    line_q.take(2)
    line_da.take(1)
    do.down_weight_grad(turned[2])
    sum_d.edge(1)
    line_db.take(1)
    do.down_weight_grad(turned[3])
    sum_d.edge(0)
    do.hidden_grad(near_side)
    do.up_weight_grad(slots[0], near_side)
    sum_un.edge(3)
    do.up_weight_grad(slots[1], near_side)
    sum_un.edge(0)
    do.up_weight_grad(slots[2], near_side)
    sum_un.edge(2)
    line_q.take(3)
    do.project(at.t, far_side)
    sum_d.hop(1, 0)
    do.up_weight_grad(slots[3], near_side)
    sum_un.edge(1)
    do.attend(0)
    line_da.take(2)
    do.attend(1)
    do.attend_grad(0)
    line_db.take(2)
    do.dense_weight_grad()
    swap_g.start()
    do.go4[pl.ds(pair * c, pair)] = do.go[:, c]
    do.attend_grad(1)
    line_da.take(3)
    sum_d.hop(1, 1)
    do.in_terms_one(tiles[0], True)
    do.qkv_weight_grad(slots[0])
    sum_q.edge(3)
    do.in_terms_one(tiles[1], False)
    sum_un.hop(1, 0)
    swap_g.finish()
    sum_o.edge(3)
    line_db.take(3)
    do.qkv_weight_grad(slots[1])
    sum_q.edge(0)
    do.out_terms(tiles[0])
    do.out_terms(tiles[1])
    plane_o.start(6, 4)
    do.hidden_grad(far_side)
    do.up_weight_grad(slots[0], far_side)
    sum_uf.edge(3)
    plane_o.fold_far()
    do.in_terms_two(tiles[0], True)
    sum_un.hop(1, 1)
    do.in_terms_two(tiles[1], False)
    plane_g.start(6, 4)
    plane_o.fold_x()
    do.out_terms(tiles[2])
    do.qkv_weight_grad(slots[2])
    sum_q.edge(2)
    plane_g.fold_far()
    do.out_terms(tiles[3])
    plane_o.start(2, 0)
    do.up_weight_grad(slots[1], far_side)
    sum_uf.edge(0)
    do.up_weight_grad(slots[2], far_side)
    sum_uf.edge(2)
    plane_o.turn_x()
    sum_d.hop(2, 0)
    do.qkv_weight_grad(slots[3])
    sum_q.edge(1)
    do.up_weight_grad(slots[3], far_side)
    sum_uf.edge(1)
    sum_q.hop(1, 0)
    plane_g.fold_x()
    plane_o.fold_near()
    plane_o.turn_y()
    do.in_terms_one(tiles[2], False)
    do.in_terms_one(tiles[3], False)
    do.in_terms_two(tiles[2], False)
    sum_uf.hop(1, 0)
    do.in_terms_two(tiles[3], False)
    plane_g.start(2, 0)
    sum_un.hop(2, 0)
    sum_o.hop(1, 0)
    do.small_terms(at.t)
    fold_v.start()
    sum_q.hop(2, 0)
    plane_g.turn_x()
    sum_q.hop(1, 1)
    plane_g.fold_near()
    sum_uf.hop(2, 0)
    plane_g.turn_y()
    sum_uf.hop(1, 1)
    fold_v.finish()
    do.small_plane(b)
    line_s.start()
    sum_q.landed()
    sum_q.total(do.fq)
    back_q.start()
    sum_o.hop(2, 0)
    sum_d.landed()
    sum_d.total(do.dd)
    out_d = mail.bring(do.dd, do.dd_to)
    sum_o.edge(2)
    sum_un.landed()
    sum_uf.landed()
    sum_un.total(do.fu)
    back_u.start()
    do.result(at.t, plane_o.finish(), plane_g.finish())
    out_x = mail.bring(do.out, do.out_to)
    out_g = mail.bring(do.in_grad, do.in_grad_to)
    sum_o.edge(1)
    sum_o.hop(1, 1)
    back_q.finish()
    line_s.finish()
    do.vt[...] = jnp.sum(do.vz[...], axis=0)
    share_v.start()
    sum_o.landed()
    sum_o.total(do.dd_o)
    out_o = mail.bring(do.dd_o, do.dd_o_to)
    back_u.finish()
    share_v.finish()
    for copied in (out_o, out_d, out_x, out_g):
        copied.wait()
    for line in (gather_x, gather_c, line_v, line_o, line_q, line_ua, line_ub, line_da, line_db, line_s, ex_v, ex_q, ex_u, back_q, back_u, fold_v, share_v, swap_w, swap_g, plane_o, plane_g, sum_o, sum_q, sum_un, sum_uf, sum_d):
        line.close()


def finish_kernel(names, planes, *refs):
    refs = dict(zip(names, refs))
    near = refs.pop(names[-1])
    do = Layer(refs)
    at = Place(planes)
    ranks, rows = do.dq.shape[:2]
    moves = []

    def move(src, dst):
        moves.append(pltpu.make_async_copy(src, dst, near.at[len(moves)]))
        moves[-1].start()

    move(do.in_grad, do.in_grad_out)
    move(do.dd, do.down_out)
    move(do.out, do.out_out)
    move(do.dd_o, do.dense_out)
    for rank in range(ranks):
        for b in range(planes):
            first = (b * ranks + rank) * LANES
            do.up_v[:, first : first + LANES] = do.du[
                rank, :, b * LANES : (b + 1) * LANES
            ].astype(jnp.float32)
    move(do.up_v, do.up_out)
    low = lax.broadcasted_iota(jnp.int32, (rows, LANES), 1) < HD
    for part in range(3):
        for core in range(2):
            for pair in range(ranks // 4):
                first, second = (
                    do.dq[2 * (2 * pair + i) + core, :, part * LANES : (part + 1) * LANES].astype(
                        jnp.float32
                    )
                    for i in range(2)
                )
                for j in range(2):
                    both = (
                        jnp.where(low, first, pltpu.roll(second, HD, 1))
                        if j == 0
                        else jnp.where(low, pltpu.roll(first, HD, 1), second)
                    )
                    start = (part * 4 + core * 2 + j) * ranks // 2 * HD + pair * LANES
                    do.qkv_v[:, start : start + LANES] = both
    move(do.qkv_v, do.qkv_out)
    piece = lax.rem(at.t, 4)
    row = (at.b * ranks + at.t) // 4
    values = do.dv[pl.ds(row, 1), 0:8, :].reshape(8, LANES)
    front = jnp.zeros((8, rows), jnp.float32)
    for i in range(4):
        cut = values[:, i * rows : (i + 1) * rows]
        front = front + jnp.where(piece == i, cut, jnp.zeros_like(cut))
    for j, ref in enumerate(
        (do.dense_bias, do.gain_one, do.shift_one, do.gain_two, do.shift_two)
    ):
        ref[...] = front[j].reshape(rows)
    do.down_bias[...] = front[0].reshape(rows)
    do.up_bias[...] = do.dv[pl.ds(at.t, 1), pl.ds(12 + at.b, 1), :].reshape(LANES)
    pieces = []
    for i in range(3):
        index = (at.b * ranks + at.t) * 3 + i
        part, inner = index // 32, lax.rem(index, 32)
        head, half = inner // 2, lax.rem(inner, 2)
        core, j, chip = head // 8, lax.rem(head // 4, 2), lax.rem(head, 4)
        value = do.dv[pl.ds(chip * 2 + core, 1), pl.ds(8 + part, 1), :].reshape(1, LANES)
        spot = 2 * j + half
        total = jnp.zeros((1, rows), jnp.float32)
        for k in range(4):
            cut = value[:, k * rows : (k + 1) * rows]
            total = total + jnp.where(spot == k, cut, jnp.zeros_like(cut))
        pieces.append(total)
    do.qkv_bias[...] = jnp.concatenate(pieces, axis=1).reshape(3 * rows)
    for made in moves:
        made.wait()


VMEM = pl.BlockSpec(memory_space=pltpu.VMEM)


def rotary_rows(length):
    half = HD // 8
    frequency = 1.0 / 10000.0 ** (np.arange(half) * (1.0 / half))
    angles = np.arange(length)[:, None] * frequency[None, :]
    table = np.zeros((3, length, HD))
    table[0] = 1.0
    table[0, :, :half] = table[0, :, half : 2 * half] = np.cos(angles)
    table[1, :, :half] = -np.sin(angles)
    table[2, :, half : 2 * half] = np.sin(angles)
    return np.tile(table, (1, 1, LANES // HD)).astype(np.float32)


def body(shape, *operands):
    residual_in, qkv_weight, down_weight = operands[0], operands[1], operands[11]
    planes = shape[BATCH]
    ranks = shape[ULY] * shape[BLK]
    tok_rows, seqs, width = residual_in.shape
    fits = (
        (shape[ULY], shape[BLK]) == (2, 4)
        and planes == 4
        and seqs == 2
        and 2 * qkv_weight.shape[0] == HD
        and width == ranks * LANES == 4 * TILE
        and ranks * tok_rows == 2 * TILE
        and TILE % (2 * tok_rows) == 0
        and down_weight.shape[0] == LANES
    )
    return fast_body(planes, *operands) if fits else general_body(*operands)


def fast_body(
    planes,
    residual_in,
    qkv_weight,
    qkv_bias,
    dense_weight,
    dense_bias,
    norm1_gain,
    norm1_bias,
    norm2_gain,
    norm2_bias,
    up_weight,
    up_bias,
    down_weight,
    down_bias,
    cotangent,
):
    single = jnp.float32
    half_type = jnp.bfloat16
    tok_rows, seqs, width = residual_in.shape
    ranks = width // LANES
    rows = qkv_weight.shape[0]
    depth = down_weight.shape[0]
    hidden = planes * depth
    pair = planes // 2
    length = ranks * tok_rows
    tokens = seqs * length
    rank = lax.axis_index(ULY) * lax.axis_size(BLK) + lax.axis_index(BLK)
    owner = lax.axis_index(BATCH) * ranks + rank

    anywhere = pl.BlockSpec(memory_space=pl.ANY)
    in_hbm = pl.BlockSpec(memory_space=pltpu.HBM)
    inputs = dict(
        x_in=(residual_in, in_hbm),
        cot_in=(cotangent, in_hbm),
        wq_in=(qkv_weight, in_hbm),
        wu_s=(up_weight, in_hbm),
        wd_s=(down_weight, in_hbm),
        wo_s=(dense_weight, in_hbm),
        table_in=(jnp.asarray(rotary_rows(length)), in_hbm),
        in_qkv=(qkv_bias, in_hbm),
        in_up=(up_bias, in_hbm),
    )
    for i, v in enumerate((dense_bias, norm1_gain, norm1_bias, norm2_gain, norm2_bias, down_bias)):
        inputs["in_vector%d" % i] = (v, in_hbm)
    shard = (seqs, tok_rows, width)
    outputs = dict(
        out_to=(residual_in.shape, half_type),
        in_grad_to=(residual_in.shape, single),
        dq=((ranks, rows, 3 * LANES), half_type),
        du=((ranks, rows, hidden), half_type),
        dd_to=((depth, width), single),
        dd_o_to=((rows, width), single),
        dv=((ranks, 16, LANES), single),
    )
    q_shape = (planes, ranks * rows, 3 * LANES)
    u_shape = (planes, ranks * rows, hidden)
    d_shape = (planes, depth, width)
    o_shape = (planes, rows, width)
    chips = ranks // 2
    scratch = dict(
        xa=((seqs, length, width), half_type),
        ca=((seqs, length, width), half_type),
        wq=(q_shape, half_type),
        wu=(u_shape, half_type),
        wd=(d_shape, half_type),
        wo=(o_shape, half_type),
        wo2=((pair, 2, rows, width), half_type),
        b_qkv=(qkv_bias.shape, half_type),
        b_up=(up_bias.shape, half_type),
        x_raw=(residual_in.shape, half_type),
        cot_raw=(residual_in.shape, half_type),
        x_own=(shard, half_type),
        cot_own=(shard, half_type),
        qkv=((tokens, 3 * LANES), single),
        wq_raw=(qkv_weight.shape, half_type),
        wq_s=((ranks, rows, 3 * LANES), half_type),
        table=((3, length, LANES), single),
        out=(residual_in.shape, half_type),
        in_grad=(residual_in.shape, single),
        dd=((depth, width), single),
        dd_o=((rows, width), single),
        vec_s=((16, LANES), single),
        vec_in=((ranks, 16, LANES), single),
        va=((planes, 32, LANES), single),
        center=((tokens, 1), single),
        inverse=((tokens, 1), single),
        act_one=((tokens, width), half_type),
        act_two=((tokens, width), half_type),
        query=((tokens, LANES), half_type),
        key=((tokens, LANES), half_type),
        value=((tokens, LANES), half_type),
        attn=((tokens, LANES), half_type),
        attn_grad=((tokens, LANES), half_type),
        qkv_grad=((tokens, 3 * LANES), half_type),
        gelu=((tokens, hidden), half_type),
        slope=((tokens, hidden), single),
        pre_grad=((tokens, hidden), half_type),
        gq=(q_shape, half_type),
        gu=(u_shape, half_type),
        gd=(d_shape, half_type),
        go=((pair, 2, rows, width), half_type),
        go4=(o_shape, half_type),
        above_q=(q_shape, half_type),
        below_q=(q_shape, half_type),
        above_u=(u_shape, half_type),
        below_u=(u_shape, half_type),
        above_d=(d_shape, half_type),
        below_d=(d_shape, half_type),
        above_o=(o_shape, half_type),
        below_o=(o_shape, half_type),
        fq=(q_shape[1:], half_type),
        fu=(u_shape[1:], half_type),
        po=((seqs, chips, 2, tok_rows, width), half_type),
        pg=((seqs, chips, 2, tok_rows, width), half_type),
        pairs_o=((seqs, chips, tok_rows, width), half_type),
        pairs_g=((seqs, chips, tok_rows, width), half_type),
        sums_o=((seqs, chips, tok_rows, width), half_type),
        sums_g=((seqs, chips, tok_rows, width), half_type),
        side_o=((3,) + shard, half_type),
        side_g=((3,) + shard, half_type),
        sums=((8, width), single),
        sm=((ranks, 8, LANES), single),
        sm_in=((ranks, 8, LANES), single),
        vz=((planes, 16, LANES), single),
        vt=((16, LANES), single),
    )
    for i in range(6):
        scratch["vector%d" % i] = (norm1_gain.shape, half_type)
    for block in range(length // TILE):
        scratch["probs%d" % block] = ((seqs * LANES // HD, TILE, (block + 1) * TILE), single)
    names = tuple(inputs) + tuple(outputs) + tuple(scratch) + ("send", "recv", "near", "second", "third")
    out, in_grad, dq, du, dd, dd_o, dv = pl.pallas_call(
        functools.partial(layer_kernel, names, planes),
        out_shape=[jax.ShapeDtypeStruct(*what) for what in outputs.values()],
        in_specs=[where for _, where in inputs.values()],
        out_specs=[anywhere] * len(outputs),
        scratch_shapes=[pltpu.VMEM(*what) for what in scratch.values()]
        + [pltpu.SemaphoreType.DMA((n,)) for n in (SEND_SLOTS, RECV_SLOTS, NEAR_SLOTS)]
        + [pltpu.SemaphoreType.REGULAR] * 2,
        compiler_params=pltpu.CompilerParams(
            collective_id=0, has_side_effects=True, vmem_limit_bytes=52 * 2**20
        ),
    )(
        *(
            pltpu.with_memory_space_constraint(value, pltpu.HBM) for value, _ in inputs.values()
        )
    )

    results = dict(
        out_out=(residual_in.shape, half_type),
        in_grad_out=(residual_in.shape, single),
        qkv_out=(qkv_weight.shape, single),
        qkv_bias=(qkv_bias.shape, single),
        dense_out=(dense_weight.shape, single),
        dense_bias=(dense_bias.shape, single),
        gain_one=(norm1_gain.shape, single),
        shift_one=(norm1_bias.shape, single),
        gain_two=(norm2_gain.shape, single),
        shift_two=(norm2_bias.shape, single),
        up_out=(up_weight.shape, single),
        up_bias=(up_bias.shape, single),
        down_out=(down_weight.shape, single),
        down_bias=(down_bias.shape, single),
    )
    given = tuple(n.removesuffix("_to") for n in outputs)
    staged = dict(up_v=results["up_out"], qkv_v=results["qkv_out"])
    return tuple(
        pl.pallas_call(
            functools.partial(
                finish_kernel, given + tuple(results) + tuple(staged) + ("near",), planes
            ),
            out_shape=[jax.ShapeDtypeStruct(*what) for what in results.values()],
            in_specs=[VMEM] * len(given),
            out_specs=[anywhere if len(what[0]) > 1 else VMEM for what in results.values()],
            scratch_shapes=[pltpu.VMEM(*what) for what in staged.values()]
            + [pltpu.SemaphoreType.DMA((8,))],
            compiler_params=pltpu.CompilerParams(vmem_limit_bytes=8 * 2**20),
        )(out, in_grad, dq, du, dd, dd_o, dv)
    )


def solution(mesh):
    placed = (
        P(TOKENS, BATCH, None),
        P(AXES, None),
        P(AXES),
        P(AXES, None),
        P(AXES),
        P(AXES),
        P(AXES),
        P(AXES),
        P(AXES),
        P(AXES, None),
        P(AXES),
        P(AXES, None),
        P(AXES),
        P(TOKENS, BATCH, None),
    )
    return jax.shard_map(
        functools.partial(body, dict(mesh.shape)),
        mesh=mesh,
        in_specs=placed,
        out_specs=(
            P(TOKENS, BATCH, None),
            P(TOKENS, BATCH, None),
            P(AXES, None),
            P(AXES),
            P(AXES, None),
            P(AXES),
            P(AXES),
            P(AXES),
            P(AXES),
            P(AXES),
            P(AXES, None),
            P(AXES),
            P(AXES, None),
            P(AXES),
        ),
        check_vma=False,
    )
```
